256 devices in a mesh: gx: 4 (over y_lo, core), gz: 8 (over y_hi, x), ta: 8 (over z).
Axes of the slice: x: 4, y: 4 (y_hi: 2, y_lo: 2; y = y_hi * 2 + y_lo), z: 8, core: 2. Of those that a mesh axis runs over, the one named last changes fastest.
Arguments:
- links: float32 [4, 2, 3, 3, 32, 32, 512], P(None, None, None, None, 'ta', 'gz', 'gx'), may hold values from -1 to 1, as said below
Outputs:
- force: float32 [4, 2, 3, 3, 32, 32, 512], P(None, None, None, None, 'ta', 'gz', 'gx')
The draws below stay inside these ranges and needn't reach their ends.
Inputs may be any that keep to these rules, and one draw needn't show every extreme that they name: Every link matrix (real part links[mu, 0], imaginary part links[mu, 1]) is special unitary, up to float32 rounding.
All inputs are finite; a program needn't handle non-finite values.
Results may differ from the reference program's by a relative error of at most 0.0003.
Values sent between devices are 32-bit elements; how exact they have to be, the bound alone decides.
A program may use at most 64 MiB of HBM per device.

```python
import jax
import jax.numpy as jnp

NX = 16
NY = 32
NZ = 32
NT = 32
NXY = 512


def draw_links(key, part):
    sample = jax.random.normal(key, (2, 4, 3, 3, NT, NZ, NXY), jnp.float32)
    real0 = sample[0][:, 0]
    imag0 = sample[1][:, 0]
    length0 = jnp.maximum(jnp.sqrt(jnp.sum(real0 * real0 + imag0 * imag0, axis=1, keepdims=True)), 1e-06)
    real0 = real0 / length0
    imag0 = imag0 / length0
    real1 = sample[0][:, 1]
    imag1 = sample[1][:, 1]
    inner_real = jnp.sum(real0 * real1 + imag0 * imag1, axis=1, keepdims=True)
    inner_imag = jnp.sum(real0 * imag1 - imag0 * real1, axis=1, keepdims=True)
    real1 = real1 - (inner_real * real0 - inner_imag * imag0)
    imag1 = imag1 - (inner_real * imag0 + inner_imag * real0)
    length1 = jnp.maximum(jnp.sqrt(jnp.sum(real1 * real1 + imag1 * imag1, axis=1, keepdims=True)), 1e-06)
    real1 = real1 / length1
    imag1 = imag1 / length1
    real_cols = []
    imag_cols = []
    for column in range(3):
        next_col = (column + 1) % 3
        last_col = (column + 2) % 3
        cross_real = real0[:, next_col] * real1[:, last_col] - imag0[:, next_col] * imag1[:, last_col] - real0[:, last_col] * real1[:, next_col] + imag0[:, last_col] * imag1[:, next_col]
        cross_imag = real0[:, next_col] * imag1[:, last_col] + imag0[:, next_col] * real1[:, last_col] - real0[:, last_col] * imag1[:, next_col] - imag0[:, last_col] * real1[:, next_col]
        real_cols.append(cross_real)
        imag_cols.append(-cross_imag)
    real2 = jnp.stack(real_cols, axis=1)
    imag2 = jnp.stack(imag_cols, axis=1)
    real_rows = jnp.stack([real0, real1, real2], axis=1)
    imag_rows = jnp.stack([imag0, imag1, imag2], axis=1)
    return jnp.stack([real_rows, imag_rows], axis=1)


def setup_inputs(seed: int = 0) -> dict:
    seeds = jax.random.split(jax.random.key(seed), 2)
    links = draw_links(jax.random.fold_in(seeds[1], 71), 0)
    return dict(links=links)


COEFF = -1.9


def matprod(left, right):
    total = left[:, 0][:, None] * right[0][None, :]
    total = total + left[:, 1][:, None] * right[1][None, :]
    return total + left[:, 2][:, None] * right[2][None, :]


def complex_mul(left, right):
    return (matprod(left[0], right[0]) - matprod(left[1], right[1]),
            matprod(left[0], right[1]) + matprod(left[1], right[0]))


def dagger(matrix):
    return (jnp.swapaxes(matrix[0], 0, 1), -jnp.swapaxes(matrix[1], 0, 1))


def unit_step(direction, sign):
    offset = [0, 0, 0, 0]
    offset[direction] = sign
    return tuple(offset)


def joined(first_step, second_step):
    return tuple(first_step[position] + second_step[position] for position in range(4))


def gauge_force(fetch_link):
    blocks = []
    still = (0, 0, 0, 0)
    for direction in range(4):
        ahead = unit_step(direction, 1)
        summed = None
        for transverse in range(4):
            if transverse == direction:
                continue
            side_up = unit_step(transverse, 1)
            side_down = unit_step(transverse, -1)
            upper = complex_mul(complex_mul(fetch_link(transverse, ahead), dagger(fetch_link(direction, side_up))),
                                dagger(fetch_link(transverse, still)))
            lower = complex_mul(complex_mul(dagger(fetch_link(transverse, joined(ahead, side_down))),
                                            dagger(fetch_link(direction, side_down))),
                                fetch_link(transverse, side_down))
            staple = (upper[0] + lower[0], upper[1] + lower[1])
            summed = staple if summed is None else (summed[0] + staple[0], summed[1] + staple[1])
        loop_matrix = complex_mul(fetch_link(direction, still), summed)
        real_part = 0.5 * (loop_matrix[0] - jnp.swapaxes(loop_matrix[0], 0, 1))
        imag_part = 0.5 * (loop_matrix[1] + jnp.swapaxes(loop_matrix[1], 0, 1))
        trace_third = (loop_matrix[1][0, 0] + loop_matrix[1][1, 1] + loop_matrix[1][2, 2]) / 3.0
        identity = jnp.eye(3, dtype=jnp.float32).reshape((3, 3) + (1,) * trace_third.ndim)
        imag_part = imag_part - identity * trace_third
        blocks.append(COEFF * jnp.stack([real_part, imag_part], axis=0))
    return jnp.stack(blocks, axis=0)


def reference(links):
    lattice = links.reshape(links.shape[:6] + (NY, NX))

    def fetch_link(direction, offset):
        field = lattice[direction]
        field = jnp.roll(field, (-offset[0], -offset[1], -offset[2], -offset[3]), axis=(3, 4, 5, 6))
        return (field[0], field[1])

    return gauge_force(fetch_link).reshape(links.shape)
```

```python
import functools

import jax
import jax.numpy as jnp
from jax import lax
from jax.experimental import pallas as pl
from jax.experimental.pallas import tpu as pltpu
from jax.sharding import PartitionSpec as P

NX = 16
COEFF = -1.9
AXES = ("ta", "gz", "gx")
SUB, LANES = 8, 128


def others(d):
    return [m for m in range(4) if m != d]


class Lattice:
    def __init__(self, depth):
        self.depth = depth
        self.per = SUB // depth
        self.ygroups = LANES // NX
        self.row = lax.broadcasted_iota(jnp.int32, (SUB, LANES), 0)
        self.lane = lax.broadcasted_iota(jnp.int32, (SUB, LANES), 1)
        self.zrow = self.row % depth
        self.xcol = self.lane % NX

    def rows(self, value, shift):
        shift %= SUB
        return pltpu.roll(value, shift, 0) if shift else value

    def lanes(self, value, shift):
        shift %= LANES
        return pltpu.roll(value, shift, 1) if shift else value


def entry(left, right, i, j, part, left_h, right_h):
    total = None
    for k in range(3):
        li = (k, i) if left_h else (i, k)
        ri = (j, k) if right_h else (k, j)
        lr, lm = left[0][li[0]][li[1]], left[1][li[0]][li[1]]
        rr, rm = right[0][ri[0]][ri[1]], right[1][ri[0]][ri[1]]
        if part == 0:
            first, second = lr * rr, lm * rm
            minus = left_h == right_h
        elif left_h:
            first, second = lr * rm, lm * rr
            minus = True
        else:
            first, second = lm * rr, lr * rm
            minus = right_h
        value = first - second if minus else first + second
        total = value if total is None else total + value
    return total


def product(left, right, left_h=False, right_h=False):
    return [
        [[entry(left, right, i, j, part, left_h, right_h) for j in range(3)] for i in range(3)]
        for part in range(2)
    ]


def projected(left, right, left_h=False, right_h=False):
    get = lambda i, j, part: entry(left, right, i, j, part, left_h, right_h)
    pairs = ((0, 1), (0, 2), (1, 2))
    real = [get(i, j, 0) - get(j, i, 0) for i, j in pairs]
    imag = [get(i, j, 1) + get(j, i, 1) for i, j in pairs]
    diag = [get(i, i, 1) for i in range(3)]
    third = (diag[0] + diag[1] + diag[2]) * (1.0 / 3.0)
    return real + imag + [diag[0] - third, diag[1] - third]


def third_row(real, imag):
    rows_r, rows_i = [], []
    for column in range(3):
        n, l = (column + 1) % 3, (column + 2) % 3
        rows_r.append(
            real[0][n] * real[1][l]
            - imag[0][n] * imag[1][l]
            - real[0][l] * real[1][n]
            + imag[0][l] * imag[1][n]
        )
        rows_i.append(
            real[0][l] * imag[1][n]
            + imag[0][l] * real[1][n]
            - real[0][n] * imag[1][l]
            - imag[0][n] * real[1][l]
        )
    return rows_r, rows_i


PLANES = ((2, 3), (0, 3), (0, 2), (1, 3), (1, 2), (0, 1))
DIAGONALS = ((0, 1), (1, 0), (0, 2), (2, 0), (1, 2), (2, 1))


def force_terms(
    counts, depth, halves, hbm, acc,
    u, ahead_s, local_s, pre_s, xs0, xs1, xs2, xr0, xr1, xr2, gs0, gs1, gs2, gr0, gr1, gr2, es, er,
    load_sem, send, recv,
):
    g = Lattice(depth)
    me = [lax.axis_index(a) for a in AXES]
    xs, xr, gs, gr = (xs0, xs1, xs2), (xr0, xr1, xr2), (gs0, gs1, gs2), (gr0, gr1, gr2)

    def device(*steps):
        where = list(me)
        for i, step in steps:
            where[i] = lax.rem(me[i] + (step + counts[i]), counts[i])
        by = dict(zip(AXES, where))
        return (by["gx"], by["gz"], by["ta"])

    barrier = pltpu.get_barrier_semaphore()
    partners = [device((i, step)) for i in (1, 0, 2) for step in (1, -1)]
    partners += [device((d, 1), (n, -1)) for d, n in DIAGONALS]
    for where in partners:
        pl.semaphore_signal(barrier, inc=1, device_id=where, device_id_type=pl.DeviceIdType.MESH)

    loads = [
        pltpu.make_async_copy(hbm.at[m], u.at[m], load_sem.at[m]) for m in range(4)
    ]
    for m in (1, 0, 2, 3):
        loads[m].start()

    def load(m, part, i, j, h):
        return u[m, part, i, j, h * SUB : (h + 1) * SUB, :]

    comps = [(part, i, j) for part in range(2) for i in range(2) for j in range(3)]

    def slot(d, m, n, h):
        k = others(d).index(m)
        if d == 0:
            return k * 48 + n // g.per * SUB, n % g.per
        if d == 1:
            return k * 48 + (n // depth * halves + h) * SUB, n % depth
        return k * 32 + (n // g.ygroups * halves + h) * SUB, n % g.ygroups

    def group(d):
        return (g.per, depth, g.ygroups)[d]

    def shifted(d, value, steps):
        if d == 0:
            return g.rows(value, depth * steps)
        return g.rows(value, steps) if d == 1 else g.lanes(value, NX * steps)

    def place(d):
        return (g.row // depth, g.zrow, g.lane // NX)[d]

    def pack(ref, d, m, h, get, layer):
        for n0 in range(0, 12, group(d)):
            value = None
            for n in range(n0, min(12, n0 + group(d))):
                r, k = slot(d, m, n, h)
                x = shifted(d, get(*comps[n]), k - layer)
                value = x if value is None else jnp.where(place(d) >= k, x, value)
            ref[r : r + SUB, :] = value

    def unpack(ref, d, m, n, h, layer):
        r, k = slot(d, m, n, h)
        return shifted(d, ref[r : r + SUB, :], layer - k)

    last = [g.per - 1, depth - 1, g.ygroups - 1]

    def face_halves(d, top):
        return range(halves) if d else ((halves - 1,) if top else (0,))

    def pack_faces(d):
        for m in others(d):
            for h in face_halves(d, False):
                pack(xs[d], d, m, h, lambda part, i, j: load(m, part, i, j, h), 0)

    def pack_edges(d, n):
        r0 = DIAGONALS.index((d, n)) * 2 * SUB
        layout = 1 if 2 not in (d, n) else 2
        for c0 in range(0, 12, SUB):
            value = None
            for k in range(min(SUB, 12 - c0)):
                c = comps[c0 + k]
                if layout == 1:
                    v = load(d, *c, halves - 1 if d == 0 else 0)
                    x = g.rows(v, k - depth if d == 0 else k - (depth - 1))
                    value = x if value is None else jnp.where(g.row >= k, x, value)
                    continue
                if 0 in (d, n):
                    v = load(d, *c, halves - 1 if d == 0 else 0)
                else:
                    at = depth - 1 if d == 1 else 0
                    step = -1 if d == 1 else 1
                    v = load(d, *c, 0)
                    for h in range(1, halves):
                        v = jnp.where(g.zrow == at + step * h, g.rows(load(d, *c, h), step * h), v)
                x = g.lanes(v, NX * (k + (1 if d == 2 else 0)))
                value = x if value is None else jnp.where(g.lane >= NX * k, x, value)
            es[r0 + c0 : r0 + c0 + SUB, :] = value

    def edge(d, n, h):
        r0 = DIAGONALS.index((d, n)) * 2 * SUB

        def get(part, i, j):
            c = part * 6 + i * 3 + j
            v = er[r0 + c // SUB * SUB : r0 + c // SUB * SUB + SUB, :]
            k = c % SUB
            if (d, n) == (0, 1):
                return g.rows(v, depth - 1 - k)
            if (d, n) == (1, 0):
                return g.rows(v, SUB - depth - k)
            v = g.lanes(v, NX * ((0 if d == 2 else g.ygroups - 1) - k))
            if (d, n) == (0, 2):
                return g.rows(v, -(SUB - depth))
            if (d, n) == (2, 0):
                return g.rows(v, SUB - depth)
            return g.rows(v, 1 - depth + h if d == 1 else depth - 1 - h)

        return complete_rows(get)

    def complete_rows(get):
        real = [[get(0, i, j) for j in range(3)] for i in range(2)]
        imag = [[get(1, i, j) for j in range(3)] for i in range(2)]
        third_r, third_i = third_row(real, imag)
        return [real + [third_r], imag + [third_i]]

    def matrix(m, h):
        return [[[load(m, part, i, j, h) for j in range(3)] for i in range(3)] for part in range(2)]

    def save(ref, index, value):
        for part in range(2):
            for i in range(len(value[part])):
                for j in range(3):
                    ref[index, part, i, j] = value[part][i][j]

    def saved(ref, index):
        return [[[ref[index, part, i, j] for j in range(3)] for i in range(3)] for part in range(2)]

    def rolled(m, d, h, part, i, j):
        v = load(m, part, i, j, h)
        if d == 3:
            return jnp.where(g.xcol == NX - 1, g.lanes(v, NX - 1), g.lanes(v, -1))
        if d == 2:
            return g.lanes(v, -NX)
        if d == 1:
            return g.rows(v, -1)
        if h + 1 < halves:
            beyond = g.rows(load(m, part, i, j, h + 1), -depth)
            return jnp.where(g.row >= SUB - depth, beyond, g.rows(v, -depth))
        return g.rows(v, -depth)

    def complete(d, h):
        return d == 3 or (d == 0 and h + 1 < halves)

    def top(d, h):
        if d == 0:
            return g.row >= SUB - depth
        return g.zrow == depth - 1 if d == 1 else g.lane >= LANES - NX

    def index(m, d, h):
        return (m * 4 + d) * halves + h

    def save_local(mu, nu):
        for h in range(halves):
            for m, d in ((nu, mu), (mu, nu)):
                save(
                    ahead_s, index(m, d, h),
                    [[[rolled(m, d, h, part, i, j) for j in range(3)] for i in range(3)] for part in range(2)],
                )
            save(
                local_s, PLANES.index((mu, nu)) * halves + h,
                product(matrix(mu, h), matrix(nu, h), left_h=True),
            )

    def pack_open(d):
        for m in others(d):
            mu, nu = min(d, m), max(d, m)
            for h in face_halves(d, True):
                b = saved(local_s, PLANES.index((mu, nu)) * halves + h)
                v = saved(ahead_s, index(d, m, h))

                def get(part, i, j):
                    value = entry(b, v, i, j, part, d > m, False)
                    if complete(m, h):
                        return value
                    if d < m:
                        short = b[part][i][j]
                    else:
                        short = b[0][j][i] if part == 0 else -b[1][j][i]
                    return jnp.where(top(m, h), short, value)

                pack(gs[d], d, m, h, get, last[d])

    def remote(src, dst, where):
        n = len(copies)
        copies.append(
            pltpu.make_async_remote_copy(
                src_ref=src, dst_ref=dst, send_sem=send.at[n], recv_sem=recv.at[n],
                device_id=where, device_id_type=pl.DeviceIdType.MESH,
            )
        )
        return copies[-1]

    def chunk(ref, d, m):
        n = ref.shape[0] // 3
        k = others(d).index(m)
        return ref.at[k * n : (k + 1) * n]

    copies, faces, opens, edges = [], {}, {}, {}
    for d, n in DIAGONALS:
        r = DIAGONALS.index((d, n)) * 2 * SUB
        rows = slice(r, r + 2 * SUB)
        edges[d, n] = remote(es.at[rows], er.at[rows], device((d, 1), (n, -1)))
    for d in range(3):
        for m in others(d):
            faces[d, m] = remote(chunk(xs[d], d, m), chunk(xr[d], d, m), device((d, -1)))
            opens[d, m] = remote(chunk(gs[d], d, m), chunk(gr[d], d, m), device((d, 1)))

    for m in (1, 0, 2, 3):
        loads[m].wait()
    pack_faces(1)
    for pair in PLANES:
        if 1 in pair:
            save_local(*pair)
    pack_open(1)
    for d, n in DIAGONALS:
        pack_edges(d, n)
    pl.semaphore_wait(barrier, len(partners))
    for key in ((1, 2), (2, 1), (0, 1), (1, 0), (0, 2), (2, 0)):
        edges[key].start()
    for m in (3, 2, 0):
        faces[1, m].start()
        opens[1, m].start()
    pack_faces(0)
    for m in (3, 2, 1):
        faces[0, m].start()
    pack_faces(2)
    for m in (3, 0, 1):
        faces[2, m].start()
    for pair in PLANES:
        if 1 not in pair:
            save_local(*pair)
    pack_open(0)
    for m in (3, 2, 1):
        opens[0, m].start()
    pack_open(2)
    for m in (3, 0, 1):
        opens[2, m].start()

    def ahead(m, d, h):
        if complete(d, h):
            return saved(ahead_s, index(m, d, h))

        def get(part, i, j):
            v = ahead_s[index(m, d, h), part, i, j]
            return jnp.where(top(d, h), unpack(xr[d], d, m, comps.index((part, i, j)), h, last[d]), v)

        return complete_rows(get)

    seen = set()

    def add(m, c, h, value):
        r = ((m * 8 + c) * halves + h) * SUB
        if (m, c, h) in seen:
            acc[r : r + SUB, :] += value
        else:
            seen.add((m, c, h))
            acc[r : r + SUB, :] = value

    def lower(m, d, h, q):
        for c in range(8):
            if d == 3:
                add(m, c, h, jnp.where(g.xcol == 0, g.lanes(q[c], 1 - NX), g.lanes(q[c], 1)))
            elif d == 2:
                add(m, c, h, jnp.where(g.lane >= NX, g.lanes(q[c], NX), 0.0))
            elif d == 1:
                add(m, c, h, jnp.where(g.zrow > 0, g.rows(q[c], 1), 0.0))
            else:
                moved = g.rows(q[c], depth)
                add(m, c, h, jnp.where(g.row >= depth, moved, 0.0))
                if h + 1 < halves:
                    add(m, c, h + 1, jnp.where(g.row < depth, moved, 0.0))

    arrived = set()

    def plane(mu, nu):
        for h in range(halves):
            n = PLANES.index((mu, nu)) * halves + h
            for d, m in ((mu, nu), (nu, mu)):
                if (d, m) not in arrived and not complete(d, h):
                    arrived.add((d, m))
                    faces[d, m].wait_recv()
            a = product(ahead(nu, mu, h), ahead(mu, nu, h), right_h=True)
            b = saved(local_s, n)
            lower(mu, nu, h, projected(a, b, left_h=True))
            lower(nu, mu, h, projected(a, b, right_h=True))
            e = product(matrix(mu, h), a)
            upper = projected(e, matrix(nu, h), right_h=True)
            for c in range(8):
                add(mu, c, h, upper[c])
                add(nu, c, h, -upper[c])

    def edge_mask(d, m, h):
        if m == 2:
            return g.lane >= LANES - NX
        if m == 1:
            return g.zrow == depth - 1
        return g.row >= SUB - depth

    def has_edge(d, m, h):
        return m in (1, 2) or (m == 0 and h == halves - 1)

    def prepare(d, m):
        if m != 3:
            edges[d, m].wait_recv()
        for h in face_halves(d, False):
            if has_edge(d, m, h):
                own = matrix(m, h)
                both = product(own, edge(d, m, h), right_h=True)
                save(
                    pre_s, index(m, d, h),
                    [
                        [
                            [jnp.where(edge_mask(d, m, h), both[p][i][j], own[p][i][j]) for j in range(3)]
                            for i in range(3)
                        ]
                        for p in range(2)
                    ],
                )

    def close(d, m):
        opens[d, m].wait_recv()
        for h in face_halves(d, False):
            own = saved(pre_s, index(m, d, h)) if has_edge(d, m, h) else matrix(m, h)
            back = complete_rows(
                lambda part, i, j: unpack(gr[d], d, m, comps.index((part, i, j)), h, 0)
            )
            q = projected(own, back, right_h=True)
            mask = (g.row < depth, g.zrow == 0, g.lane < NX)[d]
            for c in range(8):
                add(m, c, h, jnp.where(mask, q[c], 0.0))

    for pair in PLANES[:3]:
        plane(*pair)
    for d, m in ((0, 3), (2, 3), (0, 2), (2, 0), (0, 1), (2, 1)):
        prepare(d, m)
        close(d, m)
    for m in (3, 2, 0):
        prepare(1, m)
    for pair in PLANES[3:]:
        plane(*pair)
    for m in (3, 2, 0):
        close(1, m)
    for copy in copies:
        copy.wait_send()


def expand(halves, acc, hbm, out, sems):
    copies = []
    for m in range(4):
        for h in range(halves):
            rows = [((m * 8 + c) * halves + h) * SUB for c in range(8)]
            f = [acc[r : r + SUB, :] * (COEFF * 0.5 if c < 6 else COEFF) for c, r in enumerate(rows)]

            def put(part, i, j, value):
                out[m, part, i, j, h * SUB : (h + 1) * SUB, :] = value

            for n, (i, j) in enumerate(((0, 1), (0, 2), (1, 2))):
                put(0, i, j, f[n])
                put(0, j, i, -f[n])
                put(1, i, j, f[3 + n])
                put(1, j, i, f[3 + n])
            for i in range(3):
                put(0, i, i, jnp.zeros((SUB, LANES), jnp.float32))
            put(1, 0, 0, f[6])
            put(1, 1, 1, f[7])
            put(1, 2, 2, -(f[6] + f[7]))
        copies.append(pltpu.make_async_copy(out.at[m], hbm.at[m], sems.at[m]))
        copies[-1].start()
    for copy in copies:
        copy.wait()


def per_device(counts, links):
    time_len, depth, flat = links.shape[4:]
    sites = time_len * depth
    assert flat == LANES and (time_len, depth) == (4, 4)
    halves = sites // SUB
    faces = (144, 144, 96)
    vmem = lambda *s: pltpu.VMEM(s + (LANES,), jnp.float32)
    shape = links.shape[:4] + (sites, flat)
    terms = pl.pallas_call(
        functools.partial(force_terms, counts, depth, halves),
        out_shape=pltpu.VMEM((32 * sites, flat), jnp.float32),
        in_specs=[pl.BlockSpec(memory_space=pl.ANY)],
        out_specs=pl.BlockSpec(memory_space=pltpu.VMEM),
        scratch_shapes=[
            vmem(*shape[:-1]),
            vmem(16 * halves, 2, 3, 3, SUB),
            vmem(6 * halves, 2, 3, 3, SUB),
            vmem(16 * halves, 2, 3, 3, SUB),
        ]
        + [vmem(r) for r in faces * 4]
        + [vmem(6 * 2 * SUB)] * 2
        + [
            pltpu.SemaphoreType.DMA((4,)),
            pltpu.SemaphoreType.DMA((24,)),
            pltpu.SemaphoreType.DMA((24,)),
        ],
        compiler_params=pltpu.CompilerParams(collective_id=0, has_side_effects=True),
        name="force_terms",
    )(links.reshape(shape))
    out = pl.pallas_call(
        functools.partial(expand, halves),
        out_shape=jax.ShapeDtypeStruct(shape, jnp.float32),
        in_specs=[pl.BlockSpec(memory_space=pltpu.VMEM)],
        out_specs=pl.BlockSpec(memory_space=pl.ANY),
        scratch_shapes=[vmem(*shape[:-1]), pltpu.SemaphoreType.DMA((4,))],
        name="expand",
    )(pltpu.with_memory_space_constraint(terms, pltpu.VMEM))
    return out.reshape(links.shape)


def solution(mesh):
    assert mesh.axis_names == ("gx", "gz", "ta")
    counts = tuple(mesh.shape[a] for a in AXES)
    spec = P(None, None, None, None, "ta", "gz", "gx")
    return jax.shard_map(
        functools.partial(per_device, counts),
        mesh=mesh,
        in_specs=(spec,),
        out_specs=spec,
        check_vma=False,
    )
```

```python
import functools

import jax
import jax.numpy as jnp
from jax import lax
from jax.experimental import pallas as pl
from jax.experimental.pallas import tpu as pltpu
from jax.sharding import PartitionSpec as P

NX = 16
COEFF = -1.9
AXES = ("ta", "gz", "gx")
SUB, LANES = 8, 128


def others(d):
    return [m for m in range(4) if m != d]


class Lattice:
    def __init__(self, depth):
        self.depth = depth
        self.per = SUB // depth
        self.ygroups = LANES // NX
        self.row = lax.broadcasted_iota(jnp.int32, (SUB, LANES), 0)
        self.lane = lax.broadcasted_iota(jnp.int32, (SUB, LANES), 1)
        self.zrow = self.row % depth
        self.xcol = self.lane % NX

    def rows(self, value, shift):
        shift %= SUB
        return pltpu.roll(value, shift, 0) if shift else value

    def lanes(self, value, shift):
        shift %= LANES
        return pltpu.roll(value, shift, 1) if shift else value


def entry(left, right, i, j, part, left_h, right_h):
    total = None
    for k in range(3):
        li = (k, i) if left_h else (i, k)
        ri = (j, k) if right_h else (k, j)
        lr, lm = left[0][li[0]][li[1]], left[1][li[0]][li[1]]
        rr, rm = right[0][ri[0]][ri[1]], right[1][ri[0]][ri[1]]
        if part == 0:
            first, second = lr * rr, lm * rm
            minus = left_h == right_h
        elif left_h:
            first, second = lr * rm, lm * rr
            minus = True
        else:
            first, second = lm * rr, lr * rm
            minus = right_h
        value = first - second if minus else first + second
        total = value if total is None else total + value
    return total


def product(left, right, left_h=False, right_h=False):
    return [
        [[entry(left, right, i, j, part, left_h, right_h) for j in range(3)] for i in range(3)]
        for part in range(2)
    ]


def projected(left, right, left_h=False, right_h=False):
    get = lambda i, j, part: entry(left, right, i, j, part, left_h, right_h)
    pairs = ((0, 1), (0, 2), (1, 2))
    real = [get(i, j, 0) - get(j, i, 0) for i, j in pairs]
    imag = [get(i, j, 1) + get(j, i, 1) for i, j in pairs]
    diag = [get(i, i, 1) for i in range(3)]
    third = (diag[0] + diag[1] + diag[2]) * (1.0 / 3.0)
    return real + imag + [diag[0] - third, diag[1] - third]


def third_row(real, imag):
    rows_r, rows_i = [], []
    for column in range(3):
        n, l = (column + 1) % 3, (column + 2) % 3
        rows_r.append(
            real[0][n] * real[1][l]
            - imag[0][n] * imag[1][l]
            - real[0][l] * real[1][n]
            + imag[0][l] * imag[1][n]
        )
        rows_i.append(
            real[0][l] * imag[1][n]
            + imag[0][l] * real[1][n]
            - real[0][n] * imag[1][l]
            - imag[0][n] * real[1][l]
        )
    return rows_r, rows_i


PLANES = ((0, 1), (0, 2), (0, 3), (1, 2), (1, 3), (2, 3))
DIAGONALS = ((0, 2), (2, 0), (0, 1), (1, 0), (1, 2), (2, 1))
LAYOUT = (
    (((1, 0), (2, 0)), ((3, 0),)),
    (((0, 0), (0, 1), (2, 0), (2, 1)), ((3, 0), (3, 1))),
    (((0, 0), (0, 1), (1, 0), (1, 1), (3, 0), (3, 1)),),
)
ROWS = (144, 144, 96)
EDGE = 2 * SUB


def offset(kind, d):
    if kind == "e":
        return 2 * sum(ROWS) + d * EDGE
    return (sum(ROWS) if kind == "g" else 0) + sum(ROWS[:d])


TOTAL = offset("e", len(DIAGONALS))


def force_terms(
    counts, depth, halves, hbm, acc, u, out_s, in_s, face_s, b_s, pre_s, load_sem, send, recv,
):
    g = Lattice(depth)
    me = [lax.axis_index(a) for a in AXES]
    comps = [(part, i, j) for part in range(2) for i in range(2) for j in range(3)]
    last = (g.per - 1, depth - 1, g.ygroups - 1)
    place = (g.row // depth, g.zrow, g.lane // NX)

    def device(*steps):
        where = list(me)
        for i, step in steps:
            where[i] = lax.rem(me[i] + (step + counts[i]), counts[i])
        by = dict(zip(AXES, where))
        return (by["gx"], by["gz"], by["ta"])

    loads = [
        pltpu.make_async_copy(hbm.at[m, part], u.at[m, part], load_sem)
        for m in range(4)
        for part in range(2)
    ]
    for copy in loads:
        copy.start()
    barrier = pltpu.get_barrier_semaphore()
    partners = [device((i, step)) for i in (1, 0, 2) for step in (1, -1)]
    partners += [device((d, 1), (n, -1)) for d, n in DIAGONALS]
    for where in partners:
        pl.semaphore_signal(barrier, inc=1, device_id=where, device_id_type=pl.DeviceIdType.MESH)

    def remote(start, rows, slot, where):
        span = slice(start, start + rows)
        return pltpu.make_async_remote_copy(
            src_ref=out_s.at[span], dst_ref=in_s.at[span], send_sem=send, recv_sem=recv.at[slot],
            device_id=where, device_id_type=pl.DeviceIdType.MESH,
        )

    faces = [remote(offset("x", d), ROWS[d], d, device((d, -1))) for d in range(3)]
    opens = [remote(offset("g", d), ROWS[d], 3 + d, device((d, 1))) for d in range(3)]
    edges = [
        remote(offset("e", k), EDGE, 6 if k < 2 else 7, device((d, 1), (n, -1)))
        for k, (d, n) in enumerate(DIAGONALS)
    ]
    near_edges = remote(offset("e", 0), 2 * EDGE, 6, partners[0])
    far_edges = remote(offset("e", 2), 4 * EDGE, 7, partners[0])
    everything = remote(0, TOTAL, 0, partners[0])

    def load(m, part, i, j, h):
        return u[m, part, i, j, h * SUB : (h + 1) * SUB, :]

    def shifted(d, value, steps):
        if d == 0:
            return g.rows(value, depth * steps)
        return g.rows(value, steps) if d == 1 else g.lanes(value, NX * steps)

    def half(d, h, top):
        return (halves - 1 if top else 0) if d == 0 else h

    def complete(d, h):
        return d == 3 or (d == 0 and h + 1 < halves)

    def top(d, h=1):
        if d == 0:
            return g.row >= SUB - depth
        return g.zrow == depth - 1 if d == 1 else g.lane >= LANES - NX

    def bottom(d):
        return (g.row < depth, g.zrow == 0, g.lane < NX)[d]

    def open_mask(d, s, among=(0, 1, 2)):
        mask = None
        for k, (m, h) in enumerate(LAYOUT[d][s]):
            if m in among and not complete(m, h if d else 1):
                here = jnp.logical_and(place[d] == k, top(m))
                mask = here if mask is None else jnp.logical_or(mask, here)
        return mask

    def pick(mask, yes, no):
        return no if mask is None else jnp.where(mask, yes, no)

    def pack(d, s, get, up):
        value = None
        for k, (m, h) in enumerate(LAYOUT[d][s]):
            x = get(m, half(d, h, up))
            if x is None:
                continue
            x = shifted(d, x, k - (last[d] if up else 0))
            value = x if value is None else jnp.where(place[d] >= k, x, value)
        return value

    def complete_rows(get):
        real = [[get(0, i, j) for j in range(3)] for i in range(2)]
        imag = [[get(1, i, j) for j in range(3)] for i in range(2)]
        third_r, third_i = third_row(real, imag)
        return [real + [third_r], imag + [third_i]]

    def packed(d, s, get, up):
        return complete_rows(
            lambda part, i, j: pack(d, s, lambda m, h: get(m, h, part, i, j), up)
        )

    def put(kind, d, s, value):
        r = offset(kind, d)
        used = len(LAYOUT[d][s])
        for n, (part, i, j) in enumerate(comps[: 6 if s else 12]):
            v = value[part][i][j]
            if s:
                v = jnp.where(place[d] < used, v, shifted(d, value[1][i][j], used))
            at = r + (96 if s else 0) + n * SUB
            out_s[at : at + SUB, :] = v

    def fetch(ref, kind, d, s, part, i, j):
        n = part * 6 + i * 3 + j
        at = offset(kind, d) + n * SUB
        if not s:
            return ref[at : at + SUB, :]
        at += 96 - part * 6 * SUB
        v = ref[at : at + SUB, :]
        return shifted(d, v, -len(LAYOUT[d][s])) if part else v

    def fetched(ref, kind, d, s):
        return complete_rows(lambda part, i, j: fetch(ref, kind, d, s, part, i, j))

    def rolled(m, d, h, part, i, j):
        v = load(m, part, i, j, h)
        if d == 3:
            return jnp.where(g.xcol == NX - 1, g.lanes(v, NX - 1), g.lanes(v, -1))
        if d == 2:
            return g.lanes(v, -NX)
        if d == 1:
            return g.rows(v, -1)
        if h + 1 < halves:
            beyond = g.rows(load(m, part, i, j, h + 1), -depth)
            return jnp.where(g.row >= SUB - depth, beyond, g.rows(v, -depth))
        return g.rows(v, -depth)

    def matrix(get):
        return [[[get(part, i, j) for j in range(3)] for i in range(3)] for part in range(2)]

    def save(ref, index, value):
        for part in range(2):
            for i in range(ref.shape[-4]):
                for j in range(3):
                    ref[(*index, part, i, j)] = value[part][i][j]

    sets = [(d, s) for d in range(3) for s in range(len(LAYOUT[d]))]

    def kept(d, s, q):
        n = sets.index((d, s))
        return complete_rows(lambda part, i, j: face_s[n, q, part, i, j])

    def send_side(d):
        own = packed(d, 0, lambda m, h, *c: load(d, *c, h), True)
        for s in range(len(LAYOUT[d])):
            n = sets.index((d, s))
            side = packed(d, s, lambda m, h, *c: load(m, *c, h), True)
            over = packed(d, s, lambda m, h, *c: rolled(d, m, h, *c), True)
            b = product(own, side, left_h=True)
            mask = open_mask(d, s)
            put("g", d, s, [
                [
                    [pick(mask, b[p][i][j], entry(b, over, i, j, p, False, False)) for j in range(3)]
                    for i in range(2)
                ]
                for p in range(2)
            ])
            for q, value in enumerate((own, side, over)):
                save(face_s, (n, q), value)
            save(b_s, (n,), b)
            put("x", d, s, [
                [
                    [pack(d, s, lambda m, h: load(m, p, i, j, h), False) for j in range(3)]
                    for i in range(2)
                ]
                for p in range(2)
            ])

    def pack_edges(d, n):
        r0 = offset("e", DIAGONALS.index((d, n)))
        for c0 in range(0, 12, SUB):
            value = None
            for k in range(min(SUB, 12 - c0)):
                c = comps[c0 + k]
                if 2 not in (d, n):
                    v = load(d, *c, halves - 1 if d == 0 else 0)
                    x = g.rows(v, k - depth if d == 0 else k - (depth - 1))
                    value = x if value is None else jnp.where(g.row >= k, x, value)
                    continue
                if 0 in (d, n):
                    v = load(d, *c, halves - 1 if d == 0 else 0)
                else:
                    at = depth - 1 if d == 1 else 0
                    step = -1 if d == 1 else 1
                    v = load(d, *c, 0)
                    for h in range(1, halves):
                        v = jnp.where(g.zrow == at + step * h, g.rows(load(d, *c, h), step * h), v)
                x = g.lanes(v, NX * (k + (1 if d == 2 else 0)))
                value = x if value is None else jnp.where(g.lane >= NX * k, x, value)
            out_s[r0 + c0 : r0 + c0 + SUB, :] = value

    def edge(d, n, h, part, i, j):
        c = part * 6 + i * 3 + j
        r = offset("e", DIAGONALS.index((d, n))) + c // SUB * SUB
        v = in_s[r : r + SUB, :]
        k = c % SUB
        if (d, n) == (0, 1):
            return g.rows(v, depth - 1 - k)
        if (d, n) == (1, 0):
            return g.rows(v, SUB - depth - k)
        v = g.lanes(v, NX * ((0 if d == 2 else g.ygroups - 1) - k))
        if (d, n) == (0, 2):
            return g.rows(v, -(SUB - depth))
        if (d, n) == (2, 0):
            return g.rows(v, SUB - depth)
        return g.rows(v, 1 - depth + h if d == 1 else depth - 1 - h)

    everything_in = pltpu.make_async_copy(hbm, u, load_sem)
    everything_in.wait()
    for d in (1, 0, 2):
        send_side(d)
    for d, n in DIAGONALS:
        pack_edges(d, n)
    pl.semaphore_wait(barrier, len(partners))
    for copy in [opens[1], faces[1]] + edges[2:] + [opens[0], faces[0], opens[2], faces[2]] + edges[:2]:
        copy.start()

    seen, pending = set(), {}

    def add(m, c, h, value):
        key = (m, c, h)
        pending[key] = pending[key] + value if key in pending else value

    def flush():
        for (m, c, h), value in pending.items():
            r = ((m * 8 + c) * halves + h) * SUB
            if (m, c, h) in seen:
                acc[r : r + SUB, :] += value
            else:
                seen.add((m, c, h))
                acc[r : r + SUB, :] = value
        pending.clear()

    def forward(m, d, h, q):
        for c in range(8):
            if d == 3:
                add(m, c, h, jnp.where(g.xcol == 0, g.lanes(q[c], 1 - NX), g.lanes(q[c], 1)))
            elif d == 2:
                add(m, c, h, g.lanes(q[c], NX))
            elif d == 1:
                add(m, c, h, g.rows(q[c], 1))
            elif h + 1 < halves:
                moved = g.rows(q[c], depth)
                add(m, c, h, jnp.where(g.row >= depth, moved, 0.0))
                add(m, c, h + 1, jnp.where(g.row < depth, moved, 0.0))
            else:
                add(m, c, h, g.rows(q[c], depth))

    def masked(mask, a):
        return [[[pick(mask, 0.0, v) for v in line] for line in part] for part in a]

    def inner(mu, nu, h):
        own = matrix(lambda *c: load(mu, *c, h))
        side = matrix(lambda *c: load(nu, *c, h))
        a = product(
            matrix(lambda *c: rolled(nu, mu, h, *c)),
            matrix(lambda *c: rolled(mu, nu, h, *c)),
            right_h=True,
        )
        mask = None
        for d in (mu, nu):
            if not complete(d, h):
                mask = top(d) if mask is None else jnp.logical_or(mask, top(d))
        a = masked(mask, a)
        b = product(own, side, left_h=True)
        forward(mu, nu, h, projected(a, b, left_h=True))
        forward(nu, mu, h, projected(a, b, right_h=True))
        upper = projected(product(own, a), side, right_h=True)
        for c in range(8):
            add(mu, c, h, upper[c])
            add(nu, c, h, -upper[c])

    def corners(d, among):
        for s in range(len(LAYOUT[d])):
            mask = open_mask(d, s, among)
            if mask is None:
                continue
            n = sets.index((d, s))

            def corner(m, h, c):
                if m not in among or complete(m, h):
                    return None
                k = LAYOUT[m][0].index((d, 0 if m == 0 else h))
                return shifted(m, fetch(in_s, "x", m, 0, *c), last[m] - k)

            for c in comps:
                value = pack(d, s, lambda m, h: corner(m, h, c), True)
                face_s[(n, 2, *c)] = jnp.where(mask, value, face_s[(n, 2, *c)])

    def face_terms(d, closed):
        for s, spots in enumerate(LAYOUT[d]):
            n = sets.index((d, s))
            own, side, over = (kept(d, s, q) for q in range(3))
            a = product(fetched(in_s, "x", d, s), over, right_h=True)
            a = masked(open_mask(d, s, [m for m in range(3) if m not in closed]), a)
            b = matrix(lambda *c: b_s[(n, *c)])
            upper = projected(product(own, a), side, right_h=True)
            low = projected(a, b, left_h=True)
            mask = open_mask(d, s, closed)
            low = [pick(mask, 0.0, v) for v in low]
            for k, (m, h) in enumerate(spots):
                h = half(d, h, True)
                natural = lambda v: jnp.where(top(d), shifted(d, v, last[d] - k), 0.0)
                for c in range(8):
                    x = natural(upper[c])
                    add(d, c, h, x)
                    add(m, c, h, -x)
                forward(d, m, h, [natural(v) for v in low])
        flush()

    def prepare(d):
        for s in range(len(LAYOUT[d])):
            own = fetched(out_s, "x", d, s)
            mask = open_mask(d, s)
            if mask is not None:
                far = packed(
                    d, s,
                    lambda m, h, *c: None if complete(m, h if d else 1) else edge(d, m, h, *c),
                    False,
                )
                both = product(own, far, right_h=True)
                own = [
                    [[jnp.where(mask, both[p][i][j], own[p][i][j]) for j in range(3)] for i in range(3)]
                    for p in range(2)
                ]
            save(pre_s, (sets.index((d, s)),), own)

    def close(d):
        for s, spots in enumerate(LAYOUT[d]):
            n = sets.index((d, s))
            q = projected(
                matrix(lambda *c: pre_s[(n, *c)]), fetched(in_s, "g", d, s), right_h=True
            )
            for k, (m, h) in enumerate(spots):
                for c in range(8):
                    add(m, c, half(d, h, False), jnp.where(bottom(d), shifted(d, q[c], -k), 0.0))
        flush()

    for pair in PLANES:
        for h in range(halves):
            inner(*pair, h)
        flush()
    faces[2].wait_recv()
    face_terms(2, ())
    corners(0, (2,))
    faces[0].wait_recv()
    face_terms(0, (2,))
    corners(1, (0, 2))
    near_edges.wait_recv()
    far_edges.wait_recv()
    for d in (2, 0, 1):
        prepare(d)
    for d in (2, 0):
        opens[d].wait_recv()
        close(d)
    faces[1].wait_recv()
    face_terms(1, (0, 2))
    opens[1].wait_recv()
    close(1)
    everything.wait_send()


def expand(halves, acc, hbm, out, sems):
    copies = []
    for m in range(4):
        for h in range(halves):
            rows = [((m * 8 + c) * halves + h) * SUB for c in range(8)]
            f = [acc[r : r + SUB, :] * (COEFF * 0.5 if c < 6 else COEFF) for c, r in enumerate(rows)]

            def put(part, i, j, value):
                out[m, part, i, j, h * SUB : (h + 1) * SUB, :] = value

            for n, (i, j) in enumerate(((0, 1), (0, 2), (1, 2))):
                put(0, i, j, f[n])
                put(0, j, i, -f[n])
                put(1, i, j, f[3 + n])
                put(1, j, i, f[3 + n])
            for i in range(3):
                put(0, i, i, jnp.zeros((SUB, LANES), jnp.float32))
            put(1, 0, 0, f[6])
            put(1, 1, 1, f[7])
            put(1, 2, 2, -(f[6] + f[7]))
        copies.append(pltpu.make_async_copy(out.at[m], hbm.at[m], sems.at[m]))
        copies[-1].start()
    for copy in copies:
        copy.wait()


def per_device(counts, links):
    time_len, depth, flat = links.shape[4:]
    sites = time_len * depth
    assert flat == LANES and (time_len, depth) == (4, 4)
    halves = sites // SUB
    vmem = lambda *s: pltpu.VMEM(s + (LANES,), jnp.float32)
    shape = links.shape[:4] + (sites, flat)
    terms = pl.pallas_call(
        functools.partial(force_terms, counts, depth, halves),
        out_shape=pltpu.VMEM((32 * sites, flat), jnp.float32),
        in_specs=[pl.BlockSpec(memory_space=pl.ANY)],
        out_specs=pl.BlockSpec(memory_space=pltpu.VMEM),
        scratch_shapes=[
            vmem(*shape[:-1]),
            vmem(TOTAL),
            vmem(TOTAL),
            vmem(5, 3, 2, 2, 3, SUB),
            vmem(5, 2, 3, 3, SUB),
            vmem(5, 2, 3, 3, SUB),
            pltpu.SemaphoreType.DMA,
            pltpu.SemaphoreType.DMA,
            pltpu.SemaphoreType.DMA((8,)),
        ],
        compiler_params=pltpu.CompilerParams(collective_id=0, has_side_effects=True),
        name="force_terms",
    )(links.reshape(shape))
    out = pl.pallas_call(
        functools.partial(expand, halves),
        out_shape=jax.ShapeDtypeStruct(shape, jnp.float32),
        in_specs=[pl.BlockSpec(memory_space=pltpu.VMEM)],
        out_specs=pl.BlockSpec(memory_space=pl.ANY),
        scratch_shapes=[vmem(*shape[:-1]), pltpu.SemaphoreType.DMA((4,))],
        name="expand",
    )(pltpu.with_memory_space_constraint(terms, pltpu.VMEM))
    return out.reshape(links.shape)


def solution(mesh):
    assert mesh.axis_names == ("gx", "gz", "ta")
    counts = tuple(mesh.shape[a] for a in AXES)
    spec = P(None, None, None, None, "ta", "gz", "gx")
    return jax.shard_map(
        functools.partial(per_device, counts),
        mesh=mesh,
        in_specs=(spec,),
        out_specs=spec,
        check_vma=False,
    )
```

```python
import functools

import jax
import jax.numpy as jnp
from jax import lax
from jax.experimental import pallas as pl
from jax.experimental.pallas import tpu as pltpu
from jax.sharding import PartitionSpec as P

NX = 16
COEFF = -1.9
AXES = ("ta", "gz", "gx")
SUB, LANES = 8, 128


def others(d):
    return [m for m in range(4) if m != d]


class Lattice:
    def __init__(self, depth):
        self.depth = depth
        self.per = SUB // depth
        self.ygroups = LANES // NX
        self.row = lax.broadcasted_iota(jnp.int32, (SUB, LANES), 0)
        self.lane = lax.broadcasted_iota(jnp.int32, (SUB, LANES), 1)
        self.zrow = self.row % depth
        self.xcol = self.lane % NX

    def rows(self, value, shift):
        shift %= SUB
        return pltpu.roll(value, shift, 0) if shift else value

    def lanes(self, value, shift):
        shift %= LANES
        return pltpu.roll(value, shift, 1) if shift else value


def entry(left, right, i, j, part, left_h, right_h):
    total = None
    for k in range(3):
        li = (k, i) if left_h else (i, k)
        ri = (j, k) if right_h else (k, j)
        lr, lm = left[0][li[0]][li[1]], left[1][li[0]][li[1]]
        rr, rm = right[0][ri[0]][ri[1]], right[1][ri[0]][ri[1]]
        if part == 0:
            first, second = lr * rr, lm * rm
            minus = left_h == right_h
        elif left_h:
            first, second = lr * rm, lm * rr
            minus = True
        else:
            first, second = lm * rr, lr * rm
            minus = right_h
        value = first - second if minus else first + second
        total = value if total is None else total + value
    return total


def product(left, right, left_h=False, right_h=False):
    return [
        [[entry(left, right, i, j, part, left_h, right_h) for j in range(3)] for i in range(3)]
        for part in range(2)
    ]


def projected(left, right, left_h=False, right_h=False):
    get = lambda i, j, part: entry(left, right, i, j, part, left_h, right_h)
    pairs = ((0, 1), (0, 2), (1, 2))
    real = [get(i, j, 0) - get(j, i, 0) for i, j in pairs]
    imag = [get(i, j, 1) + get(j, i, 1) for i, j in pairs]
    diag = [get(i, i, 1) for i in range(3)]
    third = (diag[0] + diag[1] + diag[2]) * (1.0 / 3.0)
    return real + imag + [diag[0] - third, diag[1] - third]


def third_row(real, imag):
    rows_r, rows_i = [], []
    for column in range(3):
        n, l = (column + 1) % 3, (column + 2) % 3
        rows_r.append(
            real[0][n] * real[1][l]
            - imag[0][n] * imag[1][l]
            - real[0][l] * real[1][n]
            + imag[0][l] * imag[1][n]
        )
        rows_i.append(
            real[0][l] * imag[1][n]
            + imag[0][l] * real[1][n]
            - real[0][n] * imag[1][l]
            - imag[0][n] * real[1][l]
        )
    return rows_r, rows_i


PLANES = ((0, 1), (0, 2), (0, 3), (1, 2), (1, 3), (2, 3))
DIAGONALS = ((0, 2), (2, 0), (0, 1), (1, 0), (1, 2), (2, 1))
LAYOUT = (
    (((1, 0), (2, 0)), ((3, 0),)),
    (((0, 0), (0, 1), (2, 0), (2, 1)), ((3, 0), (3, 1))),
    (((0, 0), (0, 1), (1, 0), (1, 1), (3, 0), (3, 1)),),
)
ROWS = (144, 144, 96)
EDGE = 2 * SUB


def offset(kind, d):
    if kind == "e":
        return 2 * sum(ROWS) + d * EDGE
    return (sum(ROWS) if kind == "g" else 0) + sum(ROWS[:d])


TOTAL = offset("e", len(DIAGONALS))


def force_terms(
    counts, depth, halves, hbm, acc, u, out_s, in_s, face_s, b_s, pre_s, load_sem, send, recv,
):
    g = Lattice(depth)
    me = [lax.axis_index(a) for a in AXES]
    comps = [(part, i, j) for part in range(2) for i in range(2) for j in range(3)]
    last = (g.per - 1, depth - 1, g.ygroups - 1)
    place = (g.row // depth, g.zrow, g.lane // NX)

    def device(*steps):
        where = list(me)
        for i, step in steps:
            where[i] = lax.rem(me[i] + (step + counts[i]), counts[i])
        by = dict(zip(AXES, where))
        return (by["gx"], by["gz"], by["ta"])

    loads = [
        pltpu.make_async_copy(hbm.at[m, part], u.at[m, part], load_sem)
        for m in range(4)
        for part in range(2)
    ]
    for copy in loads:
        copy.start()
    barrier = pltpu.get_barrier_semaphore()
    partners = [device((i, step)) for i in (1, 0, 2) for step in (1, -1)]
    partners += [device((d, 1), (n, -1)) for d, n in DIAGONALS]
    for where in partners:
        pl.semaphore_signal(barrier, inc=1, device_id=where, device_id_type=pl.DeviceIdType.MESH)

    def remote(start, rows, slot, where):
        span = slice(start, start + rows)
        return pltpu.make_async_remote_copy(
            src_ref=out_s.at[span], dst_ref=in_s.at[span], send_sem=send, recv_sem=recv.at[slot],
            device_id=where, device_id_type=pl.DeviceIdType.MESH,
        )

    faces = [remote(offset("x", d), ROWS[d], d, device((d, -1))) for d in range(3)]
    opens = [remote(offset("g", d), ROWS[d], 3 + d, device((d, 1))) for d in range(3)]
    edges = [
        remote(offset("e", k), EDGE, 6 if k < 2 else 7, device((d, 1), (n, -1)))
        for k, (d, n) in enumerate(DIAGONALS)
    ]
    near_edges = remote(offset("e", 0), 2 * EDGE, 6, partners[0])
    far_edges = remote(offset("e", 2), 4 * EDGE, 7, partners[0])
    everything = remote(0, TOTAL, 0, partners[0])

    def load(m, part, i, j, h):
        return u[m, part, i, j, h * SUB : (h + 1) * SUB, :]

    def shifted(d, value, steps):
        if d == 0:
            return g.rows(value, depth * steps)
        return g.rows(value, steps) if d == 1 else g.lanes(value, NX * steps)

    def half(d, h, top):
        return (halves - 1 if top else 0) if d == 0 else h

    def complete(d, h):
        return d == 3 or (d == 0 and h + 1 < halves)

    def top(d, h=1):
        if d == 0:
            return g.row >= SUB - depth
        return g.zrow == depth - 1 if d == 1 else g.lane >= LANES - NX

    def bottom(d):
        return (g.row < depth, g.zrow == 0, g.lane < NX)[d]

    def open_mask(d, s, among=(0, 1, 2)):
        mask = None
        for k, (m, h) in enumerate(LAYOUT[d][s]):
            if m in among and not complete(m, h if d else 1):
                here = jnp.logical_and(place[d] == k, top(m))
                mask = here if mask is None else jnp.logical_or(mask, here)
        return mask

    def pick(mask, yes, no):
        return no if mask is None else jnp.where(mask, yes, no)

    def pack(d, s, get, up):
        value = None
        for k, (m, h) in enumerate(LAYOUT[d][s]):
            x = get(m, half(d, h, up))
            if x is None:
                continue
            x = shifted(d, x, k - (last[d] if up else 0))
            value = x if value is None else jnp.where(place[d] >= k, x, value)
        return value

    def complete_rows(get):
        real = [[get(0, i, j) for j in range(3)] for i in range(2)]
        imag = [[get(1, i, j) for j in range(3)] for i in range(2)]
        third_r, third_i = third_row(real, imag)
        return [real + [third_r], imag + [third_i]]

    def packed(d, s, get, up):
        return complete_rows(
            lambda part, i, j: pack(d, s, lambda m, h: get(m, h, part, i, j), up)
        )

    def put(kind, d, s, value):
        r = offset(kind, d)
        used = len(LAYOUT[d][s])
        for n, (part, i, j) in enumerate(comps[: 6 if s else 12]):
            v = value[part][i][j]
            if s:
                v = jnp.where(place[d] < used, v, shifted(d, value[1][i][j], used))
            at = r + (96 if s else 0) + n * SUB
            out_s[at : at + SUB, :] = v

    def fetch(ref, kind, d, s, part, i, j):
        n = part * 6 + i * 3 + j
        at = offset(kind, d) + n * SUB
        if not s:
            return ref[at : at + SUB, :]
        at += 96 - part * 6 * SUB
        v = ref[at : at + SUB, :]
        return shifted(d, v, -len(LAYOUT[d][s])) if part else v

    def fetched(ref, kind, d, s):
        return complete_rows(lambda part, i, j: fetch(ref, kind, d, s, part, i, j))

    def rolled(m, d, h, part, i, j):
        v = load(m, part, i, j, h)
        if d == 3:
            return jnp.where(g.xcol == NX - 1, g.lanes(v, NX - 1), g.lanes(v, -1))
        if d == 2:
            return g.lanes(v, -NX)
        if d == 1:
            return g.rows(v, -1)
        if h + 1 < halves:
            beyond = g.rows(load(m, part, i, j, h + 1), -depth)
            return jnp.where(g.row >= SUB - depth, beyond, g.rows(v, -depth))
        return g.rows(v, -depth)

    def matrix(get):
        return [[[get(part, i, j) for j in range(3)] for i in range(3)] for part in range(2)]

    def save(ref, index, value):
        for part in range(2):
            for i in range(ref.shape[-4]):
                for j in range(3):
                    ref[(*index, part, i, j)] = value[part][i][j]

    sets = [(d, s) for d in range(3) for s in range(len(LAYOUT[d]))]

    def kept(d, s, q):
        n = sets.index((d, s))
        return complete_rows(lambda part, i, j: face_s[n, q, part, i, j])

    def own_face(d):
        def get(part, i, j):
            if d != 2:
                return pack(d, 0, lambda m, h: load(d, part, i, j, h), True)
            pair = [shifted(d, load(d, part, i, j, h), h - last[d]) for h in range(halves)]
            pair = jnp.where(place[d] >= 1, pair[1], pair[0])
            value = jnp.where(place[d] >= 2, shifted(d, pair, 2), pair)
            return jnp.where(place[d] >= 4, shifted(d, pair, 4), value)

        return complete_rows(get)

    def step_in_face(d, m, v):
        if m == 3:
            return jnp.where(g.xcol == NX - 1, g.lanes(v, NX - 1), g.lanes(v, -1))
        if m == 2:
            return g.lanes(v, -NX)
        if m == 1:
            return g.rows(v, -1)
        moved = g.rows(v, -depth)
        if d == 1:
            beyond = g.rows(v, depth - 1)
            return jnp.where(jnp.logical_and(g.zrow == 0, g.row >= depth), beyond, moved)
        return jnp.where(g.row >= depth, g.lanes(moved, -NX), moved)

    def over_face(d, s, own):
        def get(part, i, j):
            value, before = None, None
            for k, (m, h) in enumerate(LAYOUT[d][s]):
                if m == before:
                    continue
                x = step_in_face(d, m, own[part][i][j])
                value = x if value is None else jnp.where(place[d] >= k, x, value)
                before = m
            return value

        return complete_rows(get)

    def send_side(d):
        own = own_face(d)
        for s in range(len(LAYOUT[d])):
            n = sets.index((d, s))
            side = packed(d, s, lambda m, h, *c: load(m, *c, h), True)
            over = over_face(d, s, own)
            b = product(own, side, left_h=True)
            mask = open_mask(d, s)
            put("g", d, s, [
                [
                    [pick(mask, b[p][i][j], entry(b, over, i, j, p, False, False)) for j in range(3)]
                    for i in range(2)
                ]
                for p in range(2)
            ])
            for q, value in enumerate((own, side, over)):
                save(face_s, (n, q), value)
            save(b_s, (n,), b)

    def send_face(d):
        for s in range(len(LAYOUT[d])):
            put("x", d, s, [
                [
                    [pack(d, s, lambda m, h: load(m, p, i, j, h), False) for j in range(3)]
                    for i in range(2)
                ]
                for p in range(2)
            ])

    def pack_edges(d, n):
        r0 = offset("e", DIAGONALS.index((d, n)))
        for c0 in range(0, 12, SUB):
            value = None
            for k in range(min(SUB, 12 - c0)):
                c = comps[c0 + k]
                if 2 not in (d, n):
                    v = load(d, *c, halves - 1 if d == 0 else 0)
                    x = g.rows(v, k - depth if d == 0 else k - (depth - 1))
                    value = x if value is None else jnp.where(g.row >= k, x, value)
                    continue
                if 0 in (d, n):
                    v = load(d, *c, halves - 1 if d == 0 else 0)
                else:
                    at = depth - 1 if d == 1 else 0
                    step = -1 if d == 1 else 1
                    v = load(d, *c, 0)
                    for h in range(1, halves):
                        v = jnp.where(g.zrow == at + step * h, g.rows(load(d, *c, h), step * h), v)
                x = g.lanes(v, NX * (k + (1 if d == 2 else 0)))
                value = x if value is None else jnp.where(g.lane >= NX * k, x, value)
            out_s[r0 + c0 : r0 + c0 + SUB, :] = value

    def edge(d, n, h, part, i, j):
        c = part * 6 + i * 3 + j
        r = offset("e", DIAGONALS.index((d, n))) + c // SUB * SUB
        v = in_s[r : r + SUB, :]
        k = c % SUB
        if (d, n) == (0, 1):
            return g.rows(v, depth - 1 - k)
        if (d, n) == (1, 0):
            return g.rows(v, SUB - depth - k)
        v = g.lanes(v, NX * ((0 if d == 2 else g.ygroups - 1) - k))
        if (d, n) == (0, 2):
            return g.rows(v, -(SUB - depth))
        if (d, n) == (2, 0):
            return g.rows(v, SUB - depth)
        return g.rows(v, 1 - depth + h if d == 1 else depth - 1 - h)

    everything_in = pltpu.make_async_copy(hbm, u, load_sem)
    everything_in.wait()
    for d, n in DIAGONALS:
        pack_edges(d, n)
    for d in (1, 0):
        send_side(d)
        send_face(d)
    send_face(2)
    pl.semaphore_wait(barrier, len(partners))
    for copy in edges[2:] + [opens[1], faces[1]] + edges[:2] + [opens[0], faces[0], faces[2]]:
        copy.start()
    send_side(2)
    opens[2].start()

    seen, pending = set(), {}

    def add(m, c, h, value):
        key = (m, c, h)
        pending[key] = pending[key] + value if key in pending else value

    def flush():
        for (m, c, h), value in pending.items():
            r = ((m * 8 + c) * halves + h) * SUB
            if (m, c, h) in seen:
                acc[r : r + SUB, :] += value
            else:
                seen.add((m, c, h))
                acc[r : r + SUB, :] = value
        pending.clear()

    def forward(m, d, h, q):
        for c in range(8):
            if d == 3:
                add(m, c, h, jnp.where(g.xcol == 0, g.lanes(q[c], 1 - NX), g.lanes(q[c], 1)))
            elif d == 2:
                add(m, c, h, g.lanes(q[c], NX))
            elif d == 1:
                add(m, c, h, g.rows(q[c], 1))
            elif h + 1 < halves:
                moved = g.rows(q[c], depth)
                add(m, c, h, jnp.where(g.row >= depth, moved, 0.0))
                add(m, c, h + 1, jnp.where(g.row < depth, moved, 0.0))
            else:
                add(m, c, h, g.rows(q[c], depth))

    def masked(mask, a):
        return [[[pick(mask, 0.0, v) for v in line] for line in part] for part in a]

    def inner(mu, nu, h):
        own = matrix(lambda *c: load(mu, *c, h))
        side = matrix(lambda *c: load(nu, *c, h))
        a = product(
            matrix(lambda *c: rolled(nu, mu, h, *c)),
            matrix(lambda *c: rolled(mu, nu, h, *c)),
            right_h=True,
        )
        mask = None
        for d in (mu, nu):
            if not complete(d, h):
                mask = top(d) if mask is None else jnp.logical_or(mask, top(d))
        a = masked(mask, a)
        b = product(own, side, left_h=True)
        forward(mu, nu, h, projected(a, b, left_h=True))
        forward(nu, mu, h, projected(a, b, right_h=True))
        upper = projected(product(own, a), side, right_h=True)
        for c in range(8):
            add(mu, c, h, upper[c])
            add(nu, c, h, -upper[c])

    def corners(d, among):
        for s in range(len(LAYOUT[d])):
            mask = open_mask(d, s, among)
            if mask is None:
                continue
            n = sets.index((d, s))

            def corner(m, h, c):
                if m not in among or complete(m, h):
                    return None
                k = LAYOUT[m][0].index((d, 0 if m == 0 else h))
                return shifted(m, fetch(in_s, "x", m, 0, *c), last[m] - k)

            for c in comps:
                value = pack(d, s, lambda m, h: corner(m, h, c), True)
                face_s[(n, 2, *c)] = jnp.where(mask, value, face_s[(n, 2, *c)])

    def face_terms(d, closed):
        for s, spots in enumerate(LAYOUT[d]):
            n = sets.index((d, s))
            own, side, over = (kept(d, s, q) for q in range(3))
            a = product(fetched(in_s, "x", d, s), over, right_h=True)
            a = masked(open_mask(d, s, [m for m in range(3) if m not in closed]), a)
            b = matrix(lambda *c: b_s[(n, *c)])
            upper = projected(product(own, a), side, right_h=True)
            low = projected(a, b, left_h=True)
            mask = open_mask(d, s, closed)
            low = [pick(mask, 0.0, v) for v in low]
            for k, (m, h) in enumerate(spots):
                h = half(d, h, True)
                natural = lambda v: jnp.where(top(d), shifted(d, v, last[d] - k), 0.0)
                for c in range(8):
                    x = natural(upper[c])
                    add(d, c, h, x)
                    add(m, c, h, -x)
                forward(d, m, h, [natural(v) for v in low])
        flush()

    def prepare(d):
        for s in range(len(LAYOUT[d])):
            own = fetched(out_s, "x", d, s)
            mask = open_mask(d, s)
            if mask is not None:
                far = packed(
                    d, s,
                    lambda m, h, *c: None if complete(m, h if d else 1) else edge(d, m, h, *c),
                    False,
                )
                both = product(own, far, right_h=True)
                own = [
                    [[jnp.where(mask, both[p][i][j], own[p][i][j]) for j in range(3)] for i in range(3)]
                    for p in range(2)
                ]
            save(pre_s, (sets.index((d, s)),), own)

    def close(d):
        for s, spots in enumerate(LAYOUT[d]):
            n = sets.index((d, s))
            q = projected(
                matrix(lambda *c: pre_s[(n, *c)]), fetched(in_s, "g", d, s), right_h=True
            )
            for k, (m, h) in enumerate(spots):
                for c in range(8):
                    add(m, c, half(d, h, False), jnp.where(bottom(d), shifted(d, q[c], -k), 0.0))
        flush()

    for pair in PLANES:
        for h in range(halves):
            inner(*pair, h)
        flush()
    faces[2].wait_recv()
    face_terms(2, ())
    corners(0, (2,))
    faces[0].wait_recv()
    face_terms(0, (2,))
    corners(1, (0, 2))
    near_edges.wait_recv()
    far_edges.wait_recv()
    for d in (2, 0, 1):
        prepare(d)
    for d in (2, 0):
        opens[d].wait_recv()
        close(d)
    faces[1].wait_recv()
    face_terms(1, (0, 2))
    opens[1].wait_recv()
    close(1)
    everything.wait_send()


def expand(halves, acc, hbm, out, sems):
    copies = []
    for m in range(4):
        for h in range(halves):
            rows = [((m * 8 + c) * halves + h) * SUB for c in range(8)]
            f = [acc[r : r + SUB, :] * (COEFF * 0.5 if c < 6 else COEFF) for c, r in enumerate(rows)]

            def put(part, i, j, value):
                out[m, part, i, j, h * SUB : (h + 1) * SUB, :] = value

            for n, (i, j) in enumerate(((0, 1), (0, 2), (1, 2))):
                put(0, i, j, f[n])
                put(0, j, i, -f[n])
                put(1, i, j, f[3 + n])
                put(1, j, i, f[3 + n])
            for i in range(3):
                put(0, i, i, jnp.zeros((SUB, LANES), jnp.float32))
            put(1, 0, 0, f[6])
            put(1, 1, 1, f[7])
            put(1, 2, 2, -(f[6] + f[7]))
        copies.append(pltpu.make_async_copy(out.at[m], hbm.at[m], sems.at[m]))
        copies[-1].start()
    for copy in copies:
        copy.wait()


def per_device(counts, links):
    time_len, depth, flat = links.shape[4:]
    sites = time_len * depth
    assert flat == LANES and (time_len, depth) == (4, 4)
    halves = sites // SUB
    vmem = lambda *s: pltpu.VMEM(s + (LANES,), jnp.float32)
    shape = links.shape[:4] + (sites, flat)
    terms = pl.pallas_call(
        functools.partial(force_terms, counts, depth, halves),
        out_shape=pltpu.VMEM((32 * sites, flat), jnp.float32),
        in_specs=[pl.BlockSpec(memory_space=pl.ANY)],
        out_specs=pl.BlockSpec(memory_space=pltpu.VMEM),
        scratch_shapes=[
            vmem(*shape[:-1]),
            vmem(TOTAL),
            vmem(TOTAL),
            vmem(5, 3, 2, 2, 3, SUB),
            vmem(5, 2, 3, 3, SUB),
            vmem(5, 2, 3, 3, SUB),
            pltpu.SemaphoreType.DMA,
            pltpu.SemaphoreType.DMA,
            pltpu.SemaphoreType.DMA((8,)),
        ],
        compiler_params=pltpu.CompilerParams(collective_id=0, has_side_effects=True),
        name="force_terms",
    )(links.reshape(shape))
    out = pl.pallas_call(
        functools.partial(expand, halves),
        out_shape=jax.ShapeDtypeStruct(shape, jnp.float32),
        in_specs=[pl.BlockSpec(memory_space=pltpu.VMEM)],
        out_specs=pl.BlockSpec(memory_space=pl.ANY),
        scratch_shapes=[vmem(*shape[:-1]), pltpu.SemaphoreType.DMA((4,))],
        name="expand",
    )(pltpu.with_memory_space_constraint(terms, pltpu.VMEM))
    return out.reshape(links.shape)


def solution(mesh):
    assert mesh.axis_names == ("gx", "gz", "ta")
    counts = tuple(mesh.shape[a] for a in AXES)
    spec = P(None, None, None, None, "ta", "gz", "gx")
    return jax.shard_map(
        functools.partial(per_device, counts),
        mesh=mesh,
        in_specs=(spec,),
        out_specs=spec,
        check_vma=False,
    )
```

```python
import functools

import jax
import jax.numpy as jnp
from jax import lax
from jax.experimental import pallas as pl
from jax.experimental.pallas import tpu as pltpu
from jax.sharding import PartitionSpec as P

NX = 16
COEFF = -1.9
AXES = ("ta", "gz", "gx")
SUB, LANES = 8, 128


def others(d):
    return [m for m in range(4) if m != d]


class Lattice:
    def __init__(self, depth):
        self.depth = depth
        self.per = SUB // depth
        self.ygroups = LANES // NX
        self.row = lax.broadcasted_iota(jnp.int32, (SUB, LANES), 0)
        self.lane = lax.broadcasted_iota(jnp.int32, (SUB, LANES), 1)
        self.zrow = self.row % depth
        self.xcol = self.lane % NX

    def rows(self, value, shift):
        shift %= SUB
        return pltpu.roll(value, shift, 0) if shift else value

    def lanes(self, value, shift):
        shift %= LANES
        return pltpu.roll(value, shift, 1) if shift else value


def entry(left, right, i, j, part, left_h, right_h):
    total = None
    for k in range(3):
        li = (k, i) if left_h else (i, k)
        ri = (j, k) if right_h else (k, j)
        lr, lm = left[0][li[0]][li[1]], left[1][li[0]][li[1]]
        rr, rm = right[0][ri[0]][ri[1]], right[1][ri[0]][ri[1]]
        if part == 0:
            first, second = lr * rr, lm * rm
            minus = left_h == right_h
        elif left_h:
            first, second = lr * rm, lm * rr
            minus = True
        else:
            first, second = lm * rr, lr * rm
            minus = right_h
        value = first - second if minus else first + second
        total = value if total is None else total + value
    return total


def product(left, right, left_h=False, right_h=False):
    return [
        [[entry(left, right, i, j, part, left_h, right_h) for j in range(3)] for i in range(3)]
        for part in range(2)
    ]


def projected(left, right, left_h=False, right_h=False):
    get = lambda i, j, part: entry(left, right, i, j, part, left_h, right_h)
    pairs = ((0, 1), (0, 2), (1, 2))
    real = [get(i, j, 0) - get(j, i, 0) for i, j in pairs]
    imag = [get(i, j, 1) + get(j, i, 1) for i, j in pairs]
    diag = [get(i, i, 1) for i in range(3)]
    third = (diag[0] + diag[1] + diag[2]) * (1.0 / 3.0)
    return real + imag + [diag[0] - third, diag[1] - third]


def third_row(real, imag):
    rows_r, rows_i = [], []
    for column in range(3):
        n, l = (column + 1) % 3, (column + 2) % 3
        rows_r.append(
            real[0][n] * real[1][l]
            - imag[0][n] * imag[1][l]
            - real[0][l] * real[1][n]
            + imag[0][l] * imag[1][n]
        )
        rows_i.append(
            real[0][l] * imag[1][n]
            + imag[0][l] * real[1][n]
            - real[0][n] * imag[1][l]
            - imag[0][n] * real[1][l]
        )
    return rows_r, rows_i


PLANES = ((0, 1), (0, 2), (0, 3), (1, 2), (1, 3), (2, 3))
DIAGONALS = ((0, 2), (2, 0), (0, 1), (1, 0), (1, 2), (2, 1))
LAYOUT = (
    (((1, 0), (2, 0)), ((3, 0),)),
    (((0, 0), (0, 1), (2, 0), (2, 1)), ((3, 0), (3, 1))),
    (((0, 0), (0, 1), (1, 0), (1, 1), (3, 0), (3, 1)),),
)
ROWS = (144, 144, 96)
EDGE = 2 * SUB


def offset(kind, d):
    if kind == "e":
        return 2 * sum(ROWS) + d * EDGE
    return (sum(ROWS) if kind == "g" else 0) + sum(ROWS[:d])


TOTAL = offset("e", len(DIAGONALS))


def force_terms(
    counts, depth, halves, hbm, acc, u, out_s, in_s, face_s, b_s, pre_s, load_sem, send, recv, met,
):
    g = Lattice(depth)
    me = [lax.axis_index(a) for a in AXES]
    comps = [(part, i, j) for part in range(2) for i in range(2) for j in range(3)]
    last = (g.per - 1, depth - 1, g.ygroups - 1)
    place = (g.row // depth, g.zrow, g.lane // NX)

    def device(*steps):
        where = list(me)
        for i, step in steps:
            where[i] = lax.rem(me[i] + (step + counts[i]), counts[i])
        by = dict(zip(AXES, where))
        return (by["gx"], by["gz"], by["ta"])

    loads = [
        pltpu.make_async_copy(hbm.at[m, part, i], u.at[m, part, i], load_sem)
        for m in range(4)
        for part in range(2)
        for i in range(3)
    ]
    for copy in loads:
        copy.start()
    barrier = pltpu.get_barrier_semaphore()
    partners = [device((i, step)) for i in (1, 0, 2) for step in (1, -1)]
    for where in partners:
        pl.semaphore_signal(barrier, inc=1, device_id=where, device_id_type=pl.DeviceIdType.MESH)

    def remote(start, rows, slot, where):
        span = slice(start, start + rows)
        return pltpu.make_async_remote_copy(
            src_ref=out_s.at[span], dst_ref=in_s.at[span], send_sem=send, recv_sem=recv.at[slot],
            device_id=where, device_id_type=pl.DeviceIdType.MESH,
        )

    faces = [remote(offset("x", d), ROWS[d], d, device((d, -1))) for d in range(3)]
    opens = [remote(offset("g", d), ROWS[d], 3 + d, device((d, 1))) for d in range(3)]
    edges = [
        remote(offset("e", k), EDGE, 6 if k < 2 else 7, device((d, 1), (n, -1)))
        for k, (d, n) in enumerate(DIAGONALS)
    ]
    near_edges = remote(offset("e", 0), 2 * EDGE, 6, partners[0])
    far_edges = remote(offset("e", 2), 4 * EDGE, 7, partners[0])
    everything = remote(0, TOTAL, 0, partners[0])

    def load(m, part, i, j, h):
        return u[m, part, i, j, h * SUB : (h + 1) * SUB, :]

    def shifted(d, value, steps):
        if d == 0:
            return g.rows(value, depth * steps)
        return g.rows(value, steps) if d == 1 else g.lanes(value, NX * steps)

    def half(d, h, top):
        return (halves - 1 if top else 0) if d == 0 else h

    def complete(d, h):
        return d == 3 or (d == 0 and h + 1 < halves)

    def top(d, h=1):
        if d == 0:
            return g.row >= SUB - depth
        return g.zrow == depth - 1 if d == 1 else g.lane >= LANES - NX

    def bottom(d):
        return (g.row < depth, g.zrow == 0, g.lane < NX)[d]

    def open_mask(d, s, among=(0, 1, 2)):
        mask = None
        for k, (m, h) in enumerate(LAYOUT[d][s]):
            if m in among and not complete(m, h if d else 1):
                here = jnp.logical_and(place[d] == k, top(m))
                mask = here if mask is None else jnp.logical_or(mask, here)
        return mask

    def pick(mask, yes, no):
        return no if mask is None else jnp.where(mask, yes, no)

    def pack(d, s, get, up):
        value = None
        for k, (m, h) in enumerate(LAYOUT[d][s]):
            x = get(m, half(d, h, up))
            if x is None:
                continue
            x = shifted(d, x, k - (last[d] if up else 0))
            value = x if value is None else jnp.where(place[d] >= k, x, value)
        return value

    def complete_rows(get):
        real = [[get(0, i, j) for j in range(3)] for i in range(2)]
        imag = [[get(1, i, j) for j in range(3)] for i in range(2)]
        third_r, third_i = third_row(real, imag)
        return [real + [third_r], imag + [third_i]]

    def packed(d, s, get, up):
        return complete_rows(
            lambda part, i, j: pack(d, s, lambda m, h: get(m, h, part, i, j), up)
        )

    def put(kind, d, s, value):
        r = offset(kind, d)
        used = len(LAYOUT[d][s])
        for n, (part, i, j) in enumerate(comps[: 6 if s else 12]):
            v = value[part][i][j]
            if s:
                v = jnp.where(place[d] < used, v, shifted(d, value[1][i][j], used))
            at = r + (96 if s else 0) + n * SUB
            out_s[at : at + SUB, :] = v

    def fetch(ref, kind, d, s, part, i, j):
        n = part * 6 + i * 3 + j
        at = offset(kind, d) + n * SUB
        if not s:
            return ref[at : at + SUB, :]
        at += 96 - part * 6 * SUB
        v = ref[at : at + SUB, :]
        return shifted(d, v, -len(LAYOUT[d][s])) if part else v

    def fetched(ref, kind, d, s):
        return complete_rows(lambda part, i, j: fetch(ref, kind, d, s, part, i, j))

    def rolled(m, d, h, part, i, j):
        v = load(m, part, i, j, h)
        if d == 3:
            return jnp.where(g.xcol == NX - 1, g.lanes(v, NX - 1), g.lanes(v, -1))
        if d == 2:
            return g.lanes(v, -NX)
        if d == 1:
            return g.rows(v, -1)
        if h + 1 < halves:
            beyond = g.rows(load(m, part, i, j, h + 1), -depth)
            return jnp.where(g.row >= SUB - depth, beyond, g.rows(v, -depth))
        return g.rows(v, -depth)

    def matrix(get):
        return [[[get(part, i, j) for j in range(3)] for i in range(3)] for part in range(2)]

    def save(ref, index, value):
        for part in range(2):
            for i in range(ref.shape[-4]):
                for j in range(3):
                    ref[(*index, part, i, j)] = value[part][i][j]

    sets = [(d, s) for d in range(3) for s in range(len(LAYOUT[d]))]

    def kept(d, s, q):
        n = sets.index((d, s))
        return complete_rows(lambda part, i, j: face_s[n, q, part, i, j])

    def own_face(d):
        def get(part, i, j):
            if d != 2:
                return pack(d, 0, lambda m, h: load(d, part, i, j, h), True)
            pair = [shifted(d, load(d, part, i, j, h), h - last[d]) for h in range(halves)]
            pair = jnp.where(place[d] >= 1, pair[1], pair[0])
            value = jnp.where(place[d] >= 2, shifted(d, pair, 2), pair)
            return jnp.where(place[d] >= 4, shifted(d, pair, 4), value)

        return complete_rows(get)

    def step_in_face(d, m, v):
        if m == 3:
            return jnp.where(g.xcol == NX - 1, g.lanes(v, NX - 1), g.lanes(v, -1))
        if m == 2:
            return g.lanes(v, -NX)
        if m == 1:
            return g.rows(v, -1)
        moved = g.rows(v, -depth)
        if d == 1:
            beyond = g.rows(v, depth - 1)
            return jnp.where(jnp.logical_and(g.zrow == 0, g.row >= depth), beyond, moved)
        return jnp.where(g.row >= depth, g.lanes(moved, -NX), moved)

    def over_face(d, s, own):
        def get(part, i, j):
            value, before = None, None
            for k, (m, h) in enumerate(LAYOUT[d][s]):
                if m == before:
                    continue
                x = step_in_face(d, m, own[part][i][j])
                value = x if value is None else jnp.where(place[d] >= k, x, value)
                before = m
            return value

        return complete_rows(get)

    def send_side(d):
        own = own_face(d)
        for s in range(len(LAYOUT[d])):
            n = sets.index((d, s))
            side = packed(d, s, lambda m, h, *c: load(m, *c, h), True)
            over = over_face(d, s, own)
            b = product(own, side, left_h=True)
            mask = open_mask(d, s)
            put("g", d, s, [
                [
                    [pick(mask, b[p][i][j], entry(b, over, i, j, p, False, False)) for j in range(3)]
                    for i in range(2)
                ]
                for p in range(2)
            ])
            for q, value in enumerate((own, side, over)):
                save(face_s, (n, q), value)
            save(b_s, (n,), b)

    def send_face(d):
        for s in range(len(LAYOUT[d])):
            put("x", d, s, [
                [
                    [pack(d, s, lambda m, h: load(m, p, i, j, h), False) for j in range(3)]
                    for i in range(2)
                ]
                for p in range(2)
            ])

    def pack_edges(d, n):
        r0 = offset("e", DIAGONALS.index((d, n)))
        for c0 in range(0, 12, SUB):
            value = None
            for k in range(min(SUB, 12 - c0)):
                c = comps[c0 + k]
                if 2 not in (d, n):
                    v = load(d, *c, halves - 1 if d == 0 else 0)
                    x = g.rows(v, k - depth if d == 0 else k - (depth - 1))
                    value = x if value is None else jnp.where(g.row >= k, x, value)
                    continue
                if 0 in (d, n):
                    v = load(d, *c, halves - 1 if d == 0 else 0)
                else:
                    at = depth - 1 if d == 1 else 0
                    step = -1 if d == 1 else 1
                    v = load(d, *c, 0)
                    for h in range(1, halves):
                        v = jnp.where(g.zrow == at + step * h, g.rows(load(d, *c, h), step * h), v)
                x = g.lanes(v, NX * (k + (1 if d == 2 else 0)))
                value = x if value is None else jnp.where(g.lane >= NX * k, x, value)
            out_s[r0 + c0 : r0 + c0 + SUB, :] = value

    def edge(d, n, h, part, i, j):
        c = part * 6 + i * 3 + j
        r = offset("e", DIAGONALS.index((d, n))) + c // SUB * SUB
        v = in_s[r : r + SUB, :]
        k = c % SUB
        if (d, n) == (0, 1):
            return g.rows(v, depth - 1 - k)
        if (d, n) == (1, 0):
            return g.rows(v, SUB - depth - k)
        v = g.lanes(v, NX * ((0 if d == 2 else g.ygroups - 1) - k))
        if (d, n) == (0, 2):
            return g.rows(v, -(SUB - depth))
        if (d, n) == (2, 0):
            return g.rows(v, SUB - depth)
        return g.rows(v, 1 - depth + h if d == 1 else depth - 1 - h)

    everything_in = pltpu.make_async_copy(hbm, u, load_sem)
    everything_in.wait()
    for d, n in DIAGONALS:
        pack_edges(d, n)
    for d in (1, 0):
        send_side(d)
        send_face(d)
    send_face(2)
    pl.semaphore_wait(barrier, len(partners))
    for where in partners[2:]:
        pl.semaphore_signal(met, inc=1, device_id=where, device_id_type=pl.DeviceIdType.MESH)
    for copy in [opens[1], faces[1], opens[0], faces[0], faces[2]]:
        copy.start()
    send_side(2)
    opens[2].start()

    seen, pending = set(), {}

    def add(m, c, h, value):
        key = (m, c, h)
        pending[key] = pending[key] + value if key in pending else value

    def flush():
        for (m, c, h), value in pending.items():
            r = ((m * 8 + c) * halves + h) * SUB
            if (m, c, h) in seen:
                acc[r : r + SUB, :] += value
            else:
                seen.add((m, c, h))
                acc[r : r + SUB, :] = value
        pending.clear()

    def forward(m, d, h, q):
        for c in range(8):
            if d == 3:
                add(m, c, h, jnp.where(g.xcol == 0, g.lanes(q[c], 1 - NX), g.lanes(q[c], 1)))
            elif d == 2:
                add(m, c, h, g.lanes(q[c], NX))
            elif d == 1:
                add(m, c, h, g.rows(q[c], 1))
            elif h + 1 < halves:
                moved = g.rows(q[c], depth)
                add(m, c, h, jnp.where(g.row >= depth, moved, 0.0))
                add(m, c, h + 1, jnp.where(g.row < depth, moved, 0.0))
            else:
                add(m, c, h, g.rows(q[c], depth))

    def masked(mask, a):
        return [[[pick(mask, 0.0, v) for v in line] for line in part] for part in a]

    def inner(mu, nu, h):
        own = matrix(lambda *c: load(mu, *c, h))
        side = matrix(lambda *c: load(nu, *c, h))
        a = product(
            matrix(lambda *c: rolled(nu, mu, h, *c)),
            matrix(lambda *c: rolled(mu, nu, h, *c)),
            right_h=True,
        )
        mask = None
        for d in (mu, nu):
            if not complete(d, h):
                mask = top(d) if mask is None else jnp.logical_or(mask, top(d))
        a = masked(mask, a)
        b = product(own, side, left_h=True)
        forward(mu, nu, h, projected(a, b, left_h=True))
        forward(nu, mu, h, projected(a, b, right_h=True))
        upper = projected(product(own, a), side, right_h=True)
        for c in range(8):
            add(mu, c, h, upper[c])
            add(nu, c, h, -upper[c])

    def corners(d, among):
        for s in range(len(LAYOUT[d])):
            mask = open_mask(d, s, among)
            if mask is None:
                continue
            n = sets.index((d, s))

            def corner(m, h, c):
                if m not in among or complete(m, h):
                    return None
                k = LAYOUT[m][0].index((d, 0 if m == 0 else h))
                return shifted(m, fetch(in_s, "x", m, 0, *c), last[m] - k)

            for c in comps:
                value = pack(d, s, lambda m, h: corner(m, h, c), True)
                face_s[(n, 2, *c)] = jnp.where(mask, value, face_s[(n, 2, *c)])

    def face_terms(d, closed):
        for s, spots in enumerate(LAYOUT[d]):
            n = sets.index((d, s))
            own, side, over = (kept(d, s, q) for q in range(3))
            a = product(fetched(in_s, "x", d, s), over, right_h=True)
            a = masked(open_mask(d, s, [m for m in range(3) if m not in closed]), a)
            b = matrix(lambda *c: b_s[(n, *c)])
            upper = projected(product(own, a), side, right_h=True)
            low = projected(a, b, left_h=True)
            mask = open_mask(d, s, closed)
            low = [pick(mask, 0.0, v) for v in low]
            for k, (m, h) in enumerate(spots):
                h = half(d, h, True)
                natural = lambda v: jnp.where(top(d), shifted(d, v, last[d] - k), 0.0)
                for c in range(8):
                    x = natural(upper[c])
                    add(d, c, h, x)
                    add(m, c, h, -x)
                forward(d, m, h, [natural(v) for v in low])
        flush()

    def prepare(d):
        for s in range(len(LAYOUT[d])):
            own = fetched(out_s, "x", d, s)
            mask = open_mask(d, s)
            if mask is not None:
                far = packed(
                    d, s,
                    lambda m, h, *c: None if complete(m, h if d else 1) else edge(d, m, h, *c),
                    False,
                )
                both = product(own, far, right_h=True)
                own = [
                    [[jnp.where(mask, both[p][i][j], own[p][i][j]) for j in range(3)] for i in range(3)]
                    for p in range(2)
                ]
            save(pre_s, (sets.index((d, s)),), own)

    def close(d):
        for s, spots in enumerate(LAYOUT[d]):
            n = sets.index((d, s))
            q = projected(
                matrix(lambda *c: pre_s[(n, *c)]), fetched(in_s, "g", d, s), right_h=True
            )
            for k, (m, h) in enumerate(spots):
                for c in range(8):
                    add(m, c, half(d, h, False), jnp.where(bottom(d), shifted(d, q[c], -k), 0.0))
        flush()

    for n, pair in enumerate(PLANES):
        if n == 3:
            pl.semaphore_wait(met, len(partners) - 2)
            for copy in edges[2:] + edges[:2]:
                copy.start()
        for h in range(halves):
            inner(*pair, h)
        flush()
    faces[2].wait_recv()
    face_terms(2, ())
    corners(0, (2,))
    faces[0].wait_recv()
    face_terms(0, (2,))
    corners(1, (0, 2))
    near_edges.wait_recv()
    far_edges.wait_recv()
    for d in (2, 0, 1):
        prepare(d)
    for d in (2, 0):
        opens[d].wait_recv()
        close(d)
    faces[1].wait_recv()
    face_terms(1, (0, 2))
    opens[1].wait_recv()
    close(1)
    everything.wait_send()


def expand(halves, acc, hbm, out, sem):
    for m in range(4):
        for h in range(halves):
            rows = [((m * 8 + c) * halves + h) * SUB for c in range(8)]
            f = [acc[r : r + SUB, :] * (COEFF * 0.5 if c < 6 else COEFF) for c, r in enumerate(rows)]

            def put(part, i, j, value):
                out[m, part, i, j, h * SUB : (h + 1) * SUB, :] = value

            for n, (i, j) in enumerate(((0, 1), (0, 2), (1, 2))):
                put(0, i, j, f[n])
                put(0, j, i, -f[n])
                put(1, i, j, f[3 + n])
                put(1, j, i, f[3 + n])
            for i in range(3):
                put(0, i, i, jnp.zeros((SUB, LANES), jnp.float32))
            put(1, 0, 0, f[6])
            put(1, 1, 1, f[7])
            put(1, 2, 2, -(f[6] + f[7]))
        for part in range(2):
            for i in range(3):
                pltpu.make_async_copy(out.at[m, part, i], hbm.at[m, part, i], sem).start()
    pltpu.make_async_copy(out, hbm, sem).wait()


def per_device(counts, links):
    time_len, depth, flat = links.shape[4:]
    sites = time_len * depth
    assert flat == LANES and (time_len, depth) == (4, 4)
    halves = sites // SUB
    vmem = lambda *s: pltpu.VMEM(s + (LANES,), jnp.float32)
    shape = links.shape[:4] + (sites, flat)
    terms = pl.pallas_call(
        functools.partial(force_terms, counts, depth, halves),
        out_shape=pltpu.VMEM((32 * sites, flat), jnp.float32),
        in_specs=[pl.BlockSpec(memory_space=pl.ANY)],
        out_specs=pl.BlockSpec(memory_space=pltpu.VMEM),
        scratch_shapes=[
            vmem(*shape[:-1]),
            vmem(TOTAL),
            vmem(TOTAL),
            vmem(5, 3, 2, 2, 3, SUB),
            vmem(5, 2, 3, 3, SUB),
            vmem(5, 2, 3, 3, SUB),
            pltpu.SemaphoreType.DMA,
            pltpu.SemaphoreType.DMA,
            pltpu.SemaphoreType.DMA((8,)),
            pltpu.SemaphoreType.REGULAR,
        ],
        compiler_params=pltpu.CompilerParams(collective_id=0, has_side_effects=True),
        name="force_terms",
    )(links.reshape(shape))
    out = pl.pallas_call(
        functools.partial(expand, halves),
        out_shape=jax.ShapeDtypeStruct(shape, jnp.float32),
        in_specs=[pl.BlockSpec(memory_space=pltpu.VMEM)],
        out_specs=pl.BlockSpec(memory_space=pl.ANY),
        scratch_shapes=[vmem(*shape[:-1]), pltpu.SemaphoreType.DMA],
        name="expand",
    )(pltpu.with_memory_space_constraint(terms, pltpu.VMEM))
    return out.reshape(links.shape)


def solution(mesh):
    assert mesh.axis_names == ("gx", "gz", "ta")
    counts = tuple(mesh.shape[a] for a in AXES)
    spec = P(None, None, None, None, "ta", "gz", "gx")
    return jax.shard_map(
        functools.partial(per_device, counts),
        mesh=mesh,
        in_specs=(spec,),
        out_specs=spec,
        check_vma=False,
    )
```

```python
import functools

import jax
import jax.numpy as jnp
from jax import lax
from jax.experimental import pallas as pl
from jax.experimental.pallas import tpu as pltpu
from jax.sharding import PartitionSpec as P

NX = 16
COEFF = -1.9
AXES = ("ta", "gz", "gx")
SUB, LANES = 8, 128


def others(d):
    return [m for m in range(4) if m != d]


class Lattice:
    def __init__(self, depth):
        self.depth = depth
        self.per = SUB // depth
        self.ygroups = LANES // NX
        self.row = lax.broadcasted_iota(jnp.int32, (SUB, LANES), 0)
        self.lane = lax.broadcasted_iota(jnp.int32, (SUB, LANES), 1)
        self.zrow = self.row % depth
        self.xcol = self.lane % NX

    def rows(self, value, shift):
        shift %= SUB
        return pltpu.roll(value, shift, 0) if shift else value

    def lanes(self, value, shift):
        shift %= LANES
        return pltpu.roll(value, shift, 1) if shift else value


def entry(left, right, i, j, part, left_h, right_h):
    total = None
    for k in range(3):
        li = (k, i) if left_h else (i, k)
        ri = (j, k) if right_h else (k, j)
        lr, lm = left[0][li[0]][li[1]], left[1][li[0]][li[1]]
        rr, rm = right[0][ri[0]][ri[1]], right[1][ri[0]][ri[1]]
        if part == 0:
            first, second = lr * rr, lm * rm
            minus = left_h == right_h
        elif left_h:
            first, second = lr * rm, lm * rr
            minus = True
        else:
            first, second = lm * rr, lr * rm
            minus = right_h
        value = first - second if minus else first + second
        total = value if total is None else total + value
    return total


def product(left, right, left_h=False, right_h=False):
    return [
        [[entry(left, right, i, j, part, left_h, right_h) for j in range(3)] for i in range(3)]
        for part in range(2)
    ]


def projected(left, right, left_h=False, right_h=False):
    get = lambda i, j, part: entry(left, right, i, j, part, left_h, right_h)
    pairs = ((0, 1), (0, 2), (1, 2))
    real = [get(i, j, 0) - get(j, i, 0) for i, j in pairs]
    imag = [get(i, j, 1) + get(j, i, 1) for i, j in pairs]
    diag = [get(i, i, 1) for i in range(3)]
    third = (diag[0] + diag[1] + diag[2]) * (1.0 / 3.0)
    return real + imag + [diag[0] - third, diag[1] - third]


def third_row(real, imag):
    rows_r, rows_i = [], []
    for column in range(3):
        n, l = (column + 1) % 3, (column + 2) % 3
        rows_r.append(
            real[0][n] * real[1][l]
            - imag[0][n] * imag[1][l]
            - real[0][l] * real[1][n]
            + imag[0][l] * imag[1][n]
        )
        rows_i.append(
            real[0][l] * imag[1][n]
            + imag[0][l] * real[1][n]
            - real[0][n] * imag[1][l]
            - imag[0][n] * real[1][l]
        )
    return rows_r, rows_i


PLANES = ((0, 1), (0, 2), (0, 3), (1, 2), (1, 3), (2, 3))
DIAGONALS = ((0, 1), (1, 0), (1, 2), (2, 1), (0, 2), (2, 0))
LEGS = (
    ((0, 1), (1, -1)),
    ((0, -1), (1, 1)),
    ((2, -1), (1, 1)),
    ((2, 1), (1, -1)),
    ((2, -1), (0, 1)),
    ((2, 1), (0, -1)),
)
LAYOUT = (
    (((1, 0), (2, 0)), ((3, 0),)),
    (((0, 0), (0, 1), (2, 0), (2, 1)), ((3, 0), (3, 1))),
    (((0, 0), (0, 1), (1, 0), (1, 1), (3, 0), (3, 1)),),
)
ROWS = (144, 144, 96)
EDGE = 2 * SUB


def offset(kind, d):
    if kind == "e":
        return 2 * sum(ROWS) + d * EDGE
    return (sum(ROWS) if kind == "g" else 0) + sum(ROWS[:d])


TOTAL = offset("e", len(DIAGONALS))


def force_terms(
    counts, depth, halves, hbm, acc, u, out_s, in_s, relay_s, face_s, b_s, pre_s,
    load_sem, send, recv, passed,
):
    g = Lattice(depth)
    me = [lax.axis_index(a) for a in AXES]
    comps = [(part, i, j) for part in range(2) for i in range(2) for j in range(3)]
    last = (g.per - 1, depth - 1, g.ygroups - 1)
    place = (g.row // depth, g.zrow, g.lane // NX)

    def device(*steps):
        where = list(me)
        for i, step in steps:
            where[i] = lax.rem(me[i] + (step + counts[i]), counts[i])
        by = dict(zip(AXES, where))
        return (by["gx"], by["gz"], by["ta"])

    loads = [
        pltpu.make_async_copy(hbm.at[m, part, i], u.at[m, part, i], load_sem)
        for m in range(4)
        for part in range(2)
        for i in range(3)
    ]
    for copy in loads:
        copy.start()
    barrier = pltpu.get_barrier_semaphore()
    partners = [device((i, step)) for i in (1, 0, 2) for step in (1, -1)]
    for where in partners:
        pl.semaphore_signal(barrier, inc=1, device_id=where, device_id_type=pl.DeviceIdType.MESH)

    def remote(start, rows, slot, where):
        span = slice(start, start + rows)
        return pltpu.make_async_remote_copy(
            src_ref=out_s.at[span], dst_ref=in_s.at[span], send_sem=send, recv_sem=recv.at[slot],
            device_id=where, device_id_type=pl.DeviceIdType.MESH,
        )

    faces = [remote(offset("x", d), ROWS[d], d, device((d, -1))) for d in range(3)]
    opens = [remote(offset("g", d), ROWS[d], 3 + d, device((d, 1))) for d in range(3)]
    first_legs, second_legs = [], []
    for k, (leg, then) in enumerate(LEGS):
        span = slice(k * EDGE, (k + 1) * EDGE)
        at = slice(offset("e", k), offset("e", k + 1))
        first_legs.append(
            pltpu.make_async_remote_copy(
                src_ref=out_s.at[at], dst_ref=relay_s.at[span], send_sem=send, recv_sem=recv.at[6],
                device_id=device(leg), device_id_type=pl.DeviceIdType.MESH,
            )
        )
        second_legs.append(
            pltpu.make_async_remote_copy(
                src_ref=relay_s.at[span], dst_ref=in_s.at[at], send_sem=passed, recv_sem=recv.at[7],
                device_id=device(then), device_id_type=pl.DeviceIdType.MESH,
            )
        )
    edge_rows = slice(offset("e", 0), TOTAL)
    relayed = pltpu.make_async_remote_copy(
        src_ref=relay_s, dst_ref=relay_s, send_sem=passed, recv_sem=recv.at[6],
        device_id=partners[0], device_id_type=pl.DeviceIdType.MESH,
    )
    edges = pltpu.make_async_remote_copy(
        src_ref=relay_s, dst_ref=in_s.at[edge_rows], send_sem=passed, recv_sem=recv.at[7],
        device_id=partners[0], device_id_type=pl.DeviceIdType.MESH,
    )
    everything = remote(0, TOTAL, 0, partners[0])

    def load(m, part, i, j, h):
        return u[m, part, i, j, h * SUB : (h + 1) * SUB, :]

    def shifted(d, value, steps):
        if d == 0:
            return g.rows(value, depth * steps)
        return g.rows(value, steps) if d == 1 else g.lanes(value, NX * steps)

    def half(d, h, top):
        return (halves - 1 if top else 0) if d == 0 else h

    def complete(d, h):
        return d == 3 or (d == 0 and h + 1 < halves)

    def top(d, h=1):
        if d == 0:
            return g.row >= SUB - depth
        return g.zrow == depth - 1 if d == 1 else g.lane >= LANES - NX

    def bottom(d):
        return (g.row < depth, g.zrow == 0, g.lane < NX)[d]

    def open_mask(d, s, among=(0, 1, 2)):
        mask = None
        for k, (m, h) in enumerate(LAYOUT[d][s]):
            if m in among and not complete(m, h if d else 1):
                here = jnp.logical_and(place[d] == k, top(m))
                mask = here if mask is None else jnp.logical_or(mask, here)
        return mask

    def pick(mask, yes, no):
        return no if mask is None else jnp.where(mask, yes, no)

    def pack(d, s, get, up):
        value = None
        for k, (m, h) in enumerate(LAYOUT[d][s]):
            x = get(m, half(d, h, up))
            if x is None:
                continue
            x = shifted(d, x, k - (last[d] if up else 0))
            value = x if value is None else jnp.where(place[d] >= k, x, value)
        return value

    def complete_rows(get):
        real = [[get(0, i, j) for j in range(3)] for i in range(2)]
        imag = [[get(1, i, j) for j in range(3)] for i in range(2)]
        third_r, third_i = third_row(real, imag)
        return [real + [third_r], imag + [third_i]]

    def packed(d, s, get, up):
        return complete_rows(
            lambda part, i, j: pack(d, s, lambda m, h: get(m, h, part, i, j), up)
        )

    def put(kind, d, s, value):
        r = offset(kind, d)
        used = len(LAYOUT[d][s])
        for n, (part, i, j) in enumerate(comps[: 6 if s else 12]):
            v = value[part][i][j]
            if s:
                v = jnp.where(place[d] < used, v, shifted(d, value[1][i][j], used))
            at = r + (96 if s else 0) + n * SUB
            out_s[at : at + SUB, :] = v

    def fetch(ref, kind, d, s, part, i, j):
        n = part * 6 + i * 3 + j
        at = offset(kind, d) + n * SUB
        if not s:
            return ref[at : at + SUB, :]
        at += 96 - part * 6 * SUB
        v = ref[at : at + SUB, :]
        return shifted(d, v, -len(LAYOUT[d][s])) if part else v

    def fetched(ref, kind, d, s):
        return complete_rows(lambda part, i, j: fetch(ref, kind, d, s, part, i, j))

    def rolled(m, d, h, part, i, j):
        v = load(m, part, i, j, h)
        if d == 3:
            return jnp.where(g.xcol == NX - 1, g.lanes(v, NX - 1), g.lanes(v, -1))
        if d == 2:
            return g.lanes(v, -NX)
        if d == 1:
            return g.rows(v, -1)
        if h + 1 < halves:
            beyond = g.rows(load(m, part, i, j, h + 1), -depth)
            return jnp.where(g.row >= SUB - depth, beyond, g.rows(v, -depth))
        return g.rows(v, -depth)

    def matrix(get):
        return [[[get(part, i, j) for j in range(3)] for i in range(3)] for part in range(2)]

    def save(ref, index, value):
        for part in range(2):
            for i in range(ref.shape[-4]):
                for j in range(3):
                    ref[(*index, part, i, j)] = value[part][i][j]

    sets = [(d, s) for d in range(3) for s in range(len(LAYOUT[d]))]

    def kept(d, s, q):
        n = sets.index((d, s))
        return complete_rows(lambda part, i, j: face_s[n, q, part, i, j])

    def own_face(d):
        def get(part, i, j):
            if d != 2:
                return pack(d, 0, lambda m, h: load(d, part, i, j, h), True)
            pair = [shifted(d, load(d, part, i, j, h), h - last[d]) for h in range(halves)]
            pair = jnp.where(place[d] >= 1, pair[1], pair[0])
            value = jnp.where(place[d] >= 2, shifted(d, pair, 2), pair)
            return jnp.where(place[d] >= 4, shifted(d, pair, 4), value)

        return complete_rows(get)

    def step_in_face(d, m, v):
        if m == 3:
            return jnp.where(g.xcol == NX - 1, g.lanes(v, NX - 1), g.lanes(v, -1))
        if m == 2:
            return g.lanes(v, -NX)
        if m == 1:
            return g.rows(v, -1)
        moved = g.rows(v, -depth)
        if d == 1:
            beyond = g.rows(v, depth - 1)
            return jnp.where(jnp.logical_and(g.zrow == 0, g.row >= depth), beyond, moved)
        return jnp.where(g.row >= depth, g.lanes(moved, -NX), moved)

    def over_face(d, s, own):
        def get(part, i, j):
            value, before = None, None
            for k, (m, h) in enumerate(LAYOUT[d][s]):
                if m == before:
                    continue
                x = step_in_face(d, m, own[part][i][j])
                value = x if value is None else jnp.where(place[d] >= k, x, value)
                before = m
            return value

        return complete_rows(get)

    def send_side(d):
        own = own_face(d)
        for s in range(len(LAYOUT[d])):
            n = sets.index((d, s))
            side = packed(d, s, lambda m, h, *c: load(m, *c, h), True)
            over = over_face(d, s, own)
            b = product(own, side, left_h=True)
            mask = open_mask(d, s)
            put("g", d, s, [
                [
                    [pick(mask, b[p][i][j], entry(b, over, i, j, p, False, False)) for j in range(3)]
                    for i in range(2)
                ]
                for p in range(2)
            ])
            for q, value in enumerate((own, side, over)):
                save(face_s, (n, q), value)
            save(b_s, (n,), b)

    def send_face(d):
        for s in range(len(LAYOUT[d])):
            put("x", d, s, [
                [
                    [pack(d, s, lambda m, h: load(m, p, i, j, h), False) for j in range(3)]
                    for i in range(2)
                ]
                for p in range(2)
            ])

    def pack_edges(d, n):
        r0 = offset("e", DIAGONALS.index((d, n)))
        for c0 in range(0, 12, SUB):
            value = None
            for k in range(min(SUB, 12 - c0)):
                c = comps[c0 + k]
                if 2 not in (d, n):
                    v = load(d, *c, halves - 1 if d == 0 else 0)
                    x = g.rows(v, k - depth if d == 0 else k - (depth - 1))
                    value = x if value is None else jnp.where(g.row >= k, x, value)
                    continue
                if 0 in (d, n):
                    v = load(d, *c, halves - 1 if d == 0 else 0)
                else:
                    at = depth - 1 if d == 1 else 0
                    step = -1 if d == 1 else 1
                    v = load(d, *c, 0)
                    for h in range(1, halves):
                        v = jnp.where(g.zrow == at + step * h, g.rows(load(d, *c, h), step * h), v)
                x = g.lanes(v, NX * (k + (1 if d == 2 else 0)))
                value = x if value is None else jnp.where(g.lane >= NX * k, x, value)
            out_s[r0 + c0 : r0 + c0 + SUB, :] = value

    def edge(d, n, h, part, i, j):
        c = part * 6 + i * 3 + j
        r = offset("e", DIAGONALS.index((d, n))) + c // SUB * SUB
        v = in_s[r : r + SUB, :]
        k = c % SUB
        if (d, n) == (0, 1):
            return g.rows(v, depth - 1 - k)
        if (d, n) == (1, 0):
            return g.rows(v, SUB - depth - k)
        v = g.lanes(v, NX * ((0 if d == 2 else g.ygroups - 1) - k))
        if (d, n) == (0, 2):
            return g.rows(v, -(SUB - depth))
        if (d, n) == (2, 0):
            return g.rows(v, SUB - depth)
        return g.rows(v, 1 - depth + h if d == 1 else depth - 1 - h)

    everything_in = pltpu.make_async_copy(hbm, u, load_sem)
    everything_in.wait()
    for d, n in DIAGONALS:
        pack_edges(d, n)
    for d in (1, 0):
        send_side(d)
        send_face(d)
    send_face(2)
    pl.semaphore_wait(barrier, len(partners))
    for copy in first_legs + [opens[1], faces[1], opens[0], faces[0], faces[2]]:
        copy.start()
    send_side(2)
    opens[2].start()
    relayed.wait_recv()
    for copy in second_legs:
        copy.start()

    seen, pending = set(), {}

    def add(m, c, h, value):
        key = (m, c, h)
        pending[key] = pending[key] + value if key in pending else value

    def flush():
        for (m, c, h), value in pending.items():
            r = ((m * 8 + c) * halves + h) * SUB
            if (m, c, h) in seen:
                acc[r : r + SUB, :] += value
            else:
                seen.add((m, c, h))
                acc[r : r + SUB, :] = value
        pending.clear()

    def forward(m, d, h, q):
        for c in range(8):
            if d == 3:
                add(m, c, h, jnp.where(g.xcol == 0, g.lanes(q[c], 1 - NX), g.lanes(q[c], 1)))
            elif d == 2:
                add(m, c, h, g.lanes(q[c], NX))
            elif d == 1:
                add(m, c, h, g.rows(q[c], 1))
            elif h + 1 < halves:
                moved = g.rows(q[c], depth)
                add(m, c, h, jnp.where(g.row >= depth, moved, 0.0))
                add(m, c, h + 1, jnp.where(g.row < depth, moved, 0.0))
            else:
                add(m, c, h, g.rows(q[c], depth))

    def masked(mask, a):
        return [[[pick(mask, 0.0, v) for v in line] for line in part] for part in a]

    def inner(mu, nu, h):
        own = matrix(lambda *c: load(mu, *c, h))
        side = matrix(lambda *c: load(nu, *c, h))
        a = product(
            matrix(lambda *c: rolled(nu, mu, h, *c)),
            matrix(lambda *c: rolled(mu, nu, h, *c)),
            right_h=True,
        )
        mask = None
        for d in (mu, nu):
            if not complete(d, h):
                mask = top(d) if mask is None else jnp.logical_or(mask, top(d))
        a = masked(mask, a)
        b = product(own, side, left_h=True)
        forward(mu, nu, h, projected(a, b, left_h=True))
        forward(nu, mu, h, projected(a, b, right_h=True))
        upper = projected(product(own, a), side, right_h=True)
        for c in range(8):
            add(mu, c, h, upper[c])
            add(nu, c, h, -upper[c])

    def corners(d, among):
        for s in range(len(LAYOUT[d])):
            mask = open_mask(d, s, among)
            if mask is None:
                continue
            n = sets.index((d, s))

            def corner(m, h, c):
                if m not in among or complete(m, h):
                    return None
                k = LAYOUT[m][0].index((d, 0 if m == 0 else h))
                return shifted(m, fetch(in_s, "x", m, 0, *c), last[m] - k)

            for c in comps:
                value = pack(d, s, lambda m, h: corner(m, h, c), True)
                face_s[(n, 2, *c)] = jnp.where(mask, value, face_s[(n, 2, *c)])

    def face_terms(d, closed):
        for s, spots in enumerate(LAYOUT[d]):
            n = sets.index((d, s))
            own, side, over = (kept(d, s, q) for q in range(3))
            a = product(fetched(in_s, "x", d, s), over, right_h=True)
            a = masked(open_mask(d, s, [m for m in range(3) if m not in closed]), a)
            b = matrix(lambda *c: b_s[(n, *c)])
            upper = projected(product(own, a), side, right_h=True)
            low = projected(a, b, left_h=True)
            mask = open_mask(d, s, closed)
            low = [pick(mask, 0.0, v) for v in low]
            for k, (m, h) in enumerate(spots):
                h = half(d, h, True)
                natural = lambda v: jnp.where(top(d), shifted(d, v, last[d] - k), 0.0)
                for c in range(8):
                    x = natural(upper[c])
                    add(d, c, h, x)
                    add(m, c, h, -x)
                forward(d, m, h, [natural(v) for v in low])
        flush()

    def prepare(d):
        for s in range(len(LAYOUT[d])):
            own = fetched(out_s, "x", d, s)
            mask = open_mask(d, s)
            if mask is not None:
                far = packed(
                    d, s,
                    lambda m, h, *c: None if complete(m, h if d else 1) else edge(d, m, h, *c),
                    False,
                )
                both = product(own, far, right_h=True)
                own = [
                    [[jnp.where(mask, both[p][i][j], own[p][i][j]) for j in range(3)] for i in range(3)]
                    for p in range(2)
                ]
            save(pre_s, (sets.index((d, s)),), own)

    def close(d):
        for s, spots in enumerate(LAYOUT[d]):
            n = sets.index((d, s))
            q = projected(
                matrix(lambda *c: pre_s[(n, *c)]), fetched(in_s, "g", d, s), right_h=True
            )
            for k, (m, h) in enumerate(spots):
                for c in range(8):
                    add(m, c, half(d, h, False), jnp.where(bottom(d), shifted(d, q[c], -k), 0.0))
        flush()

    for pair in PLANES:
        for h in range(halves):
            inner(*pair, h)
        flush()
    faces[2].wait_recv()
    face_terms(2, ())
    corners(0, (2,))
    faces[0].wait_recv()
    face_terms(0, (2,))
    corners(1, (0, 2))
    faces[1].wait_recv()
    face_terms(1, (0, 2))
    edges.wait_recv()
    for d in (2, 0, 1):
        prepare(d)
    for d in (2, 0, 1):
        opens[d].wait_recv()
        close(d)
    relayed.wait_send()
    everything.wait_send()


def expand(halves, acc, hbm, out, sem):
    for m in range(4):
        for h in range(halves):
            rows = [((m * 8 + c) * halves + h) * SUB for c in range(8)]
            f = [acc[r : r + SUB, :] * (COEFF * 0.5 if c < 6 else COEFF) for c, r in enumerate(rows)]

            def put(part, i, j, value):
                out[m, part, i, j, h * SUB : (h + 1) * SUB, :] = value

            for n, (i, j) in enumerate(((0, 1), (0, 2), (1, 2))):
                put(0, i, j, f[n])
                put(0, j, i, -f[n])
                put(1, i, j, f[3 + n])
                put(1, j, i, f[3 + n])
            for i in range(3):
                put(0, i, i, jnp.zeros((SUB, LANES), jnp.float32))
            put(1, 0, 0, f[6])
            put(1, 1, 1, f[7])
            put(1, 2, 2, -(f[6] + f[7]))
        for part in range(2):
            for i in range(3):
                pltpu.make_async_copy(out.at[m, part, i], hbm.at[m, part, i], sem).start()
    pltpu.make_async_copy(out, hbm, sem).wait()


def per_device(counts, links):
    time_len, depth, flat = links.shape[4:]
    sites = time_len * depth
    assert flat == LANES and (time_len, depth) == (4, 4)
    halves = sites // SUB
    vmem = lambda *s: pltpu.VMEM(s + (LANES,), jnp.float32)
    shape = links.shape[:4] + (sites, flat)
    terms = pl.pallas_call(
        functools.partial(force_terms, counts, depth, halves),
        out_shape=pltpu.VMEM((32 * sites, flat), jnp.float32),
        in_specs=[pl.BlockSpec(memory_space=pl.ANY)],
        out_specs=pl.BlockSpec(memory_space=pltpu.VMEM),
        scratch_shapes=[
            vmem(*shape[:-1]),
            vmem(TOTAL),
            vmem(TOTAL),
            vmem(len(LEGS) * EDGE),
            vmem(5, 3, 2, 2, 3, SUB),
            vmem(5, 2, 3, 3, SUB),
            vmem(5, 2, 3, 3, SUB),
            pltpu.SemaphoreType.DMA,
            pltpu.SemaphoreType.DMA,
            pltpu.SemaphoreType.DMA((8,)),
            pltpu.SemaphoreType.DMA,
        ],
        compiler_params=pltpu.CompilerParams(collective_id=0, has_side_effects=True),
        name="force_terms",
    )(links.reshape(shape))
    out = pl.pallas_call(
        functools.partial(expand, halves),
        out_shape=jax.ShapeDtypeStruct(shape, jnp.float32),
        in_specs=[pl.BlockSpec(memory_space=pltpu.VMEM)],
        out_specs=pl.BlockSpec(memory_space=pl.ANY),
        scratch_shapes=[vmem(*shape[:-1]), pltpu.SemaphoreType.DMA],
        name="expand",
    )(pltpu.with_memory_space_constraint(terms, pltpu.VMEM))
    return out.reshape(links.shape)


def solution(mesh):
    assert mesh.axis_names == ("gx", "gz", "ta")
    counts = tuple(mesh.shape[a] for a in AXES)
    spec = P(None, None, None, None, "ta", "gz", "gx")
    return jax.shard_map(
        functools.partial(per_device, counts),
        mesh=mesh,
        in_specs=(spec,),
        out_specs=spec,
        check_vma=False,
    )
```

```python
import functools

import jax
import jax.numpy as jnp
from jax import lax
from jax.experimental import pallas as pl
from jax.experimental.pallas import tpu as pltpu
from jax.sharding import PartitionSpec as P

NX = 16
COEFF = -1.9
AXES = ("ta", "gz", "gx")
SUB, LANES = 8, 128


def others(d):
    return [m for m in range(4) if m != d]


class Lattice:
    def __init__(self, depth):
        self.depth = depth
        self.per = SUB // depth
        self.ygroups = LANES // NX
        self.row = lax.broadcasted_iota(jnp.int32, (SUB, LANES), 0)
        self.lane = lax.broadcasted_iota(jnp.int32, (SUB, LANES), 1)
        self.zrow = self.row % depth
        self.xcol = self.lane % NX

    def rows(self, value, shift):
        shift %= SUB
        return pltpu.roll(value, shift, 0) if shift else value

    def lanes(self, value, shift):
        shift %= LANES
        return pltpu.roll(value, shift, 1) if shift else value


def entry(left, right, i, j, part, left_h, right_h):
    total = None
    for k in range(3):
        li = (k, i) if left_h else (i, k)
        ri = (j, k) if right_h else (k, j)
        lr, lm = left[0][li[0]][li[1]], left[1][li[0]][li[1]]
        rr, rm = right[0][ri[0]][ri[1]], right[1][ri[0]][ri[1]]
        if part == 0:
            first, second = lr * rr, lm * rm
            minus = left_h == right_h
        elif left_h:
            first, second = lr * rm, lm * rr
            minus = True
        else:
            first, second = lm * rr, lr * rm
            minus = right_h
        value = first - second if minus else first + second
        total = value if total is None else total + value
    return total


def product(left, right, left_h=False, right_h=False):
    return [
        [[entry(left, right, i, j, part, left_h, right_h) for j in range(3)] for i in range(3)]
        for part in range(2)
    ]


def projected(left, right, left_h=False, right_h=False):
    get = lambda i, j, part: entry(left, right, i, j, part, left_h, right_h)
    pairs = ((0, 1), (0, 2), (1, 2))
    real = [get(i, j, 0) - get(j, i, 0) for i, j in pairs]
    imag = [get(i, j, 1) + get(j, i, 1) for i, j in pairs]
    diag = [get(i, i, 1) for i in range(3)]
    third = (diag[0] + diag[1] + diag[2]) * (1.0 / 3.0)
    return real + imag + [diag[0] - third, diag[1] - third]


def third_row(real, imag):
    rows_r, rows_i = [], []
    for column in range(3):
        n, l = (column + 1) % 3, (column + 2) % 3
        rows_r.append(
            real[0][n] * real[1][l]
            - imag[0][n] * imag[1][l]
            - real[0][l] * real[1][n]
            + imag[0][l] * imag[1][n]
        )
        rows_i.append(
            real[0][l] * imag[1][n]
            + imag[0][l] * real[1][n]
            - real[0][n] * imag[1][l]
            - imag[0][n] * real[1][l]
        )
    return rows_r, rows_i


PLANES = ((0, 1), (0, 2), (0, 3), (1, 2), (1, 3), (2, 3))
DIAGONALS = ((0, 2), (2, 0), (0, 1), (1, 0), (1, 2), (2, 1))
LAYOUT = (
    (((1, 0), (2, 0)), ((3, 0),)),
    (((0, 0), (0, 1), (2, 0), (2, 1)), ((3, 0), (3, 1))),
    (((0, 0), (0, 1), (1, 0), (1, 1), (3, 0), (3, 1)),),
)
ROWS = (144, 144, 96)
EDGES = (8, 8, 16, 16, 8, 8)


def offset(kind, d):
    if kind == "e":
        return 2 * sum(ROWS) + sum(EDGES[:d])
    return (sum(ROWS) if kind == "g" else 0) + sum(ROWS[:d])


TOTAL = offset("e", len(DIAGONALS))


def force_terms(
    counts, depth, halves, hbm, acc, u, out_s, in_s, face_s, b_s, pre_s, load_sem, send, recv,
):
    g = Lattice(depth)
    me = [lax.axis_index(a) for a in AXES]
    comps = [(part, i, j) for part in range(2) for i in range(2) for j in range(3)]
    last = (g.per - 1, depth - 1, g.ygroups - 1)
    place = (g.row // depth, g.zrow, g.lane // NX)

    def device(*steps):
        where = list(me)
        for i, step in steps:
            where[i] = lax.rem(me[i] + (step + counts[i]), counts[i])
        by = dict(zip(AXES, where))
        return (by["gx"], by["gz"], by["ta"])

    loads = [
        pltpu.make_async_copy(hbm.at[m, part, i], u.at[m, part, i], load_sem)
        for m in range(4)
        for part in range(2)
        for i in range(3)
    ]
    for copy in loads:
        copy.start()
    barrier = pltpu.get_barrier_semaphore()
    partners = [device((i, step)) for i in (1, 0, 2) for step in (1, -1)]
    partners += [device((d, 1), (n, -1)) for d, n in DIAGONALS]
    for where in partners[6:] + partners[:6]:
        pl.semaphore_signal(barrier, inc=1, device_id=where, device_id_type=pl.DeviceIdType.MESH)

    def remote(start, rows, slot, where):
        span = slice(start, start + rows)
        return pltpu.make_async_remote_copy(
            src_ref=out_s.at[span], dst_ref=in_s.at[span], send_sem=send, recv_sem=recv.at[slot],
            device_id=where, device_id_type=pl.DeviceIdType.MESH,
        )

    faces = [remote(offset("x", d), ROWS[d], d, device((d, -1))) for d in range(3)]
    opens = [remote(offset("g", d), ROWS[d], 3 + d, device((d, 1))) for d in range(3)]
    edges = [
        remote(offset("e", k), EDGES[k], 6, device((d, 1), (n, -1)))
        for k, (d, n) in enumerate(DIAGONALS)
    ]
    all_edges = remote(offset("e", 0), sum(EDGES), 6, partners[0])
    everything = remote(0, TOTAL, 0, partners[0])

    def load(m, part, i, j, h):
        return u[m, part, i, j, h * SUB : (h + 1) * SUB, :]

    def shifted(d, value, steps):
        if d == 0:
            return g.rows(value, depth * steps)
        return g.rows(value, steps) if d == 1 else g.lanes(value, NX * steps)

    def half(d, h, top):
        return (halves - 1 if top else 0) if d == 0 else h

    def complete(d, h):
        return d == 3 or (d == 0 and h + 1 < halves)

    def top(d, h=1):
        if d == 0:
            return g.row >= SUB - depth
        return g.zrow == depth - 1 if d == 1 else g.lane >= LANES - NX

    def bottom(d):
        return (g.row < depth, g.zrow == 0, g.lane < NX)[d]

    def open_mask(d, s, among=(0, 1, 2)):
        mask = None
        for k, (m, h) in enumerate(LAYOUT[d][s]):
            if m in among and not complete(m, h if d else 1):
                here = jnp.logical_and(place[d] == k, top(m))
                mask = here if mask is None else jnp.logical_or(mask, here)
        return mask

    def pick(mask, yes, no):
        return no if mask is None else jnp.where(mask, yes, no)

    def pack(d, s, get, up):
        value = None
        for k, (m, h) in enumerate(LAYOUT[d][s]):
            x = get(m, half(d, h, up))
            if x is None:
                continue
            x = shifted(d, x, k - (last[d] if up else 0))
            value = x if value is None else jnp.where(place[d] >= k, x, value)
        return value

    def complete_rows(get):
        real = [[get(0, i, j) for j in range(3)] for i in range(2)]
        imag = [[get(1, i, j) for j in range(3)] for i in range(2)]
        third_r, third_i = third_row(real, imag)
        return [real + [third_r], imag + [third_i]]

    def packed(d, s, get, up):
        return complete_rows(
            lambda part, i, j: pack(d, s, lambda m, h: get(m, h, part, i, j), up)
        )

    def put(kind, d, s, value):
        r = offset(kind, d)
        used = len(LAYOUT[d][s])
        for n, (part, i, j) in enumerate(comps[: 6 if s else 12]):
            v = value[part][i][j]
            if s:
                v = jnp.where(place[d] < used, v, shifted(d, value[1][i][j], used))
            at = r + (96 if s else 0) + n * SUB
            out_s[at : at + SUB, :] = v

    def fetch(ref, kind, d, s, part, i, j):
        n = part * 6 + i * 3 + j
        at = offset(kind, d) + n * SUB
        if not s:
            return ref[at : at + SUB, :]
        at += 96 - part * 6 * SUB
        v = ref[at : at + SUB, :]
        return shifted(d, v, -len(LAYOUT[d][s])) if part else v

    def fetched(ref, kind, d, s):
        return complete_rows(lambda part, i, j: fetch(ref, kind, d, s, part, i, j))

    def rolled(m, d, h, part, i, j):
        v = load(m, part, i, j, h)
        if d == 3:
            return jnp.where(g.xcol == NX - 1, g.lanes(v, NX - 1), g.lanes(v, -1))
        if d == 2:
            return g.lanes(v, -NX)
        if d == 1:
            return g.rows(v, -1)
        if h + 1 < halves:
            beyond = g.rows(load(m, part, i, j, h + 1), -depth)
            return jnp.where(g.row >= SUB - depth, beyond, g.rows(v, -depth))
        return g.rows(v, -depth)

    def matrix(get):
        return [[[get(part, i, j) for j in range(3)] for i in range(3)] for part in range(2)]

    def save(ref, index, value):
        for part in range(2):
            for i in range(ref.shape[-4]):
                for j in range(3):
                    ref[(*index, part, i, j)] = value[part][i][j]

    sets = [(d, s) for d in range(3) for s in range(len(LAYOUT[d]))]

    def kept(d, s, q):
        n = sets.index((d, s))
        return complete_rows(lambda part, i, j: face_s[n, q, part, i, j])

    def own_face(d):
        def get(part, i, j):
            if d != 2:
                return pack(d, 0, lambda m, h: load(d, part, i, j, h), True)
            pair = [shifted(d, load(d, part, i, j, h), h - last[d]) for h in range(halves)]
            pair = jnp.where(place[d] >= 1, pair[1], pair[0])
            value = jnp.where(place[d] >= 2, shifted(d, pair, 2), pair)
            return jnp.where(place[d] >= 4, shifted(d, pair, 4), value)

        return complete_rows(get)

    def step_in_face(d, m, v):
        if m == 3:
            return jnp.where(g.xcol == NX - 1, g.lanes(v, NX - 1), g.lanes(v, -1))
        if m == 2:
            return g.lanes(v, -NX)
        if m == 1:
            return g.rows(v, -1)
        moved = g.rows(v, -depth)
        if d == 1:
            beyond = g.rows(v, depth - 1)
            return jnp.where(jnp.logical_and(g.zrow == 0, g.row >= depth), beyond, moved)
        return jnp.where(g.row >= depth, g.lanes(moved, -NX), moved)

    def over_face(d, s, own):
        def get(part, i, j):
            value, before = None, None
            for k, (m, h) in enumerate(LAYOUT[d][s]):
                if m == before:
                    continue
                x = step_in_face(d, m, own[part][i][j])
                value = x if value is None else jnp.where(place[d] >= k, x, value)
                before = m
            return value

        return complete_rows(get)

    def send_side(d):
        own = own_face(d)
        for s in range(len(LAYOUT[d])):
            n = sets.index((d, s))
            side = packed(d, s, lambda m, h, *c: load(m, *c, h), True)
            over = over_face(d, s, own)
            b = product(own, side, left_h=True)
            mask = open_mask(d, s)
            put("g", d, s, [
                [
                    [pick(mask, b[p][i][j], entry(b, over, i, j, p, False, False)) for j in range(3)]
                    for i in range(2)
                ]
                for p in range(2)
            ])
            for q, value in enumerate((own, side, over)):
                save(face_s, (n, q), value)
            save(b_s, (n,), b)

    def send_face(d):
        for s in range(len(LAYOUT[d])):
            put("x", d, s, [
                [
                    [pack(d, s, lambda m, h: load(m, p, i, j, h), False) for j in range(3)]
                    for i in range(2)
                ]
                for p in range(2)
            ])

    def pack_edges(d, n):
        r0 = offset("e", DIAGONALS.index((d, n)))
        if 2 not in (d, n):
            for c0 in range(0, 12, SUB):
                value = None
                for k in range(min(SUB, 12 - c0)):
                    v = load(d, *comps[c0 + k], halves - 1 if d == 0 else 0)
                    x = g.rows(v, k - depth if d == 0 else k - (depth - 1))
                    value = x if value is None else jnp.where(g.row >= k, x, value)
                out_s[r0 + c0 : r0 + c0 + SUB, :] = value
            return
        value = None
        for k in range(g.ygroups):
            v = dense_rows(d, n, comps[k])
            if k + g.ygroups < 12:
                w = dense_rows(d, n, comps[k + g.ygroups])
                step, mask = spare(d, n)
                v = jnp.where(mask, v, g.rows(w, step))
            x = g.lanes(v, NX * (k + (1 if d == 2 else 0)))
            value = x if value is None else jnp.where(g.lane >= NX * k, x, value)
        out_s[r0 : r0 + SUB, :] = value

    def spare(d, n):
        if (d, n) == (0, 2):
            return depth, g.row >= depth
        if (d, n) == (2, 0):
            return depth, g.row < depth
        return (-2, g.zrow >= 2) if d == 1 else (2, g.zrow < 2)

    def dense_rows(d, n, c):
        if 0 in (d, n):
            return load(d, *c, halves - 1 if d == 0 else 0)
        at = depth - 1 if d == 1 else 0
        step = -1 if d == 1 else 1
        v = load(d, *c, 0)
        for h in range(1, halves):
            v = jnp.where(g.zrow == at + step * h, g.rows(load(d, *c, h), step * h), v)
        return v

    def edge(d, n, h, part, i, j):
        c = part * 6 + i * 3 + j
        r = offset("e", DIAGONALS.index((d, n)))
        if 2 not in (d, n):
            v = in_s[r + c // SUB * SUB : r + c // SUB * SUB + SUB, :]
            k = c % SUB
            return g.rows(v, depth - 1 - k if d == 0 else SUB - depth - k)
        k, back = c % g.ygroups, c >= g.ygroups
        v = g.lanes(in_s[r : r + SUB, :], NX * ((0 if d == 2 else g.ygroups - 1) - k))
        step = -spare(d, n)[0] if back else 0
        if (d, n) == (0, 2):
            return g.rows(v, step - (SUB - depth))
        if (d, n) == (2, 0):
            return g.rows(v, step + SUB - depth)
        return g.rows(v, step + (1 - depth + h if d == 1 else depth - 1 - h))

    everything_in = pltpu.make_async_copy(hbm, u, load_sem)
    everything_in.wait()
    for d, n in DIAGONALS:
        pack_edges(d, n)
    for d in (1, 0):
        send_side(d)
        send_face(d)
    send_face(2)
    pl.semaphore_wait(barrier, len(partners))
    for copy in edges[2:] + [opens[1], faces[1]] + edges[:2] + [opens[0], faces[0]]:
        copy.start()
    send_side(2)
    faces[2].start()
    opens[2].start()

    seen, pending = set(), {}

    def add(m, c, h, value):
        key = (m, c, h)
        pending[key] = pending[key] + value if key in pending else value

    def flush():
        for (m, c, h), value in pending.items():
            r = ((m * 8 + c) * halves + h) * SUB
            if (m, c, h) in seen:
                acc[r : r + SUB, :] += value
            else:
                seen.add((m, c, h))
                acc[r : r + SUB, :] = value
        pending.clear()

    def forward(m, d, h, q):
        for c in range(8):
            if d == 3:
                add(m, c, h, jnp.where(g.xcol == 0, g.lanes(q[c], 1 - NX), g.lanes(q[c], 1)))
            elif d == 2:
                add(m, c, h, g.lanes(q[c], NX))
            elif d == 1:
                add(m, c, h, g.rows(q[c], 1))
            elif h + 1 < halves:
                moved = g.rows(q[c], depth)
                add(m, c, h, jnp.where(g.row >= depth, moved, 0.0))
                add(m, c, h + 1, jnp.where(g.row < depth, moved, 0.0))
            else:
                add(m, c, h, g.rows(q[c], depth))

    def masked(mask, a):
        return [[[pick(mask, 0.0, v) for v in line] for line in part] for part in a]

    def inner(mu, nu, h):
        own = matrix(lambda *c: load(mu, *c, h))
        side = matrix(lambda *c: load(nu, *c, h))
        a = product(
            matrix(lambda *c: rolled(nu, mu, h, *c)),
            matrix(lambda *c: rolled(mu, nu, h, *c)),
            right_h=True,
        )
        mask = None
        for d in (mu, nu):
            if not complete(d, h):
                mask = top(d) if mask is None else jnp.logical_or(mask, top(d))
        a = masked(mask, a)
        b = product(own, side, left_h=True)
        forward(mu, nu, h, projected(a, b, left_h=True))
        forward(nu, mu, h, projected(a, b, right_h=True))
        upper = projected(product(own, a), side, right_h=True)
        for c in range(8):
            add(mu, c, h, upper[c])
            add(nu, c, h, -upper[c])

    def corners(d, among):
        for s in range(len(LAYOUT[d])):
            mask = open_mask(d, s, among)
            if mask is None:
                continue
            n = sets.index((d, s))

            def corner(m, h, c):
                if m not in among or complete(m, h):
                    return None
                k = LAYOUT[m][0].index((d, 0 if m == 0 else h))
                return shifted(m, fetch(in_s, "x", m, 0, *c), last[m] - k)

            for c in comps:
                value = pack(d, s, lambda m, h: corner(m, h, c), True)
                face_s[(n, 2, *c)] = jnp.where(mask, value, face_s[(n, 2, *c)])

    def face_terms(d, closed):
        for s, spots in enumerate(LAYOUT[d]):
            n = sets.index((d, s))
            own, side, over = (kept(d, s, q) for q in range(3))
            a = product(fetched(in_s, "x", d, s), over, right_h=True)
            a = masked(open_mask(d, s, [m for m in range(3) if m not in closed]), a)
            b = matrix(lambda *c: b_s[(n, *c)])
            upper = projected(product(own, a), side, right_h=True)
            low = projected(a, b, left_h=True)
            mask = open_mask(d, s, closed)
            low = [pick(mask, 0.0, v) for v in low]
            for k, (m, h) in enumerate(spots):
                h = half(d, h, True)
                natural = lambda v: jnp.where(top(d), shifted(d, v, last[d] - k), 0.0)
                for c in range(8):
                    x = natural(upper[c])
                    add(d, c, h, x)
                    add(m, c, h, -x)
                forward(d, m, h, [natural(v) for v in low])
        flush()

    def prepare(d):
        for s in range(len(LAYOUT[d])):
            own = fetched(out_s, "x", d, s)
            mask = open_mask(d, s)
            if mask is not None:
                far = packed(
                    d, s,
                    lambda m, h, *c: None if complete(m, h if d else 1) else edge(d, m, h, *c),
                    False,
                )
                both = product(own, far, right_h=True)
                own = [
                    [[jnp.where(mask, both[p][i][j], own[p][i][j]) for j in range(3)] for i in range(3)]
                    for p in range(2)
                ]
            save(pre_s, (sets.index((d, s)),), own)

    def close(d):
        for s, spots in enumerate(LAYOUT[d]):
            n = sets.index((d, s))
            q = projected(
                matrix(lambda *c: pre_s[(n, *c)]), fetched(in_s, "g", d, s), right_h=True
            )
            for k, (m, h) in enumerate(spots):
                for c in range(8):
                    add(m, c, half(d, h, False), jnp.where(bottom(d), shifted(d, q[c], -k), 0.0))
        flush()

    for pair in PLANES:
        for h in range(halves):
            inner(*pair, h)
        flush()
    faces[2].wait_recv()
    face_terms(2, ())
    corners(0, (2,))
    faces[0].wait_recv()
    face_terms(0, (2,))
    corners(1, (0, 2))
    all_edges.wait_recv()
    for d in (2, 0, 1):
        prepare(d)
    for d in (2, 0):
        opens[d].wait_recv()
        close(d)
    faces[1].wait_recv()
    face_terms(1, (0, 2))
    opens[1].wait_recv()
    close(1)
    everything.wait_send()


def expand(halves, acc, hbm, out, sem):
    for m in range(4):
        for h in range(halves):
            rows = [((m * 8 + c) * halves + h) * SUB for c in range(8)]
            f = [acc[r : r + SUB, :] * (COEFF * 0.5 if c < 6 else COEFF) for c, r in enumerate(rows)]

            def put(part, i, j, value):
                out[m, part, i, j, h * SUB : (h + 1) * SUB, :] = value

            for n, (i, j) in enumerate(((0, 1), (0, 2), (1, 2))):
                put(0, i, j, f[n])
                put(0, j, i, -f[n])
                put(1, i, j, f[3 + n])
                put(1, j, i, f[3 + n])
            for i in range(3):
                put(0, i, i, jnp.zeros((SUB, LANES), jnp.float32))
            put(1, 0, 0, f[6])
            put(1, 1, 1, f[7])
            put(1, 2, 2, -(f[6] + f[7]))
        for part in range(2):
            for i in range(3):
                pltpu.make_async_copy(out.at[m, part, i], hbm.at[m, part, i], sem).start()
    pltpu.make_async_copy(out, hbm, sem).wait()


def per_device(counts, links):
    time_len, depth, flat = links.shape[4:]
    sites = time_len * depth
    assert flat == LANES and (time_len, depth) == (4, 4)
    halves = sites // SUB
    vmem = lambda *s: pltpu.VMEM(s + (LANES,), jnp.float32)
    shape = links.shape[:4] + (sites, flat)
    terms = pl.pallas_call(
        functools.partial(force_terms, counts, depth, halves),
        out_shape=pltpu.VMEM((32 * sites, flat), jnp.float32),
        in_specs=[pl.BlockSpec(memory_space=pl.ANY)],
        out_specs=pl.BlockSpec(memory_space=pltpu.VMEM),
        scratch_shapes=[
            vmem(*shape[:-1]),
            vmem(TOTAL),
            vmem(TOTAL),
            vmem(5, 3, 2, 2, 3, SUB),
            vmem(5, 2, 3, 3, SUB),
            vmem(5, 2, 3, 3, SUB),
            pltpu.SemaphoreType.DMA,
            pltpu.SemaphoreType.DMA,
            pltpu.SemaphoreType.DMA((7,)),
        ],
        compiler_params=pltpu.CompilerParams(collective_id=0, has_side_effects=True),
        name="force_terms",
    )(links.reshape(shape))
    out = pl.pallas_call(
        functools.partial(expand, halves),
        out_shape=jax.ShapeDtypeStruct(shape, jnp.float32),
        in_specs=[pl.BlockSpec(memory_space=pltpu.VMEM)],
        out_specs=pl.BlockSpec(memory_space=pl.ANY),
        scratch_shapes=[vmem(*shape[:-1]), pltpu.SemaphoreType.DMA],
        name="expand",
    )(pltpu.with_memory_space_constraint(terms, pltpu.VMEM))
    return out.reshape(links.shape)


def solution(mesh):
    assert mesh.axis_names == ("gx", "gz", "ta")
    counts = tuple(mesh.shape[a] for a in AXES)
    spec = P(None, None, None, None, "ta", "gz", "gx")
    return jax.shard_map(
        functools.partial(per_device, counts),
        mesh=mesh,
        in_specs=(spec,),
        out_specs=spec,
        check_vma=False,
    )
```

```python
import functools

import jax
import jax.numpy as jnp
from jax import lax
from jax.experimental import pallas as pl
from jax.experimental.pallas import tpu as pltpu
from jax.sharding import PartitionSpec as P

NX = 16
COEFF = -1.9
AXES = ("ta", "gz", "gx")
SUB, LANES = 8, 128


def others(d):
    return [m for m in range(4) if m != d]


class Lattice:
    def __init__(self, depth):
        self.depth = depth
        self.per = SUB // depth
        self.ygroups = LANES // NX
        self.row = lax.broadcasted_iota(jnp.int32, (SUB, LANES), 0)
        self.lane = lax.broadcasted_iota(jnp.int32, (SUB, LANES), 1)
        self.zrow = self.row % depth
        self.xcol = self.lane % NX

    def rows(self, value, shift):
        shift %= SUB
        return pltpu.roll(value, shift, 0) if shift else value

    def lanes(self, value, shift):
        shift %= LANES
        return pltpu.roll(value, shift, 1) if shift else value


def entry(left, right, i, j, part, left_h, right_h):
    total = None
    for k in range(3):
        li = (k, i) if left_h else (i, k)
        ri = (j, k) if right_h else (k, j)
        lr, lm = left[0][li[0]][li[1]], left[1][li[0]][li[1]]
        rr, rm = right[0][ri[0]][ri[1]], right[1][ri[0]][ri[1]]
        if part == 0:
            first, second = lr * rr, lm * rm
            minus = left_h == right_h
        elif left_h:
            first, second = lr * rm, lm * rr
            minus = True
        else:
            first, second = lm * rr, lr * rm
            minus = right_h
        value = first - second if minus else first + second
        total = value if total is None else total + value
    return total


def product(left, right, left_h=False, right_h=False):
    return [
        [[entry(left, right, i, j, part, left_h, right_h) for j in range(3)] for i in range(3)]
        for part in range(2)
    ]


def projected(left, right, left_h=False, right_h=False):
    get = lambda i, j, part: entry(left, right, i, j, part, left_h, right_h)
    pairs = ((0, 1), (0, 2), (1, 2))
    real = [get(i, j, 0) - get(j, i, 0) for i, j in pairs]
    imag = [get(i, j, 1) + get(j, i, 1) for i, j in pairs]
    diag = [get(i, i, 1) for i in range(3)]
    third = (diag[0] + diag[1] + diag[2]) * (1.0 / 3.0)
    return real + imag + [diag[0] - third, diag[1] - third]


def third_row(real, imag):
    rows_r, rows_i = [], []
    for column in range(3):
        n, l = (column + 1) % 3, (column + 2) % 3
        rows_r.append(
            real[0][n] * real[1][l]
            - imag[0][n] * imag[1][l]
            - real[0][l] * real[1][n]
            + imag[0][l] * imag[1][n]
        )
        rows_i.append(
            real[0][l] * imag[1][n]
            + imag[0][l] * real[1][n]
            - real[0][n] * imag[1][l]
            - imag[0][n] * real[1][l]
        )
    return rows_r, rows_i


PLANES = ((0, 1), (0, 2), (0, 3), (1, 2), (1, 3), (2, 3))
DIAGONALS = ((0, 2), (2, 0), (0, 1), (1, 0), (1, 2), (2, 1))
LAYOUT = (
    (((1, 0), (2, 0)), ((3, 0),)),
    (((0, 0), (0, 1), (2, 0), (2, 1)), ((3, 0), (3, 1))),
    (((0, 0), (0, 1), (1, 0), (1, 1), (3, 0), (3, 1)),),
)
ROWS = (144, 144, 96)
EDGES = (8, 8, 16, 16, 8, 8)


def offset(kind, d):
    if kind == "e":
        return 2 * sum(ROWS) + sum(EDGES[:d])
    return (sum(ROWS) if kind == "g" else 0) + sum(ROWS[:d])


TOTAL = offset("e", len(DIAGONALS))


def force_terms(
    counts, depth, halves, hbm, acc, u, out_s, in_s, face_s, b_s, pre_s, load_sem, send, recv, met,
):
    g = Lattice(depth)
    me = [lax.axis_index(a) for a in AXES]
    comps = [(part, i, j) for part in range(2) for i in range(2) for j in range(3)]
    last = (g.per - 1, depth - 1, g.ygroups - 1)
    place = (g.row // depth, g.zrow, g.lane // NX)

    def device(*steps):
        where = list(me)
        for i, step in steps:
            where[i] = lax.rem(me[i] + (step + counts[i]), counts[i])
        by = dict(zip(AXES, where))
        return (by["gx"], by["gz"], by["ta"])

    loads = [
        pltpu.make_async_copy(hbm.at[m, part, i], u.at[m, part, i], load_sem)
        for m in range(4)
        for part in range(2)
        for i in range(3)
    ]
    for copy in loads:
        copy.start()
    barrier = pltpu.get_barrier_semaphore()
    partners = [device((i, step)) for i in (1, 0, 2) for step in (1, -1)]
    partners += [device((d, 1), (n, -1)) for d, n in DIAGONALS[2:]]
    for where in partners[6:] + partners[:6]:
        pl.semaphore_signal(barrier, inc=1, device_id=where, device_id_type=pl.DeviceIdType.MESH)

    def remote(start, rows, slot, where):
        span = slice(start, start + rows)
        return pltpu.make_async_remote_copy(
            src_ref=out_s.at[span], dst_ref=in_s.at[span], send_sem=send, recv_sem=recv.at[slot],
            device_id=where, device_id_type=pl.DeviceIdType.MESH,
        )

    faces = [remote(offset("x", d), ROWS[d], d, device((d, -1))) for d in range(3)]
    opens = [remote(offset("g", d), ROWS[d], 3 + d, device((d, 1))) for d in range(3)]
    edges = [
        remote(offset("e", k), EDGES[k], 6, device((d, 1), (n, -1)))
        for k, (d, n) in enumerate(DIAGONALS)
    ]
    all_edges = remote(offset("e", 0), sum(EDGES), 6, partners[0])
    everything = remote(0, TOTAL, 0, partners[0])

    def load(m, part, i, j, h):
        return u[m, part, i, j, h * SUB : (h + 1) * SUB, :]

    def shifted(d, value, steps):
        if d == 0:
            return g.rows(value, depth * steps)
        return g.rows(value, steps) if d == 1 else g.lanes(value, NX * steps)

    def half(d, h, top):
        return (halves - 1 if top else 0) if d == 0 else h

    def complete(d, h):
        return d == 3 or (d == 0 and h + 1 < halves)

    def top(d, h=1):
        if d == 0:
            return g.row >= SUB - depth
        return g.zrow == depth - 1 if d == 1 else g.lane >= LANES - NX

    def bottom(d):
        return (g.row < depth, g.zrow == 0, g.lane < NX)[d]

    def open_mask(d, s, among=(0, 1, 2)):
        mask = None
        for k, (m, h) in enumerate(LAYOUT[d][s]):
            if m in among and not complete(m, h if d else 1):
                here = jnp.logical_and(place[d] == k, top(m))
                mask = here if mask is None else jnp.logical_or(mask, here)
        return mask

    def pick(mask, yes, no):
        return no if mask is None else jnp.where(mask, yes, no)

    def pack(d, s, get, up):
        value = None
        for k, (m, h) in enumerate(LAYOUT[d][s]):
            x = get(m, half(d, h, up))
            if x is None:
                continue
            x = shifted(d, x, k - (last[d] if up else 0))
            value = x if value is None else jnp.where(place[d] >= k, x, value)
        return value

    def complete_rows(get):
        real = [[get(0, i, j) for j in range(3)] for i in range(2)]
        imag = [[get(1, i, j) for j in range(3)] for i in range(2)]
        third_r, third_i = third_row(real, imag)
        return [real + [third_r], imag + [third_i]]

    def packed(d, s, get, up):
        return complete_rows(
            lambda part, i, j: pack(d, s, lambda m, h: get(m, h, part, i, j), up)
        )

    def put(kind, d, s, value):
        r = offset(kind, d)
        used = len(LAYOUT[d][s])
        for n, (part, i, j) in enumerate(comps[: 6 if s else 12]):
            v = value[part][i][j]
            if s:
                v = jnp.where(place[d] < used, v, shifted(d, value[1][i][j], used))
            at = r + (96 if s else 0) + n * SUB
            out_s[at : at + SUB, :] = v

    def fetch(ref, kind, d, s, part, i, j):
        n = part * 6 + i * 3 + j
        at = offset(kind, d) + n * SUB
        if not s:
            return ref[at : at + SUB, :]
        at += 96 - part * 6 * SUB
        v = ref[at : at + SUB, :]
        return shifted(d, v, -len(LAYOUT[d][s])) if part else v

    def fetched(ref, kind, d, s):
        return complete_rows(lambda part, i, j: fetch(ref, kind, d, s, part, i, j))

    def rolled(m, d, h, part, i, j):
        v = load(m, part, i, j, h)
        if d == 3:
            return jnp.where(g.xcol == NX - 1, g.lanes(v, NX - 1), g.lanes(v, -1))
        if d == 2:
            return g.lanes(v, -NX)
        if d == 1:
            return g.rows(v, -1)
        if h + 1 < halves:
            beyond = g.rows(load(m, part, i, j, h + 1), -depth)
            return jnp.where(g.row >= SUB - depth, beyond, g.rows(v, -depth))
        return g.rows(v, -depth)

    def matrix(get):
        return [[[get(part, i, j) for j in range(3)] for i in range(3)] for part in range(2)]

    def save(ref, index, value):
        for part in range(2):
            for i in range(ref.shape[-4]):
                for j in range(3):
                    ref[(*index, part, i, j)] = value[part][i][j]

    sets = [(d, s) for d in range(3) for s in range(len(LAYOUT[d]))]

    def kept(d, s, q):
        n = sets.index((d, s))
        return complete_rows(lambda part, i, j: face_s[n, q, part, i, j])

    def own_face(d):
        def get(part, i, j):
            if d != 2:
                return pack(d, 0, lambda m, h: load(d, part, i, j, h), True)
            pair = [shifted(d, load(d, part, i, j, h), h - last[d]) for h in range(halves)]
            pair = jnp.where(place[d] >= 1, pair[1], pair[0])
            value = jnp.where(place[d] >= 2, shifted(d, pair, 2), pair)
            return jnp.where(place[d] >= 4, shifted(d, pair, 4), value)

        return complete_rows(get)

    def step_in_face(d, m, v):
        if m == 3:
            return jnp.where(g.xcol == NX - 1, g.lanes(v, NX - 1), g.lanes(v, -1))
        if m == 2:
            return g.lanes(v, -NX)
        if m == 1:
            return g.rows(v, -1)
        moved = g.rows(v, -depth)
        if d == 1:
            beyond = g.rows(v, depth - 1)
            return jnp.where(jnp.logical_and(g.zrow == 0, g.row >= depth), beyond, moved)
        return jnp.where(g.row >= depth, g.lanes(moved, -NX), moved)

    def over_face(d, s, own):
        def get(part, i, j):
            value, before = None, None
            for k, (m, h) in enumerate(LAYOUT[d][s]):
                if m == before:
                    continue
                x = step_in_face(d, m, own[part][i][j])
                value = x if value is None else jnp.where(place[d] >= k, x, value)
                before = m
            return value

        return complete_rows(get)

    def send_side(d):
        own = own_face(d)
        for s in range(len(LAYOUT[d])):
            n = sets.index((d, s))
            side = packed(d, s, lambda m, h, *c: load(m, *c, h), True)
            over = over_face(d, s, own)
            b = product(own, side, left_h=True)
            mask = open_mask(d, s)
            put("g", d, s, [
                [
                    [pick(mask, b[p][i][j], entry(b, over, i, j, p, False, False)) for j in range(3)]
                    for i in range(2)
                ]
                for p in range(2)
            ])
            for q, value in enumerate((own, side, over)):
                save(face_s, (n, q), value)
            save(b_s, (n,), b)

    def send_face(d):
        for s in range(len(LAYOUT[d])):
            put("x", d, s, [
                [
                    [pack(d, s, lambda m, h: load(m, p, i, j, h), False) for j in range(3)]
                    for i in range(2)
                ]
                for p in range(2)
            ])

    def pack_edges(d, n):
        r0 = offset("e", DIAGONALS.index((d, n)))
        if 2 not in (d, n):
            for c0 in range(0, 12, SUB):
                value = None
                for k in range(min(SUB, 12 - c0)):
                    v = load(d, *comps[c0 + k], halves - 1 if d == 0 else 0)
                    x = g.rows(v, k - depth if d == 0 else k - (depth - 1))
                    value = x if value is None else jnp.where(g.row >= k, x, value)
                out_s[r0 + c0 : r0 + c0 + SUB, :] = value
            return
        value = None
        for k in range(g.ygroups):
            v = dense_rows(d, n, comps[k])
            if k + g.ygroups < 12:
                w = dense_rows(d, n, comps[k + g.ygroups])
                step, mask = spare(d, n)
                v = jnp.where(mask, v, g.rows(w, step))
            x = g.lanes(v, NX * (k + (1 if d == 2 else 0)))
            value = x if value is None else jnp.where(g.lane >= NX * k, x, value)
        out_s[r0 : r0 + SUB, :] = value

    def spare(d, n):
        if (d, n) == (0, 2):
            return depth, g.row >= depth
        if (d, n) == (2, 0):
            return depth, g.row < depth
        return (-2, g.zrow >= 2) if d == 1 else (2, g.zrow < 2)

    def dense_rows(d, n, c):
        if 0 in (d, n):
            return load(d, *c, halves - 1 if d == 0 else 0)
        at = depth - 1 if d == 1 else 0
        step = -1 if d == 1 else 1
        v = load(d, *c, 0)
        for h in range(1, halves):
            v = jnp.where(g.zrow == at + step * h, g.rows(load(d, *c, h), step * h), v)
        return v

    def edge(d, n, h, part, i, j):
        c = part * 6 + i * 3 + j
        r = offset("e", DIAGONALS.index((d, n)))
        if 2 not in (d, n):
            v = in_s[r + c // SUB * SUB : r + c // SUB * SUB + SUB, :]
            k = c % SUB
            return g.rows(v, depth - 1 - k if d == 0 else SUB - depth - k)
        k, back = c % g.ygroups, c >= g.ygroups
        v = g.lanes(in_s[r : r + SUB, :], NX * ((0 if d == 2 else g.ygroups - 1) - k))
        step = -spare(d, n)[0] if back else 0
        if (d, n) == (0, 2):
            return g.rows(v, step - (SUB - depth))
        if (d, n) == (2, 0):
            return g.rows(v, step + SUB - depth)
        return g.rows(v, step + (1 - depth + h if d == 1 else depth - 1 - h))

    everything_in = pltpu.make_async_copy(hbm, u, load_sem)
    everything_in.wait()
    for d, n in DIAGONALS:
        pack_edges(d, n)
    for d in (1, 0):
        send_side(d)
        send_face(d)
    send_face(2)
    pl.semaphore_wait(barrier, len(partners))
    for where in partners[4:6]:
        pl.semaphore_signal(met, inc=1, device_id=where, device_id_type=pl.DeviceIdType.MESH)
    for copy in edges[2:] + [opens[1], faces[1], opens[0], faces[0]]:
        copy.start()
    send_side(2)
    faces[2].start()
    opens[2].start()

    seen, pending = set(), {}

    def add(m, c, h, value):
        key = (m, c, h)
        pending[key] = pending[key] + value if key in pending else value

    def flush():
        for (m, c, h), value in pending.items():
            r = ((m * 8 + c) * halves + h) * SUB
            if (m, c, h) in seen:
                acc[r : r + SUB, :] += value
            else:
                seen.add((m, c, h))
                acc[r : r + SUB, :] = value
        pending.clear()

    def forward(m, d, h, q):
        for c in range(8):
            if d == 3:
                add(m, c, h, jnp.where(g.xcol == 0, g.lanes(q[c], 1 - NX), g.lanes(q[c], 1)))
            elif d == 2:
                add(m, c, h, g.lanes(q[c], NX))
            elif d == 1:
                add(m, c, h, g.rows(q[c], 1))
            elif h + 1 < halves:
                moved = g.rows(q[c], depth)
                add(m, c, h, jnp.where(g.row >= depth, moved, 0.0))
                add(m, c, h + 1, jnp.where(g.row < depth, moved, 0.0))
            else:
                add(m, c, h, g.rows(q[c], depth))

    def masked(mask, a):
        return [[[pick(mask, 0.0, v) for v in line] for line in part] for part in a]

    def inner(mu, nu, h):
        own = matrix(lambda *c: load(mu, *c, h))
        side = matrix(lambda *c: load(nu, *c, h))
        a = product(
            matrix(lambda *c: rolled(nu, mu, h, *c)),
            matrix(lambda *c: rolled(mu, nu, h, *c)),
            right_h=True,
        )
        mask = None
        for d in (mu, nu):
            if not complete(d, h):
                mask = top(d) if mask is None else jnp.logical_or(mask, top(d))
        a = masked(mask, a)
        b = product(own, side, left_h=True)
        forward(mu, nu, h, projected(a, b, left_h=True))
        forward(nu, mu, h, projected(a, b, right_h=True))
        upper = projected(product(own, a), side, right_h=True)
        for c in range(8):
            add(mu, c, h, upper[c])
            add(nu, c, h, -upper[c])

    def corners(d, among):
        for s in range(len(LAYOUT[d])):
            mask = open_mask(d, s, among)
            if mask is None:
                continue
            n = sets.index((d, s))

            def corner(m, h, c):
                if m not in among or complete(m, h):
                    return None
                k = LAYOUT[m][0].index((d, 0 if m == 0 else h))
                return shifted(m, fetch(in_s, "x", m, 0, *c), last[m] - k)

            for c in comps:
                value = pack(d, s, lambda m, h: corner(m, h, c), True)
                face_s[(n, 2, *c)] = jnp.where(mask, value, face_s[(n, 2, *c)])

    def face_terms(d, closed):
        for s, spots in enumerate(LAYOUT[d]):
            n = sets.index((d, s))
            own, side, over = (kept(d, s, q) for q in range(3))
            a = product(fetched(in_s, "x", d, s), over, right_h=True)
            a = masked(open_mask(d, s, [m for m in range(3) if m not in closed]), a)
            b = matrix(lambda *c: b_s[(n, *c)])
            upper = projected(product(own, a), side, right_h=True)
            low = projected(a, b, left_h=True)
            mask = open_mask(d, s, closed)
            low = [pick(mask, 0.0, v) for v in low]
            for k, (m, h) in enumerate(spots):
                h = half(d, h, True)
                natural = lambda v: jnp.where(top(d), shifted(d, v, last[d] - k), 0.0)
                for c in range(8):
                    x = natural(upper[c])
                    add(d, c, h, x)
                    add(m, c, h, -x)
                forward(d, m, h, [natural(v) for v in low])
        flush()

    def prepare(d):
        for s in range(len(LAYOUT[d])):
            own = fetched(out_s, "x", d, s)
            mask = open_mask(d, s)
            if mask is not None:
                far = packed(
                    d, s,
                    lambda m, h, *c: None if complete(m, h if d else 1) else edge(d, m, h, *c),
                    False,
                )
                both = product(own, far, right_h=True)
                own = [
                    [[jnp.where(mask, both[p][i][j], own[p][i][j]) for j in range(3)] for i in range(3)]
                    for p in range(2)
                ]
            save(pre_s, (sets.index((d, s)),), own)

    def close(d):
        for s, spots in enumerate(LAYOUT[d]):
            n = sets.index((d, s))
            q = projected(
                matrix(lambda *c: pre_s[(n, *c)]), fetched(in_s, "g", d, s), right_h=True
            )
            for k, (m, h) in enumerate(spots):
                for c in range(8):
                    add(m, c, half(d, h, False), jnp.where(bottom(d), shifted(d, q[c], -k), 0.0))
        flush()

    for n, pair in enumerate(PLANES):
        if n == 2:
            pl.semaphore_wait(met, 2)
            for copy in edges[:2]:
                copy.start()
        for h in range(halves):
            inner(*pair, h)
        flush()
    faces[2].wait_recv()
    face_terms(2, ())
    corners(0, (2,))
    faces[0].wait_recv()
    face_terms(0, (2,))
    corners(1, (0, 2))
    faces[1].wait_recv()
    face_terms(1, (0, 2))
    all_edges.wait_recv()
    for d in (2, 0, 1):
        prepare(d)
    for d in (2, 0, 1):
        opens[d].wait_recv()
    for d in (2, 0, 1):
        close(d)
    everything.wait_send()


def expand(halves, acc, hbm, out, sem):
    for m in range(4):
        for h in range(halves):
            rows = [((m * 8 + c) * halves + h) * SUB for c in range(8)]
            f = [acc[r : r + SUB, :] * (COEFF * 0.5 if c < 6 else COEFF) for c, r in enumerate(rows)]

            def put(part, i, j, value):
                out[m, part, i, j, h * SUB : (h + 1) * SUB, :] = value

            for n, (i, j) in enumerate(((0, 1), (0, 2), (1, 2))):
                put(0, i, j, f[n])
                put(0, j, i, -f[n])
                put(1, i, j, f[3 + n])
                put(1, j, i, f[3 + n])
            for i in range(3):
                put(0, i, i, jnp.zeros((SUB, LANES), jnp.float32))
            put(1, 0, 0, f[6])
            put(1, 1, 1, f[7])
            put(1, 2, 2, -(f[6] + f[7]))
        for part in range(2):
            for i in range(3):
                pltpu.make_async_copy(out.at[m, part, i], hbm.at[m, part, i], sem).start()
    pltpu.make_async_copy(out, hbm, sem).wait()


def per_device(counts, links):
    time_len, depth, flat = links.shape[4:]
    sites = time_len * depth
    assert flat == LANES and (time_len, depth) == (4, 4)
    halves = sites // SUB
    vmem = lambda *s: pltpu.VMEM(s + (LANES,), jnp.float32)
    shape = links.shape[:4] + (sites, flat)
    terms = pl.pallas_call(
        functools.partial(force_terms, counts, depth, halves),
        out_shape=pltpu.VMEM((32 * sites, flat), jnp.float32),
        in_specs=[pl.BlockSpec(memory_space=pl.ANY)],
        out_specs=pl.BlockSpec(memory_space=pltpu.VMEM),
        scratch_shapes=[
            vmem(*shape[:-1]),
            vmem(TOTAL),
            vmem(TOTAL),
            vmem(5, 3, 2, 2, 3, SUB),
            vmem(5, 2, 3, 3, SUB),
            vmem(5, 2, 3, 3, SUB),
            pltpu.SemaphoreType.DMA,
            pltpu.SemaphoreType.DMA,
            pltpu.SemaphoreType.DMA((7,)),
            pltpu.SemaphoreType.REGULAR,
        ],
        compiler_params=pltpu.CompilerParams(collective_id=0, has_side_effects=True),
        name="force_terms",
    )(links.reshape(shape))
    out = pl.pallas_call(
        functools.partial(expand, halves),
        out_shape=jax.ShapeDtypeStruct(shape, jnp.float32),
        in_specs=[pl.BlockSpec(memory_space=pltpu.VMEM)],
        out_specs=pl.BlockSpec(memory_space=pl.ANY),
        scratch_shapes=[vmem(*shape[:-1]), pltpu.SemaphoreType.DMA],
        name="expand",
    )(pltpu.with_memory_space_constraint(terms, pltpu.VMEM))
    return out.reshape(links.shape)


def solution(mesh):
    assert mesh.axis_names == ("gx", "gz", "ta")
    counts = tuple(mesh.shape[a] for a in AXES)
    spec = P(None, None, None, None, "ta", "gz", "gx")
    return jax.shard_map(
        functools.partial(per_device, counts),
        mesh=mesh,
        in_specs=(spec,),
        out_specs=spec,
        check_vma=False,
    )
```

```python
import functools

import jax
import jax.numpy as jnp
from jax import lax
from jax.experimental import pallas as pl
from jax.experimental.pallas import tpu as pltpu
from jax.sharding import PartitionSpec as P

NX = 16
COEFF = -1.9
AXES = ("ta", "gz", "gx")
SUB, LANES = 8, 128


def others(d):
    return [m for m in range(4) if m != d]


class Lattice:
    def __init__(self, depth):
        self.depth = depth
        self.per = SUB // depth
        self.ygroups = LANES // NX
        self.row = lax.broadcasted_iota(jnp.int32, (SUB, LANES), 0)
        self.lane = lax.broadcasted_iota(jnp.int32, (SUB, LANES), 1)
        self.zrow = self.row % depth
        self.xcol = self.lane % NX

    def rows(self, value, shift):
        shift %= SUB
        return pltpu.roll(value, shift, 0) if shift else value

    def lanes(self, value, shift):
        shift %= LANES
        return pltpu.roll(value, shift, 1) if shift else value


def entry(left, right, i, j, part, left_h, right_h):
    total = None
    for k in range(3):
        li = (k, i) if left_h else (i, k)
        ri = (j, k) if right_h else (k, j)
        lr, lm = left[0][li[0]][li[1]], left[1][li[0]][li[1]]
        rr, rm = right[0][ri[0]][ri[1]], right[1][ri[0]][ri[1]]
        if part == 0:
            first, second = lr * rr, lm * rm
            minus = left_h == right_h
        elif left_h:
            first, second = lr * rm, lm * rr
            minus = True
        else:
            first, second = lm * rr, lr * rm
            minus = right_h
        value = first - second if minus else first + second
        total = value if total is None else total + value
    return total


def product(left, right, left_h=False, right_h=False):
    return [
        [[entry(left, right, i, j, part, left_h, right_h) for j in range(3)] for i in range(3)]
        for part in range(2)
    ]


def projected(left, right, left_h=False, right_h=False):
    get = lambda i, j, part: entry(left, right, i, j, part, left_h, right_h)
    pairs = ((0, 1), (0, 2), (1, 2))
    real = [get(i, j, 0) - get(j, i, 0) for i, j in pairs]
    imag = [get(i, j, 1) + get(j, i, 1) for i, j in pairs]
    diag = [get(i, i, 1) for i in range(3)]
    third = (diag[0] + diag[1] + diag[2]) * (1.0 / 3.0)
    return real + imag + [diag[0] - third, diag[1] - third]


def third_row(real, imag):
    rows_r, rows_i = [], []
    for column in range(3):
        n, l = (column + 1) % 3, (column + 2) % 3
        rows_r.append(
            real[0][n] * real[1][l]
            - imag[0][n] * imag[1][l]
            - real[0][l] * real[1][n]
            + imag[0][l] * imag[1][n]
        )
        rows_i.append(
            real[0][l] * imag[1][n]
            + imag[0][l] * real[1][n]
            - real[0][n] * imag[1][l]
            - imag[0][n] * real[1][l]
        )
    return rows_r, rows_i


PLANES = ((0, 1), (0, 2), (0, 3), (1, 2), (1, 3), (2, 3))
DIAGONALS = ((0, 2), (2, 0), (0, 1), (1, 0), (1, 2), (2, 1))
LAYOUT = (
    (((1, 0), (2, 0)), ((3, 0),)),
    (((0, 0), (0, 1), (2, 0), (2, 1)), ((3, 0), (3, 1))),
    (((0, 0), (0, 1), (1, 0), (1, 1), (3, 0), (3, 1)),),
)
ROWS = (144, 144, 96)
EDGES = (8, 8, 16, 16, 8, 8)


def offset(kind, d):
    if kind == "e":
        return 2 * sum(ROWS) + sum(EDGES[:d])
    return (sum(ROWS) if kind == "g" else 0) + sum(ROWS[:d])


TOTAL = offset("e", len(DIAGONALS))


def force_terms(
    counts, depth, halves, hbm, acc, u, out_s, in_s, face_s, b_s, pre_s, load_sem, send, recv, met,
):
    g = Lattice(depth)
    me = [lax.axis_index(a) for a in AXES]
    comps = [(part, i, j) for part in range(2) for i in range(2) for j in range(3)]
    last = (g.per - 1, depth - 1, g.ygroups - 1)
    place = (g.row // depth, g.zrow, g.lane // NX)

    def device(*steps):
        where = list(me)
        for i, step in steps:
            where[i] = lax.rem(me[i] + (step + counts[i]), counts[i])
        by = dict(zip(AXES, where))
        return (by["gx"], by["gz"], by["ta"])

    loads = [
        pltpu.make_async_copy(hbm.at[m, part, i], u.at[m, part, i], load_sem)
        for m in range(4)
        for part in range(2)
        for i in range(3)
    ]
    for copy in loads:
        copy.start()
    barrier = pltpu.get_barrier_semaphore()
    partners = [device((i, step)) for i in (1, 0, 2) for step in (1, -1)]
    partners += [device((d, 1), (n, -1)) for d, n in DIAGONALS[2:]] + [device((0, -1), (2, 1))]
    for where in partners[6:] + partners[:6]:
        pl.semaphore_signal(barrier, inc=1, device_id=where, device_id_type=pl.DeviceIdType.MESH)

    def remote(start, rows, slot, where):
        span = slice(start, start + rows)
        return pltpu.make_async_remote_copy(
            src_ref=out_s.at[span], dst_ref=in_s.at[span], send_sem=send, recv_sem=recv.at[slot],
            device_id=where, device_id_type=pl.DeviceIdType.MESH,
        )

    faces = [remote(offset("x", d), ROWS[d], d, device((d, -1))) for d in range(3)]
    opens = [remote(offset("g", d), ROWS[d], 3 + d, device((d, 1))) for d in range(3)]
    edges = [
        remote(offset("e", k), EDGES[k], 6, device((d, 1), (n, -1)))
        for k, (d, n) in enumerate(DIAGONALS)
    ]
    all_edges = remote(offset("e", 0), sum(EDGES), 6, partners[0])
    everything = remote(0, TOTAL, 0, partners[0])

    def load(m, part, i, j, h):
        return u[m, part, i, j, h * SUB : (h + 1) * SUB, :]

    def shifted(d, value, steps):
        if d == 0:
            return g.rows(value, depth * steps)
        return g.rows(value, steps) if d == 1 else g.lanes(value, NX * steps)

    def half(d, h, top):
        return (halves - 1 if top else 0) if d == 0 else h

    def complete(d, h):
        return d == 3 or (d == 0 and h + 1 < halves)

    def top(d, h=1):
        if d == 0:
            return g.row >= SUB - depth
        return g.zrow == depth - 1 if d == 1 else g.lane >= LANES - NX

    def bottom(d):
        return (g.row < depth, g.zrow == 0, g.lane < NX)[d]

    def open_mask(d, s, among=(0, 1, 2)):
        mask = None
        for k, (m, h) in enumerate(LAYOUT[d][s]):
            if m in among and not complete(m, h if d else 1):
                here = jnp.logical_and(place[d] == k, top(m))
                mask = here if mask is None else jnp.logical_or(mask, here)
        return mask

    def pick(mask, yes, no):
        return no if mask is None else jnp.where(mask, yes, no)

    def pack(d, s, get, up):
        value = None
        for k, (m, h) in enumerate(LAYOUT[d][s]):
            x = get(m, half(d, h, up))
            if x is None:
                continue
            x = shifted(d, x, k - (last[d] if up else 0))
            value = x if value is None else jnp.where(place[d] >= k, x, value)
        return value

    def complete_rows(get):
        real = [[get(0, i, j) for j in range(3)] for i in range(2)]
        imag = [[get(1, i, j) for j in range(3)] for i in range(2)]
        third_r, third_i = third_row(real, imag)
        return [real + [third_r], imag + [third_i]]

    def packed(d, s, get, up):
        return complete_rows(
            lambda part, i, j: pack(d, s, lambda m, h: get(m, h, part, i, j), up)
        )

    def put(kind, d, s, value):
        r = offset(kind, d)
        used = len(LAYOUT[d][s])
        for n, (part, i, j) in enumerate(comps[: 6 if s else 12]):
            v = value[part][i][j]
            if s:
                v = jnp.where(place[d] < used, v, shifted(d, value[1][i][j], used))
            at = r + (96 if s else 0) + n * SUB
            out_s[at : at + SUB, :] = v

    def fetch(ref, kind, d, s, part, i, j):
        n = part * 6 + i * 3 + j
        at = offset(kind, d) + n * SUB
        if not s:
            return ref[at : at + SUB, :]
        at += 96 - part * 6 * SUB
        v = ref[at : at + SUB, :]
        return shifted(d, v, -len(LAYOUT[d][s])) if part else v

    def fetched(ref, kind, d, s):
        return complete_rows(lambda part, i, j: fetch(ref, kind, d, s, part, i, j))

    def rolled(m, d, h, part, i, j):
        v = load(m, part, i, j, h)
        if d == 3:
            return jnp.where(g.xcol == NX - 1, g.lanes(v, NX - 1), g.lanes(v, -1))
        if d == 2:
            return g.lanes(v, -NX)
        if d == 1:
            return g.rows(v, -1)
        if h + 1 < halves:
            beyond = g.rows(load(m, part, i, j, h + 1), -depth)
            return jnp.where(g.row >= SUB - depth, beyond, g.rows(v, -depth))
        return g.rows(v, -depth)

    def matrix(get):
        return [[[get(part, i, j) for j in range(3)] for i in range(3)] for part in range(2)]

    def save(ref, index, value):
        for part in range(2):
            for i in range(ref.shape[-4]):
                for j in range(3):
                    ref[(*index, part, i, j)] = value[part][i][j]

    sets = [(d, s) for d in range(3) for s in range(len(LAYOUT[d]))]

    def kept(d, s, q):
        n = sets.index((d, s))
        return complete_rows(lambda part, i, j: face_s[n, q, part, i, j])

    def own_face(d):
        def get(part, i, j):
            if d != 2:
                return pack(d, 0, lambda m, h: load(d, part, i, j, h), True)
            pair = [shifted(d, load(d, part, i, j, h), h - last[d]) for h in range(halves)]
            pair = jnp.where(place[d] >= 1, pair[1], pair[0])
            value = jnp.where(place[d] >= 2, shifted(d, pair, 2), pair)
            return jnp.where(place[d] >= 4, shifted(d, pair, 4), value)

        return complete_rows(get)

    def step_in_face(d, m, v):
        if m == 3:
            return jnp.where(g.xcol == NX - 1, g.lanes(v, NX - 1), g.lanes(v, -1))
        if m == 2:
            return g.lanes(v, -NX)
        if m == 1:
            return g.rows(v, -1)
        moved = g.rows(v, -depth)
        if d == 1:
            beyond = g.rows(v, depth - 1)
            return jnp.where(jnp.logical_and(g.zrow == 0, g.row >= depth), beyond, moved)
        return jnp.where(g.row >= depth, g.lanes(moved, -NX), moved)

    def over_face(d, s, own):
        def get(part, i, j):
            value, before = None, None
            for k, (m, h) in enumerate(LAYOUT[d][s]):
                if m == before:
                    continue
                x = step_in_face(d, m, own[part][i][j])
                value = x if value is None else jnp.where(place[d] >= k, x, value)
                before = m
            return value

        return complete_rows(get)

    def send_side(d):
        own = own_face(d)
        for s in range(len(LAYOUT[d])):
            n = sets.index((d, s))
            side = packed(d, s, lambda m, h, *c: load(m, *c, h), True)
            over = over_face(d, s, own)
            b = product(own, side, left_h=True)
            mask = open_mask(d, s)
            put("g", d, s, [
                [
                    [pick(mask, b[p][i][j], entry(b, over, i, j, p, False, False)) for j in range(3)]
                    for i in range(2)
                ]
                for p in range(2)
            ])
            for q, value in enumerate((own, side, over)):
                save(face_s, (n, q), value)
            save(b_s, (n,), b)

    def send_face(d):
        for s in range(len(LAYOUT[d])):
            put("x", d, s, [
                [
                    [pack(d, s, lambda m, h: load(m, p, i, j, h), False) for j in range(3)]
                    for i in range(2)
                ]
                for p in range(2)
            ])

    def pack_edges(d, n):
        r0 = offset("e", DIAGONALS.index((d, n)))
        if 2 not in (d, n):
            for c0 in range(0, 12, SUB):
                value = None
                for k in range(min(SUB, 12 - c0)):
                    v = load(d, *comps[c0 + k], halves - 1 if d == 0 else 0)
                    x = g.rows(v, k - depth if d == 0 else k - (depth - 1))
                    value = x if value is None else jnp.where(g.row >= k, x, value)
                out_s[r0 + c0 : r0 + c0 + SUB, :] = value
            return
        value = None
        for k in range(g.ygroups):
            v = dense_rows(d, n, comps[k])
            if k + g.ygroups < 12:
                w = dense_rows(d, n, comps[k + g.ygroups])
                step, mask = spare(d, n)
                v = jnp.where(mask, v, g.rows(w, step))
            x = g.lanes(v, NX * (k + (1 if d == 2 else 0)))
            value = x if value is None else jnp.where(g.lane >= NX * k, x, value)
        out_s[r0 : r0 + SUB, :] = value

    def spare(d, n):
        if (d, n) == (0, 2):
            return depth, g.row >= depth
        if (d, n) == (2, 0):
            return depth, g.row < depth
        return (-2, g.zrow >= 2) if d == 1 else (2, g.zrow < 2)

    def dense_rows(d, n, c):
        if 0 in (d, n):
            return load(d, *c, halves - 1 if d == 0 else 0)
        at = depth - 1 if d == 1 else 0
        step = -1 if d == 1 else 1
        v = load(d, *c, 0)
        for h in range(1, halves):
            v = jnp.where(g.zrow == at + step * h, g.rows(load(d, *c, h), step * h), v)
        return v

    def edge(d, n, h, part, i, j):
        c = part * 6 + i * 3 + j
        r = offset("e", DIAGONALS.index((d, n)))
        if 2 not in (d, n):
            v = in_s[r + c // SUB * SUB : r + c // SUB * SUB + SUB, :]
            k = c % SUB
            return g.rows(v, depth - 1 - k if d == 0 else SUB - depth - k)
        k, back = c % g.ygroups, c >= g.ygroups
        v = g.lanes(in_s[r : r + SUB, :], NX * ((0 if d == 2 else g.ygroups - 1) - k))
        step = -spare(d, n)[0] if back else 0
        if (d, n) == (0, 2):
            return g.rows(v, step - (SUB - depth))
        if (d, n) == (2, 0):
            return g.rows(v, step + SUB - depth)
        return g.rows(v, step + (1 - depth + h if d == 1 else depth - 1 - h))

    everything_in = pltpu.make_async_copy(hbm, u, load_sem)
    everything_in.wait()
    for d, n in DIAGONALS:
        pack_edges(d, n)
    for d in (1, 0):
        send_side(d)
        send_face(d)
    send_face(2)
    pl.semaphore_wait(barrier, len(partners))
    pl.semaphore_signal(met, inc=1, device_id=partners[5], device_id_type=pl.DeviceIdType.MESH)
    for copy in edges[2:] + edges[:1] + [opens[1], faces[1], opens[0], faces[0]]:
        copy.start()
    send_side(2)
    faces[2].start()
    opens[2].start()

    seen, pending = set(), {}

    def add(m, c, h, value):
        key = (m, c, h)
        pending[key] = pending[key] + value if key in pending else value

    def flush():
        for (m, c, h), value in pending.items():
            r = ((m * 8 + c) * halves + h) * SUB
            if (m, c, h) in seen:
                acc[r : r + SUB, :] += value
            else:
                seen.add((m, c, h))
                acc[r : r + SUB, :] = value
        pending.clear()

    def forward(m, d, h, q):
        for c in range(8):
            if d == 3:
                add(m, c, h, jnp.where(g.xcol == 0, g.lanes(q[c], 1 - NX), g.lanes(q[c], 1)))
            elif d == 2:
                add(m, c, h, g.lanes(q[c], NX))
            elif d == 1:
                add(m, c, h, g.rows(q[c], 1))
            elif h + 1 < halves:
                moved = g.rows(q[c], depth)
                add(m, c, h, jnp.where(g.row >= depth, moved, 0.0))
                add(m, c, h + 1, jnp.where(g.row < depth, moved, 0.0))
            else:
                add(m, c, h, g.rows(q[c], depth))

    def masked(mask, a):
        return [[[pick(mask, 0.0, v) for v in line] for line in part] for part in a]

    def inner(mu, nu, h):
        own = matrix(lambda *c: load(mu, *c, h))
        side = matrix(lambda *c: load(nu, *c, h))
        a = product(
            matrix(lambda *c: rolled(nu, mu, h, *c)),
            matrix(lambda *c: rolled(mu, nu, h, *c)),
            right_h=True,
        )
        mask = None
        for d in (mu, nu):
            if not complete(d, h):
                mask = top(d) if mask is None else jnp.logical_or(mask, top(d))
        a = masked(mask, a)
        b = product(own, side, left_h=True)
        forward(mu, nu, h, projected(a, b, left_h=True))
        forward(nu, mu, h, projected(a, b, right_h=True))
        upper = projected(product(own, a), side, right_h=True)
        for c in range(8):
            add(mu, c, h, upper[c])
            add(nu, c, h, -upper[c])

    def corners(d, among):
        for s in range(len(LAYOUT[d])):
            mask = open_mask(d, s, among)
            if mask is None:
                continue
            n = sets.index((d, s))

            def corner(m, h, c):
                if m not in among or complete(m, h):
                    return None
                k = LAYOUT[m][0].index((d, 0 if m == 0 else h))
                return shifted(m, fetch(in_s, "x", m, 0, *c), last[m] - k)

            for c in comps:
                value = pack(d, s, lambda m, h: corner(m, h, c), True)
                face_s[(n, 2, *c)] = jnp.where(mask, value, face_s[(n, 2, *c)])

    def face_terms(d, closed):
        for s, spots in enumerate(LAYOUT[d]):
            n = sets.index((d, s))
            own, side, over = (kept(d, s, q) for q in range(3))
            a = product(fetched(in_s, "x", d, s), over, right_h=True)
            a = masked(open_mask(d, s, [m for m in range(3) if m not in closed]), a)
            b = matrix(lambda *c: b_s[(n, *c)])
            upper = projected(product(own, a), side, right_h=True)
            low = projected(a, b, left_h=True)
            mask = open_mask(d, s, closed)
            low = [pick(mask, 0.0, v) for v in low]
            for k, (m, h) in enumerate(spots):
                h = half(d, h, True)
                natural = lambda v: jnp.where(top(d), shifted(d, v, last[d] - k), 0.0)
                for c in range(8):
                    x = natural(upper[c])
                    add(d, c, h, x)
                    add(m, c, h, -x)
                forward(d, m, h, [natural(v) for v in low])
        flush()

    def prepare(d):
        for s in range(len(LAYOUT[d])):
            own = fetched(out_s, "x", d, s)
            mask = open_mask(d, s)
            if mask is not None:
                far = packed(
                    d, s,
                    lambda m, h, *c: None if complete(m, h if d else 1) else edge(d, m, h, *c),
                    False,
                )
                both = product(own, far, right_h=True)
                own = [
                    [[jnp.where(mask, both[p][i][j], own[p][i][j]) for j in range(3)] for i in range(3)]
                    for p in range(2)
                ]
            save(pre_s, (sets.index((d, s)),), own)

    def close(d):
        for s, spots in enumerate(LAYOUT[d]):
            n = sets.index((d, s))
            q = projected(
                matrix(lambda *c: pre_s[(n, *c)]), fetched(in_s, "g", d, s), right_h=True
            )
            for k, (m, h) in enumerate(spots):
                for c in range(8):
                    add(m, c, half(d, h, False), jnp.where(bottom(d), shifted(d, q[c], -k), 0.0))
        flush()

    for n, pair in enumerate(PLANES):
        if n == 2:
            pl.semaphore_wait(met, 1)
            edges[1].start()
        for h in range(halves):
            inner(*pair, h)
        flush()
    faces[2].wait_recv()
    face_terms(2, ())
    corners(0, (2,))
    faces[0].wait_recv()
    face_terms(0, (2,))
    corners(1, (0, 2))
    faces[1].wait_recv()
    face_terms(1, (0, 2))
    all_edges.wait_recv()
    for d in (2, 0, 1):
        prepare(d)
    for d in (2, 0, 1):
        opens[d].wait_recv()
    for d in (2, 0, 1):
        close(d)
    everything.wait_send()


def expand(halves, acc, hbm, out, sem):
    for m in range(4):
        for h in range(halves):
            rows = [((m * 8 + c) * halves + h) * SUB for c in range(8)]
            f = [acc[r : r + SUB, :] * (COEFF * 0.5 if c < 6 else COEFF) for c, r in enumerate(rows)]

            def put(part, i, j, value):
                out[m, part, i, j, h * SUB : (h + 1) * SUB, :] = value

            for n, (i, j) in enumerate(((0, 1), (0, 2), (1, 2))):
                put(0, i, j, f[n])
                put(0, j, i, -f[n])
                put(1, i, j, f[3 + n])
                put(1, j, i, f[3 + n])
            for i in range(3):
                put(0, i, i, jnp.zeros((SUB, LANES), jnp.float32))
            put(1, 0, 0, f[6])
            put(1, 1, 1, f[7])
            put(1, 2, 2, -(f[6] + f[7]))
        for part in range(2):
            for i in range(3):
                pltpu.make_async_copy(out.at[m, part, i], hbm.at[m, part, i], sem).start()
    pltpu.make_async_copy(out, hbm, sem).wait()


def per_device(counts, links):
    time_len, depth, flat = links.shape[4:]
    sites = time_len * depth
    assert flat == LANES and (time_len, depth) == (4, 4)
    halves = sites // SUB
    vmem = lambda *s: pltpu.VMEM(s + (LANES,), jnp.float32)
    shape = links.shape[:4] + (sites, flat)
    terms = pl.pallas_call(
        functools.partial(force_terms, counts, depth, halves),
        out_shape=pltpu.VMEM((32 * sites, flat), jnp.float32),
        in_specs=[pl.BlockSpec(memory_space=pl.ANY)],
        out_specs=pl.BlockSpec(memory_space=pltpu.VMEM),
        scratch_shapes=[
            vmem(*shape[:-1]),
            vmem(TOTAL),
            vmem(TOTAL),
            vmem(5, 3, 2, 2, 3, SUB),
            vmem(5, 2, 3, 3, SUB),
            vmem(5, 2, 3, 3, SUB),
            pltpu.SemaphoreType.DMA,
            pltpu.SemaphoreType.DMA,
            pltpu.SemaphoreType.DMA((7,)),
            pltpu.SemaphoreType.REGULAR,
        ],
        compiler_params=pltpu.CompilerParams(collective_id=0, has_side_effects=True),
        name="force_terms",
    )(links.reshape(shape))
    out = pl.pallas_call(
        functools.partial(expand, halves),
        out_shape=jax.ShapeDtypeStruct(shape, jnp.float32),
        in_specs=[pl.BlockSpec(memory_space=pltpu.VMEM)],
        out_specs=pl.BlockSpec(memory_space=pl.ANY),
        scratch_shapes=[vmem(*shape[:-1]), pltpu.SemaphoreType.DMA],
        name="expand",
    )(pltpu.with_memory_space_constraint(terms, pltpu.VMEM))
    return out.reshape(links.shape)


def solution(mesh):
    assert mesh.axis_names == ("gx", "gz", "ta")
    counts = tuple(mesh.shape[a] for a in AXES)
    spec = P(None, None, None, None, "ta", "gz", "gx")
    return jax.shard_map(
        functools.partial(per_device, counts),
        mesh=mesh,
        in_specs=(spec,),
        out_specs=spec,
        check_vma=False,
    )
```

```python
import functools

import jax
import jax.numpy as jnp
from jax import lax
from jax.experimental import pallas as pl
from jax.experimental.pallas import tpu as pltpu
from jax.sharding import PartitionSpec as P

NX = 16
COEFF = -1.9
AXES = ("ta", "gz", "gx")
SUB, LANES = 8, 128


def others(d):
    return [m for m in range(4) if m != d]


class Lattice:
    def __init__(self, depth):
        self.depth = depth
        self.per = SUB // depth
        self.ygroups = LANES // NX
        self.row = lax.broadcasted_iota(jnp.int32, (SUB, LANES), 0)
        self.lane = lax.broadcasted_iota(jnp.int32, (SUB, LANES), 1)
        self.zrow = self.row % depth
        self.xcol = self.lane % NX

    def rows(self, value, shift):
        shift %= SUB
        return pltpu.roll(value, shift, 0) if shift else value

    def lanes(self, value, shift):
        shift %= LANES
        return pltpu.roll(value, shift, 1) if shift else value


def entry(left, right, i, j, part, left_h, right_h):
    total = None
    for k in range(3):
        li = (k, i) if left_h else (i, k)
        ri = (j, k) if right_h else (k, j)
        lr, lm = left[0][li[0]][li[1]], left[1][li[0]][li[1]]
        rr, rm = right[0][ri[0]][ri[1]], right[1][ri[0]][ri[1]]
        if part == 0:
            first, second = lr * rr, lm * rm
            minus = left_h == right_h
        elif left_h:
            first, second = lr * rm, lm * rr
            minus = True
        else:
            first, second = lm * rr, lr * rm
            minus = right_h
        value = first - second if minus else first + second
        total = value if total is None else total + value
    return total


def product(left, right, left_h=False, right_h=False):
    return [
        [[entry(left, right, i, j, part, left_h, right_h) for j in range(3)] for i in range(3)]
        for part in range(2)
    ]


def projected(left, right, left_h=False, right_h=False):
    get = lambda i, j, part: entry(left, right, i, j, part, left_h, right_h)
    pairs = ((0, 1), (0, 2), (1, 2))
    real = [get(i, j, 0) - get(j, i, 0) for i, j in pairs]
    imag = [get(i, j, 1) + get(j, i, 1) for i, j in pairs]
    diag = [get(i, i, 1) for i in range(3)]
    third = (diag[0] + diag[1] + diag[2]) * (1.0 / 3.0)
    return real + imag + [diag[0] - third, diag[1] - third]


def third_row(real, imag):
    rows_r, rows_i = [], []
    for column in range(3):
        n, l = (column + 1) % 3, (column + 2) % 3
        rows_r.append(
            real[0][n] * real[1][l]
            - imag[0][n] * imag[1][l]
            - real[0][l] * real[1][n]
            + imag[0][l] * imag[1][n]
        )
        rows_i.append(
            real[0][l] * imag[1][n]
            + imag[0][l] * real[1][n]
            - real[0][n] * imag[1][l]
            - imag[0][n] * real[1][l]
        )
    return rows_r, rows_i


PLANES = ((0, 1), (0, 2), (0, 3), (1, 2), (1, 3), (2, 3))
DIAGONALS = ((0, 2), (2, 0), (0, 1), (1, 0), (1, 2), (2, 1))
LAYOUT = (
    (((1, 0), (2, 0)), ((3, 0),)),
    (((0, 0), (0, 1), (2, 0), (2, 1)), ((3, 0), (3, 1))),
    (((0, 0), (0, 1), (1, 0), (1, 1), (3, 0), (3, 1)),),
)
ROWS = (144, 144, 96)
EDGES = (8, 8, 16, 16, 8, 8)


def offset(kind, d):
    if kind == "e":
        return 2 * sum(ROWS) + sum(EDGES[:d])
    return (sum(ROWS) if kind == "g" else 0) + sum(ROWS[:d])


TOTAL = offset("e", len(DIAGONALS))


def force_terms(
    counts, depth, halves, hbm, acc, u, out_s, in_s, face_s, b_s, pre_s, load_sem, send, recv, met, met_t, met_z,
):
    g = Lattice(depth)
    me = [lax.axis_index(a) for a in AXES]
    comps = [(part, i, j) for part in range(2) for i in range(2) for j in range(3)]
    last = (g.per - 1, depth - 1, g.ygroups - 1)
    place = (g.row // depth, g.zrow, g.lane // NX)

    def device(*steps):
        where = list(me)
        for i, step in steps:
            where[i] = lax.rem(me[i] + (step + counts[i]), counts[i])
        by = dict(zip(AXES, where))
        return (by["gx"], by["gz"], by["ta"])

    loads = [
        pltpu.make_async_copy(hbm.at[m, part, i], u.at[m, part, i], load_sem)
        for m in range(4)
        for part in range(2)
        for i in range(3)
    ]
    for copy in loads:
        copy.start()
    barrier = pltpu.get_barrier_semaphore()
    first_t, last_t = me[0] == 0, me[0] == counts[0] - 1
    first_z, last_z = me[1] == 0, me[1] == counts[1] - 1
    more_t, more_z = jnp.logical_not(last_t), jnp.logical_not(last_z)
    rest_t, rest_z = jnp.logical_not(first_t), jnp.logical_not(first_z)
    one = lambda flag: jnp.where(flag, 1, 0)

    def signal(semaphore, *steps):
        pl.semaphore_signal(
            semaphore, inc=1, device_id=device(*steps), device_id_type=pl.DeviceIdType.MESH
        )

    for steps in (((1, -1),), ((2, 1), (1, -1)), ((0, -1), (2, 1)), ((0, -1),), ((2, 1),), ((2, -1),)):
        signal(barrier, *steps)

    @pl.when(more_z)
    def _():
        signal(barrier, (1, 1))
        signal(barrier, (1, 1), (2, -1))

    @pl.when(jnp.logical_or(more_z, first_t))
    def _():
        signal(barrier, (1, 1), (0, -1))

    @pl.when(more_t)
    def _():
        signal(barrier, (0, 1))
        signal(barrier, (0, 1), (1, -1))

    expected = 11 - 2 * one(first_t) - 2 * one(first_z) - one(jnp.logical_and(first_z, more_t))

    def remote(start, rows, slot, where):
        span = slice(start, start + rows)
        return pltpu.make_async_remote_copy(
            src_ref=out_s.at[span], dst_ref=in_s.at[span], send_sem=send, recv_sem=recv.at[slot],
            device_id=where, device_id_type=pl.DeviceIdType.MESH,
        )

    faces = [remote(offset("x", d), ROWS[d], d, device((d, -1))) for d in range(3)]
    opens = [remote(offset("g", d), ROWS[d], 3 + d, device((d, 1))) for d in range(3)]
    edges = [
        remote(offset("e", k), EDGES[k], 6, device((d, 1), (n, -1)))
        for k, (d, n) in enumerate(DIAGONALS)
    ]
    all_edges = remote(offset("e", 0), sum(EDGES), 6, device((1, 1)))
    everything = remote(0, TOTAL, 0, device((1, 1)))

    def load(m, part, i, j, h):
        return u[m, part, i, j, h * SUB : (h + 1) * SUB, :]

    def shifted(d, value, steps):
        if d == 0:
            return g.rows(value, depth * steps)
        return g.rows(value, steps) if d == 1 else g.lanes(value, NX * steps)

    def half(d, h, top):
        return (halves - 1 if top else 0) if d == 0 else h

    def complete(d, h):
        return d == 3 or (d == 0 and h + 1 < halves)

    def top(d, h=1):
        if d == 0:
            return g.row >= SUB - depth
        return g.zrow == depth - 1 if d == 1 else g.lane >= LANES - NX

    def bottom(d):
        return (g.row < depth, g.zrow == 0, g.lane < NX)[d]

    def open_mask(d, s, among=(0, 1, 2)):
        mask = None
        for k, (m, h) in enumerate(LAYOUT[d][s]):
            if m in among and not complete(m, h if d else 1):
                here = jnp.logical_and(place[d] == k, top(m))
                mask = here if mask is None else jnp.logical_or(mask, here)
        return mask

    def pick(mask, yes, no):
        return no if mask is None else jnp.where(mask, yes, no)

    def pack(d, s, get, up):
        value = None
        for k, (m, h) in enumerate(LAYOUT[d][s]):
            x = get(m, half(d, h, up))
            if x is None:
                continue
            x = shifted(d, x, k - (last[d] if up else 0))
            value = x if value is None else jnp.where(place[d] >= k, x, value)
        return value

    def complete_rows(get):
        real = [[get(0, i, j) for j in range(3)] for i in range(2)]
        imag = [[get(1, i, j) for j in range(3)] for i in range(2)]
        third_r, third_i = third_row(real, imag)
        return [real + [third_r], imag + [third_i]]

    def packed(d, s, get, up):
        return complete_rows(
            lambda part, i, j: pack(d, s, lambda m, h: get(m, h, part, i, j), up)
        )

    def put(kind, d, s, value):
        r = offset(kind, d)
        used = len(LAYOUT[d][s])
        for n, (part, i, j) in enumerate(comps[: 6 if s else 12]):
            v = value[part][i][j]
            if s:
                v = jnp.where(place[d] < used, v, shifted(d, value[1][i][j], used))
            at = r + (96 if s else 0) + n * SUB
            out_s[at : at + SUB, :] = v

    def fetch(ref, kind, d, s, part, i, j):
        n = part * 6 + i * 3 + j
        at = offset(kind, d) + n * SUB
        if not s:
            return ref[at : at + SUB, :]
        at += 96 - part * 6 * SUB
        v = ref[at : at + SUB, :]
        return shifted(d, v, -len(LAYOUT[d][s])) if part else v

    def fetched(ref, kind, d, s):
        return complete_rows(lambda part, i, j: fetch(ref, kind, d, s, part, i, j))

    def rolled(m, d, h, part, i, j):
        v = load(m, part, i, j, h)
        if d == 3:
            return jnp.where(g.xcol == NX - 1, g.lanes(v, NX - 1), g.lanes(v, -1))
        if d == 2:
            return g.lanes(v, -NX)
        if d == 1:
            return g.rows(v, -1)
        if h + 1 < halves:
            beyond = g.rows(load(m, part, i, j, h + 1), -depth)
            return jnp.where(g.row >= SUB - depth, beyond, g.rows(v, -depth))
        return g.rows(v, -depth)

    def matrix(get):
        return [[[get(part, i, j) for j in range(3)] for i in range(3)] for part in range(2)]

    def save(ref, index, value):
        for part in range(2):
            for i in range(ref.shape[-4]):
                for j in range(3):
                    ref[(*index, part, i, j)] = value[part][i][j]

    sets = [(d, s) for d in range(3) for s in range(len(LAYOUT[d]))]

    def kept(d, s, q):
        n = sets.index((d, s))
        return complete_rows(lambda part, i, j: face_s[n, q, part, i, j])

    def own_face(d):
        def get(part, i, j):
            if d != 2:
                return pack(d, 0, lambda m, h: load(d, part, i, j, h), True)
            pair = [shifted(d, load(d, part, i, j, h), h - last[d]) for h in range(halves)]
            pair = jnp.where(place[d] >= 1, pair[1], pair[0])
            value = jnp.where(place[d] >= 2, shifted(d, pair, 2), pair)
            return jnp.where(place[d] >= 4, shifted(d, pair, 4), value)

        return complete_rows(get)

    def step_in_face(d, m, v):
        if m == 3:
            return jnp.where(g.xcol == NX - 1, g.lanes(v, NX - 1), g.lanes(v, -1))
        if m == 2:
            return g.lanes(v, -NX)
        if m == 1:
            return g.rows(v, -1)
        moved = g.rows(v, -depth)
        if d == 1:
            beyond = g.rows(v, depth - 1)
            return jnp.where(jnp.logical_and(g.zrow == 0, g.row >= depth), beyond, moved)
        return jnp.where(g.row >= depth, g.lanes(moved, -NX), moved)

    def over_face(d, s, own):
        def get(part, i, j):
            value, before = None, None
            for k, (m, h) in enumerate(LAYOUT[d][s]):
                if m == before:
                    continue
                x = step_in_face(d, m, own[part][i][j])
                value = x if value is None else jnp.where(place[d] >= k, x, value)
                before = m
            return value

        return complete_rows(get)

    def send_side(d):
        own = own_face(d)
        for s in range(len(LAYOUT[d])):
            n = sets.index((d, s))
            side = packed(d, s, lambda m, h, *c: load(m, *c, h), True)
            over = over_face(d, s, own)
            b = product(own, side, left_h=True)
            mask = open_mask(d, s)
            put("g", d, s, [
                [
                    [pick(mask, b[p][i][j], entry(b, over, i, j, p, False, False)) for j in range(3)]
                    for i in range(2)
                ]
                for p in range(2)
            ])
            for q, value in enumerate((own, side, over)):
                save(face_s, (n, q), value)
            save(b_s, (n,), b)

    def send_face(d):
        for s in range(len(LAYOUT[d])):
            put("x", d, s, [
                [
                    [pack(d, s, lambda m, h: load(m, p, i, j, h), False) for j in range(3)]
                    for i in range(2)
                ]
                for p in range(2)
            ])

    def pack_edges(d, n):
        r0 = offset("e", DIAGONALS.index((d, n)))
        if 2 not in (d, n):
            for c0 in range(0, 12, SUB):
                value = None
                for k in range(min(SUB, 12 - c0)):
                    v = load(d, *comps[c0 + k], halves - 1 if d == 0 else 0)
                    x = g.rows(v, k - depth if d == 0 else k - (depth - 1))
                    value = x if value is None else jnp.where(g.row >= k, x, value)
                out_s[r0 + c0 : r0 + c0 + SUB, :] = value
            return
        value = None
        for k in range(g.ygroups):
            v = dense_rows(d, n, comps[k])
            if k + g.ygroups < 12:
                w = dense_rows(d, n, comps[k + g.ygroups])
                step, mask = spare(d, n)
                v = jnp.where(mask, v, g.rows(w, step))
            x = g.lanes(v, NX * (k + (1 if d == 2 else 0)))
            value = x if value is None else jnp.where(g.lane >= NX * k, x, value)
        out_s[r0 : r0 + SUB, :] = value

    def spare(d, n):
        if (d, n) == (0, 2):
            return depth, g.row >= depth
        if (d, n) == (2, 0):
            return depth, g.row < depth
        return (-2, g.zrow >= 2) if d == 1 else (2, g.zrow < 2)

    def dense_rows(d, n, c):
        if 0 in (d, n):
            return load(d, *c, halves - 1 if d == 0 else 0)
        at = depth - 1 if d == 1 else 0
        step = -1 if d == 1 else 1
        v = load(d, *c, 0)
        for h in range(1, halves):
            v = jnp.where(g.zrow == at + step * h, g.rows(load(d, *c, h), step * h), v)
        return v

    def edge(d, n, h, part, i, j):
        c = part * 6 + i * 3 + j
        r = offset("e", DIAGONALS.index((d, n)))
        if 2 not in (d, n):
            v = in_s[r + c // SUB * SUB : r + c // SUB * SUB + SUB, :]
            k = c % SUB
            return g.rows(v, depth - 1 - k if d == 0 else SUB - depth - k)
        k, back = c % g.ygroups, c >= g.ygroups
        v = g.lanes(in_s[r : r + SUB, :], NX * ((0 if d == 2 else g.ygroups - 1) - k))
        step = -spare(d, n)[0] if back else 0
        if (d, n) == (0, 2):
            return g.rows(v, step - (SUB - depth))
        if (d, n) == (2, 0):
            return g.rows(v, step + SUB - depth)
        return g.rows(v, step + (1 - depth + h if d == 1 else depth - 1 - h))

    everything_in = pltpu.make_async_copy(hbm, u, load_sem)
    everything_in.wait()
    for d, n in DIAGONALS:
        pack_edges(d, n)
    for d in (1, 0):
        send_side(d)
        send_face(d)
    send_face(2)
    pl.semaphore_wait(barrier, expected)
    for copy in [edges[4], edges[0], opens[1], opens[0]]:
        copy.start()
    signal(met, (2, -1))

    @pl.when(last_t)
    def _():
        signal(met_t, (0, 1))

    @pl.when(last_z)
    def _():
        signal(met_z, (1, 1))

    @pl.when(rest_t)
    def _():
        edges[3].start()
        faces[0].start()

    @pl.when(rest_z)
    def _():
        edges[5].start()
        faces[1].start()

    @pl.when(jnp.logical_or(rest_z, last_t))
    def _():
        edges[2].start()

    send_side(2)
    faces[2].start()
    opens[2].start()

    seen, pending = set(), {}

    def add(m, c, h, value):
        key = (m, c, h)
        pending[key] = pending[key] + value if key in pending else value

    def flush():
        for (m, c, h), value in pending.items():
            r = ((m * 8 + c) * halves + h) * SUB
            if (m, c, h) in seen:
                acc[r : r + SUB, :] += value
            else:
                seen.add((m, c, h))
                acc[r : r + SUB, :] = value
        pending.clear()

    def forward(m, d, h, q):
        for c in range(8):
            if d == 3:
                add(m, c, h, jnp.where(g.xcol == 0, g.lanes(q[c], 1 - NX), g.lanes(q[c], 1)))
            elif d == 2:
                add(m, c, h, g.lanes(q[c], NX))
            elif d == 1:
                add(m, c, h, g.rows(q[c], 1))
            elif h + 1 < halves:
                moved = g.rows(q[c], depth)
                add(m, c, h, jnp.where(g.row >= depth, moved, 0.0))
                add(m, c, h + 1, jnp.where(g.row < depth, moved, 0.0))
            else:
                add(m, c, h, g.rows(q[c], depth))

    def masked(mask, a):
        return [[[pick(mask, 0.0, v) for v in line] for line in part] for part in a]

    def inner(mu, nu, h):
        own = matrix(lambda *c: load(mu, *c, h))
        side = matrix(lambda *c: load(nu, *c, h))
        a = product(
            matrix(lambda *c: rolled(nu, mu, h, *c)),
            matrix(lambda *c: rolled(mu, nu, h, *c)),
            right_h=True,
        )
        mask = None
        for d in (mu, nu):
            if not complete(d, h):
                mask = top(d) if mask is None else jnp.logical_or(mask, top(d))
        a = masked(mask, a)
        b = product(own, side, left_h=True)
        forward(mu, nu, h, projected(a, b, left_h=True))
        forward(nu, mu, h, projected(a, b, right_h=True))
        upper = projected(product(own, a), side, right_h=True)
        for c in range(8):
            add(mu, c, h, upper[c])
            add(nu, c, h, -upper[c])

    def corners(d, among):
        for s in range(len(LAYOUT[d])):
            mask = open_mask(d, s, among)
            if mask is None:
                continue
            n = sets.index((d, s))

            def corner(m, h, c):
                if m not in among or complete(m, h):
                    return None
                k = LAYOUT[m][0].index((d, 0 if m == 0 else h))
                return shifted(m, fetch(in_s, "x", m, 0, *c), last[m] - k)

            for c in comps:
                value = pack(d, s, lambda m, h: corner(m, h, c), True)
                face_s[(n, 2, *c)] = jnp.where(mask, value, face_s[(n, 2, *c)])

    def face_terms(d, closed):
        for s, spots in enumerate(LAYOUT[d]):
            n = sets.index((d, s))
            own, side, over = (kept(d, s, q) for q in range(3))
            a = product(fetched(in_s, "x", d, s), over, right_h=True)
            a = masked(open_mask(d, s, [m for m in range(3) if m not in closed]), a)
            b = matrix(lambda *c: b_s[(n, *c)])
            upper = projected(product(own, a), side, right_h=True)
            low = projected(a, b, left_h=True)
            mask = open_mask(d, s, closed)
            low = [pick(mask, 0.0, v) for v in low]
            for k, (m, h) in enumerate(spots):
                h = half(d, h, True)
                natural = lambda v: jnp.where(top(d), shifted(d, v, last[d] - k), 0.0)
                for c in range(8):
                    x = natural(upper[c])
                    add(d, c, h, x)
                    add(m, c, h, -x)
                forward(d, m, h, [natural(v) for v in low])
        flush()

    def prepare(d):
        for s in range(len(LAYOUT[d])):
            own = fetched(out_s, "x", d, s)
            mask = open_mask(d, s)
            if mask is not None:
                far = packed(
                    d, s,
                    lambda m, h, *c: None if complete(m, h if d else 1) else edge(d, m, h, *c),
                    False,
                )
                both = product(own, far, right_h=True)
                own = [
                    [[jnp.where(mask, both[p][i][j], own[p][i][j]) for j in range(3)] for i in range(3)]
                    for p in range(2)
                ]
            save(pre_s, (sets.index((d, s)),), own)

    def close(d):
        for s, spots in enumerate(LAYOUT[d]):
            n = sets.index((d, s))
            q = projected(
                matrix(lambda *c: pre_s[(n, *c)]), fetched(in_s, "g", d, s), right_h=True
            )
            for k, (m, h) in enumerate(spots):
                for c in range(8):
                    add(m, c, half(d, h, False), jnp.where(bottom(d), shifted(d, q[c], -k), 0.0))
        flush()

    for n, pair in enumerate(PLANES):
        if n == 2:
            pl.semaphore_wait(met, 1)

            @pl.when(rest_t)
            def _():
                edges[1].start()

        for h in range(halves):
            inner(*pair, h)
        flush()

    @pl.when(first_t)
    def _():
        pl.semaphore_wait(met_t, 1)
        for copy in (edges[3], edges[1], faces[0]):
            copy.start()

    @pl.when(first_z)
    def _():
        pl.semaphore_wait(met_z, 1)
        edges[5].start()
        faces[1].start()

    @pl.when(jnp.logical_and(first_z, more_t))
    def _():
        edges[2].start()

    faces[2].wait_recv()
    face_terms(2, ())
    corners(0, (2,))
    faces[0].wait_recv()
    face_terms(0, (2,))
    corners(1, (0, 2))
    faces[1].wait_recv()
    face_terms(1, (0, 2))
    all_edges.wait_recv()
    for d in (2, 0, 1):
        prepare(d)
    for d in (2, 0, 1):
        opens[d].wait_recv()
    for d in (2, 0, 1):
        close(d)
    everything.wait_send()


def expand(halves, acc, hbm, out, sem):
    for m in range(4):
        for h in range(halves):
            rows = [((m * 8 + c) * halves + h) * SUB for c in range(8)]
            f = [acc[r : r + SUB, :] * (COEFF * 0.5 if c < 6 else COEFF) for c, r in enumerate(rows)]

            def put(part, i, j, value):
                out[m, part, i, j, h * SUB : (h + 1) * SUB, :] = value

            for n, (i, j) in enumerate(((0, 1), (0, 2), (1, 2))):
                put(0, i, j, f[n])
                put(0, j, i, -f[n])
                put(1, i, j, f[3 + n])
                put(1, j, i, f[3 + n])
            for i in range(3):
                put(0, i, i, jnp.zeros((SUB, LANES), jnp.float32))
            put(1, 0, 0, f[6])
            put(1, 1, 1, f[7])
            put(1, 2, 2, -(f[6] + f[7]))
        for part in range(2):
            for i in range(3):
                pltpu.make_async_copy(out.at[m, part, i], hbm.at[m, part, i], sem).start()
    pltpu.make_async_copy(out, hbm, sem).wait()


def per_device(counts, links):
    time_len, depth, flat = links.shape[4:]
    sites = time_len * depth
    assert flat == LANES and (time_len, depth) == (4, 4)
    halves = sites // SUB
    vmem = lambda *s: pltpu.VMEM(s + (LANES,), jnp.float32)
    shape = links.shape[:4] + (sites, flat)
    terms = pl.pallas_call(
        functools.partial(force_terms, counts, depth, halves),
        out_shape=pltpu.VMEM((32 * sites, flat), jnp.float32),
        in_specs=[pl.BlockSpec(memory_space=pl.ANY)],
        out_specs=pl.BlockSpec(memory_space=pltpu.VMEM),
        scratch_shapes=[
            vmem(*shape[:-1]),
            vmem(TOTAL),
            vmem(TOTAL),
            vmem(5, 3, 2, 2, 3, SUB),
            vmem(5, 2, 3, 3, SUB),
            vmem(5, 2, 3, 3, SUB),
            pltpu.SemaphoreType.DMA,
            pltpu.SemaphoreType.DMA,
            pltpu.SemaphoreType.DMA((7,)),
            pltpu.SemaphoreType.REGULAR,
            pltpu.SemaphoreType.REGULAR,
            pltpu.SemaphoreType.REGULAR,
        ],
        compiler_params=pltpu.CompilerParams(collective_id=0, has_side_effects=True),
        name="force_terms",
    )(links.reshape(shape))
    out = pl.pallas_call(
        functools.partial(expand, halves),
        out_shape=jax.ShapeDtypeStruct(shape, jnp.float32),
        in_specs=[pl.BlockSpec(memory_space=pltpu.VMEM)],
        out_specs=pl.BlockSpec(memory_space=pl.ANY),
        scratch_shapes=[vmem(*shape[:-1]), pltpu.SemaphoreType.DMA],
        name="expand",
    )(pltpu.with_memory_space_constraint(terms, pltpu.VMEM))
    return out.reshape(links.shape)


def solution(mesh):
    assert mesh.axis_names == ("gx", "gz", "ta")
    counts = tuple(mesh.shape[a] for a in AXES)
    spec = P(None, None, None, None, "ta", "gz", "gx")
    return jax.shard_map(
        functools.partial(per_device, counts),
        mesh=mesh,
        in_specs=(spec,),
        out_specs=spec,
        check_vma=False,
    )
```

```python
import functools

import jax
import jax.numpy as jnp
from jax import lax
from jax.experimental import pallas as pl
from jax.experimental.pallas import tpu as pltpu
from jax.sharding import PartitionSpec as P

NX = 16
COEFF = -1.9
AXES = ("ta", "gz", "gx")
SUB, LANES = 8, 128


def others(d):
    return [m for m in range(4) if m != d]


class Lattice:
    def __init__(self, depth):
        self.depth = depth
        self.per = SUB // depth
        self.ygroups = LANES // NX
        self.row = lax.broadcasted_iota(jnp.int32, (SUB, LANES), 0)
        self.lane = lax.broadcasted_iota(jnp.int32, (SUB, LANES), 1)
        self.zrow = self.row % depth
        self.xcol = self.lane % NX

    def rows(self, value, shift):
        shift %= SUB
        return pltpu.roll(value, shift, 0) if shift else value

    def lanes(self, value, shift):
        shift %= LANES
        return pltpu.roll(value, shift, 1) if shift else value


def entry(left, right, i, j, part, left_h, right_h):
    total = None
    for k in range(3):
        li = (k, i) if left_h else (i, k)
        ri = (j, k) if right_h else (k, j)
        lr, lm = left[0][li[0]][li[1]], left[1][li[0]][li[1]]
        rr, rm = right[0][ri[0]][ri[1]], right[1][ri[0]][ri[1]]
        if part == 0:
            first, second = lr * rr, lm * rm
            minus = left_h == right_h
        elif left_h:
            first, second = lr * rm, lm * rr
            minus = True
        else:
            first, second = lm * rr, lr * rm
            minus = right_h
        value = first - second if minus else first + second
        total = value if total is None else total + value
    return total


def product(left, right, left_h=False, right_h=False):
    return [
        [[entry(left, right, i, j, part, left_h, right_h) for j in range(3)] for i in range(3)]
        for part in range(2)
    ]


def projected(left, right, left_h=False, right_h=False):
    get = lambda i, j, part: entry(left, right, i, j, part, left_h, right_h)
    pairs = ((0, 1), (0, 2), (1, 2))
    real = [get(i, j, 0) - get(j, i, 0) for i, j in pairs]
    imag = [get(i, j, 1) + get(j, i, 1) for i, j in pairs]
    diag = [get(i, i, 1) for i in range(3)]
    third = (diag[0] + diag[1] + diag[2]) * (1.0 / 3.0)
    return real + imag + [diag[0] - third, diag[1] - third]


def third_row(real, imag):
    rows_r, rows_i = [], []
    for column in range(3):
        n, l = (column + 1) % 3, (column + 2) % 3
        rows_r.append(
            real[0][n] * real[1][l]
            - imag[0][n] * imag[1][l]
            - real[0][l] * real[1][n]
            + imag[0][l] * imag[1][n]
        )
        rows_i.append(
            real[0][l] * imag[1][n]
            + imag[0][l] * real[1][n]
            - real[0][n] * imag[1][l]
            - imag[0][n] * real[1][l]
        )
    return rows_r, rows_i


PLANES = ((0, 1), (0, 2), (0, 3), (1, 2), (1, 3), (2, 3))
DIAGONALS = ((0, 2), (2, 0), (0, 1), (1, 0), (1, 2), (2, 1))
LAYOUT = (
    (((1, 0), (2, 0)), ((3, 0),)),
    (((0, 0), (0, 1), (2, 0), (2, 1)), ((3, 0), (3, 1))),
    (((0, 0), (0, 1), (1, 0), (1, 1), (3, 0), (3, 1)),),
)
ROWS = (144, 144, 96)
EDGES = (8, 8, 16, 16, 8, 8)


def offset(kind, d):
    if kind == "e":
        return 2 * sum(ROWS) + sum(EDGES[:d])
    return (sum(ROWS) if kind == "g" else 0) + sum(ROWS[:d])


TOTAL = offset("e", len(DIAGONALS))


def force_terms(
    counts, depth, halves, hbm, acc, u, out_s, in_s, face_s, b_s, pre_s, load_sem, send, recv, met, met_t, met_z,
):
    g = Lattice(depth)
    me = [lax.axis_index(a) for a in AXES]
    comps = [(part, i, j) for part in range(2) for i in range(2) for j in range(3)]
    last = (g.per - 1, depth - 1, g.ygroups - 1)
    place = (g.row // depth, g.zrow, g.lane // NX)

    def device(*steps):
        where = list(me)
        for i, step in steps:
            where[i] = lax.rem(me[i] + (step + counts[i]), counts[i])
        by = dict(zip(AXES, where))
        return (by["gx"], by["gz"], by["ta"])

    loads = [
        pltpu.make_async_copy(hbm.at[m, part, i], u.at[m, part, i], load_sem)
        for m in range(4)
        for part in range(2)
        for i in range(3)
    ]
    for copy in loads:
        copy.start()
    barrier = pltpu.get_barrier_semaphore()
    first_t, last_t = me[0] == 0, me[0] == counts[0] - 1
    more_t, rest_t = jnp.logical_not(last_t), jnp.logical_not(first_t)
    middle = counts[1] // 2
    first_z = jnp.logical_or(me[1] == 0, jnp.logical_and(me[1] == middle, rest_t))
    last_z = jnp.logical_or(
        me[1] == counts[1] - 1, jnp.logical_and(me[1] == middle - 1, rest_t)
    )
    silent = jnp.logical_or(
        jnp.logical_and(me[1] == counts[1] - 1, rest_t),
        jnp.logical_and(me[1] == middle - 1, me[0] > 1),
    )
    more_z, rest_z = jnp.logical_not(last_z), jnp.logical_not(first_z)
    one = lambda flag: jnp.where(flag, 1, 0)

    def signal(semaphore, *steps):
        pl.semaphore_signal(
            semaphore, inc=1, device_id=device(*steps), device_id_type=pl.DeviceIdType.MESH
        )

    for steps in (((1, -1),), ((2, 1), (1, -1)), ((0, -1), (2, 1)), ((0, -1),), ((2, 1),), ((2, -1),)):
        signal(barrier, *steps)

    @pl.when(more_z)
    def _():
        signal(barrier, (1, 1))
        signal(barrier, (1, 1), (2, -1))

    @pl.when(jnp.logical_not(silent))
    def _():
        signal(barrier, (1, 1), (0, -1))

    @pl.when(more_t)
    def _():
        signal(barrier, (0, 1))
        signal(barrier, (0, 1), (1, -1))

    expected = 11 - 2 * one(first_t) - 2 * one(first_z) - one(jnp.logical_and(first_z, more_t))

    def remote(start, rows, slot, where):
        span = slice(start, start + rows)
        return pltpu.make_async_remote_copy(
            src_ref=out_s.at[span], dst_ref=in_s.at[span], send_sem=send, recv_sem=recv.at[slot],
            device_id=where, device_id_type=pl.DeviceIdType.MESH,
        )

    faces = [remote(offset("x", d), ROWS[d], d, device((d, -1))) for d in range(3)]
    opens = [remote(offset("g", d), ROWS[d], 3 + d, device((d, 1))) for d in range(3)]
    edges = [
        remote(offset("e", k), EDGES[k], 6, device((d, 1), (n, -1)))
        for k, (d, n) in enumerate(DIAGONALS)
    ]
    all_edges = remote(offset("e", 0), sum(EDGES), 6, device((1, 1)))
    everything = remote(0, TOTAL, 0, device((1, 1)))

    def load(m, part, i, j, h):
        return u[m, part, i, j, h * SUB : (h + 1) * SUB, :]

    def shifted(d, value, steps):
        if d == 0:
            return g.rows(value, depth * steps)
        return g.rows(value, steps) if d == 1 else g.lanes(value, NX * steps)

    def half(d, h, top):
        return (halves - 1 if top else 0) if d == 0 else h

    def complete(d, h):
        return d == 3 or (d == 0 and h + 1 < halves)

    def top(d, h=1):
        if d == 0:
            return g.row >= SUB - depth
        return g.zrow == depth - 1 if d == 1 else g.lane >= LANES - NX

    def bottom(d):
        return (g.row < depth, g.zrow == 0, g.lane < NX)[d]

    def open_mask(d, s, among=(0, 1, 2)):
        mask = None
        for k, (m, h) in enumerate(LAYOUT[d][s]):
            if m in among and not complete(m, h if d else 1):
                here = jnp.logical_and(place[d] == k, top(m))
                mask = here if mask is None else jnp.logical_or(mask, here)
        return mask

    def pick(mask, yes, no):
        return no if mask is None else jnp.where(mask, yes, no)

    def pack(d, s, get, up):
        value = None
        for k, (m, h) in enumerate(LAYOUT[d][s]):
            x = get(m, half(d, h, up))
            if x is None:
                continue
            x = shifted(d, x, k - (last[d] if up else 0))
            value = x if value is None else jnp.where(place[d] >= k, x, value)
        return value

    def complete_rows(get):
        real = [[get(0, i, j) for j in range(3)] for i in range(2)]
        imag = [[get(1, i, j) for j in range(3)] for i in range(2)]
        third_r, third_i = third_row(real, imag)
        return [real + [third_r], imag + [third_i]]

    def packed(d, s, get, up):
        return complete_rows(
            lambda part, i, j: pack(d, s, lambda m, h: get(m, h, part, i, j), up)
        )

    def put(kind, d, s, value):
        r = offset(kind, d)
        used = len(LAYOUT[d][s])
        for n, (part, i, j) in enumerate(comps[: 6 if s else 12]):
            v = value[part][i][j]
            if s:
                v = jnp.where(place[d] < used, v, shifted(d, value[1][i][j], used))
            at = r + (96 if s else 0) + n * SUB
            out_s[at : at + SUB, :] = v

    def fetch(ref, kind, d, s, part, i, j):
        n = part * 6 + i * 3 + j
        at = offset(kind, d) + n * SUB
        if not s:
            return ref[at : at + SUB, :]
        at += 96 - part * 6 * SUB
        v = ref[at : at + SUB, :]
        return shifted(d, v, -len(LAYOUT[d][s])) if part else v

    def fetched(ref, kind, d, s):
        return complete_rows(lambda part, i, j: fetch(ref, kind, d, s, part, i, j))

    def rolled(m, d, h, part, i, j):
        v = load(m, part, i, j, h)
        if d == 3:
            return jnp.where(g.xcol == NX - 1, g.lanes(v, NX - 1), g.lanes(v, -1))
        if d == 2:
            return g.lanes(v, -NX)
        if d == 1:
            return g.rows(v, -1)
        if h + 1 < halves:
            beyond = g.rows(load(m, part, i, j, h + 1), -depth)
            return jnp.where(g.row >= SUB - depth, beyond, g.rows(v, -depth))
        return g.rows(v, -depth)

    def matrix(get):
        return [[[get(part, i, j) for j in range(3)] for i in range(3)] for part in range(2)]

    def save(ref, index, value):
        for part in range(2):
            for i in range(ref.shape[-4]):
                for j in range(3):
                    ref[(*index, part, i, j)] = value[part][i][j]

    sets = [(d, s) for d in range(3) for s in range(len(LAYOUT[d]))]

    def kept(d, s, q):
        n = sets.index((d, s))
        return complete_rows(lambda part, i, j: face_s[n, q, part, i, j])

    def own_face(d):
        def get(part, i, j):
            if d != 2:
                return pack(d, 0, lambda m, h: load(d, part, i, j, h), True)
            pair = [shifted(d, load(d, part, i, j, h), h - last[d]) for h in range(halves)]
            pair = jnp.where(place[d] >= 1, pair[1], pair[0])
            value = jnp.where(place[d] >= 2, shifted(d, pair, 2), pair)
            return jnp.where(place[d] >= 4, shifted(d, pair, 4), value)

        return complete_rows(get)

    def step_in_face(d, m, v):
        if m == 3:
            return jnp.where(g.xcol == NX - 1, g.lanes(v, NX - 1), g.lanes(v, -1))
        if m == 2:
            return g.lanes(v, -NX)
        if m == 1:
            return g.rows(v, -1)
        moved = g.rows(v, -depth)
        if d == 1:
            beyond = g.rows(v, depth - 1)
            return jnp.where(jnp.logical_and(g.zrow == 0, g.row >= depth), beyond, moved)
        return jnp.where(g.row >= depth, g.lanes(moved, -NX), moved)

    def over_face(d, s, own):
        def get(part, i, j):
            value, before = None, None
            for k, (m, h) in enumerate(LAYOUT[d][s]):
                if m == before:
                    continue
                x = step_in_face(d, m, own[part][i][j])
                value = x if value is None else jnp.where(place[d] >= k, x, value)
                before = m
            return value

        return complete_rows(get)

    def send_side(d):
        own = own_face(d)
        for s in range(len(LAYOUT[d])):
            n = sets.index((d, s))
            side = packed(d, s, lambda m, h, *c: load(m, *c, h), True)
            over = over_face(d, s, own)
            b = product(own, side, left_h=True)
            mask = open_mask(d, s)
            put("g", d, s, [
                [
                    [pick(mask, b[p][i][j], entry(b, over, i, j, p, False, False)) for j in range(3)]
                    for i in range(2)
                ]
                for p in range(2)
            ])
            for q, value in enumerate((own, side, over)):
                save(face_s, (n, q), value)
            save(b_s, (n,), b)

    def send_face(d):
        for s in range(len(LAYOUT[d])):
            put("x", d, s, [
                [
                    [pack(d, s, lambda m, h: load(m, p, i, j, h), False) for j in range(3)]
                    for i in range(2)
                ]
                for p in range(2)
            ])

    def pack_edges(d, n):
        r0 = offset("e", DIAGONALS.index((d, n)))
        if 2 not in (d, n):
            for c0 in range(0, 12, SUB):
                value = None
                for k in range(min(SUB, 12 - c0)):
                    v = load(d, *comps[c0 + k], halves - 1 if d == 0 else 0)
                    x = g.rows(v, k - depth if d == 0 else k - (depth - 1))
                    value = x if value is None else jnp.where(g.row >= k, x, value)
                out_s[r0 + c0 : r0 + c0 + SUB, :] = value
            return
        value = None
        for k in range(g.ygroups):
            v = dense_rows(d, n, comps[k])
            if k + g.ygroups < 12:
                w = dense_rows(d, n, comps[k + g.ygroups])
                step, mask = spare(d, n)
                v = jnp.where(mask, v, g.rows(w, step))
            x = g.lanes(v, NX * (k + (1 if d == 2 else 0)))
            value = x if value is None else jnp.where(g.lane >= NX * k, x, value)
        out_s[r0 : r0 + SUB, :] = value

    def spare(d, n):
        if (d, n) == (0, 2):
            return depth, g.row >= depth
        if (d, n) == (2, 0):
            return depth, g.row < depth
        return (-2, g.zrow >= 2) if d == 1 else (2, g.zrow < 2)

    def dense_rows(d, n, c):
        if 0 in (d, n):
            return load(d, *c, halves - 1 if d == 0 else 0)
        at = depth - 1 if d == 1 else 0
        step = -1 if d == 1 else 1
        v = load(d, *c, 0)
        for h in range(1, halves):
            v = jnp.where(g.zrow == at + step * h, g.rows(load(d, *c, h), step * h), v)
        return v

    def edge(d, n, h, part, i, j):
        c = part * 6 + i * 3 + j
        r = offset("e", DIAGONALS.index((d, n)))
        if 2 not in (d, n):
            v = in_s[r + c // SUB * SUB : r + c // SUB * SUB + SUB, :]
            k = c % SUB
            return g.rows(v, depth - 1 - k if d == 0 else SUB - depth - k)
        k, back = c % g.ygroups, c >= g.ygroups
        v = g.lanes(in_s[r : r + SUB, :], NX * ((0 if d == 2 else g.ygroups - 1) - k))
        step = -spare(d, n)[0] if back else 0
        if (d, n) == (0, 2):
            return g.rows(v, step - (SUB - depth))
        if (d, n) == (2, 0):
            return g.rows(v, step + SUB - depth)
        return g.rows(v, step + (1 - depth + h if d == 1 else depth - 1 - h))

    everything_in = pltpu.make_async_copy(hbm, u, load_sem)
    everything_in.wait()
    for d, n in DIAGONALS:
        pack_edges(d, n)
    for d in (1, 0):
        send_side(d)
        send_face(d)
    send_face(2)
    pl.semaphore_wait(barrier, expected)
    for copy in [edges[4], edges[0], opens[1], opens[0]]:
        copy.start()
    signal(met, (2, -1))

    @pl.when(last_t)
    def _():
        signal(met_t, (0, 1))

    @pl.when(last_z)
    def _():
        signal(met_z, (1, 1))

    @pl.when(rest_t)
    def _():
        edges[3].start()
        faces[0].start()

    @pl.when(rest_z)
    def _():
        edges[5].start()
        faces[1].start()

    @pl.when(jnp.logical_or(rest_z, last_t))
    def _():
        edges[2].start()

    send_side(2)
    faces[2].start()
    opens[2].start()

    seen, pending = set(), {}

    def add(m, c, h, value):
        key = (m, c, h)
        pending[key] = pending[key] + value if key in pending else value

    def flush():
        for (m, c, h), value in pending.items():
            r = ((m * 8 + c) * halves + h) * SUB
            if (m, c, h) in seen:
                acc[r : r + SUB, :] += value
            else:
                seen.add((m, c, h))
                acc[r : r + SUB, :] = value
        pending.clear()

    def forward(m, d, h, q):
        for c in range(8):
            if d == 3:
                add(m, c, h, jnp.where(g.xcol == 0, g.lanes(q[c], 1 - NX), g.lanes(q[c], 1)))
            elif d == 2:
                add(m, c, h, g.lanes(q[c], NX))
            elif d == 1:
                add(m, c, h, g.rows(q[c], 1))
            elif h + 1 < halves:
                moved = g.rows(q[c], depth)
                add(m, c, h, jnp.where(g.row >= depth, moved, 0.0))
                add(m, c, h + 1, jnp.where(g.row < depth, moved, 0.0))
            else:
                add(m, c, h, g.rows(q[c], depth))

    def masked(mask, a):
        return [[[pick(mask, 0.0, v) for v in line] for line in part] for part in a]

    def inner(mu, nu, h):
        own = matrix(lambda *c: load(mu, *c, h))
        side = matrix(lambda *c: load(nu, *c, h))
        a = product(
            matrix(lambda *c: rolled(nu, mu, h, *c)),
            matrix(lambda *c: rolled(mu, nu, h, *c)),
            right_h=True,
        )
        mask = None
        for d in (mu, nu):
            if not complete(d, h):
                mask = top(d) if mask is None else jnp.logical_or(mask, top(d))
        a = masked(mask, a)
        b = product(own, side, left_h=True)
        forward(mu, nu, h, projected(a, b, left_h=True))
        forward(nu, mu, h, projected(a, b, right_h=True))
        upper = projected(product(own, a), side, right_h=True)
        for c in range(8):
            add(mu, c, h, upper[c])
            add(nu, c, h, -upper[c])

    def corners(d, among):
        for s in range(len(LAYOUT[d])):
            mask = open_mask(d, s, among)
            if mask is None:
                continue
            n = sets.index((d, s))

            def corner(m, h, c):
                if m not in among or complete(m, h):
                    return None
                k = LAYOUT[m][0].index((d, 0 if m == 0 else h))
                return shifted(m, fetch(in_s, "x", m, 0, *c), last[m] - k)

            for c in comps:
                value = pack(d, s, lambda m, h: corner(m, h, c), True)
                face_s[(n, 2, *c)] = jnp.where(mask, value, face_s[(n, 2, *c)])

    def face_terms(d, closed):
        for s, spots in enumerate(LAYOUT[d]):
            n = sets.index((d, s))
            own, side, over = (kept(d, s, q) for q in range(3))
            a = product(fetched(in_s, "x", d, s), over, right_h=True)
            a = masked(open_mask(d, s, [m for m in range(3) if m not in closed]), a)
            b = matrix(lambda *c: b_s[(n, *c)])
            upper = projected(product(own, a), side, right_h=True)
            low = projected(a, b, left_h=True)
            mask = open_mask(d, s, closed)
            low = [pick(mask, 0.0, v) for v in low]
            for k, (m, h) in enumerate(spots):
                h = half(d, h, True)
                natural = lambda v: jnp.where(top(d), shifted(d, v, last[d] - k), 0.0)
                for c in range(8):
                    x = natural(upper[c])
                    add(d, c, h, x)
                    add(m, c, h, -x)
                forward(d, m, h, [natural(v) for v in low])
        flush()

    def prepare(d):
        for s in range(len(LAYOUT[d])):
            own = fetched(out_s, "x", d, s)
            mask = open_mask(d, s)
            if mask is not None:
                far = packed(
                    d, s,
                    lambda m, h, *c: None if complete(m, h if d else 1) else edge(d, m, h, *c),
                    False,
                )
                both = product(own, far, right_h=True)
                own = [
                    [[jnp.where(mask, both[p][i][j], own[p][i][j]) for j in range(3)] for i in range(3)]
                    for p in range(2)
                ]
            save(pre_s, (sets.index((d, s)),), own)

    def close(d):
        for s, spots in enumerate(LAYOUT[d]):
            n = sets.index((d, s))
            q = projected(
                matrix(lambda *c: pre_s[(n, *c)]), fetched(in_s, "g", d, s), right_h=True
            )
            for k, (m, h) in enumerate(spots):
                for c in range(8):
                    add(m, c, half(d, h, False), jnp.where(bottom(d), shifted(d, q[c], -k), 0.0))
        flush()

    for n, pair in enumerate(PLANES):
        if n == 2:
            pl.semaphore_wait(met, 1)

            @pl.when(rest_t)
            def _():
                edges[1].start()

        for h in range(halves):
            inner(*pair, h)
        flush()

    @pl.when(first_t)
    def _():
        pl.semaphore_wait(met_t, 1)
        for copy in (edges[3], edges[1], faces[0]):
            copy.start()

    @pl.when(first_z)
    def _():
        pl.semaphore_wait(met_z, 1)
        edges[5].start()
        faces[1].start()

    @pl.when(jnp.logical_and(first_z, more_t))
    def _():
        edges[2].start()

    faces[2].wait_recv()
    face_terms(2, ())
    corners(0, (2,))
    faces[0].wait_recv()
    face_terms(0, (2,))
    corners(1, (0, 2))
    faces[1].wait_recv()
    face_terms(1, (0, 2))
    all_edges.wait_recv()
    for d in (2, 0, 1):
        prepare(d)
    for d in (2, 0, 1):
        opens[d].wait_recv()
    for d in (2, 0, 1):
        close(d)
    everything.wait_send()


def expand(halves, acc, hbm, out, sem):
    for m in range(4):
        for h in range(halves):
            rows = [((m * 8 + c) * halves + h) * SUB for c in range(8)]
            f = [acc[r : r + SUB, :] * (COEFF * 0.5 if c < 6 else COEFF) for c, r in enumerate(rows)]

            def put(part, i, j, value):
                out[m, part, i, j, h * SUB : (h + 1) * SUB, :] = value

            for n, (i, j) in enumerate(((0, 1), (0, 2), (1, 2))):
                put(0, i, j, f[n])
                put(0, j, i, -f[n])
                put(1, i, j, f[3 + n])
                put(1, j, i, f[3 + n])
            for i in range(3):
                put(0, i, i, jnp.zeros((SUB, LANES), jnp.float32))
            put(1, 0, 0, f[6])
            put(1, 1, 1, f[7])
            put(1, 2, 2, -(f[6] + f[7]))
        for part in range(2):
            for i in range(3):
                pltpu.make_async_copy(out.at[m, part, i], hbm.at[m, part, i], sem).start()
    pltpu.make_async_copy(out, hbm, sem).wait()


def per_device(counts, links):
    time_len, depth, flat = links.shape[4:]
    sites = time_len * depth
    assert flat == LANES and (time_len, depth) == (4, 4)
    halves = sites // SUB
    vmem = lambda *s: pltpu.VMEM(s + (LANES,), jnp.float32)
    shape = links.shape[:4] + (sites, flat)
    terms = pl.pallas_call(
        functools.partial(force_terms, counts, depth, halves),
        out_shape=pltpu.VMEM((32 * sites, flat), jnp.float32),
        in_specs=[pl.BlockSpec(memory_space=pl.ANY)],
        out_specs=pl.BlockSpec(memory_space=pltpu.VMEM),
        scratch_shapes=[
            vmem(*shape[:-1]),
            vmem(TOTAL),
            vmem(TOTAL),
            vmem(5, 3, 2, 2, 3, SUB),
            vmem(5, 2, 3, 3, SUB),
            vmem(5, 2, 3, 3, SUB),
            pltpu.SemaphoreType.DMA,
            pltpu.SemaphoreType.DMA,
            pltpu.SemaphoreType.DMA((7,)),
            pltpu.SemaphoreType.REGULAR,
            pltpu.SemaphoreType.REGULAR,
            pltpu.SemaphoreType.REGULAR,
        ],
        compiler_params=pltpu.CompilerParams(collective_id=0, has_side_effects=True),
        name="force_terms",
    )(links.reshape(shape))
    out = pl.pallas_call(
        functools.partial(expand, halves),
        out_shape=jax.ShapeDtypeStruct(shape, jnp.float32),
        in_specs=[pl.BlockSpec(memory_space=pltpu.VMEM)],
        out_specs=pl.BlockSpec(memory_space=pl.ANY),
        scratch_shapes=[vmem(*shape[:-1]), pltpu.SemaphoreType.DMA],
        name="expand",
    )(pltpu.with_memory_space_constraint(terms, pltpu.VMEM))
    return out.reshape(links.shape)


def solution(mesh):
    assert mesh.axis_names == ("gx", "gz", "ta")
    counts = tuple(mesh.shape[a] for a in AXES)
    spec = P(None, None, None, None, "ta", "gz", "gx")
    return jax.shard_map(
        functools.partial(per_device, counts),
        mesh=mesh,
        in_specs=(spec,),
        out_specs=spec,
        check_vma=False,
    )
```

```python
import functools

import jax
import jax.numpy as jnp
from jax import lax
from jax.experimental import pallas as pl
from jax.experimental.pallas import tpu as pltpu
from jax.sharding import PartitionSpec as P

NX = 16
COEFF = -1.9
AXES = ("ta", "gz", "gx")
SUB, LANES = 8, 128


def others(d):
    return [m for m in range(4) if m != d]


class Lattice:
    def __init__(self, depth):
        self.depth = depth
        self.per = SUB // depth
        self.ygroups = LANES // NX
        self.row = lax.broadcasted_iota(jnp.int32, (SUB, LANES), 0)
        self.lane = lax.broadcasted_iota(jnp.int32, (SUB, LANES), 1)
        self.zrow = self.row % depth
        self.xcol = self.lane % NX

    def rows(self, value, shift):
        shift %= SUB
        return pltpu.roll(value, shift, 0) if shift else value

    def lanes(self, value, shift):
        shift %= LANES
        return pltpu.roll(value, shift, 1) if shift else value


def entry(left, right, i, j, part, left_h, right_h):
    total = None
    for k in range(3):
        li = (k, i) if left_h else (i, k)
        ri = (j, k) if right_h else (k, j)
        lr, lm = left[0][li[0]][li[1]], left[1][li[0]][li[1]]
        rr, rm = right[0][ri[0]][ri[1]], right[1][ri[0]][ri[1]]
        if part == 0:
            first, second = lr * rr, lm * rm
            minus = left_h == right_h
        elif left_h:
            first, second = lr * rm, lm * rr
            minus = True
        else:
            first, second = lm * rr, lr * rm
            minus = right_h
        value = first - second if minus else first + second
        total = value if total is None else total + value
    return total


def product(left, right, left_h=False, right_h=False):
    return [
        [[entry(left, right, i, j, part, left_h, right_h) for j in range(3)] for i in range(3)]
        for part in range(2)
    ]


def projected(left, right, left_h=False, right_h=False):
    get = lambda i, j, part: entry(left, right, i, j, part, left_h, right_h)
    pairs = ((0, 1), (0, 2), (1, 2))
    real = [get(i, j, 0) - get(j, i, 0) for i, j in pairs]
    imag = [get(i, j, 1) + get(j, i, 1) for i, j in pairs]
    diag = [get(i, i, 1) for i in range(3)]
    third = (diag[0] + diag[1] + diag[2]) * (1.0 / 3.0)
    return real + imag + [diag[0] - third, diag[1] - third]


def third_row(real, imag):
    rows_r, rows_i = [], []
    for column in range(3):
        n, l = (column + 1) % 3, (column + 2) % 3
        rows_r.append(
            real[0][n] * real[1][l]
            - imag[0][n] * imag[1][l]
            - real[0][l] * real[1][n]
            + imag[0][l] * imag[1][n]
        )
        rows_i.append(
            real[0][l] * imag[1][n]
            + imag[0][l] * real[1][n]
            - real[0][n] * imag[1][l]
            - imag[0][n] * real[1][l]
        )
    return rows_r, rows_i


PLANES = ((0, 1), (0, 2), (0, 3), (1, 2), (1, 3), (2, 3))
DIAGONALS = ((0, 2), (2, 0), (0, 1), (1, 0), (1, 2), (2, 1))
LAYOUT = (
    (((1, 0), (2, 0)), ((3, 0),)),
    (((0, 0), (0, 1), (2, 0), (2, 1)), ((3, 0), (3, 1))),
    (((0, 0), (0, 1), (1, 0), (1, 1), (3, 0), (3, 1)),),
)
ROWS = (144, 144, 96)
EDGES = (8, 8, 16, 16, 8, 8)


def offset(kind, d):
    if kind == "e":
        return 2 * sum(ROWS) + sum(EDGES[:d])
    return (sum(ROWS) if kind == "g" else 0) + sum(ROWS[:d])


TOTAL = offset("e", len(DIAGONALS))


def force_terms(
    counts, depth, halves, hbm, acc, u, out_s, in_s, face_s, b_s, pre_s, load_sem, send, recv, met, met_t, met_z,
):
    g = Lattice(depth)
    me = [lax.axis_index(a) for a in AXES]
    comps = [(part, i, j) for part in range(2) for i in range(2) for j in range(3)]
    last = (g.per - 1, depth - 1, g.ygroups - 1)
    place = (g.row // depth, g.zrow, g.lane // NX)

    def device(*steps):
        where = list(me)
        for i, step in steps:
            where[i] = lax.rem(me[i] + (step + counts[i]), counts[i])
        by = dict(zip(AXES, where))
        return (by["gx"], by["gz"], by["ta"])

    loads = [
        pltpu.make_async_copy(hbm.at[m, part, i], u.at[m, part, i], load_sem)
        for m in range(4)
        for part in range(2)
        for i in range(3)
    ]
    for copy in loads:
        copy.start()
    barrier = pltpu.get_barrier_semaphore()
    first_t, last_t = me[0] == 0, me[0] == counts[0] - 1
    more_t, rest_t = jnp.logical_not(last_t), jnp.logical_not(first_t)
    middle = counts[1] // 2
    first_z = jnp.logical_or(me[1] == 0, jnp.logical_and(me[1] == middle, rest_t))
    last_z = jnp.logical_or(
        me[1] == counts[1] - 1, jnp.logical_and(me[1] == middle - 1, rest_t)
    )
    silent = jnp.logical_or(
        jnp.logical_and(me[1] == counts[1] - 1, rest_t),
        jnp.logical_and(me[1] == middle - 1, me[0] > 1),
    )
    more_z, rest_z = jnp.logical_not(last_z), jnp.logical_not(first_z)
    one = lambda flag: jnp.where(flag, 1, 0)

    def signal(semaphore, *steps):
        pl.semaphore_signal(
            semaphore, inc=1, device_id=device(*steps), device_id_type=pl.DeviceIdType.MESH
        )

    for steps in (((1, -1),), ((2, 1), (1, -1)), ((0, -1), (2, 1)), ((0, -1),), ((2, 1),), ((2, -1),)):
        signal(barrier, *steps)

    @pl.when(more_z)
    def _():
        signal(barrier, (1, 1))
        signal(barrier, (1, 1), (2, -1))

    @pl.when(jnp.logical_not(silent))
    def _():
        signal(barrier, (1, 1), (0, -1))

    @pl.when(more_t)
    def _():
        signal(barrier, (0, 1))
        signal(barrier, (0, 1), (1, -1))

    expected = 11 - 2 * one(first_t) - 2 * one(first_z) - one(jnp.logical_and(first_z, more_t))

    def remote(start, rows, slot, where):
        span = slice(start, start + rows)
        return pltpu.make_async_remote_copy(
            src_ref=out_s.at[span], dst_ref=in_s.at[span], send_sem=send, recv_sem=recv.at[slot],
            device_id=where, device_id_type=pl.DeviceIdType.MESH,
        )

    faces = [remote(offset("x", d), ROWS[d], d, device((d, -1))) for d in range(3)]
    opens = [remote(offset("g", d), ROWS[d], 3 + d, device((d, 1))) for d in range(3)]
    edges = [
        remote(offset("e", k), EDGES[k], 6, device((d, 1), (n, -1)))
        for k, (d, n) in enumerate(DIAGONALS)
    ]
    all_edges = remote(offset("e", 0), sum(EDGES), 6, device((1, 1)))
    everything = remote(0, TOTAL, 0, device((1, 1)))

    def load(m, part, i, j, h):
        return u[m, part, i, j, h * SUB : (h + 1) * SUB, :]

    def shifted(d, value, steps):
        if d == 0:
            return g.rows(value, depth * steps)
        return g.rows(value, steps) if d == 1 else g.lanes(value, NX * steps)

    def half(d, h, top):
        return (halves - 1 if top else 0) if d == 0 else h

    def complete(d, h):
        return d == 3 or (d == 0 and h + 1 < halves)

    def top(d, h=1):
        if d == 0:
            return g.row >= SUB - depth
        return g.zrow == depth - 1 if d == 1 else g.lane >= LANES - NX

    def bottom(d):
        return (g.row < depth, g.zrow == 0, g.lane < NX)[d]

    def open_mask(d, s, among=(0, 1, 2)):
        mask = None
        for k, (m, h) in enumerate(LAYOUT[d][s]):
            if m in among and not complete(m, h if d else 1):
                here = jnp.logical_and(place[d] == k, top(m))
                mask = here if mask is None else jnp.logical_or(mask, here)
        return mask

    def pick(mask, yes, no):
        return no if mask is None else jnp.where(mask, yes, no)

    def pack(d, s, get, up):
        value = None
        for k, (m, h) in enumerate(LAYOUT[d][s]):
            x = get(m, half(d, h, up))
            if x is None:
                continue
            x = shifted(d, x, k - (last[d] if up else 0))
            value = x if value is None else jnp.where(place[d] >= k, x, value)
        return value

    def complete_rows(get):
        real = [[get(0, i, j) for j in range(3)] for i in range(2)]
        imag = [[get(1, i, j) for j in range(3)] for i in range(2)]
        third_r, third_i = third_row(real, imag)
        return [real + [third_r], imag + [third_i]]

    def packed(d, s, get, up):
        return complete_rows(
            lambda part, i, j: pack(d, s, lambda m, h: get(m, h, part, i, j), up)
        )

    def put(kind, d, s, value):
        r = offset(kind, d)
        used = len(LAYOUT[d][s])
        for n, (part, i, j) in enumerate(comps[: 6 if s else 12]):
            v = value[part][i][j]
            if s:
                v = jnp.where(place[d] < used, v, shifted(d, value[1][i][j], used))
            at = r + (96 if s else 0) + n * SUB
            out_s[at : at + SUB, :] = v

    def fetch(ref, kind, d, s, part, i, j):
        n = part * 6 + i * 3 + j
        at = offset(kind, d) + n * SUB
        if not s:
            return ref[at : at + SUB, :]
        at += 96 - part * 6 * SUB
        v = ref[at : at + SUB, :]
        return shifted(d, v, -len(LAYOUT[d][s])) if part else v

    def fetched(ref, kind, d, s):
        return complete_rows(lambda part, i, j: fetch(ref, kind, d, s, part, i, j))

    def rolled(m, d, h, part, i, j):
        v = load(m, part, i, j, h)
        if d == 3:
            return jnp.where(g.xcol == NX - 1, g.lanes(v, NX - 1), g.lanes(v, -1))
        if d == 2:
            return g.lanes(v, -NX)
        if d == 1:
            return g.rows(v, -1)
        if h + 1 < halves:
            beyond = g.rows(load(m, part, i, j, h + 1), -depth)
            return jnp.where(g.row >= SUB - depth, beyond, g.rows(v, -depth))
        return g.rows(v, -depth)

    def matrix(get):
        return [[[get(part, i, j) for j in range(3)] for i in range(3)] for part in range(2)]

    def save(ref, index, value):
        for part in range(2):
            for i in range(ref.shape[-4]):
                for j in range(3):
                    ref[(*index, part, i, j)] = value[part][i][j]

    sets = [(d, s) for d in range(3) for s in range(len(LAYOUT[d]))]

    def kept(d, s, q):
        n = sets.index((d, s))
        return complete_rows(lambda part, i, j: face_s[n, q, part, i, j])

    def own_face(d):
        def get(part, i, j):
            if d != 2:
                return pack(d, 0, lambda m, h: load(d, part, i, j, h), True)
            pair = [shifted(d, load(d, part, i, j, h), h - last[d]) for h in range(halves)]
            pair = jnp.where(place[d] >= 1, pair[1], pair[0])
            value = jnp.where(place[d] >= 2, shifted(d, pair, 2), pair)
            return jnp.where(place[d] >= 4, shifted(d, pair, 4), value)

        return complete_rows(get)

    def step_in_face(d, m, v):
        if m == 3:
            return jnp.where(g.xcol == NX - 1, g.lanes(v, NX - 1), g.lanes(v, -1))
        if m == 2:
            return g.lanes(v, -NX)
        if m == 1:
            return g.rows(v, -1)
        moved = g.rows(v, -depth)
        if d == 1:
            beyond = g.rows(v, depth - 1)
            return jnp.where(jnp.logical_and(g.zrow == 0, g.row >= depth), beyond, moved)
        return jnp.where(g.row >= depth, g.lanes(moved, -NX), moved)

    def over_face(d, s, own):
        def get(part, i, j):
            value, before = None, None
            for k, (m, h) in enumerate(LAYOUT[d][s]):
                if m == before:
                    continue
                x = step_in_face(d, m, own[part][i][j])
                value = x if value is None else jnp.where(place[d] >= k, x, value)
                before = m
            return value

        return complete_rows(get)

    def send_side(d):
        own = own_face(d)
        for s in range(len(LAYOUT[d])):
            n = sets.index((d, s))
            side = packed(d, s, lambda m, h, *c: load(m, *c, h), True)
            over = over_face(d, s, own)
            b = product(own, side, left_h=True)
            mask = open_mask(d, s)
            put("g", d, s, [
                [
                    [pick(mask, b[p][i][j], entry(b, over, i, j, p, False, False)) for j in range(3)]
                    for i in range(2)
                ]
                for p in range(2)
            ])
            for q, value in enumerate((own, side, over)):
                save(face_s, (n, q), value)
            save(b_s, (n,), b)

    def send_face(d):
        for s in range(len(LAYOUT[d])):
            put("x", d, s, [
                [
                    [pack(d, s, lambda m, h: load(m, p, i, j, h), False) for j in range(3)]
                    for i in range(2)
                ]
                for p in range(2)
            ])

    def pack_edges(d, n):
        r0 = offset("e", DIAGONALS.index((d, n)))
        if 2 not in (d, n):
            for c0 in range(0, 12, SUB):
                value = None
                for k in range(min(SUB, 12 - c0)):
                    v = load(d, *comps[c0 + k], halves - 1 if d == 0 else 0)
                    x = g.rows(v, k - depth if d == 0 else k - (depth - 1))
                    value = x if value is None else jnp.where(g.row >= k, x, value)
                out_s[r0 + c0 : r0 + c0 + SUB, :] = value
            return
        value = None
        for k in range(g.ygroups):
            v = dense_rows(d, n, comps[k])
            if k + g.ygroups < 12:
                w = dense_rows(d, n, comps[k + g.ygroups])
                step, mask = spare(d, n)
                v = jnp.where(mask, v, g.rows(w, step))
            x = g.lanes(v, NX * (k + (1 if d == 2 else 0)))
            value = x if value is None else jnp.where(g.lane >= NX * k, x, value)
        out_s[r0 : r0 + SUB, :] = value

    def spare(d, n):
        if (d, n) == (0, 2):
            return depth, g.row >= depth
        if (d, n) == (2, 0):
            return depth, g.row < depth
        return (-2, g.zrow >= 2) if d == 1 else (2, g.zrow < 2)

    def dense_rows(d, n, c):
        if 0 in (d, n):
            return load(d, *c, halves - 1 if d == 0 else 0)
        at = depth - 1 if d == 1 else 0
        step = -1 if d == 1 else 1
        v = load(d, *c, 0)
        for h in range(1, halves):
            v = jnp.where(g.zrow == at + step * h, g.rows(load(d, *c, h), step * h), v)
        return v

    def edge(d, n, h, part, i, j):
        c = part * 6 + i * 3 + j
        r = offset("e", DIAGONALS.index((d, n)))
        if 2 not in (d, n):
            v = in_s[r + c // SUB * SUB : r + c // SUB * SUB + SUB, :]
            k = c % SUB
            return g.rows(v, depth - 1 - k if d == 0 else SUB - depth - k)
        k, back = c % g.ygroups, c >= g.ygroups
        v = g.lanes(in_s[r : r + SUB, :], NX * ((0 if d == 2 else g.ygroups - 1) - k))
        step = -spare(d, n)[0] if back else 0
        if (d, n) == (0, 2):
            return g.rows(v, step - (SUB - depth))
        if (d, n) == (2, 0):
            return g.rows(v, step + SUB - depth)
        return g.rows(v, step + (1 - depth + h if d == 1 else depth - 1 - h))

    everything_in = pltpu.make_async_copy(hbm, u, load_sem)
    everything_in.wait()
    for d, n in DIAGONALS:
        pack_edges(d, n)
    for d in (1, 0):
        send_side(d)
        send_face(d)
    send_face(2)
    pl.semaphore_wait(barrier, expected)
    signal(met, (2, -1))

    @pl.when(last_t)
    def _():
        signal(met_t, (0, 1))

    @pl.when(last_z)
    def _():
        signal(met_z, (1, 1))

    @pl.when(jnp.logical_or(rest_z, last_t))
    def _():
        edges[2].start()

    for copy in (edges[4], edges[0]):
        copy.start()

    @pl.when(rest_t)
    def _():
        edges[3].start()
        faces[0].start()

    @pl.when(rest_z)
    def _():
        edges[5].start()
        faces[1].start()

    for copy in (opens[1], opens[0]):
        copy.start()
    send_side(2)
    faces[2].start()
    opens[2].start()

    seen, pending = set(), {}

    def add(m, c, h, value):
        key = (m, c, h)
        pending[key] = pending[key] + value if key in pending else value

    def flush():
        for (m, c, h), value in pending.items():
            r = ((m * 8 + c) * halves + h) * SUB
            if (m, c, h) in seen:
                acc[r : r + SUB, :] += value
            else:
                seen.add((m, c, h))
                acc[r : r + SUB, :] = value
        pending.clear()

    def forward(m, d, h, q):
        for c in range(8):
            if d == 3:
                add(m, c, h, jnp.where(g.xcol == 0, g.lanes(q[c], 1 - NX), g.lanes(q[c], 1)))
            elif d == 2:
                add(m, c, h, g.lanes(q[c], NX))
            elif d == 1:
                add(m, c, h, g.rows(q[c], 1))
            elif h + 1 < halves:
                moved = g.rows(q[c], depth)
                add(m, c, h, jnp.where(g.row >= depth, moved, 0.0))
                add(m, c, h + 1, jnp.where(g.row < depth, moved, 0.0))
            else:
                add(m, c, h, g.rows(q[c], depth))

    def masked(mask, a):
        return [[[pick(mask, 0.0, v) for v in line] for line in part] for part in a]

    def inner(mu, nu, h):
        own = matrix(lambda *c: load(mu, *c, h))
        side = matrix(lambda *c: load(nu, *c, h))
        a = product(
            matrix(lambda *c: rolled(nu, mu, h, *c)),
            matrix(lambda *c: rolled(mu, nu, h, *c)),
            right_h=True,
        )
        mask = None
        for d in (mu, nu):
            if not complete(d, h):
                mask = top(d) if mask is None else jnp.logical_or(mask, top(d))
        a = masked(mask, a)
        b = product(own, side, left_h=True)
        forward(mu, nu, h, projected(a, b, left_h=True))
        forward(nu, mu, h, projected(a, b, right_h=True))
        upper = projected(product(own, a), side, right_h=True)
        for c in range(8):
            add(mu, c, h, upper[c])
            add(nu, c, h, -upper[c])

    def corners(d, among):
        for s in range(len(LAYOUT[d])):
            mask = open_mask(d, s, among)
            if mask is None:
                continue
            n = sets.index((d, s))

            def corner(m, h, c):
                if m not in among or complete(m, h):
                    return None
                k = LAYOUT[m][0].index((d, 0 if m == 0 else h))
                return shifted(m, fetch(in_s, "x", m, 0, *c), last[m] - k)

            for c in comps:
                value = pack(d, s, lambda m, h: corner(m, h, c), True)
                face_s[(n, 2, *c)] = jnp.where(mask, value, face_s[(n, 2, *c)])

    def face_terms(d, closed):
        for s, spots in enumerate(LAYOUT[d]):
            n = sets.index((d, s))
            own, side, over = (kept(d, s, q) for q in range(3))
            a = product(fetched(in_s, "x", d, s), over, right_h=True)
            a = masked(open_mask(d, s, [m for m in range(3) if m not in closed]), a)
            b = matrix(lambda *c: b_s[(n, *c)])
            upper = projected(product(own, a), side, right_h=True)
            low = projected(a, b, left_h=True)
            mask = open_mask(d, s, closed)
            low = [pick(mask, 0.0, v) for v in low]
            for k, (m, h) in enumerate(spots):
                h = half(d, h, True)
                natural = lambda v: jnp.where(top(d), shifted(d, v, last[d] - k), 0.0)
                for c in range(8):
                    x = natural(upper[c])
                    add(d, c, h, x)
                    add(m, c, h, -x)
                forward(d, m, h, [natural(v) for v in low])
        flush()

    def prepare(d):
        for s in range(len(LAYOUT[d])):
            own = fetched(out_s, "x", d, s)
            mask = open_mask(d, s)
            if mask is not None:
                far = packed(
                    d, s,
                    lambda m, h, *c: None if complete(m, h if d else 1) else edge(d, m, h, *c),
                    False,
                )
                both = product(own, far, right_h=True)
                own = [
                    [[jnp.where(mask, both[p][i][j], own[p][i][j]) for j in range(3)] for i in range(3)]
                    for p in range(2)
                ]
            save(pre_s, (sets.index((d, s)),), own)

    def close(d):
        for s, spots in enumerate(LAYOUT[d]):
            n = sets.index((d, s))
            q = projected(
                matrix(lambda *c: pre_s[(n, *c)]), fetched(in_s, "g", d, s), right_h=True
            )
            for k, (m, h) in enumerate(spots):
                for c in range(8):
                    add(m, c, half(d, h, False), jnp.where(bottom(d), shifted(d, q[c], -k), 0.0))
        flush()

    for n, pair in enumerate(PLANES):
        if n == 2:
            pl.semaphore_wait(met, 1)

            @pl.when(rest_t)
            def _():
                edges[1].start()

        for h in range(halves):
            inner(*pair, h)
        flush()

    @pl.when(first_t)
    def _():
        pl.semaphore_wait(met_t, 1)
        for copy in (edges[3], edges[1], faces[0]):
            copy.start()

    @pl.when(first_z)
    def _():
        pl.semaphore_wait(met_z, 1)
        edges[5].start()
        faces[1].start()

    @pl.when(jnp.logical_and(first_z, more_t))
    def _():
        edges[2].start()

    faces[2].wait_recv()
    face_terms(2, ())
    corners(0, (2,))
    faces[0].wait_recv()
    face_terms(0, (2,))
    corners(1, (0, 2))
    faces[1].wait_recv()
    face_terms(1, (0, 2))
    all_edges.wait_recv()
    for d in (2, 0, 1):
        prepare(d)
    for d in (2, 0, 1):
        opens[d].wait_recv()
    for d in (2, 0, 1):
        close(d)
    everything.wait_send()


def expand(halves, acc, hbm, out, sem):
    for m in range(4):
        for h in range(halves):
            rows = [((m * 8 + c) * halves + h) * SUB for c in range(8)]
            f = [acc[r : r + SUB, :] * (COEFF * 0.5 if c < 6 else COEFF) for c, r in enumerate(rows)]

            def put(part, i, j, value):
                out[m, part, i, j, h * SUB : (h + 1) * SUB, :] = value

            for n, (i, j) in enumerate(((0, 1), (0, 2), (1, 2))):
                put(0, i, j, f[n])
                put(0, j, i, -f[n])
                put(1, i, j, f[3 + n])
                put(1, j, i, f[3 + n])
            for i in range(3):
                put(0, i, i, jnp.zeros((SUB, LANES), jnp.float32))
            put(1, 0, 0, f[6])
            put(1, 1, 1, f[7])
            put(1, 2, 2, -(f[6] + f[7]))
        for part in range(2):
            for i in range(3):
                pltpu.make_async_copy(out.at[m, part, i], hbm.at[m, part, i], sem).start()
    pltpu.make_async_copy(out, hbm, sem).wait()


def per_device(counts, links):
    time_len, depth, flat = links.shape[4:]
    sites = time_len * depth
    assert flat == LANES and (time_len, depth) == (4, 4)
    halves = sites // SUB
    vmem = lambda *s: pltpu.VMEM(s + (LANES,), jnp.float32)
    shape = links.shape[:4] + (sites, flat)
    terms = pl.pallas_call(
        functools.partial(force_terms, counts, depth, halves),
        out_shape=pltpu.VMEM((32 * sites, flat), jnp.float32),
        in_specs=[pl.BlockSpec(memory_space=pl.ANY)],
        out_specs=pl.BlockSpec(memory_space=pltpu.VMEM),
        scratch_shapes=[
            vmem(*shape[:-1]),
            vmem(TOTAL),
            vmem(TOTAL),
            vmem(5, 3, 2, 2, 3, SUB),
            vmem(5, 2, 3, 3, SUB),
            vmem(5, 2, 3, 3, SUB),
            pltpu.SemaphoreType.DMA,
            pltpu.SemaphoreType.DMA,
            pltpu.SemaphoreType.DMA((7,)),
            pltpu.SemaphoreType.REGULAR,
            pltpu.SemaphoreType.REGULAR,
            pltpu.SemaphoreType.REGULAR,
        ],
        compiler_params=pltpu.CompilerParams(collective_id=0, has_side_effects=True),
        name="force_terms",
    )(links.reshape(shape))
    out = pl.pallas_call(
        functools.partial(expand, halves),
        out_shape=jax.ShapeDtypeStruct(shape, jnp.float32),
        in_specs=[pl.BlockSpec(memory_space=pltpu.VMEM)],
        out_specs=pl.BlockSpec(memory_space=pl.ANY),
        scratch_shapes=[vmem(*shape[:-1]), pltpu.SemaphoreType.DMA],
        name="expand",
    )(pltpu.with_memory_space_constraint(terms, pltpu.VMEM))
    return out.reshape(links.shape)


def solution(mesh):
    assert mesh.axis_names == ("gx", "gz", "ta")
    counts = tuple(mesh.shape[a] for a in AXES)
    spec = P(None, None, None, None, "ta", "gz", "gx")
    return jax.shard_map(
        functools.partial(per_device, counts),
        mesh=mesh,
        in_specs=(spec,),
        out_specs=spec,
        check_vma=False,
    )
```

```python
import functools

import jax
import jax.numpy as jnp
from jax import lax
from jax.experimental import pallas as pl
from jax.experimental.pallas import tpu as pltpu
from jax.sharding import PartitionSpec as P

NX = 16
COEFF = -1.9
AXES = ("ta", "gz", "gx")
SUB, LANES = 8, 128


def others(d):
    return [m for m in range(4) if m != d]


class Lattice:
    def __init__(self, depth):
        self.depth = depth
        self.per = SUB // depth
        self.ygroups = LANES // NX
        self.row = lax.broadcasted_iota(jnp.int32, (SUB, LANES), 0)
        self.lane = lax.broadcasted_iota(jnp.int32, (SUB, LANES), 1)
        self.zrow = self.row % depth
        self.xcol = self.lane % NX

    def rows(self, value, shift):
        shift %= SUB
        return pltpu.roll(value, shift, 0) if shift else value

    def lanes(self, value, shift):
        shift %= LANES
        return pltpu.roll(value, shift, 1) if shift else value


def entry(left, right, i, j, part, left_h, right_h):
    total = None
    for k in range(3):
        li = (k, i) if left_h else (i, k)
        ri = (j, k) if right_h else (k, j)
        lr, lm = left[0][li[0]][li[1]], left[1][li[0]][li[1]]
        rr, rm = right[0][ri[0]][ri[1]], right[1][ri[0]][ri[1]]
        if part == 0:
            first, second = lr * rr, lm * rm
            minus = left_h == right_h
        elif left_h:
            first, second = lr * rm, lm * rr
            minus = True
        else:
            first, second = lm * rr, lr * rm
            minus = right_h
        value = first - second if minus else first + second
        total = value if total is None else total + value
    return total


def product(left, right, left_h=False, right_h=False):
    return [
        [[entry(left, right, i, j, part, left_h, right_h) for j in range(3)] for i in range(3)]
        for part in range(2)
    ]


def projected(left, right, left_h=False, right_h=False):
    get = lambda i, j, part: entry(left, right, i, j, part, left_h, right_h)
    pairs = ((0, 1), (0, 2), (1, 2))
    real = [get(i, j, 0) - get(j, i, 0) for i, j in pairs]
    imag = [get(i, j, 1) + get(j, i, 1) for i, j in pairs]
    diag = [get(i, i, 1) for i in range(3)]
    third = (diag[0] + diag[1] + diag[2]) * (1.0 / 3.0)
    return real + imag + [diag[0] - third, diag[1] - third]


def third_row(real, imag):
    rows_r, rows_i = [], []
    for column in range(3):
        n, l = (column + 1) % 3, (column + 2) % 3
        rows_r.append(
            real[0][n] * real[1][l]
            - imag[0][n] * imag[1][l]
            - real[0][l] * real[1][n]
            + imag[0][l] * imag[1][n]
        )
        rows_i.append(
            real[0][l] * imag[1][n]
            + imag[0][l] * real[1][n]
            - real[0][n] * imag[1][l]
            - imag[0][n] * real[1][l]
        )
    return rows_r, rows_i


PLANES = ((0, 1), (0, 2), (0, 3), (1, 2), (1, 3), (2, 3))
DIAGONALS = ((0, 2), (2, 0), (0, 1), (1, 0), (1, 2), (2, 1))
LAYOUT = (
    (((1, 0), (2, 0)), ((3, 0),)),
    (((0, 0), (0, 1), (2, 0), (2, 1)), ((3, 0), (3, 1))),
    (((0, 0), (0, 1), (1, 0), (1, 1), (3, 0), (3, 1)),),
)
ROWS = (144, 144, 96)
EDGES = (8, 8, 16, 16, 8, 8)


def offset(kind, d):
    if kind == "e":
        return 2 * sum(ROWS) + sum(EDGES[:d])
    return (sum(ROWS) if kind == "g" else 0) + sum(ROWS[:d])


TOTAL = offset("e", len(DIAGONALS))


def force_terms(
    counts, depth, halves, hbm, acc, u, out_s, in_s, face_s, b_s, pre_s, load_sem, send, recv, met, met_t, met_z,
):
    g = Lattice(depth)
    me = [lax.axis_index(a) for a in AXES]
    comps = [(part, i, j) for part in range(2) for i in range(2) for j in range(3)]
    last = (g.per - 1, depth - 1, g.ygroups - 1)
    place = (g.row // depth, g.zrow, g.lane // NX)

    def device(*steps):
        where = list(me)
        for i, step in steps:
            where[i] = lax.rem(me[i] + (step + counts[i]), counts[i])
        by = dict(zip(AXES, where))
        return (by["gx"], by["gz"], by["ta"])

    loads = [
        pltpu.make_async_copy(hbm.at[m, part, i], u.at[m, part, i], load_sem)
        for m in range(4)
        for part in range(2)
        for i in range(3)
    ]
    for copy in loads:
        copy.start()
    barrier = pltpu.get_barrier_semaphore()
    first_t, last_t = me[0] == 0, me[0] == counts[0] - 1
    more_t, rest_t = jnp.logical_not(last_t), jnp.logical_not(first_t)
    middle = counts[1] // 2
    first_z = jnp.logical_or(me[1] == 0, jnp.logical_and(me[1] == middle, last_t))
    last_z = jnp.logical_or(
        me[1] == counts[1] - 1, jnp.logical_and(me[1] == middle - 1, last_t)
    )
    silent = jnp.logical_and(me[1] == counts[1] - 1, rest_t)
    more_z, rest_z = jnp.logical_not(last_z), jnp.logical_not(first_z)
    one = lambda flag: jnp.where(flag, 1, 0)

    def signal(semaphore, *steps):
        pl.semaphore_signal(
            semaphore, inc=1, device_id=device(*steps), device_id_type=pl.DeviceIdType.MESH
        )

    for steps in (((1, -1),), ((2, 1), (1, -1)), ((0, -1), (2, 1)), ((0, -1),), ((2, 1),), ((2, -1),)):
        signal(barrier, *steps)

    @pl.when(more_z)
    def _():
        signal(barrier, (1, 1))
        signal(barrier, (1, 1), (2, -1))

    @pl.when(jnp.logical_not(silent))
    def _():
        signal(barrier, (1, 1), (0, -1))

    @pl.when(more_t)
    def _():
        signal(barrier, (0, 1))
        signal(barrier, (0, 1), (1, -1))

    expected = 11 - 2 * one(first_t) - 2 * one(first_z) - one(jnp.logical_and(first_z, more_t))

    def remote(start, rows, slot, where):
        span = slice(start, start + rows)
        return pltpu.make_async_remote_copy(
            src_ref=out_s.at[span], dst_ref=in_s.at[span], send_sem=send, recv_sem=recv.at[slot],
            device_id=where, device_id_type=pl.DeviceIdType.MESH,
        )

    faces = [remote(offset("x", d), ROWS[d], d, device((d, -1))) for d in range(3)]
    opens = [remote(offset("g", d), ROWS[d], 3 + d, device((d, 1))) for d in range(3)]
    edges = [
        remote(offset("e", k), EDGES[k], 6, device((d, 1), (n, -1)))
        for k, (d, n) in enumerate(DIAGONALS)
    ]
    all_edges = remote(offset("e", 0), sum(EDGES), 6, device((1, 1)))
    everything = remote(0, TOTAL, 0, device((1, 1)))

    def load(m, part, i, j, h):
        return u[m, part, i, j, h * SUB : (h + 1) * SUB, :]

    def shifted(d, value, steps):
        if d == 0:
            return g.rows(value, depth * steps)
        return g.rows(value, steps) if d == 1 else g.lanes(value, NX * steps)

    def half(d, h, top):
        return (halves - 1 if top else 0) if d == 0 else h

    def complete(d, h):
        return d == 3 or (d == 0 and h + 1 < halves)

    def top(d, h=1):
        if d == 0:
            return g.row >= SUB - depth
        return g.zrow == depth - 1 if d == 1 else g.lane >= LANES - NX

    def bottom(d):
        return (g.row < depth, g.zrow == 0, g.lane < NX)[d]

    def open_mask(d, s, among=(0, 1, 2)):
        mask = None
        for k, (m, h) in enumerate(LAYOUT[d][s]):
            if m in among and not complete(m, h if d else 1):
                here = jnp.logical_and(place[d] == k, top(m))
                mask = here if mask is None else jnp.logical_or(mask, here)
        return mask

    def pick(mask, yes, no):
        return no if mask is None else jnp.where(mask, yes, no)

    def pack(d, s, get, up):
        value = None
        for k, (m, h) in enumerate(LAYOUT[d][s]):
            x = get(m, half(d, h, up))
            if x is None:
                continue
            x = shifted(d, x, k - (last[d] if up else 0))
            value = x if value is None else jnp.where(place[d] >= k, x, value)
        return value

    def complete_rows(get):
        real = [[get(0, i, j) for j in range(3)] for i in range(2)]
        imag = [[get(1, i, j) for j in range(3)] for i in range(2)]
        third_r, third_i = third_row(real, imag)
        return [real + [third_r], imag + [third_i]]

    def packed(d, s, get, up):
        return complete_rows(
            lambda part, i, j: pack(d, s, lambda m, h: get(m, h, part, i, j), up)
        )

    def put(kind, d, s, value):
        r = offset(kind, d)
        used = len(LAYOUT[d][s])
        for n, (part, i, j) in enumerate(comps[: 6 if s else 12]):
            v = value[part][i][j]
            if s:
                v = jnp.where(place[d] < used, v, shifted(d, value[1][i][j], used))
            at = r + (96 if s else 0) + n * SUB
            out_s[at : at + SUB, :] = v

    def fetch(ref, kind, d, s, part, i, j):
        n = part * 6 + i * 3 + j
        at = offset(kind, d) + n * SUB
        if not s:
            return ref[at : at + SUB, :]
        at += 96 - part * 6 * SUB
        v = ref[at : at + SUB, :]
        return shifted(d, v, -len(LAYOUT[d][s])) if part else v

    def fetched(ref, kind, d, s):
        return complete_rows(lambda part, i, j: fetch(ref, kind, d, s, part, i, j))

    def rolled(m, d, h, part, i, j):
        v = load(m, part, i, j, h)
        if d == 3:
            return jnp.where(g.xcol == NX - 1, g.lanes(v, NX - 1), g.lanes(v, -1))
        if d == 2:
            return g.lanes(v, -NX)
        if d == 1:
            return g.rows(v, -1)
        if h + 1 < halves:
            beyond = g.rows(load(m, part, i, j, h + 1), -depth)
            return jnp.where(g.row >= SUB - depth, beyond, g.rows(v, -depth))
        return g.rows(v, -depth)

    def matrix(get):
        return [[[get(part, i, j) for j in range(3)] for i in range(3)] for part in range(2)]

    def save(ref, index, value):
        for part in range(2):
            for i in range(ref.shape[-4]):
                for j in range(3):
                    ref[(*index, part, i, j)] = value[part][i][j]

    sets = [(d, s) for d in range(3) for s in range(len(LAYOUT[d]))]

    def kept(d, s, q):
        n = sets.index((d, s))
        return complete_rows(lambda part, i, j: face_s[n, q, part, i, j])

    def own_face(d):
        def get(part, i, j):
            if d != 2:
                return pack(d, 0, lambda m, h: load(d, part, i, j, h), True)
            pair = [shifted(d, load(d, part, i, j, h), h - last[d]) for h in range(halves)]
            pair = jnp.where(place[d] >= 1, pair[1], pair[0])
            value = jnp.where(place[d] >= 2, shifted(d, pair, 2), pair)
            return jnp.where(place[d] >= 4, shifted(d, pair, 4), value)

        return complete_rows(get)

    def step_in_face(d, m, v):
        if m == 3:
            return jnp.where(g.xcol == NX - 1, g.lanes(v, NX - 1), g.lanes(v, -1))
        if m == 2:
            return g.lanes(v, -NX)
        if m == 1:
            return g.rows(v, -1)
        moved = g.rows(v, -depth)
        if d == 1:
            beyond = g.rows(v, depth - 1)
            return jnp.where(jnp.logical_and(g.zrow == 0, g.row >= depth), beyond, moved)
        return jnp.where(g.row >= depth, g.lanes(moved, -NX), moved)

    def over_face(d, s, own):
        def get(part, i, j):
            value, before = None, None
            for k, (m, h) in enumerate(LAYOUT[d][s]):
                if m == before:
                    continue
                x = step_in_face(d, m, own[part][i][j])
                value = x if value is None else jnp.where(place[d] >= k, x, value)
                before = m
            return value

        return complete_rows(get)

    def send_side(d):
        own = own_face(d)
        for s in range(len(LAYOUT[d])):
            n = sets.index((d, s))
            side = packed(d, s, lambda m, h, *c: load(m, *c, h), True)
            over = over_face(d, s, own)
            b = product(own, side, left_h=True)
            mask = open_mask(d, s)
            put("g", d, s, [
                [
                    [pick(mask, b[p][i][j], entry(b, over, i, j, p, False, False)) for j in range(3)]
                    for i in range(2)
                ]
                for p in range(2)
            ])
            for q, value in enumerate((own, side, over)):
                save(face_s, (n, q), value)
            save(b_s, (n,), b)

    def send_face(d):
        for s in range(len(LAYOUT[d])):
            put("x", d, s, [
                [
                    [pack(d, s, lambda m, h: load(m, p, i, j, h), False) for j in range(3)]
                    for i in range(2)
                ]
                for p in range(2)
            ])

    def pack_edges(d, n):
        r0 = offset("e", DIAGONALS.index((d, n)))
        if 2 not in (d, n):
            for c0 in range(0, 12, SUB):
                value = None
                for k in range(min(SUB, 12 - c0)):
                    v = load(d, *comps[c0 + k], halves - 1 if d == 0 else 0)
                    x = g.rows(v, k - depth if d == 0 else k - (depth - 1))
                    value = x if value is None else jnp.where(g.row >= k, x, value)
                out_s[r0 + c0 : r0 + c0 + SUB, :] = value
            return
        value = None
        for k in range(g.ygroups):
            v = dense_rows(d, n, comps[k])
            if k + g.ygroups < 12:
                w = dense_rows(d, n, comps[k + g.ygroups])
                step, mask = spare(d, n)
                v = jnp.where(mask, v, g.rows(w, step))
            x = g.lanes(v, NX * (k + (1 if d == 2 else 0)))
            value = x if value is None else jnp.where(g.lane >= NX * k, x, value)
        out_s[r0 : r0 + SUB, :] = value

    def spare(d, n):
        if (d, n) == (0, 2):
            return depth, g.row >= depth
        if (d, n) == (2, 0):
            return depth, g.row < depth
        return (-2, g.zrow >= 2) if d == 1 else (2, g.zrow < 2)

    def dense_rows(d, n, c):
        if 0 in (d, n):
            return load(d, *c, halves - 1 if d == 0 else 0)
        at = depth - 1 if d == 1 else 0
        step = -1 if d == 1 else 1
        v = load(d, *c, 0)
        for h in range(1, halves):
            v = jnp.where(g.zrow == at + step * h, g.rows(load(d, *c, h), step * h), v)
        return v

    def edge(d, n, h, part, i, j):
        c = part * 6 + i * 3 + j
        r = offset("e", DIAGONALS.index((d, n)))
        if 2 not in (d, n):
            v = in_s[r + c // SUB * SUB : r + c // SUB * SUB + SUB, :]
            k = c % SUB
            return g.rows(v, depth - 1 - k if d == 0 else SUB - depth - k)
        k, back = c % g.ygroups, c >= g.ygroups
        v = g.lanes(in_s[r : r + SUB, :], NX * ((0 if d == 2 else g.ygroups - 1) - k))
        step = -spare(d, n)[0] if back else 0
        if (d, n) == (0, 2):
            return g.rows(v, step - (SUB - depth))
        if (d, n) == (2, 0):
            return g.rows(v, step + SUB - depth)
        return g.rows(v, step + (1 - depth + h if d == 1 else depth - 1 - h))

    everything_in = pltpu.make_async_copy(hbm, u, load_sem)
    everything_in.wait()
    for d, n in DIAGONALS:
        pack_edges(d, n)
    for d in (1, 0):
        send_side(d)
        send_face(d)
    send_face(2)
    pl.semaphore_wait(barrier, expected)
    signal(met, (2, -1))

    @pl.when(last_t)
    def _():
        signal(met_t, (0, 1))

    @pl.when(last_z)
    def _():
        signal(met_z, (1, 1))

    @pl.when(jnp.logical_or(rest_z, last_t))
    def _():
        edges[2].start()

    for copy in (edges[4], edges[0]):
        copy.start()

    @pl.when(rest_t)
    def _():
        edges[3].start()
        faces[0].start()

    @pl.when(rest_z)
    def _():
        edges[5].start()
        faces[1].start()

    for copy in (opens[1], opens[0]):
        copy.start()
    send_side(2)
    faces[2].start()
    opens[2].start()

    seen, pending = set(), {}

    def add(m, c, h, value):
        key = (m, c, h)
        pending[key] = pending[key] + value if key in pending else value

    def flush():
        for (m, c, h), value in pending.items():
            r = ((m * 8 + c) * halves + h) * SUB
            if (m, c, h) in seen:
                acc[r : r + SUB, :] += value
            else:
                seen.add((m, c, h))
                acc[r : r + SUB, :] = value
        pending.clear()

    def forward(m, d, h, q):
        for c in range(8):
            if d == 3:
                add(m, c, h, jnp.where(g.xcol == 0, g.lanes(q[c], 1 - NX), g.lanes(q[c], 1)))
            elif d == 2:
                add(m, c, h, g.lanes(q[c], NX))
            elif d == 1:
                add(m, c, h, g.rows(q[c], 1))
            elif h + 1 < halves:
                moved = g.rows(q[c], depth)
                add(m, c, h, jnp.where(g.row >= depth, moved, 0.0))
                add(m, c, h + 1, jnp.where(g.row < depth, moved, 0.0))
            else:
                add(m, c, h, g.rows(q[c], depth))

    def masked(mask, a):
        return [[[pick(mask, 0.0, v) for v in line] for line in part] for part in a]

    def inner(mu, nu, h):
        own = matrix(lambda *c: load(mu, *c, h))
        side = matrix(lambda *c: load(nu, *c, h))
        a = product(
            matrix(lambda *c: rolled(nu, mu, h, *c)),
            matrix(lambda *c: rolled(mu, nu, h, *c)),
            right_h=True,
        )
        mask = None
        for d in (mu, nu):
            if not complete(d, h):
                mask = top(d) if mask is None else jnp.logical_or(mask, top(d))
        a = masked(mask, a)
        b = product(own, side, left_h=True)
        forward(mu, nu, h, projected(a, b, left_h=True))
        forward(nu, mu, h, projected(a, b, right_h=True))
        upper = projected(product(own, a), side, right_h=True)
        for c in range(8):
            add(mu, c, h, upper[c])
            add(nu, c, h, -upper[c])

    def corners(d, among):
        for s in range(len(LAYOUT[d])):
            mask = open_mask(d, s, among)
            if mask is None:
                continue
            n = sets.index((d, s))

            def corner(m, h, c):
                if m not in among or complete(m, h):
                    return None
                k = LAYOUT[m][0].index((d, 0 if m == 0 else h))
                return shifted(m, fetch(in_s, "x", m, 0, *c), last[m] - k)

            for c in comps:
                value = pack(d, s, lambda m, h: corner(m, h, c), True)
                face_s[(n, 2, *c)] = jnp.where(mask, value, face_s[(n, 2, *c)])

    def face_terms(d, closed):
        for s, spots in enumerate(LAYOUT[d]):
            n = sets.index((d, s))
            own, side, over = (kept(d, s, q) for q in range(3))
            a = product(fetched(in_s, "x", d, s), over, right_h=True)
            a = masked(open_mask(d, s, [m for m in range(3) if m not in closed]), a)
            b = matrix(lambda *c: b_s[(n, *c)])
            upper = projected(product(own, a), side, right_h=True)
            low = projected(a, b, left_h=True)
            mask = open_mask(d, s, closed)
            low = [pick(mask, 0.0, v) for v in low]
            for k, (m, h) in enumerate(spots):
                h = half(d, h, True)
                natural = lambda v: jnp.where(top(d), shifted(d, v, last[d] - k), 0.0)
                for c in range(8):
                    x = natural(upper[c])
                    add(d, c, h, x)
                    add(m, c, h, -x)
                forward(d, m, h, [natural(v) for v in low])
        flush()

    def prepare(d):
        for s in range(len(LAYOUT[d])):
            own = fetched(out_s, "x", d, s)
            mask = open_mask(d, s)
            if mask is not None:
                far = packed(
                    d, s,
                    lambda m, h, *c: None if complete(m, h if d else 1) else edge(d, m, h, *c),
                    False,
                )
                both = product(own, far, right_h=True)
                own = [
                    [[jnp.where(mask, both[p][i][j], own[p][i][j]) for j in range(3)] for i in range(3)]
                    for p in range(2)
                ]
            save(pre_s, (sets.index((d, s)),), own)

    def close(d):
        for s, spots in enumerate(LAYOUT[d]):
            n = sets.index((d, s))
            q = projected(
                matrix(lambda *c: pre_s[(n, *c)]), fetched(in_s, "g", d, s), right_h=True
            )
            for k, (m, h) in enumerate(spots):
                for c in range(8):
                    add(m, c, half(d, h, False), jnp.where(bottom(d), shifted(d, q[c], -k), 0.0))
        flush()

    for n, pair in enumerate(PLANES):
        if n == 2:
            pl.semaphore_wait(met, 1)

            @pl.when(rest_t)
            def _():
                edges[1].start()

        for h in range(halves):
            inner(*pair, h)
        flush()

    @pl.when(first_t)
    def _():
        pl.semaphore_wait(met_t, 1)
        for copy in (edges[3], edges[1], faces[0]):
            copy.start()

    @pl.when(first_z)
    def _():
        pl.semaphore_wait(met_z, 1)
        edges[5].start()
        faces[1].start()

    @pl.when(jnp.logical_and(first_z, more_t))
    def _():
        edges[2].start()

    faces[2].wait_recv()
    face_terms(2, ())
    corners(0, (2,))
    faces[0].wait_recv()
    face_terms(0, (2,))
    corners(1, (0, 2))

    def close_all():
        for d in (2, 0, 1):
            opens[d].wait_recv()
        all_edges.wait_recv()
        for d in (2, 0, 1):
            prepare(d)
            close(d)

    def face_z():
        faces[1].wait_recv()
        face_terms(1, (0, 2))

    @pl.when(last_z)
    def _():
        close_all()
        face_z()

    @pl.when(more_z)
    def _():
        face_z()
        close_all()

    everything.wait_send()


def expand(halves, acc, hbm, out, sem):
    for m in range(4):
        for h in range(halves):
            rows = [((m * 8 + c) * halves + h) * SUB for c in range(8)]
            f = [acc[r : r + SUB, :] * (COEFF * 0.5 if c < 6 else COEFF) for c, r in enumerate(rows)]

            def put(part, i, j, value):
                out[m, part, i, j, h * SUB : (h + 1) * SUB, :] = value

            for n, (i, j) in enumerate(((0, 1), (0, 2), (1, 2))):
                put(0, i, j, f[n])
                put(0, j, i, -f[n])
                put(1, i, j, f[3 + n])
                put(1, j, i, f[3 + n])
            for i in range(3):
                put(0, i, i, jnp.zeros((SUB, LANES), jnp.float32))
            put(1, 0, 0, f[6])
            put(1, 1, 1, f[7])
            put(1, 2, 2, -(f[6] + f[7]))
        for part in range(2):
            for i in range(3):
                pltpu.make_async_copy(out.at[m, part, i], hbm.at[m, part, i], sem).start()
    pltpu.make_async_copy(out, hbm, sem).wait()


def per_device(counts, links):
    time_len, depth, flat = links.shape[4:]
    sites = time_len * depth
    assert flat == LANES and (time_len, depth) == (4, 4)
    halves = sites // SUB
    vmem = lambda *s: pltpu.VMEM(s + (LANES,), jnp.float32)
    shape = links.shape[:4] + (sites, flat)
    terms = pl.pallas_call(
        functools.partial(force_terms, counts, depth, halves),
        out_shape=pltpu.VMEM((32 * sites, flat), jnp.float32),
        in_specs=[pl.BlockSpec(memory_space=pl.ANY)],
        out_specs=pl.BlockSpec(memory_space=pltpu.VMEM),
        scratch_shapes=[
            vmem(*shape[:-1]),
            vmem(TOTAL),
            vmem(TOTAL),
            vmem(5, 3, 2, 2, 3, SUB),
            vmem(5, 2, 3, 3, SUB),
            vmem(5, 2, 3, 3, SUB),
            pltpu.SemaphoreType.DMA,
            pltpu.SemaphoreType.DMA,
            pltpu.SemaphoreType.DMA((7,)),
            pltpu.SemaphoreType.REGULAR,
            pltpu.SemaphoreType.REGULAR,
            pltpu.SemaphoreType.REGULAR,
        ],
        compiler_params=pltpu.CompilerParams(collective_id=0, has_side_effects=True),
        name="force_terms",
    )(links.reshape(shape))
    out = pl.pallas_call(
        functools.partial(expand, halves),
        out_shape=jax.ShapeDtypeStruct(shape, jnp.float32),
        in_specs=[pl.BlockSpec(memory_space=pltpu.VMEM)],
        out_specs=pl.BlockSpec(memory_space=pl.ANY),
        scratch_shapes=[vmem(*shape[:-1]), pltpu.SemaphoreType.DMA],
        name="expand",
    )(pltpu.with_memory_space_constraint(terms, pltpu.VMEM))
    return out.reshape(links.shape)


def solution(mesh):
    assert mesh.axis_names == ("gx", "gz", "ta")
    counts = tuple(mesh.shape[a] for a in AXES)
    spec = P(None, None, None, None, "ta", "gz", "gx")
    return jax.shard_map(
        functools.partial(per_device, counts),
        mesh=mesh,
        in_specs=(spec,),
        out_specs=spec,
        check_vma=False,
    )
```

```python
import functools

import jax
import jax.numpy as jnp
from jax import lax
from jax.experimental import pallas as pl
from jax.experimental.pallas import tpu as pltpu
from jax.sharding import PartitionSpec as P

NX = 16
COEFF = -1.9
AXES = ("ta", "gz", "gx")
SUB, LANES = 8, 128


def others(d):
    return [m for m in range(4) if m != d]


class Lattice:
    def __init__(self, depth):
        self.depth = depth
        self.per = SUB // depth
        self.ygroups = LANES // NX
        self.row = lax.broadcasted_iota(jnp.int32, (SUB, LANES), 0)
        self.lane = lax.broadcasted_iota(jnp.int32, (SUB, LANES), 1)
        self.zrow = self.row % depth
        self.xcol = self.lane % NX

    def rows(self, value, shift):
        shift %= SUB
        return pltpu.roll(value, shift, 0) if shift else value

    def lanes(self, value, shift):
        shift %= LANES
        return pltpu.roll(value, shift, 1) if shift else value


def entry(left, right, i, j, part, left_h, right_h):
    total = None
    for k in range(3):
        li = (k, i) if left_h else (i, k)
        ri = (j, k) if right_h else (k, j)
        lr, lm = left[0][li[0]][li[1]], left[1][li[0]][li[1]]
        rr, rm = right[0][ri[0]][ri[1]], right[1][ri[0]][ri[1]]
        if part == 0:
            first, second = lr * rr, lm * rm
            minus = left_h == right_h
        elif left_h:
            first, second = lr * rm, lm * rr
            minus = True
        else:
            first, second = lm * rr, lr * rm
            minus = right_h
        value = first - second if minus else first + second
        total = value if total is None else total + value
    return total


def product(left, right, left_h=False, right_h=False):
    return [
        [[entry(left, right, i, j, part, left_h, right_h) for j in range(3)] for i in range(3)]
        for part in range(2)
    ]


def projected(left, right, left_h=False, right_h=False):
    get = lambda i, j, part: entry(left, right, i, j, part, left_h, right_h)
    pairs = ((0, 1), (0, 2), (1, 2))
    real = [get(i, j, 0) - get(j, i, 0) for i, j in pairs]
    imag = [get(i, j, 1) + get(j, i, 1) for i, j in pairs]
    diag = [get(i, i, 1) for i in range(3)]
    third = (diag[0] + diag[1] + diag[2]) * (1.0 / 3.0)
    return real + imag + [diag[0] - third, diag[1] - third]


def third_row(real, imag):
    rows_r, rows_i = [], []
    for column in range(3):
        n, l = (column + 1) % 3, (column + 2) % 3
        rows_r.append(
            real[0][n] * real[1][l]
            - imag[0][n] * imag[1][l]
            - real[0][l] * real[1][n]
            + imag[0][l] * imag[1][n]
        )
        rows_i.append(
            real[0][l] * imag[1][n]
            + imag[0][l] * real[1][n]
            - real[0][n] * imag[1][l]
            - imag[0][n] * real[1][l]
        )
    return rows_r, rows_i


PLANES = ((0, 1), (0, 2), (0, 3), (1, 2), (1, 3), (2, 3))
DIAGONALS = ((0, 2), (2, 0), (0, 1), (1, 0), (1, 2), (2, 1))
LAYOUT = (
    (((1, 0), (2, 0)), ((3, 0),)),
    (((0, 0), (0, 1), (2, 0), (2, 1)), ((3, 0), (3, 1))),
    (((0, 0), (0, 1), (1, 0), (1, 1), (3, 0), (3, 1)),),
)
ROWS = (144, 144, 96)
EDGES = (8, 8, 16, 16, 8, 8)


def offset(kind, d):
    if kind == "e":
        return 2 * sum(ROWS) + sum(EDGES[:d])
    return (sum(ROWS) if kind == "g" else 0) + sum(ROWS[:d])


TOTAL = offset("e", len(DIAGONALS))


def force_terms(
    counts, depth, halves, hbm, acc, u, out_s, in_s, face_s, b_s, pre_s, send, recv, met, met_t, met_z,
):
    g = Lattice(depth)
    me = [lax.axis_index(a) for a in AXES]
    comps = [(part, i, j) for part in range(2) for i in range(2) for j in range(3)]
    last = (g.per - 1, depth - 1, g.ygroups - 1)
    place = (g.row // depth, g.zrow, g.lane // NX)

    def device(*steps):
        where = list(me)
        for i, step in steps:
            where[i] = lax.rem(me[i] + (step + counts[i]), counts[i])
        by = dict(zip(AXES, where))
        return (by["gx"], by["gz"], by["ta"])

    barrier = pltpu.get_barrier_semaphore()
    first_t, last_t = me[0] == 0, me[0] == counts[0] - 1
    more_t, rest_t = jnp.logical_not(last_t), jnp.logical_not(first_t)
    middle = counts[1] // 2
    first_z = jnp.logical_or(me[1] == 0, jnp.logical_and(me[1] == middle, last_t))
    last_z = jnp.logical_or(
        me[1] == counts[1] - 1, jnp.logical_and(me[1] == middle - 1, last_t)
    )
    silent = jnp.logical_and(me[1] == counts[1] - 1, rest_t)
    more_z, rest_z = jnp.logical_not(last_z), jnp.logical_not(first_z)
    one = lambda flag: jnp.where(flag, 1, 0)

    def signal(semaphore, *steps):
        pl.semaphore_signal(
            semaphore, inc=1, device_id=device(*steps), device_id_type=pl.DeviceIdType.MESH
        )

    for steps in (((1, -1),), ((2, 1), (1, -1)), ((0, -1), (2, 1)), ((0, -1),), ((2, 1),), ((2, -1),)):
        signal(barrier, *steps)

    @pl.when(more_z)
    def _():
        signal(barrier, (1, 1))
        signal(barrier, (1, 1), (2, -1))

    @pl.when(jnp.logical_not(silent))
    def _():
        signal(barrier, (1, 1), (0, -1))

    @pl.when(more_t)
    def _():
        signal(barrier, (0, 1))
        signal(barrier, (0, 1), (1, -1))

    expected = 11 - 2 * one(first_t) - 2 * one(first_z) - one(jnp.logical_and(first_z, more_t))

    loads = [
        pltpu.make_async_copy(hbm.at[m, part, i], u.at[m, part, i], send)
        for m in range(4)
        for part in range(2)
        for i in range(3)
    ]
    for copy in loads:
        copy.start()

    def remote(start, rows, slot, where):
        span = slice(start, start + rows)
        return pltpu.make_async_remote_copy(
            src_ref=out_s.at[span], dst_ref=in_s.at[span], send_sem=send, recv_sem=recv.at[slot],
            device_id=where, device_id_type=pl.DeviceIdType.MESH,
        )

    faces = [remote(offset("x", d), ROWS[d], d, device((d, -1))) for d in range(3)]
    opens = [remote(offset("g", d), ROWS[d], 3, device((d, 1))) for d in range(3)]
    edges = [
        remote(offset("e", k), EDGES[k], 3, device((d, 1), (n, -1)))
        for k, (d, n) in enumerate(DIAGONALS)
    ]
    arrivals = remote(offset("g", 0), TOTAL - offset("g", 0), 3, device((1, 1)))
    everything = remote(0, TOTAL, 0, device((1, 1)))

    def load(m, part, i, j, h):
        return u[m, part, i, j, h * SUB : (h + 1) * SUB, :]

    def shifted(d, value, steps):
        if d == 0:
            return g.rows(value, depth * steps)
        return g.rows(value, steps) if d == 1 else g.lanes(value, NX * steps)

    def half(d, h, top):
        return (halves - 1 if top else 0) if d == 0 else h

    def complete(d, h):
        return d == 3 or (d == 0 and h + 1 < halves)

    def top(d, h=1):
        if d == 0:
            return g.row >= SUB - depth
        return g.zrow == depth - 1 if d == 1 else g.lane >= LANES - NX

    def bottom(d):
        return (g.row < depth, g.zrow == 0, g.lane < NX)[d]

    def open_mask(d, s, among=(0, 1, 2)):
        mask = None
        for k, (m, h) in enumerate(LAYOUT[d][s]):
            if m in among and not complete(m, h if d else 1):
                here = jnp.logical_and(place[d] == k, top(m))
                mask = here if mask is None else jnp.logical_or(mask, here)
        return mask

    def pick(mask, yes, no):
        return no if mask is None else jnp.where(mask, yes, no)

    def pack(d, s, get, up):
        value = None
        for k, (m, h) in enumerate(LAYOUT[d][s]):
            x = get(m, half(d, h, up))
            if x is None:
                continue
            x = shifted(d, x, k - (last[d] if up else 0))
            value = x if value is None else jnp.where(place[d] >= k, x, value)
        return value

    def complete_rows(get):
        real = [[get(0, i, j) for j in range(3)] for i in range(2)]
        imag = [[get(1, i, j) for j in range(3)] for i in range(2)]
        third_r, third_i = third_row(real, imag)
        return [real + [third_r], imag + [third_i]]

    def packed(d, s, get, up):
        return complete_rows(
            lambda part, i, j: pack(d, s, lambda m, h: get(m, h, part, i, j), up)
        )

    def put(kind, d, s, value):
        r = offset(kind, d)
        used = len(LAYOUT[d][s])
        for n, (part, i, j) in enumerate(comps[: 6 if s else 12]):
            v = value[part][i][j]
            if s:
                v = jnp.where(place[d] < used, v, shifted(d, value[1][i][j], used))
            at = r + (96 if s else 0) + n * SUB
            out_s[at : at + SUB, :] = v

    def fetch(ref, kind, d, s, part, i, j):
        n = part * 6 + i * 3 + j
        at = offset(kind, d) + n * SUB
        if not s:
            return ref[at : at + SUB, :]
        at += 96 - part * 6 * SUB
        v = ref[at : at + SUB, :]
        return shifted(d, v, -len(LAYOUT[d][s])) if part else v

    def fetched(ref, kind, d, s):
        return complete_rows(lambda part, i, j: fetch(ref, kind, d, s, part, i, j))

    def rolled(m, d, h, part, i, j):
        v = load(m, part, i, j, h)
        if d == 3:
            return jnp.where(g.xcol == NX - 1, g.lanes(v, NX - 1), g.lanes(v, -1))
        if d == 2:
            return g.lanes(v, -NX)
        if d == 1:
            return g.rows(v, -1)
        if h + 1 < halves:
            beyond = g.rows(load(m, part, i, j, h + 1), -depth)
            return jnp.where(g.row >= SUB - depth, beyond, g.rows(v, -depth))
        return g.rows(v, -depth)

    def matrix(get):
        return [[[get(part, i, j) for j in range(3)] for i in range(3)] for part in range(2)]

    def save(ref, index, value):
        for part in range(2):
            for i in range(ref.shape[-4]):
                for j in range(3):
                    ref[(*index, part, i, j)] = value[part][i][j]

    sets = [(d, s) for d in range(3) for s in range(len(LAYOUT[d]))]

    def kept(d, s, q):
        n = sets.index((d, s))
        return complete_rows(lambda part, i, j: face_s[n, q, part, i, j])

    def own_face(d):
        def get(part, i, j):
            if d != 2:
                return pack(d, 0, lambda m, h: load(d, part, i, j, h), True)
            pair = [shifted(d, load(d, part, i, j, h), h - last[d]) for h in range(halves)]
            pair = jnp.where(place[d] >= 1, pair[1], pair[0])
            value = jnp.where(place[d] >= 2, shifted(d, pair, 2), pair)
            return jnp.where(place[d] >= 4, shifted(d, pair, 4), value)

        return complete_rows(get)

    def step_in_face(d, m, v):
        if m == 3:
            return jnp.where(g.xcol == NX - 1, g.lanes(v, NX - 1), g.lanes(v, -1))
        if m == 2:
            return g.lanes(v, -NX)
        if m == 1:
            return g.rows(v, -1)
        moved = g.rows(v, -depth)
        if d == 1:
            beyond = g.rows(v, depth - 1)
            return jnp.where(jnp.logical_and(g.zrow == 0, g.row >= depth), beyond, moved)
        return jnp.where(g.row >= depth, g.lanes(moved, -NX), moved)

    def over_face(d, s, own):
        def get(part, i, j):
            value, before = None, None
            for k, (m, h) in enumerate(LAYOUT[d][s]):
                if m == before:
                    continue
                x = step_in_face(d, m, own[part][i][j])
                value = x if value is None else jnp.where(place[d] >= k, x, value)
                before = m
            return value

        return complete_rows(get)

    def send_side(d):
        own = own_face(d)
        for s in range(len(LAYOUT[d])):
            n = sets.index((d, s))
            side = packed(d, s, lambda m, h, *c: load(m, *c, h), True)
            over = over_face(d, s, own)
            b = product(own, side, left_h=True)
            mask = open_mask(d, s)
            put("g", d, s, [
                [
                    [pick(mask, b[p][i][j], entry(b, over, i, j, p, False, False)) for j in range(3)]
                    for i in range(2)
                ]
                for p in range(2)
            ])
            for q, value in enumerate((own, side, over)):
                save(face_s, (n, q), value)
            save(b_s, (n,), b)

    def send_face(d):
        for s in range(len(LAYOUT[d])):
            put("x", d, s, [
                [
                    [pack(d, s, lambda m, h: load(m, p, i, j, h), False) for j in range(3)]
                    for i in range(2)
                ]
                for p in range(2)
            ])

    def pack_edges(d, n):
        r0 = offset("e", DIAGONALS.index((d, n)))
        if 2 not in (d, n):
            for c0 in range(0, 12, SUB):
                value = None
                for k in range(min(SUB, 12 - c0)):
                    v = load(d, *comps[c0 + k], halves - 1 if d == 0 else 0)
                    x = g.rows(v, k - depth if d == 0 else k - (depth - 1))
                    value = x if value is None else jnp.where(g.row >= k, x, value)
                out_s[r0 + c0 : r0 + c0 + SUB, :] = value
            return
        value = None
        for k in range(g.ygroups):
            v = dense_rows(d, n, comps[k])
            if k + g.ygroups < 12:
                w = dense_rows(d, n, comps[k + g.ygroups])
                step, mask = spare(d, n)
                v = jnp.where(mask, v, g.rows(w, step))
            x = g.lanes(v, NX * (k + (1 if d == 2 else 0)))
            value = x if value is None else jnp.where(g.lane >= NX * k, x, value)
        out_s[r0 : r0 + SUB, :] = value

    def spare(d, n):
        if (d, n) == (0, 2):
            return depth, g.row >= depth
        if (d, n) == (2, 0):
            return depth, g.row < depth
        return (-2, g.zrow >= 2) if d == 1 else (2, g.zrow < 2)

    def dense_rows(d, n, c):
        if 0 in (d, n):
            return load(d, *c, halves - 1 if d == 0 else 0)
        at = depth - 1 if d == 1 else 0
        step = -1 if d == 1 else 1
        v = load(d, *c, 0)
        for h in range(1, halves):
            v = jnp.where(g.zrow == at + step * h, g.rows(load(d, *c, h), step * h), v)
        return v

    def edge(d, n, h, part, i, j):
        c = part * 6 + i * 3 + j
        r = offset("e", DIAGONALS.index((d, n)))
        if 2 not in (d, n):
            v = in_s[r + c // SUB * SUB : r + c // SUB * SUB + SUB, :]
            k = c % SUB
            return g.rows(v, depth - 1 - k if d == 0 else SUB - depth - k)
        k, back = c % g.ygroups, c >= g.ygroups
        v = g.lanes(in_s[r : r + SUB, :], NX * ((0 if d == 2 else g.ygroups - 1) - k))
        step = -spare(d, n)[0] if back else 0
        if (d, n) == (0, 2):
            return g.rows(v, step - (SUB - depth))
        if (d, n) == (2, 0):
            return g.rows(v, step + SUB - depth)
        return g.rows(v, step + (1 - depth + h if d == 1 else depth - 1 - h))

    everything_in = pltpu.make_async_copy(hbm, u, send)
    everything_in.wait()
    for d, n in DIAGONALS:
        pack_edges(d, n)
    for d in (1, 0):
        send_side(d)
        send_face(d)
    send_face(2)
    pl.semaphore_wait(barrier, expected)
    signal(met, (2, -1))

    @pl.when(last_t)
    def _():
        signal(met_t, (0, 1))

    @pl.when(last_z)
    def _():
        signal(met_z, (1, 1))

    @pl.when(jnp.logical_or(rest_z, last_t))
    def _():
        edges[2].start()

    for copy in (edges[4], edges[0], opens[0], opens[1]):
        copy.start()

    @pl.when(rest_t)
    def _():
        edges[3].start()
        faces[0].start()

    @pl.when(rest_z)
    def _():
        edges[5].start()
        faces[1].start()

    send_side(2)
    faces[2].start()
    opens[2].start()

    seen, pending = set(), {}

    def add(m, c, h, value):
        key = (m, c, h)
        pending[key] = pending[key] + value if key in pending else value

    def flush():
        for (m, c, h), value in pending.items():
            r = ((m * 8 + c) * halves + h) * SUB
            if (m, c, h) in seen:
                acc[r : r + SUB, :] += value
            else:
                seen.add((m, c, h))
                acc[r : r + SUB, :] = value
        pending.clear()

    def forward(m, d, h, q):
        for c in range(8):
            if d == 3:
                add(m, c, h, jnp.where(g.xcol == 0, g.lanes(q[c], 1 - NX), g.lanes(q[c], 1)))
            elif d == 2:
                add(m, c, h, g.lanes(q[c], NX))
            elif d == 1:
                add(m, c, h, g.rows(q[c], 1))
            elif h + 1 < halves:
                moved = g.rows(q[c], depth)
                add(m, c, h, jnp.where(g.row >= depth, moved, 0.0))
                add(m, c, h + 1, jnp.where(g.row < depth, moved, 0.0))
            else:
                add(m, c, h, g.rows(q[c], depth))

    def masked(mask, a):
        return [[[pick(mask, 0.0, v) for v in line] for line in part] for part in a]

    def inner(mu, nu, h):
        own = matrix(lambda *c: load(mu, *c, h))
        side = matrix(lambda *c: load(nu, *c, h))
        a = product(
            matrix(lambda *c: rolled(nu, mu, h, *c)),
            matrix(lambda *c: rolled(mu, nu, h, *c)),
            right_h=True,
        )
        mask = None
        for d in (mu, nu):
            if not complete(d, h):
                mask = top(d) if mask is None else jnp.logical_or(mask, top(d))
        a = masked(mask, a)
        b = product(own, side, left_h=True)
        forward(mu, nu, h, projected(a, b, left_h=True))
        forward(nu, mu, h, projected(a, b, right_h=True))
        upper = projected(product(own, a), side, right_h=True)
        for c in range(8):
            add(mu, c, h, upper[c])
            add(nu, c, h, -upper[c])

    def corners(d, among):
        for s in range(len(LAYOUT[d])):
            mask = open_mask(d, s, among)
            if mask is None:
                continue
            n = sets.index((d, s))

            def corner(m, h, c):
                if m not in among or complete(m, h):
                    return None
                k = LAYOUT[m][0].index((d, 0 if m == 0 else h))
                return shifted(m, fetch(in_s, "x", m, 0, *c), last[m] - k)

            for c in comps:
                value = pack(d, s, lambda m, h: corner(m, h, c), True)
                face_s[(n, 2, *c)] = jnp.where(mask, value, face_s[(n, 2, *c)])

    def face_terms(d, closed):
        for s, spots in enumerate(LAYOUT[d]):
            n = sets.index((d, s))
            own, side, over = (kept(d, s, q) for q in range(3))
            a = product(fetched(in_s, "x", d, s), over, right_h=True)
            a = masked(open_mask(d, s, [m for m in range(3) if m not in closed]), a)
            b = matrix(lambda *c: b_s[(n, *c)])
            upper = projected(product(own, a), side, right_h=True)
            low = projected(a, b, left_h=True)
            mask = open_mask(d, s, closed)
            low = [pick(mask, 0.0, v) for v in low]
            for k, (m, h) in enumerate(spots):
                h = half(d, h, True)
                natural = lambda v: jnp.where(top(d), shifted(d, v, last[d] - k), 0.0)
                for c in range(8):
                    x = natural(upper[c])
                    add(d, c, h, x)
                    add(m, c, h, -x)
                forward(d, m, h, [natural(v) for v in low])
        flush()

    def prepare(d):
        for s in range(len(LAYOUT[d])):
            own = fetched(out_s, "x", d, s)
            mask = open_mask(d, s)
            if mask is not None:
                far = packed(
                    d, s,
                    lambda m, h, *c: None if complete(m, h if d else 1) else edge(d, m, h, *c),
                    False,
                )
                both = product(own, far, right_h=True)
                own = [
                    [[jnp.where(mask, both[p][i][j], own[p][i][j]) for j in range(3)] for i in range(3)]
                    for p in range(2)
                ]
            save(pre_s, (sets.index((d, s)),), own)

    def close(d):
        for s, spots in enumerate(LAYOUT[d]):
            n = sets.index((d, s))
            q = projected(
                matrix(lambda *c: pre_s[(n, *c)]), fetched(in_s, "g", d, s), right_h=True
            )
            for k, (m, h) in enumerate(spots):
                for c in range(8):
                    add(m, c, half(d, h, False), jnp.where(bottom(d), shifted(d, q[c], -k), 0.0))
        flush()

    for n, pair in enumerate(PLANES):
        if n == 2:
            pl.semaphore_wait(met, 1)

            @pl.when(rest_t)
            def _():
                edges[1].start()

        for h in range(halves):
            inner(*pair, h)
        flush()

    @pl.when(first_t)
    def _():
        pl.semaphore_wait(met_t, 1)
        for copy in (edges[3], edges[1], faces[0]):
            copy.start()

    @pl.when(first_z)
    def _():
        pl.semaphore_wait(met_z, 1)
        edges[5].start()
        faces[1].start()

    @pl.when(jnp.logical_and(first_z, more_t))
    def _():
        edges[2].start()

    faces[2].wait_recv()
    face_terms(2, ())
    corners(0, (2,))
    faces[0].wait_recv()
    face_terms(0, (2,))
    corners(1, (0, 2))

    def close_all():
        arrivals.wait_recv()
        for d in (2, 0, 1):
            prepare(d)
            close(d)

    def face_z():
        faces[1].wait_recv()
        face_terms(1, (0, 2))

    @pl.when(last_z)
    def _():
        close_all()
        face_z()

    @pl.when(more_z)
    def _():
        face_z()
        close_all()

    everything.wait_send()


def expand(halves, acc, hbm, out, sem):
    for m in range(4):
        for h in range(halves):
            rows = [((m * 8 + c) * halves + h) * SUB for c in range(8)]
            f = [acc[r : r + SUB, :] * (COEFF * 0.5 if c < 6 else COEFF) for c, r in enumerate(rows)]

            def put(part, i, j, value):
                out[m, part, i, j, h * SUB : (h + 1) * SUB, :] = value

            for n, (i, j) in enumerate(((0, 1), (0, 2), (1, 2))):
                put(0, i, j, f[n])
                put(0, j, i, -f[n])
                put(1, i, j, f[3 + n])
                put(1, j, i, f[3 + n])
            for i in range(3):
                put(0, i, i, jnp.zeros((SUB, LANES), jnp.float32))
            put(1, 0, 0, f[6])
            put(1, 1, 1, f[7])
            put(1, 2, 2, -(f[6] + f[7]))
        for part in range(2):
            for i in range(3):
                pltpu.make_async_copy(out.at[m, part, i], hbm.at[m, part, i], sem).start()
    pltpu.make_async_copy(out, hbm, sem).wait()


def per_device(counts, links):
    time_len, depth, flat = links.shape[4:]
    sites = time_len * depth
    assert flat == LANES and (time_len, depth) == (4, 4)
    halves = sites // SUB
    vmem = lambda *s: pltpu.VMEM(s + (LANES,), jnp.float32)
    shape = links.shape[:4] + (sites, flat)
    terms = pl.pallas_call(
        functools.partial(force_terms, counts, depth, halves),
        out_shape=pltpu.VMEM((32 * sites, flat), jnp.float32),
        in_specs=[pl.BlockSpec(memory_space=pl.ANY)],
        out_specs=pl.BlockSpec(memory_space=pltpu.VMEM),
        scratch_shapes=[
            vmem(*shape[:-1]),
            vmem(TOTAL),
            vmem(TOTAL),
            vmem(5, 3, 2, 2, 3, SUB),
            vmem(5, 2, 3, 3, SUB),
            vmem(5, 2, 3, 3, SUB),
            pltpu.SemaphoreType.DMA,
            pltpu.SemaphoreType.DMA((4,)),
            pltpu.SemaphoreType.REGULAR,
            pltpu.SemaphoreType.REGULAR,
            pltpu.SemaphoreType.REGULAR,
        ],
        compiler_params=pltpu.CompilerParams(collective_id=0, has_side_effects=True),
        name="force_terms",
    )(links.reshape(shape))
    out = pl.pallas_call(
        functools.partial(expand, halves),
        out_shape=jax.ShapeDtypeStruct(shape, jnp.float32),
        in_specs=[pl.BlockSpec(memory_space=pltpu.VMEM)],
        out_specs=pl.BlockSpec(memory_space=pl.ANY),
        scratch_shapes=[vmem(*shape[:-1]), pltpu.SemaphoreType.DMA],
        name="expand",
    )(pltpu.with_memory_space_constraint(terms, pltpu.VMEM))
    return out.reshape(links.shape)


def solution(mesh):
    assert mesh.axis_names == ("gx", "gz", "ta")
    counts = tuple(mesh.shape[a] for a in AXES)
    spec = P(None, None, None, None, "ta", "gz", "gx")
    return jax.shard_map(
        functools.partial(per_device, counts),
        mesh=mesh,
        in_specs=(spec,),
        out_specs=spec,
        check_vma=False,
    )
```

```python
import functools

import jax
import jax.numpy as jnp
from jax import lax
from jax.experimental import pallas as pl
from jax.experimental.pallas import tpu as pltpu
from jax.sharding import PartitionSpec as P

NX = 16
COEFF = -1.9
AXES = ("ta", "gz", "gx")
SUB, LANES = 8, 128


def others(d):
    return [m for m in range(4) if m != d]


class Lattice:
    def __init__(self, depth):
        self.depth = depth
        self.per = SUB // depth
        self.ygroups = LANES // NX
        self.row = lax.broadcasted_iota(jnp.int32, (SUB, LANES), 0)
        self.lane = lax.broadcasted_iota(jnp.int32, (SUB, LANES), 1)
        self.zrow = self.row % depth
        self.xcol = self.lane % NX

    def rows(self, value, shift):
        shift %= SUB
        return pltpu.roll(value, shift, 0) if shift else value

    def lanes(self, value, shift):
        shift %= LANES
        return pltpu.roll(value, shift, 1) if shift else value


def entry(left, right, i, j, part, left_h, right_h):
    total = None
    for k in range(3):
        li = (k, i) if left_h else (i, k)
        ri = (j, k) if right_h else (k, j)
        lr, lm = left[0][li[0]][li[1]], left[1][li[0]][li[1]]
        rr, rm = right[0][ri[0]][ri[1]], right[1][ri[0]][ri[1]]
        if part == 0:
            first, second = lr * rr, lm * rm
            minus = left_h == right_h
        elif left_h:
            first, second = lr * rm, lm * rr
            minus = True
        else:
            first, second = lm * rr, lr * rm
            minus = right_h
        value = first - second if minus else first + second
        total = value if total is None else total + value
    return total


def product(left, right, left_h=False, right_h=False):
    return [
        [[entry(left, right, i, j, part, left_h, right_h) for j in range(3)] for i in range(3)]
        for part in range(2)
    ]


def projected(left, right, left_h=False, right_h=False):
    get = lambda i, j, part: entry(left, right, i, j, part, left_h, right_h)
    pairs = ((0, 1), (0, 2), (1, 2))
    real = [get(i, j, 0) - get(j, i, 0) for i, j in pairs]
    imag = [get(i, j, 1) + get(j, i, 1) for i, j in pairs]
    diag = [get(i, i, 1) for i in range(3)]
    third = (diag[0] + diag[1] + diag[2]) * (1.0 / 3.0)
    return real + imag + [diag[0] - third, diag[1] - third]


def third_row(real, imag):
    rows_r, rows_i = [], []
    for column in range(3):
        n, l = (column + 1) % 3, (column + 2) % 3
        rows_r.append(
            real[0][n] * real[1][l]
            - imag[0][n] * imag[1][l]
            - real[0][l] * real[1][n]
            + imag[0][l] * imag[1][n]
        )
        rows_i.append(
            real[0][l] * imag[1][n]
            + imag[0][l] * real[1][n]
            - real[0][n] * imag[1][l]
            - imag[0][n] * real[1][l]
        )
    return rows_r, rows_i


PLANES = ((0, 1), (0, 2), (0, 3), (1, 2), (1, 3), (2, 3))
DIAGONALS = ((0, 2), (2, 0), (0, 1), (1, 0), (1, 2), (2, 1))
LAYOUT = (
    (((1, 0), (2, 0)), ((3, 0),)),
    (((0, 0), (0, 1), (2, 0), (2, 1)), ((3, 0), (3, 1))),
    (((0, 0), (0, 1), (1, 0), (1, 1), (3, 0), (3, 1)),),
)
ROWS = (144, 144, 96)
EDGES = (8, 8, 16, 16, 8, 8)


def offset(kind, d):
    if kind == "e":
        return 2 * sum(ROWS) + sum(EDGES[:d])
    return (sum(ROWS) if kind == "g" else 0) + sum(ROWS[:d])


TOTAL = offset("e", len(DIAGONALS))


def force_terms(
    counts, depth, halves, hbm, acc, u, out_s, in_s, face_s, b_s, pre_s, send, recv, met, met_t, met_z,
):
    g = Lattice(depth)
    me = [lax.axis_index(a) for a in AXES]
    comps = [(part, i, j) for part in range(2) for i in range(2) for j in range(3)]
    last = (g.per - 1, depth - 1, g.ygroups - 1)
    place = (g.row // depth, g.zrow, g.lane // NX)

    def device(*steps):
        where = list(me)
        for i, step in steps:
            where[i] = lax.rem(me[i] + (step + counts[i]), counts[i])
        by = dict(zip(AXES, where))
        return (by["gx"], by["gz"], by["ta"])

    barrier = pltpu.get_barrier_semaphore()
    first_t, last_t = me[0] == 0, me[0] == counts[0] - 1
    more_t, rest_t = jnp.logical_not(last_t), jnp.logical_not(first_t)
    middle = counts[1] // 2
    first_z = jnp.logical_or(me[1] == 0, jnp.logical_and(me[1] == middle, last_t))
    last_z = jnp.logical_or(
        me[1] == counts[1] - 1, jnp.logical_and(me[1] == middle - 1, last_t)
    )
    silent = jnp.logical_and(me[1] == counts[1] - 1, rest_t)
    more_z, rest_z = jnp.logical_not(last_z), jnp.logical_not(first_z)
    early = jnp.logical_and(me[1] == middle - 1, last_t)
    late = jnp.logical_and(me[1] == middle, me[0] == counts[0] - 2)
    vouch = jnp.logical_and(me[1] == middle - 1, me[0] == counts[0] - 2)
    one = lambda flag: jnp.where(flag, 1, 0)

    def signal(semaphore, *steps):
        pl.semaphore_signal(
            semaphore, inc=1, device_id=device(*steps), device_id_type=pl.DeviceIdType.MESH
        )

    for steps in (((1, -1),), ((2, 1), (1, -1)), ((0, -1), (2, 1)), ((0, -1),), ((2, 1),), ((2, -1),)):
        signal(barrier, *steps)

    @pl.when(more_z)
    def _():
        signal(barrier, (1, 1))
        signal(barrier, (1, 1), (2, -1))

    @pl.when(jnp.logical_not(silent))
    def _():
        signal(barrier, (1, 1), (0, -1))

    @pl.when(more_t)
    def _():
        signal(barrier, (0, 1))

    @pl.when(jnp.logical_not(jnp.logical_or(last_t, late)))
    def _():
        signal(barrier, (0, 1), (1, -1))

    expected = 11 - 2 * one(first_t) - 2 * one(first_z) - one(jnp.logical_and(first_z, more_t))
    expected = expected - one(early)

    loads = [
        pltpu.make_async_copy(hbm.at[m, part, i], u.at[m, part, i], send)
        for m in range(4)
        for part in range(2)
        for i in range(3)
    ]
    for copy in loads:
        copy.start()

    def remote(start, rows, slot, where):
        span = slice(start, start + rows)
        return pltpu.make_async_remote_copy(
            src_ref=out_s.at[span], dst_ref=in_s.at[span], send_sem=send, recv_sem=recv.at[slot],
            device_id=where, device_id_type=pl.DeviceIdType.MESH,
        )

    faces = [remote(offset("x", d), ROWS[d], d, device((d, -1))) for d in range(3)]
    opens = [remote(offset("g", d), ROWS[d], 3, device((d, 1))) for d in range(3)]
    edges = [
        remote(offset("e", k), EDGES[k], 3, device((d, 1), (n, -1)))
        for k, (d, n) in enumerate(DIAGONALS)
    ]
    arrivals = remote(offset("g", 0), TOTAL - offset("g", 0), 3, device((1, 1)))
    everything = remote(0, TOTAL, 0, device((1, 1)))

    def load(m, part, i, j, h):
        return u[m, part, i, j, h * SUB : (h + 1) * SUB, :]

    def shifted(d, value, steps):
        if d == 0:
            return g.rows(value, depth * steps)
        return g.rows(value, steps) if d == 1 else g.lanes(value, NX * steps)

    def half(d, h, top):
        return (halves - 1 if top else 0) if d == 0 else h

    def complete(d, h):
        return d == 3 or (d == 0 and h + 1 < halves)

    def top(d, h=1):
        if d == 0:
            return g.row >= SUB - depth
        return g.zrow == depth - 1 if d == 1 else g.lane >= LANES - NX

    def bottom(d):
        return (g.row < depth, g.zrow == 0, g.lane < NX)[d]

    def open_mask(d, s, among=(0, 1, 2)):
        mask = None
        for k, (m, h) in enumerate(LAYOUT[d][s]):
            if m in among and not complete(m, h if d else 1):
                here = jnp.logical_and(place[d] == k, top(m))
                mask = here if mask is None else jnp.logical_or(mask, here)
        return mask

    def pick(mask, yes, no):
        return no if mask is None else jnp.where(mask, yes, no)

    def pack(d, s, get, up):
        value = None
        for k, (m, h) in enumerate(LAYOUT[d][s]):
            x = get(m, half(d, h, up))
            if x is None:
                continue
            x = shifted(d, x, k - (last[d] if up else 0))
            value = x if value is None else jnp.where(place[d] >= k, x, value)
        return value

    def complete_rows(get):
        real = [[get(0, i, j) for j in range(3)] for i in range(2)]
        imag = [[get(1, i, j) for j in range(3)] for i in range(2)]
        third_r, third_i = third_row(real, imag)
        return [real + [third_r], imag + [third_i]]

    def packed(d, s, get, up):
        return complete_rows(
            lambda part, i, j: pack(d, s, lambda m, h: get(m, h, part, i, j), up)
        )

    def put(kind, d, s, value):
        r = offset(kind, d)
        used = len(LAYOUT[d][s])
        for n, (part, i, j) in enumerate(comps[: 6 if s else 12]):
            v = value[part][i][j]
            if s:
                v = jnp.where(place[d] < used, v, shifted(d, value[1][i][j], used))
            at = r + (96 if s else 0) + n * SUB
            out_s[at : at + SUB, :] = v

    def fetch(ref, kind, d, s, part, i, j):
        n = part * 6 + i * 3 + j
        at = offset(kind, d) + n * SUB
        if not s:
            return ref[at : at + SUB, :]
        at += 96 - part * 6 * SUB
        v = ref[at : at + SUB, :]
        return shifted(d, v, -len(LAYOUT[d][s])) if part else v

    def fetched(ref, kind, d, s):
        return complete_rows(lambda part, i, j: fetch(ref, kind, d, s, part, i, j))

    def rolled(m, d, h, part, i, j):
        v = load(m, part, i, j, h)
        if d == 3:
            return jnp.where(g.xcol == NX - 1, g.lanes(v, NX - 1), g.lanes(v, -1))
        if d == 2:
            return g.lanes(v, -NX)
        if d == 1:
            return g.rows(v, -1)
        if h + 1 < halves:
            beyond = g.rows(load(m, part, i, j, h + 1), -depth)
            return jnp.where(g.row >= SUB - depth, beyond, g.rows(v, -depth))
        return g.rows(v, -depth)

    def matrix(get):
        return [[[get(part, i, j) for j in range(3)] for i in range(3)] for part in range(2)]

    def save(ref, index, value):
        for part in range(2):
            for i in range(ref.shape[-4]):
                for j in range(3):
                    ref[(*index, part, i, j)] = value[part][i][j]

    sets = [(d, s) for d in range(3) for s in range(len(LAYOUT[d]))]

    def kept(d, s, q):
        n = sets.index((d, s))
        return complete_rows(lambda part, i, j: face_s[n, q, part, i, j])

    def own_face(d):
        def get(part, i, j):
            if d != 2:
                return pack(d, 0, lambda m, h: load(d, part, i, j, h), True)
            pair = [shifted(d, load(d, part, i, j, h), h - last[d]) for h in range(halves)]
            pair = jnp.where(place[d] >= 1, pair[1], pair[0])
            value = jnp.where(place[d] >= 2, shifted(d, pair, 2), pair)
            return jnp.where(place[d] >= 4, shifted(d, pair, 4), value)

        return complete_rows(get)

    def step_in_face(d, m, v):
        if m == 3:
            return jnp.where(g.xcol == NX - 1, g.lanes(v, NX - 1), g.lanes(v, -1))
        if m == 2:
            return g.lanes(v, -NX)
        if m == 1:
            return g.rows(v, -1)
        moved = g.rows(v, -depth)
        if d == 1:
            beyond = g.rows(v, depth - 1)
            return jnp.where(jnp.logical_and(g.zrow == 0, g.row >= depth), beyond, moved)
        return jnp.where(g.row >= depth, g.lanes(moved, -NX), moved)

    def over_face(d, s, own):
        def get(part, i, j):
            value, before = None, None
            for k, (m, h) in enumerate(LAYOUT[d][s]):
                if m == before:
                    continue
                x = step_in_face(d, m, own[part][i][j])
                value = x if value is None else jnp.where(place[d] >= k, x, value)
                before = m
            return value

        return complete_rows(get)

    def send_side(d):
        own = own_face(d)
        for s in range(len(LAYOUT[d])):
            n = sets.index((d, s))
            side = packed(d, s, lambda m, h, *c: load(m, *c, h), True)
            over = over_face(d, s, own)
            b = product(own, side, left_h=True)
            mask = open_mask(d, s)
            put("g", d, s, [
                [
                    [pick(mask, b[p][i][j], entry(b, over, i, j, p, False, False)) for j in range(3)]
                    for i in range(2)
                ]
                for p in range(2)
            ])
            for q, value in enumerate((own, side, over)):
                save(face_s, (n, q), value)
            save(b_s, (n,), b)

    def send_face(d):
        for s in range(len(LAYOUT[d])):
            put("x", d, s, [
                [
                    [pack(d, s, lambda m, h: load(m, p, i, j, h), False) for j in range(3)]
                    for i in range(2)
                ]
                for p in range(2)
            ])

    def pack_edges(d, n):
        r0 = offset("e", DIAGONALS.index((d, n)))
        if 2 not in (d, n):
            for c0 in range(0, 12, SUB):
                value = None
                for k in range(min(SUB, 12 - c0)):
                    v = load(d, *comps[c0 + k], halves - 1 if d == 0 else 0)
                    x = g.rows(v, k - depth if d == 0 else k - (depth - 1))
                    value = x if value is None else jnp.where(g.row >= k, x, value)
                out_s[r0 + c0 : r0 + c0 + SUB, :] = value
            return
        value = None
        for k in range(g.ygroups):
            v = dense_rows(d, n, comps[k])
            if k + g.ygroups < 12:
                w = dense_rows(d, n, comps[k + g.ygroups])
                step, mask = spare(d, n)
                v = jnp.where(mask, v, g.rows(w, step))
            x = g.lanes(v, NX * (k + (1 if d == 2 else 0)))
            value = x if value is None else jnp.where(g.lane >= NX * k, x, value)
        out_s[r0 : r0 + SUB, :] = value

    def spare(d, n):
        if (d, n) == (0, 2):
            return depth, g.row >= depth
        if (d, n) == (2, 0):
            return depth, g.row < depth
        return (-2, g.zrow >= 2) if d == 1 else (2, g.zrow < 2)

    def dense_rows(d, n, c):
        if 0 in (d, n):
            return load(d, *c, halves - 1 if d == 0 else 0)
        at = depth - 1 if d == 1 else 0
        step = -1 if d == 1 else 1
        v = load(d, *c, 0)
        for h in range(1, halves):
            v = jnp.where(g.zrow == at + step * h, g.rows(load(d, *c, h), step * h), v)
        return v

    def edge(d, n, h, part, i, j):
        c = part * 6 + i * 3 + j
        r = offset("e", DIAGONALS.index((d, n)))
        if 2 not in (d, n):
            v = in_s[r + c // SUB * SUB : r + c // SUB * SUB + SUB, :]
            k = c % SUB
            return g.rows(v, depth - 1 - k if d == 0 else SUB - depth - k)
        k, back = c % g.ygroups, c >= g.ygroups
        v = g.lanes(in_s[r : r + SUB, :], NX * ((0 if d == 2 else g.ygroups - 1) - k))
        step = -spare(d, n)[0] if back else 0
        if (d, n) == (0, 2):
            return g.rows(v, step - (SUB - depth))
        if (d, n) == (2, 0):
            return g.rows(v, step + SUB - depth)
        return g.rows(v, step + (1 - depth + h if d == 1 else depth - 1 - h))

    everything_in = pltpu.make_async_copy(hbm, u, send)
    everything_in.wait()
    for d, n in DIAGONALS:
        pack_edges(d, n)
    for d in (1, 0):
        send_side(d)
        send_face(d)
    send_face(2)
    pl.semaphore_wait(barrier, expected)
    signal(met, (2, -1))

    @pl.when(jnp.logical_or(last_t, vouch))
    def _():
        signal(met_t, (0, 1))

    @pl.when(last_z)
    def _():
        signal(met_z, (1, 1))

    @pl.when(jnp.logical_or(rest_z, last_t))
    def _():
        edges[2].start()

    for copy in (edges[4], edges[0]):
        copy.start()

    @pl.when(jnp.logical_not(jnp.logical_or(first_t, early)))
    def _():
        edges[3].start()

    @pl.when(rest_z)
    def _():
        edges[5].start()

    for copy in (opens[0], opens[1]):
        copy.start()

    @pl.when(rest_t)
    def _():
        faces[0].start()

    @pl.when(rest_z)
    def _():
        faces[1].start()

    send_side(2)
    faces[2].start()
    opens[2].start()

    seen, pending = set(), {}

    def add(m, c, h, value):
        key = (m, c, h)
        pending[key] = pending[key] + value if key in pending else value

    def flush():
        for (m, c, h), value in pending.items():
            r = ((m * 8 + c) * halves + h) * SUB
            if (m, c, h) in seen:
                acc[r : r + SUB, :] += value
            else:
                seen.add((m, c, h))
                acc[r : r + SUB, :] = value
        pending.clear()

    def forward(m, d, h, q):
        for c in range(8):
            if d == 3:
                add(m, c, h, jnp.where(g.xcol == 0, g.lanes(q[c], 1 - NX), g.lanes(q[c], 1)))
            elif d == 2:
                add(m, c, h, g.lanes(q[c], NX))
            elif d == 1:
                add(m, c, h, g.rows(q[c], 1))
            elif h + 1 < halves:
                moved = g.rows(q[c], depth)
                add(m, c, h, jnp.where(g.row >= depth, moved, 0.0))
                add(m, c, h + 1, jnp.where(g.row < depth, moved, 0.0))
            else:
                add(m, c, h, g.rows(q[c], depth))

    def masked(mask, a):
        return [[[pick(mask, 0.0, v) for v in line] for line in part] for part in a]

    def inner(mu, nu, h):
        own = matrix(lambda *c: load(mu, *c, h))
        side = matrix(lambda *c: load(nu, *c, h))
        a = product(
            matrix(lambda *c: rolled(nu, mu, h, *c)),
            matrix(lambda *c: rolled(mu, nu, h, *c)),
            right_h=True,
        )
        mask = None
        for d in (mu, nu):
            if not complete(d, h):
                mask = top(d) if mask is None else jnp.logical_or(mask, top(d))
        a = masked(mask, a)
        b = product(own, side, left_h=True)
        forward(mu, nu, h, projected(a, b, left_h=True))
        forward(nu, mu, h, projected(a, b, right_h=True))
        upper = projected(product(own, a), side, right_h=True)
        for c in range(8):
            add(mu, c, h, upper[c])
            add(nu, c, h, -upper[c])

    def corners(d, among):
        for s in range(len(LAYOUT[d])):
            mask = open_mask(d, s, among)
            if mask is None:
                continue
            n = sets.index((d, s))

            def corner(m, h, c):
                if m not in among or complete(m, h):
                    return None
                k = LAYOUT[m][0].index((d, 0 if m == 0 else h))
                return shifted(m, fetch(in_s, "x", m, 0, *c), last[m] - k)

            for c in comps:
                value = pack(d, s, lambda m, h: corner(m, h, c), True)
                face_s[(n, 2, *c)] = jnp.where(mask, value, face_s[(n, 2, *c)])

    def face_terms(d, closed):
        for s, spots in enumerate(LAYOUT[d]):
            n = sets.index((d, s))
            own, side, over = (kept(d, s, q) for q in range(3))
            a = product(fetched(in_s, "x", d, s), over, right_h=True)
            a = masked(open_mask(d, s, [m for m in range(3) if m not in closed]), a)
            b = matrix(lambda *c: b_s[(n, *c)])
            upper = projected(product(own, a), side, right_h=True)
            low = projected(a, b, left_h=True)
            mask = open_mask(d, s, closed)
            low = [pick(mask, 0.0, v) for v in low]
            for k, (m, h) in enumerate(spots):
                h = half(d, h, True)
                natural = lambda v: jnp.where(top(d), shifted(d, v, last[d] - k), 0.0)
                for c in range(8):
                    x = natural(upper[c])
                    add(d, c, h, x)
                    add(m, c, h, -x)
                forward(d, m, h, [natural(v) for v in low])
        flush()

    def prepare(d):
        for s in range(len(LAYOUT[d])):
            own = fetched(out_s, "x", d, s)
            mask = open_mask(d, s)
            if mask is not None:
                far = packed(
                    d, s,
                    lambda m, h, *c: None if complete(m, h if d else 1) else edge(d, m, h, *c),
                    False,
                )
                both = product(own, far, right_h=True)
                own = [
                    [[jnp.where(mask, both[p][i][j], own[p][i][j]) for j in range(3)] for i in range(3)]
                    for p in range(2)
                ]
            save(pre_s, (sets.index((d, s)),), own)

    def close(d):
        for s, spots in enumerate(LAYOUT[d]):
            n = sets.index((d, s))
            q = projected(
                matrix(lambda *c: pre_s[(n, *c)]), fetched(in_s, "g", d, s), right_h=True
            )
            for k, (m, h) in enumerate(spots):
                for c in range(8):
                    add(m, c, half(d, h, False), jnp.where(bottom(d), shifted(d, q[c], -k), 0.0))
        flush()

    for n, pair in enumerate(PLANES):
        if n == 2:
            pl.semaphore_wait(met, 1)

            @pl.when(rest_t)
            def _():
                edges[1].start()

        for h in range(halves):
            inner(*pair, h)
        flush()

    @pl.when(first_t)
    def _():
        pl.semaphore_wait(met_t, 1)
        for copy in (edges[3], edges[1], faces[0]):
            copy.start()

    @pl.when(early)
    def _():
        pl.semaphore_wait(met_t, 1)
        edges[3].start()

    @pl.when(first_z)
    def _():
        pl.semaphore_wait(met_z, 1)
        edges[5].start()
        faces[1].start()

    @pl.when(jnp.logical_and(first_z, more_t))
    def _():
        edges[2].start()

    faces[2].wait_recv()
    face_terms(2, ())
    corners(0, (2,))
    faces[0].wait_recv()
    face_terms(0, (2,))
    corners(1, (0, 2))

    def close_all():
        arrivals.wait_recv()
        for d in (2, 0, 1):
            prepare(d)
            close(d)

    def face_z():
        faces[1].wait_recv()
        face_terms(1, (0, 2))

    @pl.when(last_z)
    def _():
        close_all()
        face_z()

    @pl.when(more_z)
    def _():
        face_z()
        close_all()

    everything.wait_send()


def expand(halves, acc, hbm, out, sem):
    for m in range(4):
        for h in range(halves):
            rows = [((m * 8 + c) * halves + h) * SUB for c in range(8)]
            f = [acc[r : r + SUB, :] * (COEFF * 0.5 if c < 6 else COEFF) for c, r in enumerate(rows)]

            def put(part, i, j, value):
                out[m, part, i, j, h * SUB : (h + 1) * SUB, :] = value

            for n, (i, j) in enumerate(((0, 1), (0, 2), (1, 2))):
                put(0, i, j, f[n])
                put(0, j, i, -f[n])
                put(1, i, j, f[3 + n])
                put(1, j, i, f[3 + n])
            for i in range(3):
                put(0, i, i, jnp.zeros((SUB, LANES), jnp.float32))
            put(1, 0, 0, f[6])
            put(1, 1, 1, f[7])
            put(1, 2, 2, -(f[6] + f[7]))
        for part in range(2):
            for i in range(3):
                pltpu.make_async_copy(out.at[m, part, i], hbm.at[m, part, i], sem).start()
    pltpu.make_async_copy(out, hbm, sem).wait()


def per_device(counts, links):
    time_len, depth, flat = links.shape[4:]
    sites = time_len * depth
    assert flat == LANES and (time_len, depth) == (4, 4)
    halves = sites // SUB
    vmem = lambda *s: pltpu.VMEM(s + (LANES,), jnp.float32)
    shape = links.shape[:4] + (sites, flat)
    terms = pl.pallas_call(
        functools.partial(force_terms, counts, depth, halves),
        out_shape=pltpu.VMEM((32 * sites, flat), jnp.float32),
        in_specs=[pl.BlockSpec(memory_space=pl.ANY)],
        out_specs=pl.BlockSpec(memory_space=pltpu.VMEM),
        scratch_shapes=[
            vmem(*shape[:-1]),
            vmem(TOTAL),
            vmem(TOTAL),
            vmem(5, 3, 2, 2, 3, SUB),
            vmem(5, 2, 3, 3, SUB),
            vmem(5, 2, 3, 3, SUB),
            pltpu.SemaphoreType.DMA,
            pltpu.SemaphoreType.DMA((4,)),
            pltpu.SemaphoreType.REGULAR,
            pltpu.SemaphoreType.REGULAR,
            pltpu.SemaphoreType.REGULAR,
        ],
        compiler_params=pltpu.CompilerParams(collective_id=0, has_side_effects=True),
        name="force_terms",
    )(links.reshape(shape))
    out = pl.pallas_call(
        functools.partial(expand, halves),
        out_shape=jax.ShapeDtypeStruct(shape, jnp.float32),
        in_specs=[pl.BlockSpec(memory_space=pltpu.VMEM)],
        out_specs=pl.BlockSpec(memory_space=pl.ANY),
        scratch_shapes=[vmem(*shape[:-1]), pltpu.SemaphoreType.DMA],
        name="expand",
    )(pltpu.with_memory_space_constraint(terms, pltpu.VMEM))
    return out.reshape(links.shape)


def solution(mesh):
    assert mesh.axis_names == ("gx", "gz", "ta")
    counts = tuple(mesh.shape[a] for a in AXES)
    spec = P(None, None, None, None, "ta", "gz", "gx")
    return jax.shard_map(
        functools.partial(per_device, counts),
        mesh=mesh,
        in_specs=(spec,),
        out_specs=spec,
        check_vma=False,
    )
```

```python
import functools

import jax
import jax.numpy as jnp
from jax import lax
from jax.experimental import pallas as pl
from jax.experimental.pallas import tpu as pltpu
from jax.sharding import PartitionSpec as P

NX = 16
COEFF = -1.9
AXES = ("ta", "gz", "gx")
SUB, LANES = 8, 128


def others(d):
    return [m for m in range(4) if m != d]


class Lattice:
    def __init__(self, depth):
        self.depth = depth
        self.per = SUB // depth
        self.ygroups = LANES // NX
        self.row = lax.broadcasted_iota(jnp.int32, (SUB, LANES), 0)
        self.lane = lax.broadcasted_iota(jnp.int32, (SUB, LANES), 1)
        self.zrow = self.row % depth
        self.xcol = self.lane % NX

    def rows(self, value, shift):
        shift %= SUB
        return pltpu.roll(value, shift, 0) if shift else value

    def lanes(self, value, shift):
        shift %= LANES
        return pltpu.roll(value, shift, 1) if shift else value


def entry(left, right, i, j, part, left_h, right_h):
    total = None
    for k in range(3):
        li = (k, i) if left_h else (i, k)
        ri = (j, k) if right_h else (k, j)
        lr, lm = left[0][li[0]][li[1]], left[1][li[0]][li[1]]
        rr, rm = right[0][ri[0]][ri[1]], right[1][ri[0]][ri[1]]
        if part == 0:
            first, second = lr * rr, lm * rm
            minus = left_h == right_h
        elif left_h:
            first, second = lr * rm, lm * rr
            minus = True
        else:
            first, second = lm * rr, lr * rm
            minus = right_h
        value = first - second if minus else first + second
        total = value if total is None else total + value
    return total


def product(left, right, left_h=False, right_h=False):
    return [
        [[entry(left, right, i, j, part, left_h, right_h) for j in range(3)] for i in range(3)]
        for part in range(2)
    ]


def projected(left, right, left_h=False, right_h=False):
    get = lambda i, j, part: entry(left, right, i, j, part, left_h, right_h)
    pairs = ((0, 1), (0, 2), (1, 2))
    real = [get(i, j, 0) - get(j, i, 0) for i, j in pairs]
    imag = [get(i, j, 1) + get(j, i, 1) for i, j in pairs]
    diag = [get(i, i, 1) for i in range(3)]
    third = (diag[0] + diag[1] + diag[2]) * (1.0 / 3.0)
    return real + imag + [diag[0] - third, diag[1] - third]


def third_row(real, imag):
    rows_r, rows_i = [], []
    for column in range(3):
        n, l = (column + 1) % 3, (column + 2) % 3
        rows_r.append(
            real[0][n] * real[1][l]
            - imag[0][n] * imag[1][l]
            - real[0][l] * real[1][n]
            + imag[0][l] * imag[1][n]
        )
        rows_i.append(
            real[0][l] * imag[1][n]
            + imag[0][l] * real[1][n]
            - real[0][n] * imag[1][l]
            - imag[0][n] * real[1][l]
        )
    return rows_r, rows_i


PLANES = ((0, 1), (0, 2), (0, 3), (1, 2), (1, 3), (2, 3))
DIAGONALS = ((0, 2), (2, 0), (0, 1), (1, 0), (1, 2), (2, 1))
LAYOUT = (
    (((1, 0), (2, 0)), ((3, 0),)),
    (((0, 0), (0, 1), (2, 0), (2, 1)), ((3, 0), (3, 1))),
    (((0, 0), (0, 1), (1, 0), (1, 1), (3, 0), (3, 1)),),
)
ROWS = (144, 144, 96)
EDGES = (8, 8, 16, 16, 8, 8)


def group_rows(d):
    return ROWS[d] + sum(rows for pair, rows in zip(DIAGONALS, EDGES) if pair[0] == d)


def offset(kind, d):
    if kind == "x":
        return sum(ROWS[:d])
    if kind == "g":
        return sum(ROWS) + sum(group_rows(k) for k in range(d))
    own = DIAGONALS[d][0]
    before = sum(EDGES[k] for k in range(d) if DIAGONALS[k][0] == own)
    return offset("g", own) + ROWS[own] + before


TOTAL = sum(ROWS) + sum(group_rows(d) for d in range(3))


def force_terms(
    counts, depth, halves, hbm, acc, u, out_s, in_s, face_s, b_s, pre_s, send, recv, met, met_t, met_z,
):
    g = Lattice(depth)
    me = [lax.axis_index(a) for a in AXES]
    comps = [(part, i, j) for part in range(2) for i in range(2) for j in range(3)]
    last = (g.per - 1, depth - 1, g.ygroups - 1)
    place = (g.row // depth, g.zrow, g.lane // NX)

    def device(*steps):
        where = list(me)
        for i, step in steps:
            where[i] = lax.rem(me[i] + (step + counts[i]), counts[i])
        by = dict(zip(AXES, where))
        return (by["gx"], by["gz"], by["ta"])

    barrier = pltpu.get_barrier_semaphore()
    first_t, last_t = me[0] == 0, me[0] == counts[0] - 1
    more_t, rest_t = jnp.logical_not(last_t), jnp.logical_not(first_t)
    middle = counts[1] // 2
    first_z = jnp.logical_or(me[1] == 0, jnp.logical_and(me[1] == middle, last_t))
    last_z = jnp.logical_or(
        me[1] == counts[1] - 1, jnp.logical_and(me[1] == middle - 1, last_t)
    )
    silent = jnp.logical_and(me[1] == counts[1] - 1, rest_t)
    more_z, rest_z = jnp.logical_not(last_z), jnp.logical_not(first_z)
    early = jnp.logical_and(me[1] == middle - 1, last_t)
    late = jnp.logical_and(me[1] == middle, me[0] == counts[0] - 2)
    vouch = jnp.logical_and(me[1] == middle - 1, me[0] == counts[0] - 2)
    one = lambda flag: jnp.where(flag, 1, 0)

    def signal(semaphore, *steps):
        pl.semaphore_signal(
            semaphore, inc=1, device_id=device(*steps), device_id_type=pl.DeviceIdType.MESH
        )

    for steps in (((1, -1),), ((2, 1), (1, -1)), ((0, -1), (2, 1)), ((0, -1),), ((2, 1),), ((2, -1),)):
        signal(barrier, *steps)

    @pl.when(more_z)
    def _():
        signal(barrier, (1, 1))
        signal(barrier, (1, 1), (2, -1))

    @pl.when(jnp.logical_not(silent))
    def _():
        signal(barrier, (1, 1), (0, -1))

    @pl.when(more_t)
    def _():
        signal(barrier, (0, 1))

    @pl.when(jnp.logical_not(jnp.logical_or(last_t, late)))
    def _():
        signal(barrier, (0, 1), (1, -1))

    expected = 11 - 2 * one(first_t) - 2 * one(first_z) - one(jnp.logical_and(first_z, more_t))
    expected = expected - one(early)

    loads = [
        pltpu.make_async_copy(hbm.at[m, part, i], u.at[m, part, i], send)
        for m in range(4)
        for part in range(2)
        for i in range(3)
    ]
    for copy in loads:
        copy.start()

    def remote(start, rows, slot, where):
        span = slice(start, start + rows)
        return pltpu.make_async_remote_copy(
            src_ref=out_s.at[span], dst_ref=in_s.at[span], send_sem=send, recv_sem=recv.at[slot],
            device_id=where, device_id_type=pl.DeviceIdType.MESH,
        )

    faces = [remote(offset("x", d), ROWS[d], d, device((d, -1))) for d in range(3)]
    opens = [remote(offset("g", d), ROWS[d], 3 + d, device((d, 1))) for d in range(3)]
    edges = [
        remote(offset("e", k), EDGES[k], 3 + d, device((d, 1), (n, -1)))
        for k, (d, n) in enumerate(DIAGONALS)
    ]
    arrivals = [remote(offset("g", d), group_rows(d), 3 + d, device((1, 1))) for d in range(3)]
    everything = remote(0, TOTAL, 0, device((1, 1)))

    def load(m, part, i, j, h):
        return u[m, part, i, j, h * SUB : (h + 1) * SUB, :]

    def shifted(d, value, steps):
        if d == 0:
            return g.rows(value, depth * steps)
        return g.rows(value, steps) if d == 1 else g.lanes(value, NX * steps)

    def half(d, h, top):
        return (halves - 1 if top else 0) if d == 0 else h

    def complete(d, h):
        return d == 3 or (d == 0 and h + 1 < halves)

    def top(d, h=1):
        if d == 0:
            return g.row >= SUB - depth
        return g.zrow == depth - 1 if d == 1 else g.lane >= LANES - NX

    def bottom(d):
        return (g.row < depth, g.zrow == 0, g.lane < NX)[d]

    def open_mask(d, s, among=(0, 1, 2)):
        mask = None
        for k, (m, h) in enumerate(LAYOUT[d][s]):
            if m in among and not complete(m, h if d else 1):
                here = jnp.logical_and(place[d] == k, top(m))
                mask = here if mask is None else jnp.logical_or(mask, here)
        return mask

    def pick(mask, yes, no):
        return no if mask is None else jnp.where(mask, yes, no)

    def pack(d, s, get, up):
        value = None
        for k, (m, h) in enumerate(LAYOUT[d][s]):
            x = get(m, half(d, h, up))
            if x is None:
                continue
            x = shifted(d, x, k - (last[d] if up else 0))
            value = x if value is None else jnp.where(place[d] >= k, x, value)
        return value

    def complete_rows(get):
        real = [[get(0, i, j) for j in range(3)] for i in range(2)]
        imag = [[get(1, i, j) for j in range(3)] for i in range(2)]
        third_r, third_i = third_row(real, imag)
        return [real + [third_r], imag + [third_i]]

    def packed(d, s, get, up):
        return complete_rows(
            lambda part, i, j: pack(d, s, lambda m, h: get(m, h, part, i, j), up)
        )

    def put(kind, d, s, value):
        r = offset(kind, d)
        used = len(LAYOUT[d][s])
        for n, (part, i, j) in enumerate(comps[: 6 if s else 12]):
            v = value[part][i][j]
            if s:
                v = jnp.where(place[d] < used, v, shifted(d, value[1][i][j], used))
            at = r + (96 if s else 0) + n * SUB
            out_s[at : at + SUB, :] = v

    def fetch(ref, kind, d, s, part, i, j):
        n = part * 6 + i * 3 + j
        at = offset(kind, d) + n * SUB
        if not s:
            return ref[at : at + SUB, :]
        at += 96 - part * 6 * SUB
        v = ref[at : at + SUB, :]
        return shifted(d, v, -len(LAYOUT[d][s])) if part else v

    def fetched(ref, kind, d, s):
        return complete_rows(lambda part, i, j: fetch(ref, kind, d, s, part, i, j))

    def rolled(m, d, h, part, i, j):
        v = load(m, part, i, j, h)
        if d == 3:
            return jnp.where(g.xcol == NX - 1, g.lanes(v, NX - 1), g.lanes(v, -1))
        if d == 2:
            return g.lanes(v, -NX)
        if d == 1:
            return g.rows(v, -1)
        if h + 1 < halves:
            beyond = g.rows(load(m, part, i, j, h + 1), -depth)
            return jnp.where(g.row >= SUB - depth, beyond, g.rows(v, -depth))
        return g.rows(v, -depth)

    def matrix(get):
        return [[[get(part, i, j) for j in range(3)] for i in range(3)] for part in range(2)]

    def save(ref, index, value):
        for part in range(2):
            for i in range(ref.shape[-4]):
                for j in range(3):
                    ref[(*index, part, i, j)] = value[part][i][j]

    sets = [(d, s) for d in range(3) for s in range(len(LAYOUT[d]))]

    def kept(d, s, q):
        n = sets.index((d, s))
        return complete_rows(lambda part, i, j: face_s[n, q, part, i, j])

    def own_face(d):
        def get(part, i, j):
            if d != 2:
                return pack(d, 0, lambda m, h: load(d, part, i, j, h), True)
            pair = [shifted(d, load(d, part, i, j, h), h - last[d]) for h in range(halves)]
            pair = jnp.where(place[d] >= 1, pair[1], pair[0])
            value = jnp.where(place[d] >= 2, shifted(d, pair, 2), pair)
            return jnp.where(place[d] >= 4, shifted(d, pair, 4), value)

        return complete_rows(get)

    def step_in_face(d, m, v):
        if m == 3:
            return jnp.where(g.xcol == NX - 1, g.lanes(v, NX - 1), g.lanes(v, -1))
        if m == 2:
            return g.lanes(v, -NX)
        if m == 1:
            return g.rows(v, -1)
        moved = g.rows(v, -depth)
        if d == 1:
            beyond = g.rows(v, depth - 1)
            return jnp.where(jnp.logical_and(g.zrow == 0, g.row >= depth), beyond, moved)
        return jnp.where(g.row >= depth, g.lanes(moved, -NX), moved)

    def over_face(d, s, own):
        def get(part, i, j):
            value, before = None, None
            for k, (m, h) in enumerate(LAYOUT[d][s]):
                if m == before:
                    continue
                x = step_in_face(d, m, own[part][i][j])
                value = x if value is None else jnp.where(place[d] >= k, x, value)
                before = m
            return value

        return complete_rows(get)

    def send_side(d):
        own = own_face(d)
        for s in range(len(LAYOUT[d])):
            n = sets.index((d, s))
            side = packed(d, s, lambda m, h, *c: load(m, *c, h), True)
            over = over_face(d, s, own)
            b = product(own, side, left_h=True)
            mask = open_mask(d, s)
            put("g", d, s, [
                [
                    [pick(mask, b[p][i][j], entry(b, over, i, j, p, False, False)) for j in range(3)]
                    for i in range(2)
                ]
                for p in range(2)
            ])
            for q, value in enumerate((own, side, over)):
                save(face_s, (n, q), value)
            save(b_s, (n,), b)

    def send_face(d):
        for s in range(len(LAYOUT[d])):
            put("x", d, s, [
                [
                    [pack(d, s, lambda m, h: load(m, p, i, j, h), False) for j in range(3)]
                    for i in range(2)
                ]
                for p in range(2)
            ])

    def pack_edges(d, n):
        r0 = offset("e", DIAGONALS.index((d, n)))
        if 2 not in (d, n):
            for c0 in range(0, 12, SUB):
                value = None
                for k in range(min(SUB, 12 - c0)):
                    v = load(d, *comps[c0 + k], halves - 1 if d == 0 else 0)
                    x = g.rows(v, k - depth if d == 0 else k - (depth - 1))
                    value = x if value is None else jnp.where(g.row >= k, x, value)
                out_s[r0 + c0 : r0 + c0 + SUB, :] = value
            return
        value = None
        for k in range(g.ygroups):
            v = dense_rows(d, n, comps[k])
            if k + g.ygroups < 12:
                w = dense_rows(d, n, comps[k + g.ygroups])
                step, mask = spare(d, n)
                v = jnp.where(mask, v, g.rows(w, step))
            x = g.lanes(v, NX * (k + (1 if d == 2 else 0)))
            value = x if value is None else jnp.where(g.lane >= NX * k, x, value)
        out_s[r0 : r0 + SUB, :] = value

    def spare(d, n):
        if (d, n) == (0, 2):
            return depth, g.row >= depth
        if (d, n) == (2, 0):
            return depth, g.row < depth
        return (-2, g.zrow >= 2) if d == 1 else (2, g.zrow < 2)

    def dense_rows(d, n, c):
        if 0 in (d, n):
            return load(d, *c, halves - 1 if d == 0 else 0)
        at = depth - 1 if d == 1 else 0
        step = -1 if d == 1 else 1
        v = load(d, *c, 0)
        for h in range(1, halves):
            v = jnp.where(g.zrow == at + step * h, g.rows(load(d, *c, h), step * h), v)
        return v

    def edge(d, n, h, part, i, j):
        c = part * 6 + i * 3 + j
        r = offset("e", DIAGONALS.index((d, n)))
        if 2 not in (d, n):
            v = in_s[r + c // SUB * SUB : r + c // SUB * SUB + SUB, :]
            k = c % SUB
            return g.rows(v, depth - 1 - k if d == 0 else SUB - depth - k)
        k, back = c % g.ygroups, c >= g.ygroups
        v = g.lanes(in_s[r : r + SUB, :], NX * ((0 if d == 2 else g.ygroups - 1) - k))
        step = -spare(d, n)[0] if back else 0
        if (d, n) == (0, 2):
            return g.rows(v, step - (SUB - depth))
        if (d, n) == (2, 0):
            return g.rows(v, step + SUB - depth)
        return g.rows(v, step + (1 - depth + h if d == 1 else depth - 1 - h))

    everything_in = pltpu.make_async_copy(hbm, u, send)
    everything_in.wait()
    for d, n in DIAGONALS:
        pack_edges(d, n)
    for d in (1, 0):
        send_side(d)
        send_face(d)
    send_face(2)
    pl.semaphore_wait(barrier, expected)
    signal(met, (2, -1))

    @pl.when(jnp.logical_or(last_t, vouch))
    def _():
        signal(met_t, (0, 1))

    @pl.when(last_z)
    def _():
        signal(met_z, (1, 1))

    @pl.when(jnp.logical_or(rest_z, last_t))
    def _():
        edges[2].start()

    for copy in (edges[4], edges[0]):
        copy.start()

    @pl.when(jnp.logical_not(jnp.logical_or(first_t, early)))
    def _():
        edges[3].start()

    @pl.when(rest_z)
    def _():
        edges[5].start()

    for copy in (opens[0], opens[1]):
        copy.start()

    @pl.when(rest_t)
    def _():
        faces[0].start()

    @pl.when(rest_z)
    def _():
        faces[1].start()

    send_side(2)
    faces[2].start()
    opens[2].start()

    seen, pending = set(), {}

    def add(m, c, h, value):
        key = (m, c, h)
        pending[key] = pending[key] + value if key in pending else value

    def flush():
        for (m, c, h), value in pending.items():
            r = ((m * 8 + c) * halves + h) * SUB
            if (m, c, h) in seen:
                acc[r : r + SUB, :] += value
            else:
                seen.add((m, c, h))
                acc[r : r + SUB, :] = value
        pending.clear()

    def forward(m, d, h, q):
        for c in range(8):
            if d == 3:
                add(m, c, h, jnp.where(g.xcol == 0, g.lanes(q[c], 1 - NX), g.lanes(q[c], 1)))
            elif d == 2:
                add(m, c, h, g.lanes(q[c], NX))
            elif d == 1:
                add(m, c, h, g.rows(q[c], 1))
            elif h + 1 < halves:
                moved = g.rows(q[c], depth)
                add(m, c, h, jnp.where(g.row >= depth, moved, 0.0))
                add(m, c, h + 1, jnp.where(g.row < depth, moved, 0.0))
            else:
                add(m, c, h, g.rows(q[c], depth))

    def masked(mask, a):
        return [[[pick(mask, 0.0, v) for v in line] for line in part] for part in a]

    def inner(mu, nu, h):
        own = matrix(lambda *c: load(mu, *c, h))
        side = matrix(lambda *c: load(nu, *c, h))
        a = product(
            matrix(lambda *c: rolled(nu, mu, h, *c)),
            matrix(lambda *c: rolled(mu, nu, h, *c)),
            right_h=True,
        )
        mask = None
        for d in (mu, nu):
            if not complete(d, h):
                mask = top(d) if mask is None else jnp.logical_or(mask, top(d))
        a = masked(mask, a)
        b = product(own, side, left_h=True)
        forward(mu, nu, h, projected(a, b, left_h=True))
        forward(nu, mu, h, projected(a, b, right_h=True))
        upper = projected(product(own, a), side, right_h=True)
        for c in range(8):
            add(mu, c, h, upper[c])
            add(nu, c, h, -upper[c])

    def corners(d, among):
        for s in range(len(LAYOUT[d])):
            mask = open_mask(d, s, among)
            if mask is None:
                continue
            n = sets.index((d, s))

            def corner(m, h, c):
                if m not in among or complete(m, h):
                    return None
                k = LAYOUT[m][0].index((d, 0 if m == 0 else h))
                return shifted(m, fetch(in_s, "x", m, 0, *c), last[m] - k)

            for c in comps:
                value = pack(d, s, lambda m, h: corner(m, h, c), True)
                face_s[(n, 2, *c)] = jnp.where(mask, value, face_s[(n, 2, *c)])

    def face_terms(d, closed):
        for s, spots in enumerate(LAYOUT[d]):
            n = sets.index((d, s))
            own, side, over = (kept(d, s, q) for q in range(3))
            a = product(fetched(in_s, "x", d, s), over, right_h=True)
            a = masked(open_mask(d, s, [m for m in range(3) if m not in closed]), a)
            b = matrix(lambda *c: b_s[(n, *c)])
            upper = projected(product(own, a), side, right_h=True)
            low = projected(a, b, left_h=True)
            mask = open_mask(d, s, closed)
            low = [pick(mask, 0.0, v) for v in low]
            for k, (m, h) in enumerate(spots):
                h = half(d, h, True)
                natural = lambda v: jnp.where(top(d), shifted(d, v, last[d] - k), 0.0)
                for c in range(8):
                    x = natural(upper[c])
                    add(d, c, h, x)
                    add(m, c, h, -x)
                forward(d, m, h, [natural(v) for v in low])
        flush()

    def prepare(d):
        for s in range(len(LAYOUT[d])):
            own = fetched(out_s, "x", d, s)
            mask = open_mask(d, s)
            if mask is not None:
                far = packed(
                    d, s,
                    lambda m, h, *c: None if complete(m, h if d else 1) else edge(d, m, h, *c),
                    False,
                )
                both = product(own, far, right_h=True)
                own = [
                    [[jnp.where(mask, both[p][i][j], own[p][i][j]) for j in range(3)] for i in range(3)]
                    for p in range(2)
                ]
            save(pre_s, (sets.index((d, s)),), own)

    def close(d):
        for s, spots in enumerate(LAYOUT[d]):
            n = sets.index((d, s))
            q = projected(
                matrix(lambda *c: pre_s[(n, *c)]), fetched(in_s, "g", d, s), right_h=True
            )
            for k, (m, h) in enumerate(spots):
                for c in range(8):
                    add(m, c, half(d, h, False), jnp.where(bottom(d), shifted(d, q[c], -k), 0.0))
        flush()

    for n, pair in enumerate(PLANES):
        if n == 2:
            pl.semaphore_wait(met, 1)

            @pl.when(rest_t)
            def _():
                edges[1].start()

        for h in range(halves):
            inner(*pair, h)
        flush()

    @pl.when(first_t)
    def _():
        pl.semaphore_wait(met_t, 1)
        for copy in (edges[3], edges[1], faces[0]):
            copy.start()

    @pl.when(early)
    def _():
        pl.semaphore_wait(met_t, 1)
        edges[3].start()

    @pl.when(first_z)
    def _():
        pl.semaphore_wait(met_z, 1)
        edges[5].start()
        faces[1].start()

    @pl.when(jnp.logical_and(first_z, more_t))
    def _():
        edges[2].start()

    faces[2].wait_recv()
    face_terms(2, ())
    corners(0, (2,))
    faces[0].wait_recv()
    face_terms(0, (2,))
    corners(1, (0, 2))

    def close_all():
        for d in (2, 1, 0):
            arrivals[d].wait_recv()
            prepare(d)
            close(d)

    def face_z():
        faces[1].wait_recv()
        face_terms(1, (0, 2))

    @pl.when(last_z)
    def _():
        close_all()
        face_z()

    @pl.when(more_z)
    def _():
        face_z()
        close_all()

    everything.wait_send()


def expand(halves, acc, hbm, out, sem):
    for m in range(4):
        for h in range(halves):
            rows = [((m * 8 + c) * halves + h) * SUB for c in range(8)]
            f = [acc[r : r + SUB, :] * (COEFF * 0.5 if c < 6 else COEFF) for c, r in enumerate(rows)]

            def put(part, i, j, value):
                out[m, part, i, j, h * SUB : (h + 1) * SUB, :] = value

            for n, (i, j) in enumerate(((0, 1), (0, 2), (1, 2))):
                put(0, i, j, f[n])
                put(0, j, i, -f[n])
                put(1, i, j, f[3 + n])
                put(1, j, i, f[3 + n])
            for i in range(3):
                put(0, i, i, jnp.zeros((SUB, LANES), jnp.float32))
            put(1, 0, 0, f[6])
            put(1, 1, 1, f[7])
            put(1, 2, 2, -(f[6] + f[7]))
        for part in range(2):
            for i in range(3):
                pltpu.make_async_copy(out.at[m, part, i], hbm.at[m, part, i], sem).start()
    pltpu.make_async_copy(out, hbm, sem).wait()


def per_device(counts, links):
    time_len, depth, flat = links.shape[4:]
    sites = time_len * depth
    assert flat == LANES and (time_len, depth) == (4, 4)
    halves = sites // SUB
    vmem = lambda *s: pltpu.VMEM(s + (LANES,), jnp.float32)
    shape = links.shape[:4] + (sites, flat)
    terms = pl.pallas_call(
        functools.partial(force_terms, counts, depth, halves),
        out_shape=pltpu.VMEM((32 * sites, flat), jnp.float32),
        in_specs=[pl.BlockSpec(memory_space=pl.ANY)],
        out_specs=pl.BlockSpec(memory_space=pltpu.VMEM),
        scratch_shapes=[
            vmem(*shape[:-1]),
            vmem(TOTAL),
            vmem(TOTAL),
            vmem(5, 3, 2, 2, 3, SUB),
            vmem(5, 2, 3, 3, SUB),
            vmem(5, 2, 3, 3, SUB),
            pltpu.SemaphoreType.DMA,
            pltpu.SemaphoreType.DMA((6,)),
            pltpu.SemaphoreType.REGULAR,
            pltpu.SemaphoreType.REGULAR,
            pltpu.SemaphoreType.REGULAR,
        ],
        compiler_params=pltpu.CompilerParams(collective_id=0, has_side_effects=True),
        name="force_terms",
    )(links.reshape(shape))
    out = pl.pallas_call(
        functools.partial(expand, halves),
        out_shape=jax.ShapeDtypeStruct(shape, jnp.float32),
        in_specs=[pl.BlockSpec(memory_space=pltpu.VMEM)],
        out_specs=pl.BlockSpec(memory_space=pl.ANY),
        scratch_shapes=[vmem(*shape[:-1]), pltpu.SemaphoreType.DMA],
        name="expand",
    )(pltpu.with_memory_space_constraint(terms, pltpu.VMEM))
    return out.reshape(links.shape)


def solution(mesh):
    assert mesh.axis_names == ("gx", "gz", "ta")
    counts = tuple(mesh.shape[a] for a in AXES)
    spec = P(None, None, None, None, "ta", "gz", "gx")
    return jax.shard_map(
        functools.partial(per_device, counts),
        mesh=mesh,
        in_specs=(spec,),
        out_specs=spec,
        check_vma=False,
    )
```

```python
import functools

import jax
import jax.numpy as jnp
from jax import lax
from jax.experimental import pallas as pl
from jax.experimental.pallas import tpu as pltpu
from jax.sharding import PartitionSpec as P

NX = 16
COEFF = -1.9
AXES = ("ta", "gz", "gx")
SUB, LANES = 8, 128


def others(d):
    return [m for m in range(4) if m != d]


class Lattice:
    def __init__(self, depth):
        self.depth = depth
        self.per = SUB // depth
        self.ygroups = LANES // NX
        self.row = lax.broadcasted_iota(jnp.int32, (SUB, LANES), 0)
        self.lane = lax.broadcasted_iota(jnp.int32, (SUB, LANES), 1)
        self.zrow = self.row % depth
        self.xcol = self.lane % NX

    def rows(self, value, shift):
        shift %= SUB
        return pltpu.roll(value, shift, 0) if shift else value

    def lanes(self, value, shift):
        shift %= LANES
        return pltpu.roll(value, shift, 1) if shift else value


def entry(left, right, i, j, part, left_h, right_h):
    total = None
    for k in range(3):
        li = (k, i) if left_h else (i, k)
        ri = (j, k) if right_h else (k, j)
        lr, lm = left[0][li[0]][li[1]], left[1][li[0]][li[1]]
        rr, rm = right[0][ri[0]][ri[1]], right[1][ri[0]][ri[1]]
        if part == 0:
            first, second = lr * rr, lm * rm
            minus = left_h == right_h
        elif left_h:
            first, second = lr * rm, lm * rr
            minus = True
        else:
            first, second = lm * rr, lr * rm
            minus = right_h
        value = first - second if minus else first + second
        total = value if total is None else total + value
    return total


def product(left, right, left_h=False, right_h=False):
    return [
        [[entry(left, right, i, j, part, left_h, right_h) for j in range(3)] for i in range(3)]
        for part in range(2)
    ]


def projected(left, right, left_h=False, right_h=False):
    get = lambda i, j, part: entry(left, right, i, j, part, left_h, right_h)
    pairs = ((0, 1), (0, 2), (1, 2))
    real = [get(i, j, 0) - get(j, i, 0) for i, j in pairs]
    imag = [get(i, j, 1) + get(j, i, 1) for i, j in pairs]
    diag = [get(i, i, 1) for i in range(3)]
    third = (diag[0] + diag[1] + diag[2]) * (1.0 / 3.0)
    return real + imag + [diag[0] - third, diag[1] - third]


def third_row(real, imag):
    rows_r, rows_i = [], []
    for column in range(3):
        n, l = (column + 1) % 3, (column + 2) % 3
        rows_r.append(
            real[0][n] * real[1][l]
            - imag[0][n] * imag[1][l]
            - real[0][l] * real[1][n]
            + imag[0][l] * imag[1][n]
        )
        rows_i.append(
            real[0][l] * imag[1][n]
            + imag[0][l] * real[1][n]
            - real[0][n] * imag[1][l]
            - imag[0][n] * real[1][l]
        )
    return rows_r, rows_i


PLANES = ((0, 1), (0, 2), (0, 3), (1, 2), (1, 3), (2, 3))
DIAGONALS = ((0, 2), (2, 0), (0, 1), (1, 0), (1, 2), (2, 1))
LAYOUT = (
    (((1, 0), (2, 0)), ((3, 0),)),
    (((0, 0), (0, 1), (2, 0), (2, 1)), ((3, 0), (3, 1))),
    (((0, 0), (0, 1), (1, 0), (1, 1), (3, 0), (3, 1)),),
)
ROWS = (144, 144, 96)
EDGES = (8, 8, 16, 16, 8, 8)


def group_rows(d):
    return ROWS[d] + sum(rows for pair, rows in zip(DIAGONALS, EDGES) if pair[0] == d)


def offset(kind, d):
    if kind == "x":
        return sum(ROWS[:d])
    if kind == "g":
        return sum(ROWS) + sum(group_rows(k) for k in range(d))
    own = DIAGONALS[d][0]
    before = sum(EDGES[k] for k in range(d) if DIAGONALS[k][0] == own)
    return offset("g", own) + ROWS[own] + before


TOTAL = sum(ROWS) + sum(group_rows(d) for d in range(3))


def force_terms(
    counts, depth, halves, hbm, acc, u, out_s, in_s, face_s, b_s, pre_s, send, recv, met, met_t, met_z,
):
    g = Lattice(depth)
    me = [lax.axis_index(a) for a in AXES]
    comps = [(part, i, j) for part in range(2) for i in range(2) for j in range(3)]
    last = (g.per - 1, depth - 1, g.ygroups - 1)
    place = (g.row // depth, g.zrow, g.lane // NX)

    def device(*steps):
        where = list(me)
        for i, step in steps:
            where[i] = lax.rem(me[i] + (step + counts[i]), counts[i])
        by = dict(zip(AXES, where))
        return (by["gx"], by["gz"], by["ta"])

    barrier = pltpu.get_barrier_semaphore()
    first_t, last_t = me[0] == 0, me[0] == counts[0] - 1
    more_t, rest_t = jnp.logical_not(last_t), jnp.logical_not(first_t)
    middle = counts[1] // 2
    first_z = jnp.logical_or(me[1] == 0, jnp.logical_and(me[1] == middle, last_t))
    last_z = jnp.logical_or(
        me[1] == counts[1] - 1, jnp.logical_and(me[1] == middle - 1, last_t)
    )
    silent = jnp.logical_and(me[1] == counts[1] - 1, rest_t)
    more_z, rest_z = jnp.logical_not(last_z), jnp.logical_not(first_z)
    early = jnp.logical_and(me[1] == middle - 1, last_t)
    late = jnp.logical_and(me[1] == middle, me[0] == counts[0] - 2)
    vouch = jnp.logical_and(me[1] == middle - 1, me[0] == counts[0] - 2)
    one = lambda flag: jnp.where(flag, 1, 0)

    def signal(semaphore, *steps):
        pl.semaphore_signal(
            semaphore, inc=1, device_id=device(*steps), device_id_type=pl.DeviceIdType.MESH
        )

    for steps in (((1, -1),), ((2, 1), (1, -1)), ((0, -1), (2, 1)), ((0, -1),), ((2, 1),), ((2, -1),)):
        signal(barrier, *steps)

    @pl.when(more_z)
    def _():
        signal(barrier, (1, 1))
        signal(barrier, (1, 1), (2, -1))

    @pl.when(jnp.logical_not(silent))
    def _():
        signal(barrier, (1, 1), (0, -1))

    @pl.when(more_t)
    def _():
        signal(barrier, (0, 1))

    @pl.when(jnp.logical_not(jnp.logical_or(last_t, late)))
    def _():
        signal(barrier, (0, 1), (1, -1))

    expected = 11 - 2 * one(first_t) - 2 * one(first_z) - one(jnp.logical_and(first_z, more_t))
    expected = expected - one(early)

    loads = [
        pltpu.make_async_copy(hbm.at[m, part, i], u.at[m, part, i], send)
        for m in range(4)
        for part in range(2)
        for i in range(3)
    ]
    for copy in loads:
        copy.start()

    def remote(start, rows, slot, where):
        span = slice(start, start + rows)
        return pltpu.make_async_remote_copy(
            src_ref=out_s.at[span], dst_ref=in_s.at[span], send_sem=send, recv_sem=recv.at[slot],
            device_id=where, device_id_type=pl.DeviceIdType.MESH,
        )

    faces = [remote(offset("x", d), ROWS[d], d, device((d, -1))) for d in range(3)]
    opens = [remote(offset("g", d), ROWS[d], 3 + d, device((d, 1))) for d in range(3)]
    edges = [
        remote(offset("e", k), EDGES[k], 3 + d, device((d, 1), (n, -1)))
        for k, (d, n) in enumerate(DIAGONALS)
    ]
    arrivals = [remote(offset("g", d), group_rows(d), 3 + d, device((1, 1))) for d in range(3)]
    everything = remote(0, TOTAL, 0, device((1, 1)))

    def load(m, part, i, j, h):
        return u[m, part, i, j, h * SUB : (h + 1) * SUB, :]

    def shifted(d, value, steps):
        if d == 0:
            return g.rows(value, depth * steps)
        return g.rows(value, steps) if d == 1 else g.lanes(value, NX * steps)

    def half(d, h, top):
        return (halves - 1 if top else 0) if d == 0 else h

    def complete(d, h):
        return d == 3 or (d == 0 and h + 1 < halves)

    def top(d, h=1):
        if d == 0:
            return g.row >= SUB - depth
        return g.zrow == depth - 1 if d == 1 else g.lane >= LANES - NX

    def bottom(d):
        return (g.row < depth, g.zrow == 0, g.lane < NX)[d]

    def open_mask(d, s, among=(0, 1, 2)):
        mask = None
        for k, (m, h) in enumerate(LAYOUT[d][s]):
            if m in among and not complete(m, h if d else 1):
                here = jnp.logical_and(place[d] == k, top(m))
                mask = here if mask is None else jnp.logical_or(mask, here)
        return mask

    def pick(mask, yes, no):
        return no if mask is None else jnp.where(mask, yes, no)

    def pack(d, s, get, up):
        value = None
        for k, (m, h) in enumerate(LAYOUT[d][s]):
            x = get(m, half(d, h, up))
            if x is None:
                continue
            x = shifted(d, x, k - (last[d] if up else 0))
            value = x if value is None else jnp.where(place[d] >= k, x, value)
        return value

    def complete_rows(get):
        real = [[get(0, i, j) for j in range(3)] for i in range(2)]
        imag = [[get(1, i, j) for j in range(3)] for i in range(2)]
        third_r, third_i = third_row(real, imag)
        return [real + [third_r], imag + [third_i]]

    def packed(d, s, get, up):
        return complete_rows(
            lambda part, i, j: pack(d, s, lambda m, h: get(m, h, part, i, j), up)
        )

    def put(kind, d, s, value):
        r = offset(kind, d)
        used = len(LAYOUT[d][s])
        for n, (part, i, j) in enumerate(comps[: 6 if s else 12]):
            v = value[part][i][j]
            if s:
                v = jnp.where(place[d] < used, v, shifted(d, value[1][i][j], used))
            at = r + (96 if s else 0) + n * SUB
            out_s[at : at + SUB, :] = v

    def fetch(ref, kind, d, s, part, i, j):
        n = part * 6 + i * 3 + j
        at = offset(kind, d) + n * SUB
        if not s:
            return ref[at : at + SUB, :]
        at += 96 - part * 6 * SUB
        v = ref[at : at + SUB, :]
        return shifted(d, v, -len(LAYOUT[d][s])) if part else v

    def fetched(ref, kind, d, s):
        return complete_rows(lambda part, i, j: fetch(ref, kind, d, s, part, i, j))

    def rolled(m, d, h, part, i, j):
        v = load(m, part, i, j, h)
        if d == 3:
            return jnp.where(g.xcol == NX - 1, g.lanes(v, NX - 1), g.lanes(v, -1))
        if d == 2:
            return g.lanes(v, -NX)
        if d == 1:
            return g.rows(v, -1)
        if h + 1 < halves:
            beyond = g.rows(load(m, part, i, j, h + 1), -depth)
            return jnp.where(g.row >= SUB - depth, beyond, g.rows(v, -depth))
        return g.rows(v, -depth)

    def matrix(get):
        return [[[get(part, i, j) for j in range(3)] for i in range(3)] for part in range(2)]

    def save(ref, index, value):
        for part in range(2):
            for i in range(ref.shape[-4]):
                for j in range(3):
                    ref[(*index, part, i, j)] = value[part][i][j]

    sets = [(d, s) for d in range(3) for s in range(len(LAYOUT[d]))]

    def kept(d, s, q):
        n = sets.index((d, s))
        return complete_rows(lambda part, i, j: face_s[n, q, part, i, j])

    def own_face(d):
        def get(part, i, j):
            if d != 2:
                return pack(d, 0, lambda m, h: load(d, part, i, j, h), True)
            pair = [shifted(d, load(d, part, i, j, h), h - last[d]) for h in range(halves)]
            pair = jnp.where(place[d] >= 1, pair[1], pair[0])
            value = jnp.where(place[d] >= 2, shifted(d, pair, 2), pair)
            return jnp.where(place[d] >= 4, shifted(d, pair, 4), value)

        return complete_rows(get)

    def step_in_face(d, m, v):
        if m == 3:
            return jnp.where(g.xcol == NX - 1, g.lanes(v, NX - 1), g.lanes(v, -1))
        if m == 2:
            return g.lanes(v, -NX)
        if m == 1:
            return g.rows(v, -1)
        moved = g.rows(v, -depth)
        if d == 1:
            beyond = g.rows(v, depth - 1)
            return jnp.where(jnp.logical_and(g.zrow == 0, g.row >= depth), beyond, moved)
        return jnp.where(g.row >= depth, g.lanes(moved, -NX), moved)

    def over_face(d, s, own):
        def get(part, i, j):
            value, before = None, None
            for k, (m, h) in enumerate(LAYOUT[d][s]):
                if m == before:
                    continue
                x = step_in_face(d, m, own[part][i][j])
                value = x if value is None else jnp.where(place[d] >= k, x, value)
                before = m
            return value

        return complete_rows(get)

    def send_side(d):
        own = own_face(d)
        for s in range(len(LAYOUT[d])):
            n = sets.index((d, s))
            side = packed(d, s, lambda m, h, *c: load(m, *c, h), True)
            over = over_face(d, s, own)
            b = product(own, side, left_h=True)
            mask = open_mask(d, s)
            put("g", d, s, [
                [
                    [pick(mask, b[p][i][j], entry(b, over, i, j, p, False, False)) for j in range(3)]
                    for i in range(2)
                ]
                for p in range(2)
            ])
            for q, value in enumerate((own, side, over)):
                save(face_s, (n, q), value)
            save(b_s, (n,), b)

    def send_face(d):
        for s in range(len(LAYOUT[d])):
            put("x", d, s, [
                [
                    [pack(d, s, lambda m, h: load(m, p, i, j, h), False) for j in range(3)]
                    for i in range(2)
                ]
                for p in range(2)
            ])

    def pack_edges(d, n):
        r0 = offset("e", DIAGONALS.index((d, n)))
        if 2 not in (d, n):
            for c0 in range(0, 12, SUB):
                value = None
                for k in range(min(SUB, 12 - c0)):
                    v = load(d, *comps[c0 + k], halves - 1 if d == 0 else 0)
                    x = g.rows(v, k - depth if d == 0 else k - (depth - 1))
                    value = x if value is None else jnp.where(g.row >= k, x, value)
                out_s[r0 + c0 : r0 + c0 + SUB, :] = value
            return
        value = None
        for k in range(g.ygroups):
            v = dense_rows(d, n, comps[k])
            if k + g.ygroups < 12:
                w = dense_rows(d, n, comps[k + g.ygroups])
                step, mask = spare(d, n)
                v = jnp.where(mask, v, g.rows(w, step))
            x = g.lanes(v, NX * (k + (1 if d == 2 else 0)))
            value = x if value is None else jnp.where(g.lane >= NX * k, x, value)
        out_s[r0 : r0 + SUB, :] = value

    def spare(d, n):
        if (d, n) == (0, 2):
            return depth, g.row >= depth
        if (d, n) == (2, 0):
            return depth, g.row < depth
        return (-2, g.zrow >= 2) if d == 1 else (2, g.zrow < 2)

    def dense_rows(d, n, c):
        if 0 in (d, n):
            return load(d, *c, halves - 1 if d == 0 else 0)
        at = depth - 1 if d == 1 else 0
        step = -1 if d == 1 else 1
        v = load(d, *c, 0)
        for h in range(1, halves):
            v = jnp.where(g.zrow == at + step * h, g.rows(load(d, *c, h), step * h), v)
        return v

    def edge(d, n, h, part, i, j):
        c = part * 6 + i * 3 + j
        r = offset("e", DIAGONALS.index((d, n)))
        if 2 not in (d, n):
            v = in_s[r + c // SUB * SUB : r + c // SUB * SUB + SUB, :]
            k = c % SUB
            return g.rows(v, depth - 1 - k if d == 0 else SUB - depth - k)
        k, back = c % g.ygroups, c >= g.ygroups
        v = g.lanes(in_s[r : r + SUB, :], NX * ((0 if d == 2 else g.ygroups - 1) - k))
        step = -spare(d, n)[0] if back else 0
        if (d, n) == (0, 2):
            return g.rows(v, step - (SUB - depth))
        if (d, n) == (2, 0):
            return g.rows(v, step + SUB - depth)
        return g.rows(v, step + (1 - depth + h if d == 1 else depth - 1 - h))

    everything_in = pltpu.make_async_copy(hbm, u, send)
    everything_in.wait()
    for d, n in DIAGONALS:
        pack_edges(d, n)
    for d in (1, 0):
        send_side(d)
        send_face(d)
    send_face(2)
    pl.semaphore_wait(barrier, expected)
    signal(met, (2, -1))

    @pl.when(jnp.logical_or(last_t, vouch))
    def _():
        signal(met_t, (0, 1))

    @pl.when(last_z)
    def _():
        signal(met_z, (1, 1))

    @pl.when(jnp.logical_or(rest_z, last_t))
    def _():
        edges[2].start()

    for copy in (edges[4], edges[0]):
        copy.start()

    @pl.when(jnp.logical_not(jnp.logical_or(first_t, early)))
    def _():
        edges[3].start()

    @pl.when(rest_z)
    def _():
        edges[5].start()

    for copy in (opens[0], opens[1]):
        copy.start()

    @pl.when(rest_t)
    def _():
        faces[0].start()

    @pl.when(rest_z)
    def _():
        faces[1].start()

    faces[2].start()
    send_side(2)
    opens[2].start()

    seen, pending = set(), {}

    def add(m, c, h, value):
        key = (m, c, h)
        pending[key] = pending[key] + value if key in pending else value

    def flush():
        for (m, c, h), value in pending.items():
            r = ((m * 8 + c) * halves + h) * SUB
            if (m, c, h) in seen:
                acc[r : r + SUB, :] += value
            else:
                seen.add((m, c, h))
                acc[r : r + SUB, :] = value
        pending.clear()

    def forward(m, d, h, q):
        for c in range(8):
            if d == 3:
                add(m, c, h, jnp.where(g.xcol == 0, g.lanes(q[c], 1 - NX), g.lanes(q[c], 1)))
            elif d == 2:
                add(m, c, h, g.lanes(q[c], NX))
            elif d == 1:
                add(m, c, h, g.rows(q[c], 1))
            elif h + 1 < halves:
                moved = g.rows(q[c], depth)
                add(m, c, h, jnp.where(g.row >= depth, moved, 0.0))
                add(m, c, h + 1, jnp.where(g.row < depth, moved, 0.0))
            else:
                add(m, c, h, g.rows(q[c], depth))

    def masked(mask, a):
        return [[[pick(mask, 0.0, v) for v in line] for line in part] for part in a]

    def inner(mu, nu, h):
        own = matrix(lambda *c: load(mu, *c, h))
        side = matrix(lambda *c: load(nu, *c, h))
        a = product(
            matrix(lambda *c: rolled(nu, mu, h, *c)),
            matrix(lambda *c: rolled(mu, nu, h, *c)),
            right_h=True,
        )
        mask = None
        for d in (mu, nu):
            if not complete(d, h):
                mask = top(d) if mask is None else jnp.logical_or(mask, top(d))
        a = masked(mask, a)
        b = product(own, side, left_h=True)
        forward(mu, nu, h, projected(a, b, left_h=True))
        forward(nu, mu, h, projected(a, b, right_h=True))
        upper = projected(product(own, a), side, right_h=True)
        for c in range(8):
            add(mu, c, h, upper[c])
            add(nu, c, h, -upper[c])

    def corners(d, among):
        for s in range(len(LAYOUT[d])):
            mask = open_mask(d, s, among)
            if mask is None:
                continue
            n = sets.index((d, s))

            def corner(m, h, c):
                if m not in among or complete(m, h):
                    return None
                k = LAYOUT[m][0].index((d, 0 if m == 0 else h))
                return shifted(m, fetch(in_s, "x", m, 0, *c), last[m] - k)

            for c in comps:
                value = pack(d, s, lambda m, h: corner(m, h, c), True)
                face_s[(n, 2, *c)] = jnp.where(mask, value, face_s[(n, 2, *c)])

    def face_terms(d, closed):
        for s, spots in enumerate(LAYOUT[d]):
            n = sets.index((d, s))
            own, side, over = (kept(d, s, q) for q in range(3))
            a = product(fetched(in_s, "x", d, s), over, right_h=True)
            a = masked(open_mask(d, s, [m for m in range(3) if m not in closed]), a)
            b = matrix(lambda *c: b_s[(n, *c)])
            upper = projected(product(own, a), side, right_h=True)
            low = projected(a, b, left_h=True)
            mask = open_mask(d, s, closed)
            low = [pick(mask, 0.0, v) for v in low]
            for k, (m, h) in enumerate(spots):
                h = half(d, h, True)
                natural = lambda v: jnp.where(top(d), shifted(d, v, last[d] - k), 0.0)
                for c in range(8):
                    x = natural(upper[c])
                    add(d, c, h, x)
                    add(m, c, h, -x)
                forward(d, m, h, [natural(v) for v in low])
        flush()

    def prepare(d):
        for s in range(len(LAYOUT[d])):
            own = fetched(out_s, "x", d, s)
            mask = open_mask(d, s)
            if mask is not None:
                far = packed(
                    d, s,
                    lambda m, h, *c: None if complete(m, h if d else 1) else edge(d, m, h, *c),
                    False,
                )
                both = product(own, far, right_h=True)
                own = [
                    [[jnp.where(mask, both[p][i][j], own[p][i][j]) for j in range(3)] for i in range(3)]
                    for p in range(2)
                ]
            save(pre_s, (sets.index((d, s)),), own)

    def close(d):
        for s, spots in enumerate(LAYOUT[d]):
            n = sets.index((d, s))
            q = projected(
                matrix(lambda *c: pre_s[(n, *c)]), fetched(in_s, "g", d, s), right_h=True
            )
            for k, (m, h) in enumerate(spots):
                for c in range(8):
                    add(m, c, half(d, h, False), jnp.where(bottom(d), shifted(d, q[c], -k), 0.0))
        flush()

    for n, pair in enumerate(PLANES):
        if n == 2:
            pl.semaphore_wait(met, 1)

            @pl.when(rest_t)
            def _():
                edges[1].start()

        for h in range(halves):
            inner(*pair, h)
        flush()

    @pl.when(first_t)
    def _():
        pl.semaphore_wait(met_t, 1)
        for copy in (edges[3], edges[1], faces[0]):
            copy.start()

    @pl.when(early)
    def _():
        pl.semaphore_wait(met_t, 1)
        edges[3].start()

    @pl.when(first_z)
    def _():
        pl.semaphore_wait(met_z, 1)
        edges[5].start()
        faces[1].start()

    @pl.when(jnp.logical_and(first_z, more_t))
    def _():
        edges[2].start()

    faces[2].wait_recv()
    face_terms(2, ())
    corners(0, (2,))
    faces[0].wait_recv()
    face_terms(0, (2,))
    corners(1, (0, 2))

    def close_all():
        for d in (2, 1, 0):
            arrivals[d].wait_recv()
            prepare(d)
            close(d)

    def face_z():
        faces[1].wait_recv()
        face_terms(1, (0, 2))

    @pl.when(last_z)
    def _():
        close_all()
        face_z()

    @pl.when(more_z)
    def _():
        face_z()
        close_all()

    everything.wait_send()


def expand(halves, acc, hbm, out, sem):
    for m in range(4):
        for h in range(halves):
            rows = [((m * 8 + c) * halves + h) * SUB for c in range(8)]
            f = [acc[r : r + SUB, :] * (COEFF * 0.5 if c < 6 else COEFF) for c, r in enumerate(rows)]

            def put(part, i, j, value):
                out[m, part, i, j, h * SUB : (h + 1) * SUB, :] = value

            for n, (i, j) in enumerate(((0, 1), (0, 2), (1, 2))):
                put(0, i, j, f[n])
                put(0, j, i, -f[n])
                put(1, i, j, f[3 + n])
                put(1, j, i, f[3 + n])
            for i in range(3):
                put(0, i, i, jnp.zeros((SUB, LANES), jnp.float32))
            put(1, 0, 0, f[6])
            put(1, 1, 1, f[7])
            put(1, 2, 2, -(f[6] + f[7]))
        for part in range(2):
            for i in range(3):
                pltpu.make_async_copy(out.at[m, part, i], hbm.at[m, part, i], sem).start()
    pltpu.make_async_copy(out, hbm, sem).wait()


def per_device(counts, links):
    time_len, depth, flat = links.shape[4:]
    sites = time_len * depth
    assert flat == LANES and (time_len, depth) == (4, 4)
    halves = sites // SUB
    vmem = lambda *s: pltpu.VMEM(s + (LANES,), jnp.float32)
    shape = links.shape[:4] + (sites, flat)
    terms = pl.pallas_call(
        functools.partial(force_terms, counts, depth, halves),
        out_shape=pltpu.VMEM((32 * sites, flat), jnp.float32),
        in_specs=[pl.BlockSpec(memory_space=pl.ANY)],
        out_specs=pl.BlockSpec(memory_space=pltpu.VMEM),
        scratch_shapes=[
            vmem(*shape[:-1]),
            vmem(TOTAL),
            vmem(TOTAL),
            vmem(5, 3, 2, 2, 3, SUB),
            vmem(5, 2, 3, 3, SUB),
            vmem(5, 2, 3, 3, SUB),
            pltpu.SemaphoreType.DMA,
            pltpu.SemaphoreType.DMA((6,)),
            pltpu.SemaphoreType.REGULAR,
            pltpu.SemaphoreType.REGULAR,
            pltpu.SemaphoreType.REGULAR,
        ],
        compiler_params=pltpu.CompilerParams(collective_id=0, has_side_effects=True),
        name="force_terms",
    )(links.reshape(shape))
    out = pl.pallas_call(
        functools.partial(expand, halves),
        out_shape=jax.ShapeDtypeStruct(shape, jnp.float32),
        in_specs=[pl.BlockSpec(memory_space=pltpu.VMEM)],
        out_specs=pl.BlockSpec(memory_space=pl.ANY),
        scratch_shapes=[vmem(*shape[:-1]), pltpu.SemaphoreType.DMA],
        name="expand",
    )(pltpu.with_memory_space_constraint(terms, pltpu.VMEM))
    return out.reshape(links.shape)


def solution(mesh):
    assert mesh.axis_names == ("gx", "gz", "ta")
    counts = tuple(mesh.shape[a] for a in AXES)
    spec = P(None, None, None, None, "ta", "gz", "gx")
    return jax.shard_map(
        functools.partial(per_device, counts),
        mesh=mesh,
        in_specs=(spec,),
        out_specs=spec,
        check_vma=False,
    )
```

```python
import functools

import jax
import jax.numpy as jnp
from jax import lax
from jax.experimental import pallas as pl
from jax.experimental.pallas import tpu as pltpu
from jax.sharding import PartitionSpec as P

NX = 16
COEFF = -1.9
AXES = ("ta", "gz", "gx")
SUB, LANES = 8, 128


def others(d):
    return [m for m in range(4) if m != d]


class Lattice:
    def __init__(self, depth):
        self.depth = depth
        self.per = SUB // depth
        self.ygroups = LANES // NX
        self.row = lax.broadcasted_iota(jnp.int32, (SUB, LANES), 0)
        self.lane = lax.broadcasted_iota(jnp.int32, (SUB, LANES), 1)
        self.zrow = self.row % depth
        self.xcol = self.lane % NX

    def rows(self, value, shift):
        shift %= SUB
        return pltpu.roll(value, shift, 0) if shift else value

    def lanes(self, value, shift):
        shift %= LANES
        return pltpu.roll(value, shift, 1) if shift else value


def entry(left, right, i, j, part, left_h, right_h):
    total = None
    for k in range(3):
        li = (k, i) if left_h else (i, k)
        ri = (j, k) if right_h else (k, j)
        lr, lm = left[0][li[0]][li[1]], left[1][li[0]][li[1]]
        rr, rm = right[0][ri[0]][ri[1]], right[1][ri[0]][ri[1]]
        if part == 0:
            first, second = lr * rr, lm * rm
            minus = left_h == right_h
        elif left_h:
            first, second = lr * rm, lm * rr
            minus = True
        else:
            first, second = lm * rr, lr * rm
            minus = right_h
        value = first - second if minus else first + second
        total = value if total is None else total + value
    return total


def product(left, right, left_h=False, right_h=False):
    return [
        [[entry(left, right, i, j, part, left_h, right_h) for j in range(3)] for i in range(3)]
        for part in range(2)
    ]


def projected(left, right, left_h=False, right_h=False):
    get = lambda i, j, part: entry(left, right, i, j, part, left_h, right_h)
    pairs = ((0, 1), (0, 2), (1, 2))
    real = [get(i, j, 0) - get(j, i, 0) for i, j in pairs]
    imag = [get(i, j, 1) + get(j, i, 1) for i, j in pairs]
    diag = [get(i, i, 1) for i in range(3)]
    third = (diag[0] + diag[1] + diag[2]) * (1.0 / 3.0)
    return real + imag + [diag[0] - third, diag[1] - third]


def third_row(real, imag):
    rows_r, rows_i = [], []
    for column in range(3):
        n, l = (column + 1) % 3, (column + 2) % 3
        rows_r.append(
            real[0][n] * real[1][l]
            - imag[0][n] * imag[1][l]
            - real[0][l] * real[1][n]
            + imag[0][l] * imag[1][n]
        )
        rows_i.append(
            real[0][l] * imag[1][n]
            + imag[0][l] * real[1][n]
            - real[0][n] * imag[1][l]
            - imag[0][n] * real[1][l]
        )
    return rows_r, rows_i


PLANES = ((0, 1), (0, 2), (0, 3), (1, 2), (1, 3), (2, 3))
DIAGONALS = ((0, 2), (2, 0), (0, 1), (1, 0), (1, 2), (2, 1))
LAYOUT = (
    (((1, 0), (2, 0)), ((3, 0),)),
    (((0, 0), (0, 1), (2, 0), (2, 1)), ((3, 0), (3, 1))),
    (((0, 0), (0, 1), (1, 0), (1, 1), (3, 0), (3, 1)),),
)
ROWS = (144, 144, 96)
EDGES = (8, 8, 16, 16, 8, 8)


def group_rows(d):
    return ROWS[d] + sum(rows for pair, rows in zip(DIAGONALS, EDGES) if pair[0] == d)


def offset(kind, d):
    if kind == "x":
        return sum(ROWS[:d])
    if kind == "g":
        return sum(ROWS) + sum(group_rows(k) for k in range(d))
    own = DIAGONALS[d][0]
    before = sum(EDGES[k] for k in range(d) if DIAGONALS[k][0] == own)
    return offset("g", own) + ROWS[own] + before


TOTAL = sum(ROWS) + sum(group_rows(d) for d in range(3))


def force_terms(
    counts, depth, halves, hbm, acc, u, out_s, in_s, face_s, b_s, pre_s, send, recv, met, met_t, met_z,
):
    g = Lattice(depth)
    me = [lax.axis_index(a) for a in AXES]
    comps = [(part, i, j) for part in range(2) for i in range(2) for j in range(3)]
    last = (g.per - 1, depth - 1, g.ygroups - 1)
    place = (g.row // depth, g.zrow, g.lane // NX)

    def device(*steps):
        where = list(me)
        for i, step in steps:
            where[i] = lax.rem(me[i] + (step + counts[i]), counts[i])
        by = dict(zip(AXES, where))
        return (by["gx"], by["gz"], by["ta"])

    barrier = pltpu.get_barrier_semaphore()
    first_t, last_t = me[0] == 0, me[0] == counts[0] - 1
    more_t, rest_t = jnp.logical_not(last_t), jnp.logical_not(first_t)
    middle = counts[1] // 2
    first_z = jnp.logical_or(me[1] == 0, jnp.logical_and(me[1] == middle, last_t))
    last_z = jnp.logical_or(
        me[1] == counts[1] - 1, jnp.logical_and(me[1] == middle - 1, last_t)
    )
    silent = jnp.logical_and(me[1] == counts[1] - 1, rest_t)
    more_z, rest_z = jnp.logical_not(last_z), jnp.logical_not(first_z)
    early = jnp.logical_and(me[1] == middle - 1, last_t)
    late = jnp.logical_and(me[1] == middle, me[0] == counts[0] - 2)
    vouch = jnp.logical_and(me[1] == middle - 1, me[0] == counts[0] - 2)
    one = lambda flag: jnp.where(flag, 1, 0)

    def signal(semaphore, *steps):
        pl.semaphore_signal(
            semaphore, inc=1, device_id=device(*steps), device_id_type=pl.DeviceIdType.MESH
        )

    for steps in (((1, -1),), ((2, 1), (1, -1)), ((0, -1), (2, 1)), ((0, -1),), ((2, 1),), ((2, -1),)):
        signal(barrier, *steps)

    @pl.when(more_z)
    def _():
        signal(barrier, (1, 1))
        signal(barrier, (1, 1), (2, -1))

    @pl.when(jnp.logical_not(silent))
    def _():
        signal(barrier, (1, 1), (0, -1))

    @pl.when(more_t)
    def _():
        signal(barrier, (0, 1))

    @pl.when(jnp.logical_not(jnp.logical_or(last_t, late)))
    def _():
        signal(barrier, (0, 1), (1, -1))

    expected = 11 - 2 * one(first_t) - 2 * one(first_z) - one(jnp.logical_and(first_z, more_t))
    expected = expected - one(early)

    loads = [
        pltpu.make_async_copy(hbm.at[m, part, i], u.at[m, part, i], send)
        for m in range(4)
        for part in range(2)
        for i in range(3)
    ]
    for copy in loads:
        copy.start()

    def remote(start, rows, slot, where):
        span = slice(start, start + rows)
        return pltpu.make_async_remote_copy(
            src_ref=out_s.at[span], dst_ref=in_s.at[span], send_sem=send, recv_sem=recv.at[slot],
            device_id=where, device_id_type=pl.DeviceIdType.MESH,
        )

    faces = [remote(offset("x", d), ROWS[d], d, device((d, -1))) for d in range(3)]
    opens = [remote(offset("g", d), ROWS[d], 3 + d, device((d, 1))) for d in range(3)]
    edges = [
        remote(offset("e", k), EDGES[k], 3 + d, device((d, 1), (n, -1)))
        for k, (d, n) in enumerate(DIAGONALS)
    ]
    arrivals = [remote(offset("g", d), group_rows(d), 3 + d, device((1, 1))) for d in range(3)]
    everything = remote(0, TOTAL, 0, device((1, 1)))

    def load(m, part, i, j, h):
        return u[m, part, i, j, h * SUB : (h + 1) * SUB, :]

    def shifted(d, value, steps):
        if d == 0:
            return g.rows(value, depth * steps)
        return g.rows(value, steps) if d == 1 else g.lanes(value, NX * steps)

    def half(d, h, top):
        return (halves - 1 if top else 0) if d == 0 else h

    def complete(d, h):
        return d == 3 or (d == 0 and h + 1 < halves)

    def top(d, h=1):
        if d == 0:
            return g.row >= SUB - depth
        return g.zrow == depth - 1 if d == 1 else g.lane >= LANES - NX

    def bottom(d):
        return (g.row < depth, g.zrow == 0, g.lane < NX)[d]

    def open_mask(d, s, among=(0, 1, 2)):
        mask = None
        for k, (m, h) in enumerate(LAYOUT[d][s]):
            if m in among and not complete(m, h if d else 1):
                here = jnp.logical_and(place[d] == k, top(m))
                mask = here if mask is None else jnp.logical_or(mask, here)
        return mask

    def pick(mask, yes, no):
        return no if mask is None else jnp.where(mask, yes, no)

    def pack(d, s, get, up):
        value = None
        for k, (m, h) in enumerate(LAYOUT[d][s]):
            x = get(m, half(d, h, up))
            if x is None:
                continue
            x = shifted(d, x, k - (last[d] if up else 0))
            value = x if value is None else jnp.where(place[d] >= k, x, value)
        return value

    def complete_rows(get):
        real = [[get(0, i, j) for j in range(3)] for i in range(2)]
        imag = [[get(1, i, j) for j in range(3)] for i in range(2)]
        third_r, third_i = third_row(real, imag)
        return [real + [third_r], imag + [third_i]]

    def packed(d, s, get, up):
        return complete_rows(
            lambda part, i, j: pack(d, s, lambda m, h: get(m, h, part, i, j), up)
        )

    def put(kind, d, s, value):
        r = offset(kind, d)
        used = len(LAYOUT[d][s])
        for n, (part, i, j) in enumerate(comps[: 6 if s else 12]):
            v = value[part][i][j]
            if s:
                v = jnp.where(place[d] < used, v, shifted(d, value[1][i][j], used))
            at = r + (96 if s else 0) + n * SUB
            out_s[at : at + SUB, :] = v

    def fetch(ref, kind, d, s, part, i, j):
        n = part * 6 + i * 3 + j
        at = offset(kind, d) + n * SUB
        if not s:
            return ref[at : at + SUB, :]
        at += 96 - part * 6 * SUB
        v = ref[at : at + SUB, :]
        return shifted(d, v, -len(LAYOUT[d][s])) if part else v

    def fetched(ref, kind, d, s):
        return complete_rows(lambda part, i, j: fetch(ref, kind, d, s, part, i, j))

    def rolled(m, d, h, part, i, j):
        v = load(m, part, i, j, h)
        if d == 3:
            return jnp.where(g.xcol == NX - 1, g.lanes(v, NX - 1), g.lanes(v, -1))
        if d == 2:
            return g.lanes(v, -NX)
        if d == 1:
            return g.rows(v, -1)
        if h + 1 < halves:
            beyond = g.rows(load(m, part, i, j, h + 1), -depth)
            return jnp.where(g.row >= SUB - depth, beyond, g.rows(v, -depth))
        return g.rows(v, -depth)

    def matrix(get):
        return [[[get(part, i, j) for j in range(3)] for i in range(3)] for part in range(2)]

    def save(ref, index, value):
        for part in range(2):
            for i in range(ref.shape[-4]):
                for j in range(3):
                    ref[(*index, part, i, j)] = value[part][i][j]

    sets = [(d, s) for d in range(3) for s in range(len(LAYOUT[d]))]

    def kept(d, s, q):
        n = sets.index((d, s))
        return complete_rows(lambda part, i, j: face_s[n, q, part, i, j])

    def own_face(d):
        def get(part, i, j):
            if d != 2:
                return pack(d, 0, lambda m, h: load(d, part, i, j, h), True)
            pair = [shifted(d, load(d, part, i, j, h), h - last[d]) for h in range(halves)]
            pair = jnp.where(place[d] >= 1, pair[1], pair[0])
            value = jnp.where(place[d] >= 2, shifted(d, pair, 2), pair)
            return jnp.where(place[d] >= 4, shifted(d, pair, 4), value)

        return complete_rows(get)

    def step_in_face(d, m, v):
        if m == 3:
            return jnp.where(g.xcol == NX - 1, g.lanes(v, NX - 1), g.lanes(v, -1))
        if m == 2:
            return g.lanes(v, -NX)
        if m == 1:
            return g.rows(v, -1)
        moved = g.rows(v, -depth)
        if d == 1:
            beyond = g.rows(v, depth - 1)
            return jnp.where(jnp.logical_and(g.zrow == 0, g.row >= depth), beyond, moved)
        return jnp.where(g.row >= depth, g.lanes(moved, -NX), moved)

    def over_face(d, s, own):
        def get(part, i, j):
            value, before = None, None
            for k, (m, h) in enumerate(LAYOUT[d][s]):
                if m == before:
                    continue
                x = step_in_face(d, m, own[part][i][j])
                value = x if value is None else jnp.where(place[d] >= k, x, value)
                before = m
            return value

        return complete_rows(get)

    def send_side(d):
        own = own_face(d)
        for s in range(len(LAYOUT[d])):
            n = sets.index((d, s))
            side = packed(d, s, lambda m, h, *c: load(m, *c, h), True)
            over = over_face(d, s, own)
            b = product(own, side, left_h=True)
            mask = open_mask(d, s)
            put("g", d, s, [
                [
                    [pick(mask, b[p][i][j], entry(b, over, i, j, p, False, False)) for j in range(3)]
                    for i in range(2)
                ]
                for p in range(2)
            ])
            for q, value in enumerate((own, side, over)):
                save(face_s, (n, q), value)
            save(b_s, (n,), b)

    def send_face(d):
        for s in range(len(LAYOUT[d])):
            put("x", d, s, [
                [
                    [pack(d, s, lambda m, h: load(m, p, i, j, h), False) for j in range(3)]
                    for i in range(2)
                ]
                for p in range(2)
            ])

    def pack_edges(d, n):
        r0 = offset("e", DIAGONALS.index((d, n)))
        if 2 not in (d, n):
            for c0 in range(0, 12, SUB):
                value = None
                for k in range(min(SUB, 12 - c0)):
                    v = load(d, *comps[c0 + k], halves - 1 if d == 0 else 0)
                    x = g.rows(v, k - depth if d == 0 else k - (depth - 1))
                    value = x if value is None else jnp.where(g.row >= k, x, value)
                out_s[r0 + c0 : r0 + c0 + SUB, :] = value
            return
        value = None
        for k in range(g.ygroups):
            v = dense_rows(d, n, comps[k])
            if k + g.ygroups < 12:
                w = dense_rows(d, n, comps[k + g.ygroups])
                step, mask = spare(d, n)
                v = jnp.where(mask, v, g.rows(w, step))
            x = g.lanes(v, NX * (k + (1 if d == 2 else 0)))
            value = x if value is None else jnp.where(g.lane >= NX * k, x, value)
        out_s[r0 : r0 + SUB, :] = value

    def spare(d, n):
        if (d, n) == (0, 2):
            return depth, g.row >= depth
        if (d, n) == (2, 0):
            return depth, g.row < depth
        return (-2, g.zrow >= 2) if d == 1 else (2, g.zrow < 2)

    def dense_rows(d, n, c):
        if 0 in (d, n):
            return load(d, *c, halves - 1 if d == 0 else 0)
        at = depth - 1 if d == 1 else 0
        step = -1 if d == 1 else 1
        v = load(d, *c, 0)
        for h in range(1, halves):
            v = jnp.where(g.zrow == at + step * h, g.rows(load(d, *c, h), step * h), v)
        return v

    def edge(d, n, h, part, i, j):
        c = part * 6 + i * 3 + j
        r = offset("e", DIAGONALS.index((d, n)))
        if 2 not in (d, n):
            v = in_s[r + c // SUB * SUB : r + c // SUB * SUB + SUB, :]
            k = c % SUB
            return g.rows(v, depth - 1 - k if d == 0 else SUB - depth - k)
        k, back = c % g.ygroups, c >= g.ygroups
        v = g.lanes(in_s[r : r + SUB, :], NX * ((0 if d == 2 else g.ygroups - 1) - k))
        step = -spare(d, n)[0] if back else 0
        if (d, n) == (0, 2):
            return g.rows(v, step - (SUB - depth))
        if (d, n) == (2, 0):
            return g.rows(v, step + SUB - depth)
        return g.rows(v, step + (1 - depth + h if d == 1 else depth - 1 - h))

    everything_in = pltpu.make_async_copy(hbm, u, send)
    everything_in.wait()
    for d, n in DIAGONALS:
        pack_edges(d, n)
    for d in (1, 0):
        send_side(d)
        send_face(d)
    send_face(2)
    pl.semaphore_wait(barrier, expected)
    signal(met, (2, -1))

    @pl.when(jnp.logical_or(last_t, vouch))
    def _():
        signal(met_t, (0, 1))

    @pl.when(last_z)
    def _():
        signal(met_z, (1, 1))

    @pl.when(jnp.logical_or(rest_z, last_t))
    def _():
        edges[2].start()

    for copy in (edges[4], edges[0], faces[2]):
        copy.start()

    @pl.when(jnp.logical_not(jnp.logical_or(first_t, early)))
    def _():
        edges[3].start()

    @pl.when(rest_z)
    def _():
        edges[5].start()

    for copy in (opens[0], opens[1]):
        copy.start()

    @pl.when(rest_t)
    def _():
        faces[0].start()

    @pl.when(rest_z)
    def _():
        faces[1].start()

    send_side(2)
    opens[2].start()

    seen, pending = set(), {}

    def add(m, c, h, value):
        key = (m, c, h)
        pending[key] = pending[key] + value if key in pending else value

    def flush():
        for (m, c, h), value in pending.items():
            r = ((m * 8 + c) * halves + h) * SUB
            if (m, c, h) in seen:
                acc[r : r + SUB, :] += value
            else:
                seen.add((m, c, h))
                acc[r : r + SUB, :] = value
        pending.clear()

    def forward(m, d, h, q):
        for c in range(8):
            if d == 3:
                add(m, c, h, jnp.where(g.xcol == 0, g.lanes(q[c], 1 - NX), g.lanes(q[c], 1)))
            elif d == 2:
                add(m, c, h, g.lanes(q[c], NX))
            elif d == 1:
                add(m, c, h, g.rows(q[c], 1))
            elif h + 1 < halves:
                moved = g.rows(q[c], depth)
                add(m, c, h, jnp.where(g.row >= depth, moved, 0.0))
                add(m, c, h + 1, jnp.where(g.row < depth, moved, 0.0))
            else:
                add(m, c, h, g.rows(q[c], depth))

    def masked(mask, a):
        return [[[pick(mask, 0.0, v) for v in line] for line in part] for part in a]

    def inner(mu, nu, h):
        own = matrix(lambda *c: load(mu, *c, h))
        side = matrix(lambda *c: load(nu, *c, h))
        a = product(
            matrix(lambda *c: rolled(nu, mu, h, *c)),
            matrix(lambda *c: rolled(mu, nu, h, *c)),
            right_h=True,
        )
        mask = None
        for d in (mu, nu):
            if not complete(d, h):
                mask = top(d) if mask is None else jnp.logical_or(mask, top(d))
        a = masked(mask, a)
        b = product(own, side, left_h=True)
        forward(mu, nu, h, projected(a, b, left_h=True))
        forward(nu, mu, h, projected(a, b, right_h=True))
        upper = projected(product(own, a), side, right_h=True)
        for c in range(8):
            add(mu, c, h, upper[c])
            add(nu, c, h, -upper[c])

    def corners(d, among):
        for s in range(len(LAYOUT[d])):
            mask = open_mask(d, s, among)
            if mask is None:
                continue
            n = sets.index((d, s))

            def corner(m, h, c):
                if m not in among or complete(m, h):
                    return None
                k = LAYOUT[m][0].index((d, 0 if m == 0 else h))
                return shifted(m, fetch(in_s, "x", m, 0, *c), last[m] - k)

            for c in comps:
                value = pack(d, s, lambda m, h: corner(m, h, c), True)
                face_s[(n, 2, *c)] = jnp.where(mask, value, face_s[(n, 2, *c)])

    def face_terms(d, closed):
        for s, spots in enumerate(LAYOUT[d]):
            n = sets.index((d, s))
            own, side, over = (kept(d, s, q) for q in range(3))
            a = product(fetched(in_s, "x", d, s), over, right_h=True)
            a = masked(open_mask(d, s, [m for m in range(3) if m not in closed]), a)
            b = matrix(lambda *c: b_s[(n, *c)])
            upper = projected(product(own, a), side, right_h=True)
            low = projected(a, b, left_h=True)
            mask = open_mask(d, s, closed)
            low = [pick(mask, 0.0, v) for v in low]
            for k, (m, h) in enumerate(spots):
                h = half(d, h, True)
                natural = lambda v: jnp.where(top(d), shifted(d, v, last[d] - k), 0.0)
                for c in range(8):
                    x = natural(upper[c])
                    add(d, c, h, x)
                    add(m, c, h, -x)
                forward(d, m, h, [natural(v) for v in low])
        flush()

    def prepare(d):
        for s in range(len(LAYOUT[d])):
            own = fetched(out_s, "x", d, s)
            mask = open_mask(d, s)
            if mask is not None:
                far = packed(
                    d, s,
                    lambda m, h, *c: None if complete(m, h if d else 1) else edge(d, m, h, *c),
                    False,
                )
                both = product(own, far, right_h=True)
                own = [
                    [[jnp.where(mask, both[p][i][j], own[p][i][j]) for j in range(3)] for i in range(3)]
                    for p in range(2)
                ]
            save(pre_s, (sets.index((d, s)),), own)

    def close(d):
        for s, spots in enumerate(LAYOUT[d]):
            n = sets.index((d, s))
            q = projected(
                matrix(lambda *c: pre_s[(n, *c)]), fetched(in_s, "g", d, s), right_h=True
            )
            for k, (m, h) in enumerate(spots):
                for c in range(8):
                    add(m, c, half(d, h, False), jnp.where(bottom(d), shifted(d, q[c], -k), 0.0))
        flush()

    for n, pair in enumerate(PLANES):
        if n == 2:
            pl.semaphore_wait(met, 1)

            @pl.when(rest_t)
            def _():
                edges[1].start()

        for h in range(halves):
            inner(*pair, h)
        flush()

    @pl.when(first_t)
    def _():
        pl.semaphore_wait(met_t, 1)
        for copy in (edges[3], edges[1], faces[0]):
            copy.start()

    @pl.when(early)
    def _():
        pl.semaphore_wait(met_t, 1)
        edges[3].start()

    @pl.when(first_z)
    def _():
        pl.semaphore_wait(met_z, 1)
        edges[5].start()
        faces[1].start()

    @pl.when(jnp.logical_and(first_z, more_t))
    def _():
        edges[2].start()

    faces[2].wait_recv()
    face_terms(2, ())
    corners(0, (2,))
    faces[0].wait_recv()
    face_terms(0, (2,))
    corners(1, (0, 2))

    def close_all():
        for d in (2, 1, 0):
            arrivals[d].wait_recv()
            prepare(d)
            close(d)

    def face_z():
        faces[1].wait_recv()
        face_terms(1, (0, 2))

    @pl.when(last_z)
    def _():
        close_all()
        face_z()

    @pl.when(more_z)
    def _():
        face_z()
        close_all()

    everything.wait_send()


def expand(halves, acc, hbm, out, sem):
    for m in range(4):
        for h in range(halves):
            rows = [((m * 8 + c) * halves + h) * SUB for c in range(8)]
            f = [acc[r : r + SUB, :] * (COEFF * 0.5 if c < 6 else COEFF) for c, r in enumerate(rows)]

            def put(part, i, j, value):
                out[m, part, i, j, h * SUB : (h + 1) * SUB, :] = value

            for n, (i, j) in enumerate(((0, 1), (0, 2), (1, 2))):
                put(0, i, j, f[n])
                put(0, j, i, -f[n])
                put(1, i, j, f[3 + n])
                put(1, j, i, f[3 + n])
            for i in range(3):
                put(0, i, i, jnp.zeros((SUB, LANES), jnp.float32))
            put(1, 0, 0, f[6])
            put(1, 1, 1, f[7])
            put(1, 2, 2, -(f[6] + f[7]))
        for part in range(2):
            for i in range(3):
                pltpu.make_async_copy(out.at[m, part, i], hbm.at[m, part, i], sem).start()
    pltpu.make_async_copy(out, hbm, sem).wait()


def per_device(counts, links):
    time_len, depth, flat = links.shape[4:]
    sites = time_len * depth
    assert flat == LANES and (time_len, depth) == (4, 4)
    halves = sites // SUB
    vmem = lambda *s: pltpu.VMEM(s + (LANES,), jnp.float32)
    shape = links.shape[:4] + (sites, flat)
    terms = pl.pallas_call(
        functools.partial(force_terms, counts, depth, halves),
        out_shape=pltpu.VMEM((32 * sites, flat), jnp.float32),
        in_specs=[pl.BlockSpec(memory_space=pl.ANY)],
        out_specs=pl.BlockSpec(memory_space=pltpu.VMEM),
        scratch_shapes=[
            vmem(*shape[:-1]),
            vmem(TOTAL),
            vmem(TOTAL),
            vmem(5, 3, 2, 2, 3, SUB),
            vmem(5, 2, 3, 3, SUB),
            vmem(5, 2, 3, 3, SUB),
            pltpu.SemaphoreType.DMA,
            pltpu.SemaphoreType.DMA((6,)),
            pltpu.SemaphoreType.REGULAR,
            pltpu.SemaphoreType.REGULAR,
            pltpu.SemaphoreType.REGULAR,
        ],
        compiler_params=pltpu.CompilerParams(collective_id=0, has_side_effects=True),
        name="force_terms",
    )(links.reshape(shape))
    out = pl.pallas_call(
        functools.partial(expand, halves),
        out_shape=jax.ShapeDtypeStruct(shape, jnp.float32),
        in_specs=[pl.BlockSpec(memory_space=pltpu.VMEM)],
        out_specs=pl.BlockSpec(memory_space=pl.ANY),
        scratch_shapes=[vmem(*shape[:-1]), pltpu.SemaphoreType.DMA],
        name="expand",
    )(pltpu.with_memory_space_constraint(terms, pltpu.VMEM))
    return out.reshape(links.shape)


def solution(mesh):
    assert mesh.axis_names == ("gx", "gz", "ta")
    counts = tuple(mesh.shape[a] for a in AXES)
    spec = P(None, None, None, None, "ta", "gz", "gx")
    return jax.shard_map(
        functools.partial(per_device, counts),
        mesh=mesh,
        in_specs=(spec,),
        out_specs=spec,
        check_vma=False,
    )
```
